32 devices in a mesh: rep: 2 (over x), dim: 4 (over z), shard: 4 (over y, core).
Axes of the slice: x: 2, y: 2, z: 4, core: 2. Of those that a mesh axis runs over, the one named last changes fastest.
Arguments:
- queries: bfloat16 [16384, 4096], P(('rep', 'shard'), 'dim'), parts along dimension 0
- list_vecs: bfloat16 [1024, 8, 4096], P('shard', None, 'dim')
- list_ids: int32 [1024, 8], P('shard')
- probes: int32 [16384, 8], P(('rep', 'shard')), parts along dimension 0
Outputs:
- output 1: float32 [16384, 10], P(('rep', 'shard')), parts along dimension 0
- output 2: int32 [16384, 10], P(('rep', 'shard')), parts along dimension 0
There are 2 independent parts. The reference program is written for one: setup_inputs(seed, part) draws one part's arguments, and reference() takes and returns one part's arrays. A program takes and returns all parts, laid end to end along the dimension named above; an argument that names none is the same for every part.
All inputs are finite; a program needn't handle non-finite values.
Results may differ from the reference program's by a relative error of at most 0.001.
Values are sent between devices in bfloat16 or wider.
A program may use at most 1 GiB of HBM per device.

```python
import jax
import jax.numpy as jnp
from jax import lax

EMBED_DIM = 4096
NUM_LISTS = 1024
NUM_PROBES = 8
QUERY_ROWS = 2048
LIST_LEN = 8
GROUP_DEVS = 4
TOP_K = 10

QUERIES = QUERY_ROWS * GROUP_DEVS
LISTS_DEV = NUM_LISTS // GROUP_DEVS
PAIR_TOTAL = QUERY_ROWS * NUM_PROBES
SLOT_CAP = min(3 * PAIR_TOTAL // 4, 2 * PAIR_TOTAL // GROUP_DEVS)


def draw_probes(base_key):
    rest_pairs = PAIR_TOTAL - SLOT_CAP
    base_count = rest_pairs // (GROUP_DEVS - 1)
    extra_count = rest_pairs - base_count * (GROUP_DEVS - 1)
    spread = (3 * base_count) // 4

    def one_source(src_key):
        key_dest, key_bump, key_row, key_start = jax.random.split(src_key, 4)
        dest_order = jax.random.permutation(key_dest, GROUP_DEVS).astype(jnp.int32)
        count_bumps = jax.random.randint(key_bump, (GROUP_DEVS - 1,), 0, spread + 1)
        other_rank = jnp.arange(GROUP_DEVS - 1)
        other_counts = base_count + (other_rank < extra_count).astype(jnp.int32) + count_bumps - jnp.roll(count_bumps, -1)
        counts = jnp.concatenate([jnp.full((1,), SLOT_CAP, jnp.int32), other_counts.astype(jnp.int32)])
        run_end = jnp.cumsum(counts)
        run_start = run_end - counts
        row_order = jax.random.permutation(key_row, QUERY_ROWS).astype(jnp.int32)
        position = jnp.arange(NUM_PROBES, dtype=jnp.int32)[None, :] * QUERY_ROWS + row_order[:, None]
        run_rank = jnp.sum((position[:, :, None] >= run_end[None, None, :]).astype(jnp.int32), axis=2)
        first_probe = jnp.maximum(0, (run_start[run_rank] - row_order[:, None] + QUERY_ROWS - 1) // QUERY_ROWS)
        repeat_index = jnp.arange(NUM_PROBES, dtype=jnp.int32)[None, :] - first_probe
        start_list = jax.random.randint(key_start, (QUERY_ROWS, GROUP_DEVS), 0, LISTS_DEV)
        local_list = (jnp.take_along_axis(start_list, run_rank, axis=1) + repeat_index) % LISTS_DEV
        return (dest_order[run_rank] * LISTS_DEV + local_list).astype(jnp.int32)

    src_keys = jax.random.split(base_key, GROUP_DEVS)
    return jax.vmap(one_source)(src_keys).reshape(QUERIES, NUM_PROBES)


def draw_lists(base_key):
    key_vecs, key_fill, key_full, key_ids = jax.random.split(base_key, 4)
    list_vecs = jax.random.randint(key_vecs, (NUM_LISTS, LIST_LEN, EMBED_DIM), -8, 9).astype(jnp.bfloat16)
    fill_len = jax.random.randint(key_fill, (NUM_LISTS,), LIST_LEN // 4, LIST_LEN + 1)
    full_list = jax.random.randint(key_full, (), 0, NUM_LISTS)
    fill_len = jnp.where(jnp.arange(NUM_LISTS) == full_list, LIST_LEN, fill_len)
    id_pool = jax.random.permutation(key_ids, NUM_LISTS * LIST_LEN).reshape(NUM_LISTS, LIST_LEN)
    list_ids = jnp.where(jnp.arange(LIST_LEN)[None, :] < fill_len[:, None], id_pool, -1).astype(jnp.int32)
    return list_vecs, list_ids


def setup_inputs(seed: int = 0, part: int = 0) -> dict:
    root_key = jax.random.key(seed)
    key_lists, key_part = jax.random.split(root_key)
    list_vecs, list_ids = draw_lists(key_lists)
    key_query, key_probe = jax.random.split(jax.random.fold_in(key_part, part))
    queries = jax.random.randint(key_query, (QUERIES, EMBED_DIM), -8, 9).astype(jnp.bfloat16)
    probes = draw_probes(key_probe)
    return {'queries': queries, 'list_vecs': list_vecs, 'list_ids': list_ids, 'probes': probes}


def reference(queries, list_vecs, list_ids, probes):
    def one_query(query_pack):
        query_vec, probe_row = query_pack
        members = list_vecs[probe_row].reshape(NUM_PROBES * LIST_LEN, EMBED_DIM)
        member_ids = list_ids[probe_row].reshape(NUM_PROBES * LIST_LEN)
        scores = jnp.dot(members, query_vec, preferred_element_type=jnp.float32)
        neg_keys = jnp.where(member_ids >= 0, -scores, jnp.inf)
        key_sorted, ids_sorted = lax.sort((neg_keys, member_ids), num_keys=2)
        return -key_sorted[:TOP_K], ids_sorted[:TOP_K]

    top_scores, top_ids = lax.map(one_query, (queries, probes))
    return top_scores, top_ids
```

```python
import functools

import jax
import jax.numpy as jnp
from jax import lax
from jax.experimental import pallas as pl
from jax.experimental.pallas import tpu as pltpu
from jax.sharding import PartitionSpec as P

TOP_K = 10
LIST_LEN = 8
GROUP_LISTS = 8
GROUP_ROWS = GROUP_LISTS * LIST_LEN
STEP_GROUPS = 4
STEP_ROWS = STEP_GROUPS * GROUP_ROWS
LANES = 128
MESH = pl.DeviceIdType.MESH
BIG = 1e9


def flip(index, bit):
    return index + bit - 2 * bit * ((index // bit) % 2)


def search_kernel(dims, q_hbm, l_hbm, probes_ref, ids_ref, out_s, out_i,
                  raw, qv, vecs, perm, acc, parts, ids_all, cand_ids, res,
                  load_l, load_q, send_o, recv_o, send_y, recv_y, send_x, recv_x,
                  send_dy, recv_dy, send_dx, recv_dx, send_i, recv_i,
                  send_r, recv_r, send_g, recv_g):
    rows_q = qv.shape[0]
    lists_dev = ids_ref.shape[1]
    block_rows = lists_dev * LIST_LEN
    block_groups = lists_dev // GROUP_LISTS
    chunks = block_groups // 2
    block_steps = block_groups // STEP_GROUPS
    width = rows_q // dims
    x, z, s = lax.axis_index('rep'), lax.axis_index('dim'), lax.axis_index('shard')
    twin, across, far = flip(s, 1), flip(s, 2), flip(flip(s, 1), 2)
    other_x = 1 - x

    def at(**place):
        return {'rep': x, 'dim': z, 'shard': s, **place}

    def group_rows(group):
        return pl.ds(pl.multiple_of(group * GROUP_ROWS, GROUP_ROWS), GROUP_ROWS)

    def step_rows(step):
        return pl.ds(pl.multiple_of(step * STEP_ROWS, STEP_ROWS), STEP_ROWS)

    def remote(src, dst, send, recv, device):
        return pltpu.make_async_remote_copy(src_ref=src, dst_ref=dst, send_sem=send, recv_sem=recv,
                                            device_id=device, device_id_type=MESH)

    def load_list(block):
        return pltpu.make_async_copy(l_hbm.at[step_rows(block)], raw.at[step_rows(block)], load_l.at[block])

    def load_query(part):
        rows = pl.ds(pl.multiple_of(part * width, width), width)
        return pltpu.make_async_copy(q_hbm.at[rows], qv.at[rows], load_q.at[part])

    def own_copy(block):
        return remote(vecs.at[step_rows(block)], vecs.at[step_rows(block_steps + block)],
                      send_o.at[block], recv_o.at[block], at(shard=twin))

    def slot(chunk, which):
        return vecs.at[group_rows(2 * block_groups + STEP_GROUPS * chunk + which)]

    def y_copy(chunk):
        return remote(vecs.at[group_rows(chunks * x + chunk)], slot(chunk, 0), send_y.at[chunk], recv_y.at[chunk], at(shard=across))

    def x_copy(chunk):
        return remote(slot(chunk, 0), slot(chunk, 1), send_x.at[chunk], recv_x.at[chunk], at(rep=other_x))

    def dy_copy(chunk):
        return remote(slot(chunk, 0), slot(chunk, 2), send_dy.at[chunk], recv_dy.at[chunk], at(shard=twin))

    def dx_copy(chunk):
        return remote(slot(chunk, 1), slot(chunk, 3), send_dx.at[chunk], recv_dx.at[chunk], at(shard=twin))

    def id_copy(which, peer):
        return remote(ids_ref, ids_all.at[s], send_i.at[which], recv_i.at[which], at(shard=peer))

    def peer_slot(source, target):
        return (source - target - 1 + dims) % dims

    def part_copy(target, which):
        return remote(acc.at[target], parts.at[peer_slot(z, target)], send_r.at[which], recv_r.at[peer_slot(z, target)], at(dim=target))

    def res_copy(target, which):
        return remote(res.at[z], res.at[z], send_g.at[which], recv_g.at[peer_slot(z, target)], at(dim=target))

    def target_at(turn):
        if dims == 1:
            return 0
        half = dims // 2
        low = z // half == 0
        ahead = turn
        far_target = jnp.where(low, dims - 1 - ahead, ahead)
        near = turn - half
        base = jnp.where(low, 0, half)
        near_target = base + (z - base + 1 + near) % half
        return jnp.where(turn < half, far_target, near_target)

    def block_at(turn):
        return (block_steps // 2 * x + turn) % block_steps

    for turn in range(block_steps):
        load_list(block_at(turn)).start()
    for part in range(dims):
        load_query(part).start()

    barrier = pltpu.get_barrier_semaphore()
    peers = [at(shard=twin), at(shard=across), at(shard=far), at(rep=other_x)]
    peers += [at(dim=(z + hop) % dims) for hop in range(1, dims)]
    for peer in peers:
        pl.semaphore_signal(barrier, inc=1, device_id=peer, device_id_type=MESH)

    row = lax.broadcasted_iota(jnp.int32, (STEP_ROWS, STEP_ROWS), 0)
    col = lax.broadcasted_iota(jnp.int32, (STEP_ROWS, STEP_ROWS), 1)
    source = (row // GROUP_ROWS) * GROUP_ROWS + (row % GROUP_LISTS) * LIST_LEN + (row // GROUP_LISTS) % LIST_LEN
    perm[...] = jnp.where(col == source, 1.0, 0.0).astype(jnp.bfloat16)
    acc[...] = jnp.zeros_like(acc)
    ids_all[s] = ids_ref[...]

    pl.semaphore_wait(barrier, len(peers))
    for which, peer in enumerate((twin, across, far)):
        id_copy(which, peer).start()

    def send_block(turn):
        own_copy(block_at(turn)).start()

        @pl.when(turn < block_steps // 2)
        def _():
            for sub in range(STEP_GROUPS):
                y_copy(STEP_GROUPS * turn + sub).start()

    def arrange(turn, carry):
        block = block_at(turn)
        load_list(block).wait()
        moved = jnp.dot(perm[...], raw[step_rows(block), :], preferred_element_type=jnp.float32)
        vecs[step_rows(block), :] = moved.astype(jnp.bfloat16)

        @pl.when(turn > 0)
        def _():
            send_block(turn - 1)
        return carry

    lax.fori_loop(0, block_steps, arrange, 0)

    for part in range(dims):
        load_query(part).wait()
    for which, peer in enumerate((twin, across, far)):
        remote(ids_ref, ids_all.at[peer], send_i.at[which], recv_i.at[which], at(shard=peer)).wait_recv()

    def name_candidates(tile, carry):
        cols = pl.ds(pl.multiple_of(z * width + tile * LANES, LANES), LANES)
        probe = probes_ref[:, cols]
        lane, page = probe % LANES, probe // LANES
        pages = lists_dev // LANES
        for member in range(LIST_LEN):
            got = jnp.zeros((probe.shape[0], LANES), jnp.int32)
            for number in range(4 * pages):
                table = ids_all[number // pages, member:member + 1, (number % pages) * LANES:(number % pages + 1) * LANES]
                table = jnp.broadcast_to(table, (probe.shape[0], LANES))
                picked = jnp.take_along_axis(table, lane, axis=1, mode='promise_in_bounds')
                got = jnp.where(page == number, picked, got)
            cand_ids[member, :, pl.ds(pl.multiple_of(tile * LANES, LANES), LANES)] = got.astype(jnp.float32)
        return carry

    lax.fori_loop(0, width // LANES, name_candidates, 0)
    send_block(block_steps - 1)

    def score(step, heads, part):
        lists = vecs[step_rows(step), :]
        rows = pl.ds(pl.multiple_of(part * width, width), width)
        scores = lax.dot_general(lists, qv[rows, :], (((1,), (1,)), ((), ())), preferred_element_type=jnp.float32)
        for tile in range(width // LANES):
            probe = probes_ref[:, pl.ds(pl.multiple_of(part * width + tile * LANES, LANES), LANES)]
            low, head = probe % GROUP_LISTS, probe // GROUP_LISTS
            hits = [head == want for want in heads]
            lanes = slice(tile * LANES, (tile + 1) * LANES)
            for member in range(LIST_LEN):
                kept = acc[part, member, :, lanes]
                for group, hit in enumerate(hits):
                    first = group * GROUP_ROWS + member * GROUP_LISTS
                    picked = jnp.take_along_axis(scores[first:first + GROUP_LISTS, lanes], low, axis=0, mode='promise_in_bounds')
                    kept = jnp.where(hit, picked, kept)
                acc[part, member, :, lanes] = kept

    def heads_at(step):
        local = step < 2 * block_steps
        chunk = step - 2 * block_steps
        base = block_groups * jnp.where(step < block_steps, s, twin) + STEP_GROUPS * (step % block_steps)
        heads = []
        for which in range(STEP_GROUPS):
            home = across if which < 2 else far
            side = x if which % 2 == 0 else other_x
            heads.append(jnp.where(local, base + which, block_groups * home + chunks * side + chunk))
        return heads

    last = 2 * block_steps + chunks - 1
    slow_until = 2 * block_steps + 6

    def pass_on(step):
        slow = step <= slow_until
        y_chunk = jnp.where(slow, (step - 4) // 2, step - slow_until + 9)
        x_chunk = jnp.where(slow, (step - 8) // 2, step - slow_until + 7)
        turn = jnp.logical_or(jnp.logical_not(slow), step % 2 == 0)

        @pl.when(turn & (step >= 4) & (y_chunk < chunks))
        def _():
            y_copy(y_chunk).wait_recv()
            x_copy(y_chunk).start()
            dy_copy(y_chunk).start()

        @pl.when(turn & (step >= 8) & (x_chunk < chunks))
        def _():
            x_copy(x_chunk).wait_recv()
            dx_copy(x_chunk).start()

        @pl.when((step >= block_steps) & (step < 2 * block_steps))
        def _():
            own_copy(step - block_steps).wait_recv()

        @pl.when(step >= 2 * block_steps)
        def _():
            dy_copy(step - 2 * block_steps).wait_recv()
            dx_copy(step - 2 * block_steps).wait_recv()

    def main(step, carry):
        pass_on(step)
        heads = heads_at(step)
        for part in range(dims):
            score(step, heads, part)
        return carry

    lax.fori_loop(0, last, main, 0)
    pass_on(last)
    last_heads = heads_at(jnp.int32(last))

    def finish(turn, carry):
        score(last, last_heads, target_at(turn))

        @pl.when(turn > 0)
        def _():
            part_copy(target_at(turn - 1), turn - 1).start()
        return carry

    lax.fori_loop(0, dims, finish, 0)

    for which in range(dims - 1):
        remote(acc.at[z], parts.at[which], send_r.at[which], recv_r.at[which], at()).wait_recv()

    scores, names = [], []
    for member in range(LIST_LEN):
        total = acc[z, member]
        for which in range(dims - 1):
            total = total + parts[which, member]
        name = cand_ids[member]
        real = name >= 0.0
        scores.append(jnp.where(real, total, -jnp.inf))
        names.append(jnp.where(real, name, BIG))
    for place in range(TOP_K):
        best = functools.reduce(jnp.maximum, scores)
        best = jnp.max(best, axis=0, keepdims=True)
        tied = [jnp.where(score_j == best, name_j, BIG) for score_j, name_j in zip(scores, names)]
        first = jnp.min(functools.reduce(jnp.minimum, tied), axis=0, keepdims=True)
        res[z, place:place + 1, :] = best
        res[z, TOP_K + place:TOP_K + place + 1, :] = first
        if place + 1 < TOP_K:
            scores = [jnp.where(name_j == first, -jnp.inf, score_j) for score_j, name_j in zip(scores, names)]

    def drain_local(block, carry):
        own_copy(block).wait_send()
        return carry

    def drain_chunks(chunk, carry):
        y_copy(chunk).wait_send()
        x_copy(chunk).wait_send()
        dy_copy(chunk).wait_send()
        dx_copy(chunk).wait_send()
        return carry

    lax.fori_loop(0, block_steps, drain_local, 0)
    lax.fori_loop(0, chunks, drain_chunks, 0)
    for which, peer in enumerate((twin, across, far)):
        id_copy(which, peer).wait_send()
    for which in range(dims - 1):
        part_copy(target_at(which), which).wait_send()

    for which in range(dims - 1):
        res_copy(target_at(which), which).start()
    for which in range(dims - 1):
        remote(res.at[z], res.at[(z + 1 + which) % dims], send_g.at[which], recv_g.at[which], at()).wait_recv()
    for part in range(dims):
        out_s[:, part * width:(part + 1) * width] = res[part, 0:TOP_K, :]
        out_i[:, part * width:(part + 1) * width] = res[part, TOP_K:2 * TOP_K, :].astype(jnp.int32)
    for which in range(dims - 1):
        res_copy(target_at(which), which).wait_send()


def solution(mesh):
    dims = mesh.shape['dim']
    row_spec = P(('rep', 'shard'), None)

    def local_search(queries, list_vecs, list_ids, probes):
        rows_q, depth = queries.shape
        lists_dev, list_len, _ = list_vecs.shape
        probe_count = probes.shape[1]
        block_rows = lists_dev * list_len
        block_steps = block_rows // STEP_ROWS
        chunks = lists_dev // GROUP_LISTS // 2
        width = rows_q // dims
        dma = pltpu.SemaphoreType.DMA
        any_spec = pl.BlockSpec(memory_space=pl.ANY)
        vmem_spec = pl.BlockSpec(memory_space=pltpu.VMEM)
        scores, ids = pl.pallas_call(
            functools.partial(search_kernel, dims),
            out_shape=(jax.ShapeDtypeStruct((TOP_K, rows_q), jnp.float32),
                       jax.ShapeDtypeStruct((TOP_K, rows_q), jnp.int32)),
            in_specs=[any_spec, any_spec, vmem_spec, vmem_spec],
            out_specs=(vmem_spec, vmem_spec),
            scratch_shapes=[
                pltpu.VMEM((block_rows, depth), jnp.bfloat16),
                pltpu.VMEM((rows_q, depth), jnp.bfloat16),
                pltpu.VMEM((4 * block_rows, depth), jnp.bfloat16),
                pltpu.VMEM((STEP_ROWS, STEP_ROWS), jnp.bfloat16),
                pltpu.VMEM((dims, LIST_LEN, probe_count, width), jnp.float32),
                pltpu.VMEM((dims - 1, LIST_LEN, probe_count, width), jnp.float32),
                pltpu.VMEM((4, LIST_LEN, lists_dev), jnp.int32),
                pltpu.VMEM((LIST_LEN, probe_count, width), jnp.float32),
                pltpu.VMEM((dims, 24, width), jnp.float32),
                dma((block_steps,)), dma((dims,)),
                dma((block_steps,)), dma((block_steps,)),
                dma((chunks,)), dma((chunks,)), dma((chunks,)), dma((chunks,)),
                dma((chunks,)), dma((chunks,)), dma((chunks,)), dma((chunks,)),
                dma((3,)), dma((3,)),
                dma((dims - 1,)), dma((dims - 1,)), dma((dims - 1,)), dma((dims - 1,)),
            ],
            compiler_params=pltpu.CompilerParams(collective_id=0, has_side_effects=True, vmem_limit_bytes=60 * 2**20),
            name='ivf_search',
        )(queries, list_vecs.reshape(block_rows, depth), probes.T, list_ids.T)
        return scores.T, ids.T

    return jax.shard_map(local_search, mesh=mesh,
                         in_specs=(P(('rep', 'shard'), 'dim'), P('shard', None, 'dim'), P('shard', None), row_spec),
                         out_specs=(row_spec, row_spec), check_vma=False)
```

```python
import functools

import jax
import jax.numpy as jnp
from jax import lax
from jax.experimental import pallas as pl
from jax.experimental.pallas import tpu as pltpu
from jax.sharding import PartitionSpec as P

TOP_K = 10
LIST_LEN = 8
GROUP_LISTS = 8
GROUP_ROWS = GROUP_LISTS * LIST_LEN
STEP_GROUPS = 4
STEP_ROWS = STEP_GROUPS * GROUP_ROWS
PIECE_ROWS = GROUP_ROWS // 2
LANES = 128
MESH = pl.DeviceIdType.MESH
BIG = 1e9


def flip(index, bit):
    return index + bit - 2 * bit * ((index // bit) % 2)


def search_kernel(dims, q_hbm, l_hbm, probes_ref, ids_ref, res,
                  raw, qv, vecs, perm, acc, parts, ids_all, cand_ids,
                  load_l, load_q, send_o, recv_o, send_y, recv_y, send_x, recv_x,
                  send_dy, recv_dy, send_dx, recv_dx, send_i, recv_i,
                  send_r, recv_r, send_g, recv_g):
    rows_q = qv.shape[0]
    lists_dev = ids_ref.shape[1]
    block_rows = lists_dev * LIST_LEN
    block_groups = lists_dev // GROUP_LISTS
    chunks = block_groups
    block_steps = block_groups // STEP_GROUPS
    width = rows_q // dims
    x, z, s = lax.axis_index('rep'), lax.axis_index('dim'), lax.axis_index('shard')
    twin, across, far = flip(s, 1), flip(s, 2), flip(flip(s, 1), 2)
    other_x = 1 - x

    def at(**place):
        return {'rep': x, 'dim': z, 'shard': s, **place}

    def step_rows(step):
        return pl.ds(pl.multiple_of(step * STEP_ROWS, STEP_ROWS), STEP_ROWS)

    def remote(src, dst, send, recv, device):
        return pltpu.make_async_remote_copy(src_ref=src, dst_ref=dst, send_sem=send, recv_sem=recv,
                                            device_id=device, device_id_type=MESH)

    def load_list(block):
        return pltpu.make_async_copy(l_hbm.at[step_rows(block)], raw.at[step_rows(block)], load_l.at[block])

    def load_query(part):
        rows = pl.ds(pl.multiple_of(part * width, width), width)
        return pltpu.make_async_copy(q_hbm.at[rows], qv.at[rows], load_q.at[part])

    def own_copy(block):
        return remote(vecs.at[step_rows(block)], vecs.at[step_rows(block_steps + block)],
                      send_o.at[block], recv_o.at[block], at(shard=twin))

    def piece(group, chunk):
        first = pl.multiple_of(group * GROUP_ROWS + chunk % 2 * PIECE_ROWS, PIECE_ROWS)
        return vecs.at[pl.ds(first, PIECE_ROWS)]

    def slot(chunk, which):
        return piece(2 * block_groups + STEP_GROUPS * (chunk // 2) + which, chunk)

    def y_copy(chunk):
        return remote(piece(chunks // 2 * x + chunk // 2, chunk), slot(chunk, 0), send_y.at[chunk], recv_y.at[chunk], at(shard=across))

    def x_copy(chunk):
        return remote(slot(chunk, 0), slot(chunk, 1), send_x.at[chunk], recv_x.at[chunk], at(rep=other_x))

    def dy_copy(chunk):
        return remote(slot(chunk, 0), slot(chunk, 2), send_dy.at[chunk], recv_dy.at[chunk], at(shard=twin))

    def dx_copy(chunk):
        return remote(slot(chunk, 1), slot(chunk, 3), send_dx.at[chunk], recv_dx.at[chunk], at(shard=twin))

    def id_copy(which, peer):
        return remote(ids_ref, ids_all.at[s], send_i.at[which], recv_i.at[which], at(shard=peer))

    def peer_slot(source, target):
        return (source - target - 1 + dims) % dims

    def part_copy(target, which):
        return remote(acc.at[target], parts.at[peer_slot(z, target)], send_r.at[which], recv_r.at[peer_slot(z, target)], at(dim=target))

    def res_copy(target, which):
        return remote(res.at[z], res.at[z], send_g.at[which], recv_g.at[peer_slot(z, target)], at(dim=target))

    def target_at(turn):
        if dims == 1:
            return 0
        half = dims // 2
        low = z // half == 0
        ahead = turn
        far_target = jnp.where(low, dims - 1 - ahead, ahead)
        near = turn - half
        base = jnp.where(low, 0, half)
        near_target = base + (z - base + 1 + near) % half
        return jnp.where(turn < half, far_target, near_target)

    def block_at(turn):
        return (block_steps // 2 * x + turn) % block_steps

    for turn in range(block_steps):
        load_list(block_at(turn)).start()

    barrier = pltpu.get_barrier_semaphore()
    peers = [at(shard=twin), at(shard=across), at(shard=far), at(rep=other_x)]
    peers += [at(dim=(z + hop) % dims) for hop in range(1, dims)]
    for peer in peers:
        pl.semaphore_signal(barrier, inc=1, device_id=peer, device_id_type=MESH)

    row = lax.broadcasted_iota(jnp.int32, (STEP_ROWS, STEP_ROWS), 0)
    col = lax.broadcasted_iota(jnp.int32, (STEP_ROWS, STEP_ROWS), 1)
    source = (row // GROUP_ROWS) * GROUP_ROWS + (row % GROUP_LISTS) * LIST_LEN + (row // GROUP_LISTS) % LIST_LEN
    perm[...] = jnp.where(col == source, 1.0, 0.0).astype(jnp.bfloat16)

    def send_block(turn):
        @pl.when(turn < block_steps // 2)
        def _():
            for sub in range(2 * STEP_GROUPS):
                y_copy(2 * STEP_GROUPS * turn + sub).start()
        own_copy(block_at(turn)).start()

    def arrange(turn):
        block = block_at(turn)
        load_list(block).wait()
        moved = jnp.dot(perm[...], raw[step_rows(block), :], preferred_element_type=jnp.float32)
        vecs[step_rows(block), :] = moved.astype(jnp.bfloat16)

    arrange(0)
    for part in range(dims):
        load_query(part).start()
    ids_all[s] = ids_ref[...]
    pl.semaphore_wait(barrier, len(peers))

    def arrange_send(turn, carry):
        arrange(turn)
        send_block(turn - 1)
        return carry

    lax.fori_loop(1, block_steps, arrange_send, 0)
    for which, peer in enumerate((twin, across, far)):
        id_copy(which, peer).start()
    acc[...] = jnp.zeros_like(acc)
    send_block(block_steps - 1)

    for part in range(dims):
        load_query(part).wait()
    for which, peer in enumerate((twin, across, far)):
        remote(ids_ref, ids_all.at[peer], send_i.at[which], recv_i.at[which], at(shard=peer)).wait_recv()

    def name_candidates(tile, carry):
        cols = pl.ds(pl.multiple_of(z * width + tile * LANES, LANES), LANES)
        probe = probes_ref[:, cols]
        lane, page = probe % LANES, probe // LANES
        pages = lists_dev // LANES
        for member in range(LIST_LEN):
            got = jnp.zeros((probe.shape[0], LANES), jnp.int32)
            for number in range(4 * pages):
                table = ids_all[number // pages, member:member + 1, (number % pages) * LANES:(number % pages + 1) * LANES]
                table = jnp.broadcast_to(table, (probe.shape[0], LANES))
                picked = jnp.take_along_axis(table, lane, axis=1, mode='promise_in_bounds')
                got = jnp.where(page == number, picked, got)
            cand_ids[member, :, pl.ds(pl.multiple_of(tile * LANES, LANES), LANES)] = got.astype(jnp.float32)
        return carry

    lax.fori_loop(0, width // LANES, name_candidates, 0)

    def score(step, heads, part):
        lists = vecs[step_rows(step), :]
        rows = pl.ds(pl.multiple_of(part * width, width), width)
        scores = lax.dot_general(lists, qv[rows, :], (((1,), (1,)), ((), ())), preferred_element_type=jnp.float32)
        for tile in range(width // LANES):
            probe = probes_ref[:, pl.ds(pl.multiple_of(part * width + tile * LANES, LANES), LANES)]
            low, head = probe % GROUP_LISTS, probe // GROUP_LISTS
            hits = [head == want for want in heads]
            lanes = slice(tile * LANES, (tile + 1) * LANES)
            for member in range(LIST_LEN):
                kept = acc[part, member, :, lanes]
                for group, hit in enumerate(hits):
                    first = group * GROUP_ROWS + member * GROUP_LISTS
                    picked = jnp.take_along_axis(scores[first:first + GROUP_LISTS, lanes], low, axis=0, mode='promise_in_bounds')
                    kept = jnp.where(hit, picked, kept)
                acc[part, member, :, lanes] = kept

    def heads_at(step):
        local = step < 2 * block_steps
        group = step - 2 * block_steps
        base = block_groups * jnp.where(step < block_steps, s, twin) + STEP_GROUPS * (step % block_steps)
        heads = []
        for which in range(STEP_GROUPS):
            home = across if which < 2 else far
            side = x if which % 2 == 0 else other_x
            heads.append(jnp.where(local, base + which, block_groups * home + chunks // 2 * side + group))
        return heads

    last = 2 * block_steps + chunks // 2 - 1
    paced = last - 4

    def pass_y(chunk):
        y_copy(chunk).wait_recv()
        x_copy(chunk).start()
        dy_copy(chunk).start()

    def pass_x(chunk):
        x_copy(chunk).wait_recv()
        dx_copy(chunk).start()

    def pass_on(step):
        @pl.when((step >= 1) & (step < paced))
        def _():
            pass_y(step - 1)

        @pl.when((step >= 4) & (step <= paced))
        def _():
            pass_x(step - 4)

        @pl.when((step >= paced) & (step < paced + 3))
        def _():
            first = chunks - 6 + 2 * (step - paced)
            pass_y(first)
            pass_x(first - 2)
            pass_y(first + 1)
            pass_x(first - 1)

        @pl.when(step >= paced + 3)
        def _():
            pass_x(step - last + chunks - 1)

        @pl.when((step >= block_steps) & (step < 2 * block_steps))
        def _():
            own_copy(step - block_steps).wait_recv()

        @pl.when(step >= 2 * block_steps)
        def _():
            first = 2 * (step - 2 * block_steps)
            for chunk in (first, first + 1):
                dy_copy(chunk).wait_recv()
                dx_copy(chunk).wait_recv()

    def main(step, carry):
        pass_on(step)
        heads = heads_at(step)
        for part in range(dims):
            score(step, heads, part)
        return carry

    lax.fori_loop(0, last, main, 0)
    pass_on(last)
    last_heads = heads_at(jnp.int32(last))

    def finish(turn, carry):
        score(last, last_heads, target_at(turn))

        @pl.when(turn > 0)
        def _():
            part_copy(target_at(turn - 1), turn - 1).start()
        return carry

    lax.fori_loop(0, dims, finish, 0)

    for which in range(dims - 1):
        remote(acc.at[z], parts.at[which], send_r.at[which], recv_r.at[which], at()).wait_recv()

    scores, names = [], []
    for member in range(LIST_LEN):
        total = acc[z, member]
        for which in range(dims - 1):
            total = total + parts[which, member]
        name = cand_ids[member]
        real = name >= 0.0
        scores.append(jnp.where(real, total, -jnp.inf))
        names.append(jnp.where(real, name, BIG))
    for place in range(TOP_K):
        best = functools.reduce(jnp.maximum, scores)
        best = jnp.max(best, axis=0, keepdims=True)
        tied = [jnp.where(score_j == best, name_j, BIG) for score_j, name_j in zip(scores, names)]
        first = jnp.min(functools.reduce(jnp.minimum, tied), axis=0, keepdims=True)
        res[z, place:place + 1, :] = best
        res[z, TOP_K + place:TOP_K + place + 1, :] = first
        if place + 1 < TOP_K:
            scores = [jnp.where(name_j == first, -jnp.inf, score_j) for score_j, name_j in zip(scores, names)]

    def drain_local(block, carry):
        own_copy(block).wait_send()
        return carry

    def drain_chunks(chunk, carry):
        y_copy(chunk).wait_send()
        x_copy(chunk).wait_send()
        dy_copy(chunk).wait_send()
        dx_copy(chunk).wait_send()
        return carry

    lax.fori_loop(0, block_steps, drain_local, 0)
    lax.fori_loop(0, chunks, drain_chunks, 0)
    for which, peer in enumerate((twin, across, far)):
        id_copy(which, peer).wait_send()
    for which in range(dims - 1):
        part_copy(target_at(which), which).wait_send()

    for which in range(dims - 1):
        res_copy(target_at(which), which).start()
    for which in range(dims - 1):
        remote(res.at[z], res.at[(z + 1 + which) % dims], send_g.at[which], recv_g.at[which], at()).wait_recv()
    for which in range(dims - 1):
        res_copy(target_at(which), which).wait_send()


def place_kernel(res, out_s, out_i):
    dims, _, width = res.shape
    for part in range(dims):
        cols = slice(part * width, (part + 1) * width)
        out_s[:, cols] = res[part, 0:TOP_K, :]
        out_i[:, cols] = res[part, TOP_K:2 * TOP_K, :].astype(jnp.int32)


def solution(mesh):
    dims = mesh.shape['dim']
    row_spec = P(('rep', 'shard'), None)

    def local_search(queries, list_vecs, list_ids, probes):
        rows_q, depth = queries.shape
        lists_dev, list_len, _ = list_vecs.shape
        probe_count = probes.shape[1]
        block_rows = lists_dev * list_len
        block_steps = block_rows // STEP_ROWS
        chunks = lists_dev // GROUP_LISTS
        width = rows_q // dims
        dma = pltpu.SemaphoreType.DMA
        any_spec = pl.BlockSpec(memory_space=pl.ANY)
        vmem_spec = pl.BlockSpec(memory_space=pltpu.VMEM)
        found = pl.pallas_call(
            functools.partial(search_kernel, dims),
            out_shape=jax.ShapeDtypeStruct((dims, 2 * TOP_K, width), jnp.float32),
            in_specs=[any_spec, any_spec, vmem_spec, vmem_spec],
            out_specs=vmem_spec,
            scratch_shapes=[
                pltpu.VMEM((block_rows, depth), jnp.bfloat16),
                pltpu.VMEM((rows_q, depth), jnp.bfloat16),
                pltpu.VMEM((4 * block_rows, depth), jnp.bfloat16),
                pltpu.VMEM((STEP_ROWS, STEP_ROWS), jnp.bfloat16),
                pltpu.VMEM((dims, LIST_LEN, probe_count, width), jnp.float32),
                pltpu.VMEM((dims - 1, LIST_LEN, probe_count, width), jnp.float32),
                pltpu.VMEM((4, LIST_LEN, lists_dev), jnp.int32),
                pltpu.VMEM((LIST_LEN, probe_count, width), jnp.float32),
                dma((block_steps,)), dma((dims,)),
                dma((block_steps,)), dma((block_steps,)),
                dma((chunks,)), dma((chunks,)), dma((chunks,)), dma((chunks,)),
                dma((chunks,)), dma((chunks,)), dma((chunks,)), dma((chunks,)),
                dma((3,)), dma((3,)),
                dma((dims - 1,)), dma((dims - 1,)), dma((dims - 1,)), dma((dims - 1,)),
            ],
            compiler_params=pltpu.CompilerParams(collective_id=0, has_side_effects=True, vmem_limit_bytes=60 * 2**20),
            name='ivf_search',
        )(queries, list_vecs.reshape(block_rows, depth), probes.T, list_ids.T)
        scores, ids = pl.pallas_call(
            place_kernel,
            out_shape=(jax.ShapeDtypeStruct((TOP_K, rows_q), jnp.float32),
                       jax.ShapeDtypeStruct((TOP_K, rows_q), jnp.int32)),
            in_specs=[vmem_spec],
            out_specs=(vmem_spec, vmem_spec),
            name='place',
        )(found)
        return scores.T, ids.T

    return jax.shard_map(local_search, mesh=mesh,
                         in_specs=(P(('rep', 'shard'), 'dim'), P('shard', None, 'dim'), P('shard', None), row_spec),
                         out_specs=(row_spec, row_spec), check_vma=False)
```

```python
import functools

import jax
import jax.numpy as jnp
from jax import lax
from jax.experimental import pallas as pl
from jax.experimental.pallas import tpu as pltpu
from jax.sharding import PartitionSpec as P

TOP_K = 10
LIST_LEN = 8
GROUP_LISTS = 8
GROUP_ROWS = GROUP_LISTS * LIST_LEN
STEP_GROUPS = 4
STEP_ROWS = STEP_GROUPS * GROUP_ROWS
PIECE_ROWS = GROUP_ROWS // 2
LANES = 128
MESH = pl.DeviceIdType.MESH
BIG = 1e9


def flip(index, bit):
    return index + bit - 2 * bit * ((index // bit) % 2)


def search_kernel(dims, q_hbm, l_hbm, probes_ref, ids_ref, res,
                  raw, qv, vecs, perm, acc, parts, ids_all, cand_ids,
                  load_l, load_q, send_o, recv_o, send_y, recv_y, send_x, recv_x,
                  send_dy, recv_dy, send_dx, recv_dx, send_i, recv_i,
                  send_r, recv_r, send_g, recv_g):
    rows_q = qv.shape[0]
    lists_dev = ids_ref.shape[1]
    block_rows = lists_dev * LIST_LEN
    block_groups = lists_dev // GROUP_LISTS
    chunks = block_groups
    block_steps = block_groups // STEP_GROUPS
    width = rows_q // dims
    x, z, s = lax.axis_index('rep'), lax.axis_index('dim'), lax.axis_index('shard')
    twin, across, far = flip(s, 1), flip(s, 2), flip(flip(s, 1), 2)
    other_x = 1 - x

    def at(**place):
        return {'rep': x, 'dim': z, 'shard': s, **place}

    def step_rows(step):
        return pl.ds(pl.multiple_of(step * STEP_ROWS, STEP_ROWS), STEP_ROWS)

    def remote(src, dst, send, recv, device):
        return pltpu.make_async_remote_copy(src_ref=src, dst_ref=dst, send_sem=send, recv_sem=recv,
                                            device_id=device, device_id_type=MESH)

    def load_list(block):
        return pltpu.make_async_copy(l_hbm.at[step_rows(block)], raw.at[step_rows(block)], load_l.at[block])

    def load_query(part):
        rows = pl.ds(pl.multiple_of(part * width, width), width)
        return pltpu.make_async_copy(q_hbm.at[rows], qv.at[rows], load_q.at[part])

    def own_copy(block):
        return remote(vecs.at[step_rows(block)], vecs.at[step_rows(block_steps + block)],
                      send_o.at[block], recv_o.at[block], at(shard=twin))

    def piece(group, chunk):
        first = pl.multiple_of(group * GROUP_ROWS + chunk % 2 * PIECE_ROWS, PIECE_ROWS)
        return vecs.at[pl.ds(first, PIECE_ROWS)]

    def slot(chunk, which):
        return piece(2 * block_groups + STEP_GROUPS * (chunk // 2) + which, chunk)

    def y_copy(chunk):
        return remote(piece(chunks // 2 * x + chunk // 2, chunk), slot(chunk, 0), send_y.at[chunk], recv_y.at[chunk], at(shard=across))

    def x_copy(chunk):
        return remote(slot(chunk, 0), slot(chunk, 1), send_x.at[chunk], recv_x.at[chunk], at(rep=other_x))

    def dy_copy(chunk):
        return remote(slot(chunk, 0), slot(chunk, 2), send_dy.at[chunk], recv_dy.at[chunk], at(shard=twin))

    def dx_copy(chunk):
        return remote(slot(chunk, 1), slot(chunk, 3), send_dx.at[chunk], recv_dx.at[chunk], at(shard=twin))

    def id_copy(which, peer):
        return remote(ids_ref, ids_all.at[s], send_i.at[which], recv_i.at[which], at(shard=peer))

    def peer_slot(source, target):
        return (source - target - 1 + dims) % dims

    def part_copy(target, which):
        return remote(acc.at[target], parts.at[peer_slot(z, target)], send_r.at[which], recv_r.at[peer_slot(z, target)], at(dim=target))

    def res_copy(target, which):
        return remote(res.at[z], res.at[z], send_g.at[which], recv_g.at[peer_slot(z, target)], at(dim=target))

    def target_at(turn):
        if dims == 1:
            return 0
        half = dims // 2
        low = z // half == 0
        ahead = turn
        far_target = jnp.where(low, dims - 1 - ahead, ahead)
        near = turn - half
        base = jnp.where(low, 0, half)
        near_target = base + (z - base + 1 + near) % half
        return jnp.where(turn < half, far_target, near_target)

    def block_at(turn):
        return (block_steps // 2 * x + turn) % block_steps

    for turn in range(block_steps):
        load_list(block_at(turn)).start()

    barrier = pltpu.get_barrier_semaphore()
    peers = [at(shard=twin), at(shard=across), at(shard=far), at(rep=other_x)]
    peers += [at(dim=(z + hop) % dims) for hop in range(1, dims)]
    for peer in peers:
        pl.semaphore_signal(barrier, inc=1, device_id=peer, device_id_type=MESH)

    row = lax.broadcasted_iota(jnp.int32, (STEP_ROWS, STEP_ROWS), 0)
    col = lax.broadcasted_iota(jnp.int32, (STEP_ROWS, STEP_ROWS), 1)
    source = (row // GROUP_ROWS) * GROUP_ROWS + (row % GROUP_LISTS) * LIST_LEN + (row // GROUP_LISTS) % LIST_LEN
    perm[...] = jnp.where(col == source, 1.0, 0.0).astype(jnp.bfloat16)

    window = 2 * STEP_GROUPS

    def send_block(turn):
        @pl.when(turn == 0)
        def _():
            for chunk in range(window):
                y_copy(chunk).start()
        own_copy(block_at(turn)).start()

    def arrange(turn):
        block = block_at(turn)
        load_list(block).wait()
        moved = jnp.dot(perm[...], raw[step_rows(block), :], preferred_element_type=jnp.float32)
        vecs[step_rows(block), :] = moved.astype(jnp.bfloat16)

    arrange(0)
    for part in range(dims):
        load_query(part).start()
    ids_all[s] = ids_ref[...]
    pl.semaphore_wait(barrier, len(peers))

    def arrange_send(turn, carry):
        arrange(turn)
        send_block(turn - 1)
        return carry

    lax.fori_loop(1, block_steps, arrange_send, 0)
    for which, peer in enumerate((twin, across, far)):
        id_copy(which, peer).start()
    acc[...] = jnp.zeros_like(acc)
    send_block(block_steps - 1)

    for part in range(dims):
        load_query(part).wait()
    for which, peer in enumerate((twin, across, far)):
        remote(ids_ref, ids_all.at[peer], send_i.at[which], recv_i.at[which], at(shard=peer)).wait_recv()

    def name_candidates(tile, carry):
        cols = pl.ds(pl.multiple_of(z * width + tile * LANES, LANES), LANES)
        probe = probes_ref[:, cols]
        lane, page = probe % LANES, probe // LANES
        pages = lists_dev // LANES
        for member in range(LIST_LEN):
            got = jnp.zeros((probe.shape[0], LANES), jnp.int32)
            for number in range(4 * pages):
                table = ids_all[number // pages, member:member + 1, (number % pages) * LANES:(number % pages + 1) * LANES]
                table = jnp.broadcast_to(table, (probe.shape[0], LANES))
                picked = jnp.take_along_axis(table, lane, axis=1, mode='promise_in_bounds')
                got = jnp.where(page == number, picked, got)
            cand_ids[member, :, pl.ds(pl.multiple_of(tile * LANES, LANES), LANES)] = got.astype(jnp.float32)
        return carry

    lax.fori_loop(0, width // LANES, name_candidates, 0)

    def score(step, heads, part):
        lists = vecs[step_rows(step), :]
        rows = pl.ds(pl.multiple_of(part * width, width), width)
        scores = lax.dot_general(lists, qv[rows, :], (((1,), (1,)), ((), ())), preferred_element_type=jnp.float32)
        for tile in range(width // LANES):
            probe = probes_ref[:, pl.ds(pl.multiple_of(part * width + tile * LANES, LANES), LANES)]
            low, head = probe % GROUP_LISTS, probe // GROUP_LISTS
            hits = [head == want for want in heads]
            lanes = slice(tile * LANES, (tile + 1) * LANES)
            for member in range(LIST_LEN):
                kept = acc[part, member, :, lanes]
                for group, hit in enumerate(hits):
                    first = group * GROUP_ROWS + member * GROUP_LISTS
                    picked = jnp.take_along_axis(scores[first:first + GROUP_LISTS, lanes], low, axis=0, mode='promise_in_bounds')
                    kept = jnp.where(hit, picked, kept)
                acc[part, member, :, lanes] = kept

    def heads_at(step):
        local = step < 2 * block_steps
        group = step - 2 * block_steps
        base = block_groups * jnp.where(step < block_steps, s, twin) + STEP_GROUPS * (step % block_steps)
        heads = []
        for which in range(STEP_GROUPS):
            home = across if which < 2 else far
            side = x if which % 2 == 0 else other_x
            heads.append(jnp.where(local, base + which, block_groups * home + chunks // 2 * side + group))
        return heads

    last = 2 * block_steps + chunks // 2 - 1
    paced = last - 4

    def pass_y(chunk):
        y_copy(chunk).wait_recv()
        x_copy(chunk).start()
        dy_copy(chunk).start()

        @pl.when(chunk + window < chunks)
        def _():
            y_copy(chunk + window).start()

    def pass_x(chunk):
        x_copy(chunk).wait_recv()
        dx_copy(chunk).start()

    def pass_on(step):
        @pl.when((step >= 1) & (step < paced))
        def _():
            pass_y(step - 1)

        @pl.when((step >= 4) & (step <= paced))
        def _():
            pass_x(step - 4)

        @pl.when((step >= paced) & (step < paced + 3))
        def _():
            first = chunks - 6 + 2 * (step - paced)
            pass_y(first)
            pass_x(first - 2)
            pass_y(first + 1)
            pass_x(first - 1)

        @pl.when(step >= paced + 3)
        def _():
            pass_x(step - last + chunks - 1)

        @pl.when((step >= block_steps) & (step < 2 * block_steps))
        def _():
            own_copy(step - block_steps).wait_recv()

        @pl.when(step >= 2 * block_steps)
        def _():
            first = 2 * (step - 2 * block_steps)
            for chunk in (first, first + 1):
                dy_copy(chunk).wait_recv()
                dx_copy(chunk).wait_recv()

    def main(step, carry):
        pass_on(step)
        heads = heads_at(step)
        for part in range(dims):
            score(step, heads, part)
        return carry

    lax.fori_loop(0, last, main, 0)
    pass_on(last)
    last_heads = heads_at(jnp.int32(last))

    def finish(turn, carry):
        score(last, last_heads, target_at(turn))

        @pl.when(turn > 0)
        def _():
            part_copy(target_at(turn - 1), turn - 1).start()
        return carry

    lax.fori_loop(0, dims, finish, 0)

    for which in range(dims - 1):
        remote(acc.at[z], parts.at[which], send_r.at[which], recv_r.at[which], at()).wait_recv()

    scores, names = [], []
    for member in range(LIST_LEN):
        total = acc[z, member]
        for which in range(dims - 1):
            total = total + parts[which, member]
        name = cand_ids[member]
        real = name >= 0.0
        scores.append(jnp.where(real, total, -jnp.inf))
        names.append(jnp.where(real, name, BIG))
    for place in range(TOP_K):
        best = functools.reduce(jnp.maximum, scores)
        best = jnp.max(best, axis=0, keepdims=True)
        tied = [jnp.where(score_j == best, name_j, BIG) for score_j, name_j in zip(scores, names)]
        first = jnp.min(functools.reduce(jnp.minimum, tied), axis=0, keepdims=True)
        res[z, place:place + 1, :] = best
        res[z, TOP_K + place:TOP_K + place + 1, :] = first
        if place + 1 < TOP_K:
            scores = [jnp.where(name_j == first, -jnp.inf, score_j) for score_j, name_j in zip(scores, names)]

    def drain_local(block, carry):
        own_copy(block).wait_send()
        return carry

    def drain_chunks(chunk, carry):
        y_copy(chunk).wait_send()
        x_copy(chunk).wait_send()
        dy_copy(chunk).wait_send()
        dx_copy(chunk).wait_send()
        return carry

    lax.fori_loop(0, block_steps, drain_local, 0)
    lax.fori_loop(0, chunks, drain_chunks, 0)
    for which, peer in enumerate((twin, across, far)):
        id_copy(which, peer).wait_send()
    for which in range(dims - 1):
        part_copy(target_at(which), which).wait_send()

    for which in range(dims - 1):
        res_copy(target_at(which), which).start()
    for which in range(dims - 1):
        remote(res.at[z], res.at[(z + 1 + which) % dims], send_g.at[which], recv_g.at[which], at()).wait_recv()
    for which in range(dims - 1):
        res_copy(target_at(which), which).wait_send()


def place_kernel(res, out_s, out_i):
    dims, _, width = res.shape
    for part in range(dims):
        cols = slice(part * width, (part + 1) * width)
        out_s[:, cols] = res[part, 0:TOP_K, :]
        out_i[:, cols] = res[part, TOP_K:2 * TOP_K, :].astype(jnp.int32)


def solution(mesh):
    dims = mesh.shape['dim']
    row_spec = P(('rep', 'shard'), None)

    def local_search(queries, list_vecs, list_ids, probes):
        rows_q, depth = queries.shape
        lists_dev, list_len, _ = list_vecs.shape
        probe_count = probes.shape[1]
        block_rows = lists_dev * list_len
        block_steps = block_rows // STEP_ROWS
        chunks = lists_dev // GROUP_LISTS
        width = rows_q // dims
        dma = pltpu.SemaphoreType.DMA
        any_spec = pl.BlockSpec(memory_space=pl.ANY)
        vmem_spec = pl.BlockSpec(memory_space=pltpu.VMEM)
        found = pl.pallas_call(
            functools.partial(search_kernel, dims),
            out_shape=jax.ShapeDtypeStruct((dims, 2 * TOP_K, width), jnp.float32),
            in_specs=[any_spec, any_spec, vmem_spec, vmem_spec],
            out_specs=vmem_spec,
            scratch_shapes=[
                pltpu.VMEM((block_rows, depth), jnp.bfloat16),
                pltpu.VMEM((rows_q, depth), jnp.bfloat16),
                pltpu.VMEM((4 * block_rows, depth), jnp.bfloat16),
                pltpu.VMEM((STEP_ROWS, STEP_ROWS), jnp.bfloat16),
                pltpu.VMEM((dims, LIST_LEN, probe_count, width), jnp.float32),
                pltpu.VMEM((dims - 1, LIST_LEN, probe_count, width), jnp.float32),
                pltpu.VMEM((4, LIST_LEN, lists_dev), jnp.int32),
                pltpu.VMEM((LIST_LEN, probe_count, width), jnp.float32),
                dma((block_steps,)), dma((dims,)),
                dma((block_steps,)), dma((block_steps,)),
                dma((chunks,)), dma((chunks,)), dma((chunks,)), dma((chunks,)),
                dma((chunks,)), dma((chunks,)), dma((chunks,)), dma((chunks,)),
                dma((3,)), dma((3,)),
                dma((dims - 1,)), dma((dims - 1,)), dma((dims - 1,)), dma((dims - 1,)),
            ],
            compiler_params=pltpu.CompilerParams(collective_id=0, has_side_effects=True, vmem_limit_bytes=60 * 2**20),
            name='ivf_search',
        )(queries, list_vecs.reshape(block_rows, depth), probes.T, list_ids.T)
        scores, ids = pl.pallas_call(
            place_kernel,
            out_shape=(jax.ShapeDtypeStruct((TOP_K, rows_q), jnp.float32),
                       jax.ShapeDtypeStruct((TOP_K, rows_q), jnp.int32)),
            in_specs=[vmem_spec],
            out_specs=(vmem_spec, vmem_spec),
            name='place',
        )(found)
        return scores.T, ids.T

    return jax.shard_map(local_search, mesh=mesh,
                         in_specs=(P(('rep', 'shard'), 'dim'), P('shard', None, 'dim'), P('shard', None), row_spec),
                         out_specs=(row_spec, row_spec), check_vma=False)
```

```python
import functools

import jax
import jax.numpy as jnp
from jax import lax
from jax.experimental import pallas as pl
from jax.experimental.pallas import tpu as pltpu
from jax.sharding import PartitionSpec as P

TOP_K = 10
LIST_LEN = 8
GROUP_LISTS = 8
GROUP_ROWS = GROUP_LISTS * LIST_LEN
STEP_GROUPS = 4
STEP_ROWS = STEP_GROUPS * GROUP_ROWS
PIECE_ROWS = GROUP_ROWS // 2
LANES = 128
MESH = pl.DeviceIdType.MESH
BIG = 1e9


def flip(index, bit):
    return index + bit - 2 * bit * ((index // bit) % 2)


def search_kernel(dims, q_hbm, l_hbm, probes_ref, ids_ref, res,
                  raw, qv, vecs, perm, acc, parts, ids_all, cand_ids,
                  load_l, load_q, send_o, recv_o, send_y, recv_y, send_x, recv_x,
                  send_dy, recv_dy, send_dx, recv_dx, send_i, recv_i,
                  send_r, recv_r, send_g, recv_g):
    rows_q = qv.shape[0]
    lists_dev = ids_ref.shape[1]
    block_rows = lists_dev * LIST_LEN
    block_groups = lists_dev // GROUP_LISTS
    chunks = block_groups
    block_steps = block_groups // STEP_GROUPS
    width = rows_q // dims
    x, z, s = lax.axis_index('rep'), lax.axis_index('dim'), lax.axis_index('shard')
    twin, across, far = flip(s, 1), flip(s, 2), flip(flip(s, 1), 2)
    other_x = 1 - x

    def at(**place):
        return {'rep': x, 'dim': z, 'shard': s, **place}

    def step_rows(step):
        return pl.ds(pl.multiple_of(step * STEP_ROWS, STEP_ROWS), STEP_ROWS)

    def remote(src, dst, send, recv, device):
        return pltpu.make_async_remote_copy(src_ref=src, dst_ref=dst, send_sem=send, recv_sem=recv,
                                            device_id=device, device_id_type=MESH)

    def load_list(block):
        return pltpu.make_async_copy(l_hbm.at[step_rows(block)], raw.at[step_rows(block)], load_l.at[block])

    def load_query(part):
        rows = pl.ds(pl.multiple_of(part * width, width), width)
        return pltpu.make_async_copy(q_hbm.at[rows], qv.at[rows], load_q.at[part])

    def own_copy(block):
        return remote(vecs.at[step_rows(block)], vecs.at[step_rows(block_steps + block)],
                      send_o.at[block], recv_o.at[block], at(shard=twin))

    def piece(group, chunk):
        first = pl.multiple_of(group * GROUP_ROWS + chunk % 2 * PIECE_ROWS, PIECE_ROWS)
        return vecs.at[pl.ds(first, PIECE_ROWS)]

    def slot(chunk, which):
        return piece(2 * block_groups + STEP_GROUPS * (chunk // 2) + which, chunk)

    def y_copy(chunk):
        return remote(piece(chunks // 2 * x + chunk // 2, chunk), slot(chunk, 0), send_y.at[chunk], recv_y.at[chunk], at(shard=across))

    def x_copy(chunk):
        return remote(slot(chunk, 0), slot(chunk, 1), send_x.at[chunk], recv_x.at[chunk], at(rep=other_x))

    def dy_copy(chunk):
        return remote(slot(chunk, 0), slot(chunk, 2), send_dy.at[chunk], recv_dy.at[chunk], at(shard=twin))

    def dx_copy(chunk):
        return remote(slot(chunk, 1), slot(chunk, 3), send_dx.at[chunk], recv_dx.at[chunk], at(shard=twin))

    def id_copy(which, peer):
        return remote(ids_ref, ids_all.at[s], send_i.at[which], recv_i.at[which], at(shard=peer))

    def peer_slot(source, target):
        return (source - target - 1 + dims) % dims

    def part_copy(target, which):
        return remote(acc.at[target], parts.at[peer_slot(z, target)], send_r.at[which], recv_r.at[peer_slot(z, target)], at(dim=target))

    def res_copy(target, which):
        return remote(res.at[z], res.at[z], send_g.at[which], recv_g.at[peer_slot(z, target)], at(dim=target))

    def target_at(turn):
        if dims == 1:
            return 0
        half = dims // 2
        low = z // half == 0
        ahead = turn
        far_target = jnp.where(low, dims - 1 - ahead, ahead)
        near = turn - half
        base = jnp.where(low, 0, half)
        near_target = base + (z - base + 1 + near) % half
        return jnp.where(turn < half, far_target, near_target)

    def block_at(turn):
        return (block_steps // 2 * x + turn) % block_steps

    load_list(block_at(0)).start()
    for part in range(dims):
        load_query(part).start()
    for turn in range(1, block_steps):
        load_list(block_at(turn)).start()

    barrier = pltpu.get_barrier_semaphore()
    peers = [at(shard=twin), at(shard=across), at(shard=far), at(rep=other_x)]
    peers += [at(dim=(z + hop) % dims) for hop in range(1, dims)]
    for peer in peers:
        pl.semaphore_signal(barrier, inc=1, device_id=peer, device_id_type=MESH)

    row = lax.broadcasted_iota(jnp.int32, (STEP_ROWS, STEP_ROWS), 0)
    col = lax.broadcasted_iota(jnp.int32, (STEP_ROWS, STEP_ROWS), 1)
    source = (row // GROUP_ROWS) * GROUP_ROWS + (row % GROUP_LISTS) * LIST_LEN + (row // GROUP_LISTS) % LIST_LEN
    perm[...] = jnp.where(col == source, 1.0, 0.0).astype(jnp.bfloat16)

    def arrange(turn):
        block = block_at(turn)
        moved = jnp.dot(perm[...], raw[step_rows(block), :], preferred_element_type=jnp.float32)
        vecs[step_rows(block), :] = moved.astype(jnp.bfloat16)

    window = 2 * STEP_GROUPS
    load_list(block_at(0)).wait()
    arrange(0)
    pl.semaphore_wait(barrier, len(peers))
    for chunk in range(window):
        y_copy(chunk).start()
    ids_all[s] = ids_ref[...]
    acc[...] = jnp.zeros_like(acc)
    for which, peer in enumerate((twin, across, far)):
        id_copy(which, peer).start()
    for part in range(dims):
        load_query(part).wait()

    def name_candidates(tile, carry):
        cols = pl.ds(pl.multiple_of(z * width + tile * LANES, LANES), LANES)
        probe = probes_ref[:, cols]
        lane, page = probe % LANES, probe // LANES
        pages = lists_dev // LANES
        for member in range(LIST_LEN):
            got = jnp.zeros((probe.shape[0], LANES), jnp.int32)
            for number in range(4 * pages):
                table = ids_all[number // pages, member:member + 1, (number % pages) * LANES:(number % pages + 1) * LANES]
                table = jnp.broadcast_to(table, (probe.shape[0], LANES))
                picked = jnp.take_along_axis(table, lane, axis=1, mode='promise_in_bounds')
                got = jnp.where(page == number, picked, got)
            cand_ids[member, :, pl.ds(pl.multiple_of(tile * LANES, LANES), LANES)] = got.astype(jnp.float32)
        return carry

    def list_block(step):
        return jnp.where(step < block_steps, block_at(step), step % block_steps)

    def score(step, heads, part):
        lists = vecs[step_rows(jnp.where(step < block_steps, block_at(step), step)), :]
        rows = pl.ds(pl.multiple_of(part * width, width), width)
        scores = lax.dot_general(lists, qv[rows, :], (((1,), (1,)), ((), ())), preferred_element_type=jnp.float32)
        for tile in range(width // LANES):
            probe = probes_ref[:, pl.ds(pl.multiple_of(part * width + tile * LANES, LANES), LANES)]
            low, head = probe % GROUP_LISTS, probe // GROUP_LISTS
            hits = [head == want for want in heads]
            lanes = slice(tile * LANES, (tile + 1) * LANES)
            for member in range(LIST_LEN):
                kept = acc[part, member, :, lanes]
                for group, hit in enumerate(hits):
                    first = group * GROUP_ROWS + member * GROUP_LISTS
                    picked = jnp.take_along_axis(scores[first:first + GROUP_LISTS, lanes], low, axis=0, mode='promise_in_bounds')
                    kept = jnp.where(hit, picked, kept)
                acc[part, member, :, lanes] = kept

    def heads_at(step):
        local = step < 2 * block_steps
        group = step - 2 * block_steps
        base = block_groups * jnp.where(step < block_steps, s, twin) + STEP_GROUPS * list_block(step)
        heads = []
        for which in range(STEP_GROUPS):
            home = across if which < 2 else far
            side = x if which % 2 == 0 else other_x
            heads.append(jnp.where(local, base + which, block_groups * home + chunks // 2 * side + group))
        return heads

    last = 2 * block_steps + chunks // 2 - 1

    def pass_y(chunk):
        y_copy(chunk).wait_recv()
        x_copy(chunk).start()
        dy_copy(chunk).start()

        @pl.when(chunk + window < chunks)
        def _():
            y_copy(chunk + window).start()

    def pass_x(chunk):
        x_copy(chunk).wait_recv()
        dx_copy(chunk).start()

    def await_step(step):
        first = 2 * (step - 2 * block_steps)
        for chunk in (first, first + 1):
            dy_copy(chunk).wait_recv()
            dx_copy(chunk).wait_recv()

    def score_all(step):
        heads = heads_at(step)
        for part in range(dims):
            score(step, heads, part)

    def early(step, carry):
        own_copy(block_at(step)).start()

        @pl.when(step >= 2)
        def _():
            pass_y(jnp.where(step <= 5, step - 2, step - 1))

        @pl.when(step == 5)
        def _():
            pass_y(4)

        @pl.when(step >= 5)
        def _():
            pass_x(step - 5)
        load_list(block_at(step + 1)).wait()
        score_all(step)
        arrange(step + 1)
        return carry

    def middle(step, carry):
        pass_y(step - 1)
        pass_x(step - 5)

        @pl.when(step == block_steps - 1)
        def _():
            own_copy(block_at(step)).start()

        @pl.when((step >= block_steps) & (step < 2 * block_steps))
        def _():
            own_copy(step - block_steps).wait_recv()

        @pl.when(step >= 2 * block_steps)
        def _():
            await_step(step)
        score_all(step)
        return carry

    late_plan = {
        last - 5: 'y25 x21 x22',
        last - 4: 'y26 y27 x23',
        last - 3: 'y28 y29 x24 x25 y30',
        last - 2: 'y31 x26 x27',
        last - 1: 'x28 x29 x30',
    }

    def late(step, carry):
        for when, plan in late_plan.items():
            @pl.when(step == when)
            def _(plan=plan):
                for word in plan.split():
                    (pass_y if word[0] == 'y' else pass_x)(int(word[1:]))

        @pl.when(step == last - 1)
        def _():
            for which, peer in enumerate((twin, across, far)):
                remote(ids_ref, ids_all.at[peer], send_i.at[which], recv_i.at[which], at(shard=peer)).wait_recv()
            lax.fori_loop(0, width // LANES, name_candidates, 0)
        await_step(step)
        score_all(step)
        return carry

    lax.fori_loop(0, block_steps - 1, early, 0)
    lax.fori_loop(block_steps - 1, last - 5, middle, 0)
    lax.fori_loop(last - 5, last, late, 0)
    pass_x(chunks - 1)
    await_step(jnp.int32(last))
    last_heads = heads_at(jnp.int32(last))

    def finish(turn, carry):
        @pl.when(turn > 0)
        def _():
            part_copy(target_at(turn - 1), turn - 1).start()
        score(jnp.int32(last), last_heads, target_at(turn))
        return carry

    lax.fori_loop(0, dims, finish, 0)

    for which in range(dims - 1):
        remote(acc.at[z], parts.at[which], send_r.at[which], recv_r.at[which], at()).wait_recv()

    scores, names = [], []
    for member in range(LIST_LEN):
        total = acc[z, member]
        for which in range(dims - 1):
            total = total + parts[which, member]
        name = cand_ids[member]
        real = name >= 0.0
        scores.append(jnp.where(real, total, -jnp.inf))
        names.append(jnp.where(real, name, BIG))
    for place in range(TOP_K):
        best = functools.reduce(jnp.maximum, scores)
        best = jnp.max(best, axis=0, keepdims=True)
        tied = [jnp.where(score_j == best, name_j, BIG) for score_j, name_j in zip(scores, names)]
        first = jnp.min(functools.reduce(jnp.minimum, tied), axis=0, keepdims=True)
        res[z, place:place + 1, :] = best
        res[z, TOP_K + place:TOP_K + place + 1, :] = first
        if place + 1 < TOP_K:
            scores = [jnp.where(name_j == first, -jnp.inf, score_j) for score_j, name_j in zip(scores, names)]

    def drain_local(block, carry):
        own_copy(block).wait_send()
        return carry

    def drain_chunks(chunk, carry):
        y_copy(chunk).wait_send()
        x_copy(chunk).wait_send()
        dy_copy(chunk).wait_send()
        dx_copy(chunk).wait_send()
        return carry

    lax.fori_loop(0, block_steps, drain_local, 0)
    lax.fori_loop(0, chunks, drain_chunks, 0)
    for which, peer in enumerate((twin, across, far)):
        id_copy(which, peer).wait_send()
    for which in range(dims - 1):
        part_copy(target_at(which), which).wait_send()

    for which in range(dims - 1):
        res_copy(target_at(which), which).start()
    for which in range(dims - 1):
        remote(res.at[z], res.at[(z + 1 + which) % dims], send_g.at[which], recv_g.at[which], at()).wait_recv()
    for which in range(dims - 1):
        res_copy(target_at(which), which).wait_send()


def place_kernel(res, out_s, out_i):
    dims, _, width = res.shape
    for part in range(dims):
        cols = slice(part * width, (part + 1) * width)
        out_s[:, cols] = res[part, 0:TOP_K, :]
        out_i[:, cols] = res[part, TOP_K:2 * TOP_K, :].astype(jnp.int32)


def solution(mesh):
    dims = mesh.shape['dim']
    row_spec = P(('rep', 'shard'), None)

    def local_search(queries, list_vecs, list_ids, probes):
        rows_q, depth = queries.shape
        lists_dev, list_len, _ = list_vecs.shape
        probe_count = probes.shape[1]
        block_rows = lists_dev * list_len
        block_steps = block_rows // STEP_ROWS
        chunks = lists_dev // GROUP_LISTS
        width = rows_q // dims
        dma = pltpu.SemaphoreType.DMA
        any_spec = pl.BlockSpec(memory_space=pl.ANY)
        vmem_spec = pl.BlockSpec(memory_space=pltpu.VMEM)
        found = pl.pallas_call(
            functools.partial(search_kernel, dims),
            out_shape=jax.ShapeDtypeStruct((dims, 2 * TOP_K, width), jnp.float32),
            in_specs=[any_spec, any_spec, vmem_spec, vmem_spec],
            out_specs=vmem_spec,
            scratch_shapes=[
                pltpu.VMEM((block_rows, depth), jnp.bfloat16),
                pltpu.VMEM((rows_q, depth), jnp.bfloat16),
                pltpu.VMEM((4 * block_rows, depth), jnp.bfloat16),
                pltpu.VMEM((STEP_ROWS, STEP_ROWS), jnp.bfloat16),
                pltpu.VMEM((dims, LIST_LEN, probe_count, width), jnp.float32),
                pltpu.VMEM((dims - 1, LIST_LEN, probe_count, width), jnp.float32),
                pltpu.VMEM((4, LIST_LEN, lists_dev), jnp.int32),
                pltpu.VMEM((LIST_LEN, probe_count, width), jnp.float32),
                dma((block_steps,)), dma((dims,)),
                dma((block_steps,)), dma((block_steps,)),
                dma((chunks,)), dma((chunks,)), dma((chunks,)), dma((chunks,)),
                dma((chunks,)), dma((chunks,)), dma((chunks,)), dma((chunks,)),
                dma((3,)), dma((3,)),
                dma((dims - 1,)), dma((dims - 1,)), dma((dims - 1,)), dma((dims - 1,)),
            ],
            compiler_params=pltpu.CompilerParams(collective_id=0, has_side_effects=True, vmem_limit_bytes=60 * 2**20),
            name='ivf_search',
        )(queries, list_vecs.reshape(block_rows, depth), probes.T, list_ids.T)
        scores, ids = pl.pallas_call(
            place_kernel,
            out_shape=(jax.ShapeDtypeStruct((TOP_K, rows_q), jnp.float32),
                       jax.ShapeDtypeStruct((TOP_K, rows_q), jnp.int32)),
            in_specs=[vmem_spec],
            out_specs=(vmem_spec, vmem_spec),
            name='place',
        )(found)
        return scores.T, ids.T

    return jax.shard_map(local_search, mesh=mesh,
                         in_specs=(P(('rep', 'shard'), 'dim'), P('shard', None, 'dim'), P('shard', None), row_spec),
                         out_specs=(row_spec, row_spec), check_vma=False)
```

```python
import functools

import jax
import jax.numpy as jnp
from jax import lax
from jax.experimental import pallas as pl
from jax.experimental.pallas import tpu as pltpu
from jax.sharding import PartitionSpec as P

TOP_K = 10
LIST_LEN = 8
GROUP_LISTS = 8
GROUP_ROWS = GROUP_LISTS * LIST_LEN
STEP_GROUPS = 4
STEP_ROWS = STEP_GROUPS * GROUP_ROWS
PIECE_ROWS = GROUP_ROWS // 2
LANES = 128
MESH = pl.DeviceIdType.MESH
BIG = 1e9


def flip(index, bit):
    return index + bit - 2 * bit * ((index // bit) % 2)


def search_kernel(dims, q_hbm, l_hbm, probes_hbm, ids_hbm, res,
                  raw, qv, vecs, perm, acc, parts, ids_all, cand_ids, probes_ref, ids_ref, load_p, load_i,
                  load_l, load_q, send_o, recv_o, send_y, recv_y, send_x, recv_x,
                  send_dy, recv_dy, send_dx, recv_dx, send_i, recv_i,
                  send_r, recv_r, send_g, recv_g):
    rows_q = qv.shape[0]
    lists_dev = ids_ref.shape[1]
    block_rows = lists_dev * LIST_LEN
    block_groups = lists_dev // GROUP_LISTS
    chunks = block_groups
    block_steps = block_groups // STEP_GROUPS
    width = rows_q // dims
    x, z, s = lax.axis_index('rep'), lax.axis_index('dim'), lax.axis_index('shard')
    twin, across, far = flip(s, 1), flip(s, 2), flip(flip(s, 1), 2)
    other_x = 1 - x

    def at(**place):
        return {'rep': x, 'dim': z, 'shard': s, **place}

    def step_rows(step):
        return pl.ds(pl.multiple_of(step * STEP_ROWS, STEP_ROWS), STEP_ROWS)

    def remote(src, dst, send, recv, device):
        return pltpu.make_async_remote_copy(src_ref=src, dst_ref=dst, send_sem=send, recv_sem=recv,
                                            device_id=device, device_id_type=MESH)

    def load_list(block):
        return pltpu.make_async_copy(l_hbm.at[step_rows(block)], raw.at[step_rows(block)], load_l.at[block])

    def load_query(part):
        rows = pl.ds(pl.multiple_of(part * width, width), width)
        return pltpu.make_async_copy(q_hbm.at[rows], qv.at[rows], load_q.at[part])

    def own_copy(block):
        return remote(vecs.at[step_rows(block)], vecs.at[step_rows(block_steps + block)],
                      send_o.at[block], recv_o.at[block], at(shard=twin))

    def piece(group, chunk):
        first = pl.multiple_of(group * GROUP_ROWS + chunk % 2 * PIECE_ROWS, PIECE_ROWS)
        return vecs.at[pl.ds(first, PIECE_ROWS)]

    def slot(chunk, which):
        return piece(2 * block_groups + STEP_GROUPS * (chunk // 2) + which, chunk)

    def y_copy(chunk):
        return remote(piece(chunks // 2 * x + chunk // 2, chunk), slot(chunk, 0), send_y.at[chunk], recv_y.at[chunk], at(shard=across))

    def x_copy(chunk):
        return remote(slot(chunk, 0), slot(chunk, 1), send_x.at[chunk], recv_x.at[chunk], at(rep=other_x))

    def dy_copy(chunk):
        return remote(slot(chunk, 0), slot(chunk, 2), send_dy.at[chunk], recv_dy.at[chunk], at(shard=twin))

    def dx_copy(chunk):
        return remote(slot(chunk, 1), slot(chunk, 3), send_dx.at[chunk], recv_dx.at[chunk], at(shard=twin))

    def id_copy(which, peer):
        return remote(ids_ref, ids_all.at[s], send_i.at[which], recv_i.at[which], at(shard=peer))

    outer = z % 3 == 0
    mate, far_outer = flip(z, 1), jnp.where(z < 2, dims - 1, 0)
    far_inner = flip(far_outer, 1)
    halves = tuple(pl.ds(half * (LIST_LEN // 2), LIST_LEN // 2) for half in range(2))

    def part_copy(target, place, which, half):
        return remote(acc.at[target, halves[half]], parts.at[place, halves[half]], send_r.at[which, half], recv_r.at[place, half], at(dim=mate))

    def merged_copy(merge, half):
        return remote(parts.at[merge, halves[half]], parts.at[3, halves[half]], send_r.at[1 + merge, half], recv_r.at[3, half],
                      at(dim=(far_outer, far_inner)[merge]))

    def part_wait(place, half):
        remote(acc.at[z, halves[half]], parts.at[place, halves[half]], send_r.at[0, half], recv_r.at[place, half], at()).wait_recv()

    def peer_slot(source, target):
        return (source - target - 1 + dims) % dims

    def res_copy(target, which):
        return remote(res.at[z], res.at[z], send_g.at[which], recv_g.at[peer_slot(z, target)], at(dim=target))

    def target_at(turn):
        first, second, third = (jnp.where(outer, one, two) for one, two in ((far_outer, mate), (far_inner, far_outer), (mate, far_inner)))
        return jnp.where(turn == 0, first, jnp.where(turn == 1, second, jnp.where(turn == 2, third, z)))

    def block_at(turn):
        return (block_steps // 2 * x + turn) % block_steps

    load_list(block_at(0)).start()
    probes_in = pltpu.make_async_copy(probes_hbm, probes_ref, load_p)
    ids_in = pltpu.make_async_copy(ids_hbm, ids_ref, load_i)
    ids_in.start()
    probes_in.start()
    for part in range(dims):
        load_query(part).start()
    for turn in range(1, block_steps):
        load_list(block_at(turn)).start()

    barrier = pltpu.get_barrier_semaphore()
    peers = [at(shard=twin), at(shard=across), at(shard=far), at(rep=other_x)]
    peers += [at(dim=(z + hop) % dims) for hop in range(1, dims)]
    for peer in peers:
        pl.semaphore_signal(barrier, inc=1, device_id=peer, device_id_type=MESH)

    row = lax.broadcasted_iota(jnp.int32, (STEP_ROWS, STEP_ROWS), 0)
    col = lax.broadcasted_iota(jnp.int32, (STEP_ROWS, STEP_ROWS), 1)
    source = (row // GROUP_ROWS) * GROUP_ROWS + (row % GROUP_LISTS) * LIST_LEN + (row // GROUP_LISTS) % LIST_LEN
    perm[...] = jnp.where(col == source, 1.0, 0.0).astype(jnp.bfloat16)

    def arrange(turn):
        block = block_at(turn)
        moved = jnp.dot(perm[...], raw[step_rows(block), :], preferred_element_type=jnp.float32)
        vecs[step_rows(block), :] = moved.astype(jnp.bfloat16)

    window = 2 * STEP_GROUPS
    load_list(block_at(0)).wait()
    arrange(0)
    pl.semaphore_wait(barrier, len(peers))
    for chunk in range(window):
        y_copy(chunk).start()
    acc[...] = jnp.zeros_like(acc)
    ids_in.wait()
    for which, peer in enumerate((twin, across, far)):
        id_copy(which, peer).start()
    ids_all[s] = ids_ref[...]
    probes_in.wait()
    for part in range(dims):
        load_query(part).wait()

    def name_candidates(tile, carry):
        cols = pl.ds(pl.multiple_of(z * width + tile * LANES, LANES), LANES)
        probe = probes_ref[:, cols]
        lane, page = probe % LANES, probe // LANES
        pages = lists_dev // LANES
        for member in range(LIST_LEN):
            got = jnp.zeros((probe.shape[0], LANES), jnp.int32)
            for number in range(4 * pages):
                table = ids_all[number // pages, member:member + 1, (number % pages) * LANES:(number % pages + 1) * LANES]
                table = jnp.broadcast_to(table, (probe.shape[0], LANES))
                picked = jnp.take_along_axis(table, lane, axis=1, mode='promise_in_bounds')
                got = jnp.where(page == number, picked, got)
            cand_ids[member, :, pl.ds(pl.multiple_of(tile * LANES, LANES), LANES)] = got.astype(jnp.float32)
        return carry

    def list_block(step):
        return jnp.where(step < block_steps, block_at(step), step % block_steps)

    def score(step, heads, part):
        lists = vecs[step_rows(jnp.where(step < block_steps, block_at(step), step)), :]
        rows = pl.ds(pl.multiple_of(part * width, width), width)
        scores = lax.dot_general(lists, qv[rows, :], (((1,), (1,)), ((), ())), preferred_element_type=jnp.float32)
        for tile in range(width // LANES):
            probe = probes_ref[:, pl.ds(pl.multiple_of(part * width + tile * LANES, LANES), LANES)]
            low, head = probe % GROUP_LISTS, probe // GROUP_LISTS
            hits = [head == want for want in heads]
            lanes = slice(tile * LANES, (tile + 1) * LANES)
            for member in range(LIST_LEN):
                kept = acc[part, member, :, lanes]
                for group, hit in enumerate(hits):
                    first = group * GROUP_ROWS + member * GROUP_LISTS
                    picked = jnp.take_along_axis(scores[first:first + GROUP_LISTS, lanes], low, axis=0, mode='promise_in_bounds')
                    kept = jnp.where(hit, picked, kept)
                acc[part, member, :, lanes] = kept

    def heads_at(step):
        local = step < 2 * block_steps
        group = step - 2 * block_steps
        base = block_groups * jnp.where(step < block_steps, s, twin) + STEP_GROUPS * list_block(step)
        heads = []
        for which in range(STEP_GROUPS):
            home = across if which < 2 else far
            side = x if which % 2 == 0 else other_x
            heads.append(jnp.where(local, base + which, block_groups * home + chunks // 2 * side + group))
        return heads

    last = 2 * block_steps + chunks // 2 - 1

    def pass_y(chunk):
        y_copy(chunk).wait_recv()
        x_copy(chunk).start()
        dy_copy(chunk).start()

        @pl.when(chunk + window < chunks)
        def _():
            y_copy(chunk + window).start()

    def pass_x(chunk):
        x_copy(chunk).wait_recv()
        dx_copy(chunk).start()

    def await_step(step):
        first = 2 * (step - 2 * block_steps)
        for chunk in (first, first + 1):
            dy_copy(chunk).wait_recv()
            dx_copy(chunk).wait_recv()

    def score_all(step):
        heads = heads_at(step)
        for part in range(dims):
            score(step, heads, part)

    def early(step, carry):
        own_copy(block_at(step)).start()

        @pl.when(step >= 2)
        def _():
            pass_y(jnp.where(step <= 5, step - 2, step - 1))

        @pl.when(step == 5)
        def _():
            pass_y(4)

        @pl.when(step >= 5)
        def _():
            pass_x(step - 5)
        load_list(block_at(step + 1)).wait()
        score_all(step)
        arrange(step + 1)
        return carry

    def middle(step, carry):
        pass_y(step - 1)
        pass_x(step - 5)

        @pl.when(step == block_steps - 1)
        def _():
            own_copy(block_at(step)).start()

        @pl.when((step >= block_steps) & (step < 2 * block_steps))
        def _():
            own_copy(step - block_steps).wait_recv()

        @pl.when(step >= 2 * block_steps)
        def _():
            await_step(step)
        score_all(step)
        return carry

    late_plan = {
        last - 5: 'y25 x21 x22',
        last - 4: 'y26 y27 x23',
        last - 3: 'y28 y29 x24 x25 y30',
        last - 2: 'y31 x26 x27',
        last - 1: 'x28 x29 x30',
    }

    def late(step, carry):
        for when, plan in late_plan.items():
            @pl.when(step == when)
            def _(plan=plan):
                for word in plan.split():
                    (pass_y if word[0] == 'y' else pass_x)(int(word[1:]))

        @pl.when(step == last - 1)
        def _():
            for which, peer in enumerate((twin, across, far)):
                remote(ids_ref, ids_all.at[peer], send_i.at[which], recv_i.at[which], at(shard=peer)).wait_recv()
            lax.fori_loop(0, width // LANES, name_candidates, 0)
        await_step(step)
        score_all(step)
        return carry

    lax.fori_loop(0, block_steps - 1, early, 0)
    lax.fori_loop(block_steps - 1, last - 5, middle, 0)
    lax.fori_loop(last - 5, last, late, 0)
    pass_x(chunks - 1)
    await_step(jnp.int32(last))
    last_heads = heads_at(jnp.int32(last))

    def finish(turn, carry):
        @pl.when((turn > 0) & (outer | (turn == 1)))
        def _():
            for half in range(2):
                part_copy(target_at(turn - 1), jnp.where(outer, turn - 1, 2), turn - 1, half).start()
        score(jnp.int32(last), last_heads, target_at(turn))
        return carry

    lax.fori_loop(0, dims, finish, 0)

    @pl.when(jnp.logical_not(outer))
    def _():
        for merge, target in enumerate((far_outer, far_inner)):
            for half in range(2):
                part_wait(merge, half)
                parts[merge, halves[half]] += acc[target, halves[half]]
                merged_copy(merge, half).start()

    for place in (2, 3):
        for half in range(2):
            part_wait(place, half)

    tiles = width // LANES
    scores, names = [], []
    for member in range(LIST_LEN):
        total = acc[z, member]
        total = total + parts[2, member] + parts[3, member]
        name = cand_ids[member]
        real = name >= 0.0
        scores.append(jnp.where(real, total, -jnp.inf))
        names.append(jnp.where(real, name, BIG))
    for place in range(TOP_K):
        best = functools.reduce(jnp.maximum, scores)
        best = jnp.max(best, axis=0, keepdims=True)
        tied = [jnp.where(score_j == best, name_j, BIG) for score_j, name_j in zip(scores, names)]
        first = jnp.min(functools.reduce(jnp.minimum, tied), axis=0, keepdims=True)
        for tile in range(tiles):
            lanes = slice(tile * LANES, (tile + 1) * LANES)
            line = place * tiles + tile
            res[z, line:line + 1, :] = best[:, lanes]
            res[z, TOP_K * tiles + line:TOP_K * tiles + line + 1, :] = first[:, lanes]
        if place + 1 < TOP_K:
            scores = [jnp.where(name_j == first, -jnp.inf, score_j) for score_j, name_j in zip(scores, names)]

    def drain_local(block, carry):
        own_copy(block).wait_send()
        return carry

    def drain_chunks(chunk, carry):
        y_copy(chunk).wait_send()
        x_copy(chunk).wait_send()
        dy_copy(chunk).wait_send()
        dx_copy(chunk).wait_send()
        return carry

    lax.fori_loop(0, block_steps, drain_local, 0)
    lax.fori_loop(0, chunks, drain_chunks, 0)
    for which, peer in enumerate((twin, across, far)):
        id_copy(which, peer).wait_send()
    for which in range(3):
        for half in range(2):
            part_copy(z, 2, which, half).wait_send()

    for which in range(dims - 1):
        res_copy(target_at(which), which).start()
    for which in range(dims - 1):
        remote(res.at[z], res.at[(z + 1 + which) % dims], send_g.at[which], recv_g.at[which], at()).wait_recv()
    for which in range(dims - 1):
        res_copy(target_at(which), which).wait_send()


def place_kernel(res, out_s, out_i):
    dims, lines, _ = res.shape
    tiles = lines // (2 * TOP_K)
    for part in range(dims):
        for tile in range(tiles):
            first = (part * tiles + tile) * LANES
            out_s[:, first:first + LANES] = res[part, pl.ds(tile, TOP_K, stride=tiles), :]
            out_i[:, first:first + LANES] = res[part, pl.ds(TOP_K * tiles + tile, TOP_K, stride=tiles), :].astype(jnp.int32)


def solution(mesh):
    dims = mesh.shape['dim']
    row_spec = P(('rep', 'shard'), None)

    def local_search(queries, list_vecs, list_ids, probes):
        rows_q, depth = queries.shape
        lists_dev, list_len, _ = list_vecs.shape
        probe_count = probes.shape[1]
        block_rows = lists_dev * list_len
        block_steps = block_rows // STEP_ROWS
        chunks = lists_dev // GROUP_LISTS
        width = rows_q // dims
        dma = pltpu.SemaphoreType.DMA
        any_spec = pl.BlockSpec(memory_space=pl.ANY)
        vmem_spec = pl.BlockSpec(memory_space=pltpu.VMEM)
        found = pl.pallas_call(
            functools.partial(search_kernel, dims),
            out_shape=pltpu.VMEM((dims, 2 * TOP_K * width // LANES, LANES), jnp.float32),
            in_specs=[any_spec] * 4,
            out_specs=vmem_spec,
            scratch_shapes=[
                pltpu.VMEM((block_rows, depth), jnp.bfloat16),
                pltpu.VMEM((rows_q, depth), jnp.bfloat16),
                pltpu.VMEM((4 * block_rows, depth), jnp.bfloat16),
                pltpu.VMEM((STEP_ROWS, STEP_ROWS), jnp.bfloat16),
                pltpu.VMEM((dims, LIST_LEN, probe_count, width), jnp.float32),
                pltpu.VMEM((4, LIST_LEN, probe_count, width), jnp.float32),
                pltpu.VMEM((4, LIST_LEN, lists_dev), jnp.int32),
                pltpu.VMEM((LIST_LEN, probe_count, width), jnp.float32),
                pltpu.VMEM((probe_count, rows_q), jnp.int32),
                pltpu.VMEM((LIST_LEN, lists_dev), jnp.int32),
                dma, dma,
                dma((block_steps,)), dma((dims,)),
                dma((block_steps,)), dma((block_steps,)),
                dma((chunks,)), dma((chunks,)), dma((chunks,)), dma((chunks,)),
                dma((chunks,)), dma((chunks,)), dma((chunks,)), dma((chunks,)),
                dma((3,)), dma((3,)),
                dma((3, 2)), dma((4, 2)), dma((dims - 1,)), dma((dims - 1,)),
            ],
            compiler_params=pltpu.CompilerParams(collective_id=0, has_side_effects=True, vmem_limit_bytes=60 * 2**20),
            name='ivf_search',
        )(queries, list_vecs.reshape(block_rows, depth), probes.T, list_ids.T)
        scores, ids = pl.pallas_call(
            place_kernel,
            out_shape=(jax.ShapeDtypeStruct((TOP_K, rows_q), jnp.float32),
                       jax.ShapeDtypeStruct((TOP_K, rows_q), jnp.int32)),
            in_specs=[vmem_spec],
            out_specs=(vmem_spec, vmem_spec),
            compiler_params=pltpu.CompilerParams(vmem_limit_bytes=4 * 2**20),
            name='place',
        )(found)
        return scores.T, ids.T

    return jax.shard_map(local_search, mesh=mesh,
                         in_specs=(P(('rep', 'shard'), 'dim'), P('shard', None, 'dim'), P('shard', None), row_spec),
                         out_specs=(row_spec, row_spec), check_vma=False)
```

```python
import functools

import jax
import jax.numpy as jnp
from jax import lax
from jax.experimental import pallas as pl
from jax.experimental.pallas import tpu as pltpu
from jax.sharding import PartitionSpec as P

TOP_K = 10
LIST_LEN = 8
GROUP_LISTS = 8
GROUP_ROWS = GROUP_LISTS * LIST_LEN
STEP_GROUPS = 4
STEP_ROWS = STEP_GROUPS * GROUP_ROWS
PIECE_ROWS = GROUP_ROWS // 2
LANES = 128
MESH = pl.DeviceIdType.MESH
BIG = 1e9


def flip(index, bit):
    return index + bit - 2 * bit * ((index // bit) % 2)


def search_kernel(dims, q_hbm, l_hbm, probes_hbm, ids_hbm, res,
                  raw, qv, vecs, perm, acc, parts, ids_all, cand_ids, probes_ref, ids_ref, load_p, load_i,
                  load_l, load_q, send_o, recv_o, send_y, recv_y, send_x, recv_x,
                  send_dy, recv_dy, send_dx, recv_dx, send_i, recv_i,
                  send_r, recv_r, send_g, recv_g):
    rows_q = qv.shape[0]
    lists_dev = ids_ref.shape[1]
    block_rows = lists_dev * LIST_LEN
    block_groups = lists_dev // GROUP_LISTS
    chunks = block_groups
    block_steps = block_groups // STEP_GROUPS
    width = rows_q // dims
    x, z, s = lax.axis_index('rep'), lax.axis_index('dim'), lax.axis_index('shard')
    twin, across, far = flip(s, 1), flip(s, 2), flip(flip(s, 1), 2)
    other_x = 1 - x

    def at(**place):
        return {'rep': x, 'dim': z, 'shard': s, **place}

    def step_rows(step):
        return pl.ds(pl.multiple_of(step * STEP_ROWS, STEP_ROWS), STEP_ROWS)

    def remote(src, dst, send, recv, device):
        return pltpu.make_async_remote_copy(src_ref=src, dst_ref=dst, send_sem=send, recv_sem=recv,
                                            device_id=device, device_id_type=MESH)

    def load_list(block):
        return pltpu.make_async_copy(l_hbm.at[step_rows(block)], raw.at[step_rows(block)], load_l.at[block])

    def load_query(part):
        rows = pl.ds(pl.multiple_of(part * width, width), width)
        return pltpu.make_async_copy(q_hbm.at[rows], qv.at[rows], load_q.at[part])

    def own_copy(block):
        return remote(vecs.at[step_rows(block)], vecs.at[step_rows(block_steps + block)],
                      send_o.at[block], recv_o.at[block], at(shard=twin))

    def piece(group, chunk):
        first = pl.multiple_of(group * GROUP_ROWS + chunk % 2 * PIECE_ROWS, PIECE_ROWS)
        return vecs.at[pl.ds(first, PIECE_ROWS)]

    def slot(chunk, which):
        return piece(2 * block_groups + STEP_GROUPS * (chunk // 2) + which, chunk)

    def y_copy(chunk):
        return remote(piece(chunks // 2 * x + chunk // 2, chunk), slot(chunk, 0), send_y.at[chunk], recv_y.at[chunk], at(shard=across))

    def x_copy(chunk):
        return remote(slot(chunk, 0), slot(chunk, 1), send_x.at[chunk], recv_x.at[chunk], at(rep=other_x))

    def dy_copy(chunk):
        return remote(slot(chunk, 0), slot(chunk, 2), send_dy.at[chunk], recv_dy.at[chunk], at(shard=twin))

    def dx_copy(chunk):
        return remote(slot(chunk, 1), slot(chunk, 3), send_dx.at[chunk], recv_dx.at[chunk], at(shard=twin))

    def id_copy(which, peer):
        return remote(ids_ref, ids_all.at[s], send_i.at[which], recv_i.at[which], at(shard=peer))

    outer = z % 3 == 0
    mate, far_outer = flip(z, 1), jnp.where(z < 2, dims - 1, 0)
    far_inner = flip(far_outer, 1)

    def part_copy(target, place, which, half):
        return remote(acc.at[target, half], parts.at[place, half], send_r.at[which, half], recv_r.at[place, half], at(dim=mate))

    def merged_copy(merge, half):
        return remote(parts.at[merge, half], parts.at[3, half], send_r.at[1 + merge, half], recv_r.at[3, half],
                      at(dim=(far_outer, far_inner)[merge]))

    def part_wait(place, half):
        remote(acc.at[z, half], parts.at[place, half], send_r.at[0, half], recv_r.at[place, half], at()).wait_recv()

    def peer_slot(source, target):
        return (source - target - 1 + dims) % dims

    def res_copy(target, which, half):
        return remote(res.at[z, half], res.at[z, half], send_g.at[which, half], recv_g.at[peer_slot(z, target), half], at(dim=target))

    def target_at(turn):
        first, second, third = (jnp.where(outer, one, two) for one, two in ((far_outer, mate), (far_inner, far_outer), (mate, far_inner)))
        return jnp.where(turn == 0, first, jnp.where(turn == 1, second, jnp.where(turn == 2, third, z)))

    def block_at(turn):
        return (block_steps // 2 * x + turn) % block_steps

    load_list(block_at(0)).start()
    probes_in = pltpu.make_async_copy(probes_hbm, probes_ref, load_p)
    ids_in = pltpu.make_async_copy(ids_hbm, ids_ref, load_i)
    ids_in.start()
    probes_in.start()
    for part in range(dims):
        load_query(part).start()
    for turn in range(1, block_steps):
        load_list(block_at(turn)).start()

    barrier = pltpu.get_barrier_semaphore()
    peers = [at(shard=twin), at(shard=across), at(shard=far), at(rep=other_x)]
    peers += [at(dim=(z + hop) % dims) for hop in range(1, dims)]
    for peer in peers:
        pl.semaphore_signal(barrier, inc=1, device_id=peer, device_id_type=MESH)

    row = lax.broadcasted_iota(jnp.int32, (STEP_ROWS, STEP_ROWS), 0)
    col = lax.broadcasted_iota(jnp.int32, (STEP_ROWS, STEP_ROWS), 1)
    source = (row // GROUP_ROWS) * GROUP_ROWS + (row % GROUP_LISTS) * LIST_LEN + (row // GROUP_LISTS) % LIST_LEN
    perm[...] = jnp.where(col == source, 1.0, 0.0).astype(jnp.bfloat16)

    def arrange(turn):
        block = block_at(turn)
        moved = jnp.dot(perm[...], raw[step_rows(block), :], preferred_element_type=jnp.float32)
        vecs[step_rows(block), :] = moved.astype(jnp.bfloat16)

    window = 2 * STEP_GROUPS
    load_list(block_at(0)).wait()
    arrange(0)
    pl.semaphore_wait(barrier, len(peers))
    for chunk in range(window):
        y_copy(chunk).start()
    acc[...] = jnp.zeros_like(acc)
    ids_in.wait()
    for which, peer in enumerate((twin, across, far)):
        id_copy(which, peer).start()
    ids_all[s] = ids_ref[...]
    probes_in.wait()
    for part in range(dims):
        load_query(part).wait()

    def name_candidates(tile, carry):
        cols = pl.ds(pl.multiple_of(z * width + tile * LANES, LANES), LANES)
        probe = probes_ref[:, cols]
        lane, page = probe % LANES, probe // LANES
        pages = lists_dev // LANES
        for member in range(LIST_LEN):
            got = jnp.zeros((probe.shape[0], LANES), jnp.int32)
            for number in range(4 * pages):
                table = ids_all[number // pages, member:member + 1, (number % pages) * LANES:(number % pages + 1) * LANES]
                table = jnp.broadcast_to(table, (probe.shape[0], LANES))
                picked = jnp.take_along_axis(table, lane, axis=1, mode='promise_in_bounds')
                got = jnp.where(page == number, picked, got)
            tiles_half = width // 2 // LANES
            place = pl.ds(pl.multiple_of(tile % tiles_half * LANES, LANES), LANES)
            cand_ids[tile // tiles_half, member, :, place] = got.astype(jnp.float32)
        return carry

    def list_block(step):
        return jnp.where(step < block_steps, block_at(step), step % block_steps)

    def score(step, heads, part):
        lists = vecs[step_rows(jnp.where(step < block_steps, block_at(step), step)), :]
        rows = pl.ds(pl.multiple_of(part * width, width), width)
        scores = lax.dot_general(lists, qv[rows, :], (((1,), (1,)), ((), ())), preferred_element_type=jnp.float32)
        for tile in range(width // LANES):
            probe = probes_ref[:, pl.ds(pl.multiple_of(part * width + tile * LANES, LANES), LANES)]
            low, head = probe % GROUP_LISTS, probe // GROUP_LISTS
            hits = [head == want for want in heads]
            lanes = slice(tile * LANES, (tile + 1) * LANES)
            half, place = divmod(tile * LANES, width // 2)
            kept_lanes = slice(place, place + LANES)
            for member in range(LIST_LEN):
                kept = acc[part, half, member, :, kept_lanes]
                for group, hit in enumerate(hits):
                    first = group * GROUP_ROWS + member * GROUP_LISTS
                    picked = jnp.take_along_axis(scores[first:first + GROUP_LISTS, lanes], low, axis=0, mode='promise_in_bounds')
                    kept = jnp.where(hit, picked, kept)
                acc[part, half, member, :, kept_lanes] = kept

    def heads_at(step):
        local = step < 2 * block_steps
        group = step - 2 * block_steps
        base = block_groups * jnp.where(step < block_steps, s, twin) + STEP_GROUPS * list_block(step)
        heads = []
        for which in range(STEP_GROUPS):
            home = across if which < 2 else far
            side = x if which % 2 == 0 else other_x
            heads.append(jnp.where(local, base + which, block_groups * home + chunks // 2 * side + group))
        return heads

    last = 2 * block_steps + chunks // 2 - 1

    spare_copy = remote(piece(chunks // 2 * other_x + (chunks - 1) // 2, chunks - 1), slot(chunks - 1, 1),
                        send_x.at[chunks - 1], recv_x.at[chunks - 1], at(shard=across))

    def pass_y(chunk):
        y_copy(chunk).wait_recv()
        if not (isinstance(chunk, int) and chunk == chunks - 1):
            x_copy(chunk).start()
        dy_copy(chunk).start()

        @pl.when(chunk + window < chunks)
        def _():
            y_copy(chunk + window).start()

        @pl.when(chunk + window == chunks)
        def _():
            spare_copy.start()

    def pass_x(chunk):
        x_copy(chunk).wait_recv()
        dx_copy(chunk).start()

    def await_step(step):
        first = 2 * (step - 2 * block_steps)
        for chunk in (first, first + 1):
            dy_copy(chunk).wait_recv()
            dx_copy(chunk).wait_recv()

    def score_all(step):
        heads = heads_at(step)
        for part in range(dims):
            score(step, heads, part)

    def early(step, carry):
        own_copy(block_at(step)).start()

        @pl.when(step >= 1)
        def _():
            pass_y(step - 1)

        @pl.when(step >= 5)
        def _():
            pass_x(step - 5)
        load_list(block_at(step + 1)).wait()
        score_all(step)
        arrange(step + 1)
        return carry

    def middle(step, carry):
        pass_y(step - 1)
        pass_x(step - 5)

        @pl.when(step == block_steps - 1)
        def _():
            own_copy(block_at(step)).start()

        @pl.when((step >= block_steps) & (step < 2 * block_steps))
        def _():
            own_copy(step - block_steps).wait_recv()

        @pl.when(step >= 2 * block_steps)
        def _():
            await_step(step)
        score_all(step)
        return carry

    late_plan = {
        last - 5: 'y25 x21 x22',
        last - 4: 'y26 x23 y27 x24',
        last - 3: 'y28 x25 y29 x26',
        last - 2: 'y30 x27 y31 x28',
        last - 1: 'x31 x29',
    }

    def late(step, carry):
        for when, plan in late_plan.items():
            @pl.when(step == when)
            def _(plan=plan):
                for word in plan.split():
                    (pass_y if word[0] == 'y' else pass_x)(int(word[1:]))

        @pl.when(step == last - 1)
        def _():
            for which, peer in enumerate((twin, across, far)):
                remote(ids_ref, ids_all.at[peer], send_i.at[which], recv_i.at[which], at(shard=peer)).wait_recv()
            lax.fori_loop(0, width // LANES, name_candidates, 0)
            pass_x(chunks - 2)
        await_step(step)
        score_all(step)
        return carry

    lax.fori_loop(0, block_steps - 1, early, 0)
    lax.fori_loop(block_steps - 1, last - 5, middle, 0)
    lax.fori_loop(last - 5, last, late, 0)
    await_step(jnp.int32(last))
    last_heads = heads_at(jnp.int32(last))

    def finish(turn, carry):
        @pl.when(outer & (turn == 1))
        def _():
            part_copy(far_outer, 0, 0, 0).start()

        @pl.when(outer & (turn == 2))
        def _():
            part_copy(far_inner, 1, 1, 0).start()
            part_copy(far_outer, 0, 0, 1).start()
            part_copy(far_inner, 1, 1, 1).start()

        @pl.when(jnp.where(outer, turn == 3, turn == 1))
        def _():
            for half in range(2):
                part_copy(mate, 2, jnp.where(outer, 2, 0), half).start()
        score(jnp.int32(last), last_heads, target_at(turn))
        return carry

    lax.fori_loop(0, dims, finish, 0)

    @pl.when(jnp.logical_not(outer))
    def _():
        for half in range(2):
            for merge, target in enumerate((far_outer, far_inner)):
                part_wait(merge, half)
                parts[merge, half] += acc[target, half]
                merged_copy(merge, half).start()

    def drain_local(block, carry):
        own_copy(block).wait_send()
        return carry

    def drain_chunks(chunk, carry):
        y_copy(chunk).wait_send()
        x_copy(chunk).wait_send()
        dy_copy(chunk).wait_send()
        dx_copy(chunk).wait_send()
        return carry

    tiles = width // 2 // LANES
    for half in range(2):
        for place in (2, 3):
            part_wait(place, half)
        scores, names = [], []
        for member in range(LIST_LEN):
            total = acc[z, half, member] + parts[2, half, member] + parts[3, half, member]
            name = cand_ids[half, member]
            real = name >= 0.0
            scores.append(jnp.where(real, total, -jnp.inf))
            names.append(jnp.where(real, name, BIG))
        for place in range(TOP_K):
            best = functools.reduce(jnp.maximum, scores)
            best = jnp.max(best, axis=0, keepdims=True)
            tied = [jnp.where(score_j == best, name_j, BIG) for score_j, name_j in zip(scores, names)]
            first = jnp.min(functools.reduce(jnp.minimum, tied), axis=0, keepdims=True)
            for tile in range(tiles):
                lanes = slice(tile * LANES, (tile + 1) * LANES)
                line = place * tiles + tile
                res[z, half, line:line + 1, :] = best[:, lanes]
                res[z, half, TOP_K * tiles + line:TOP_K * tiles + line + 1, :] = first[:, lanes]
            if place + 1 < TOP_K:
                scores = [jnp.where(name_j == first, -jnp.inf, score_j) for score_j, name_j in zip(scores, names)]
        if half == 0:
            lax.fori_loop(0, block_steps, drain_local, 0)
        else:
            for which, peer in enumerate((twin, across, far)):
                id_copy(which, peer).wait_send()
        for which in range(dims - 1):
            res_copy(target_at(which), which, half).start()

    lax.fori_loop(0, chunks, drain_chunks, 0)
    for which in range(3):
        for half in range(2):
            part_copy(z, 2, which, half).wait_send()
    for which in range(dims - 1):
        for half in range(2):
            remote(res.at[z, half], res.at[z, half], send_g.at[which, half], recv_g.at[which, half], at()).wait_recv()
    for which in range(dims - 1):
        for half in range(2):
            res_copy(target_at(which), which, half).wait_send()


def place_kernel(res, out_s, out_i):
    dims, halves, lines, _ = res.shape
    tiles = lines // (2 * TOP_K)
    for part in range(dims):
        for half in range(halves):
            for tile in range(tiles):
                first = ((part * halves + half) * tiles + tile) * LANES
                out_s[:, first:first + LANES] = res[part, half, pl.ds(tile, TOP_K, stride=tiles), :]
                out_i[:, first:first + LANES] = res[part, half, pl.ds(TOP_K * tiles + tile, TOP_K, stride=tiles), :].astype(jnp.int32)


def solution(mesh):
    dims = mesh.shape['dim']
    row_spec = P(('rep', 'shard'), None)

    def local_search(queries, list_vecs, list_ids, probes):
        rows_q, depth = queries.shape
        lists_dev, list_len, _ = list_vecs.shape
        probe_count = probes.shape[1]
        block_rows = lists_dev * list_len
        block_steps = block_rows // STEP_ROWS
        chunks = lists_dev // GROUP_LISTS
        width = rows_q // dims
        dma = pltpu.SemaphoreType.DMA
        any_spec = pl.BlockSpec(memory_space=pl.ANY)
        vmem_spec = pl.BlockSpec(memory_space=pltpu.VMEM)
        found = pl.pallas_call(
            functools.partial(search_kernel, dims),
            out_shape=pltpu.VMEM((dims, 2, TOP_K * width // LANES, LANES), jnp.float32),
            in_specs=[any_spec] * 4,
            out_specs=vmem_spec,
            scratch_shapes=[
                pltpu.VMEM((block_rows, depth), jnp.bfloat16),
                pltpu.VMEM((rows_q, depth), jnp.bfloat16),
                pltpu.VMEM((4 * block_rows, depth), jnp.bfloat16),
                pltpu.VMEM((STEP_ROWS, STEP_ROWS), jnp.bfloat16),
                pltpu.VMEM((dims, 2, LIST_LEN, probe_count, width // 2), jnp.float32),
                pltpu.VMEM((4, 2, LIST_LEN, probe_count, width // 2), jnp.float32),
                pltpu.VMEM((4, LIST_LEN, lists_dev), jnp.int32),
                pltpu.VMEM((2, LIST_LEN, probe_count, width // 2), jnp.float32),
                pltpu.VMEM((probe_count, rows_q), jnp.int32),
                pltpu.VMEM((LIST_LEN, lists_dev), jnp.int32),
                dma, dma,
                dma((block_steps,)), dma((dims,)),
                dma((block_steps,)), dma((block_steps,)),
                dma((chunks,)), dma((chunks,)), dma((chunks,)), dma((chunks,)),
                dma((chunks,)), dma((chunks,)), dma((chunks,)), dma((chunks,)),
                dma((3,)), dma((3,)),
                dma((3, 2)), dma((4, 2)), dma((dims - 1, 2)), dma((dims - 1, 2)),
            ],
            compiler_params=pltpu.CompilerParams(collective_id=0, has_side_effects=True, vmem_limit_bytes=60 * 2**20),
            name='ivf_search',
        )(queries, list_vecs.reshape(block_rows, depth), probes.T, list_ids.T)
        scores, ids = pl.pallas_call(
            place_kernel,
            out_shape=(jax.ShapeDtypeStruct((TOP_K, rows_q), jnp.float32),
                       jax.ShapeDtypeStruct((TOP_K, rows_q), jnp.int32)),
            in_specs=[vmem_spec],
            out_specs=(vmem_spec, vmem_spec),
            compiler_params=pltpu.CompilerParams(vmem_limit_bytes=4 * 2**20),
            name='place',
        )(found)
        return scores.T, ids.T

    return jax.shard_map(local_search, mesh=mesh,
                         in_specs=(P(('rep', 'shard'), 'dim'), P('shard', None, 'dim'), P('shard', None), row_spec),
                         out_specs=(row_spec, row_spec), check_vma=False)
```

```python
import functools

import jax
import jax.numpy as jnp
from jax import lax
from jax.experimental import pallas as pl
from jax.experimental.pallas import tpu as pltpu
from jax.sharding import PartitionSpec as P

TOP_K = 10
LIST_LEN = 8
GROUP_LISTS = 8
GROUP_ROWS = GROUP_LISTS * LIST_LEN
STEP_GROUPS = 4
STEP_ROWS = STEP_GROUPS * GROUP_ROWS
PIECE_ROWS = GROUP_ROWS // 2
LANES = 128
REUSE = 16
MESH = pl.DeviceIdType.MESH
BIG = 1e9


def flip(index, bit):
    return index + bit - 2 * bit * ((index // bit) % 2)


def search_kernel(dims, q_hbm, l_hbm, probes_hbm, ids_hbm, res,
                  raw, qv, vecs, perm, acc, parts, ids_all, cand_ids, probes_ref, ids_ref, load_p, load_i,
                  load_l, load_q, send_o, recv_o, send_y, recv_y, send_x, recv_x,
                  send_d, recv_d, send_i, recv_i, send_r, recv_r, send_g, recv_g):
    rows_q = qv.shape[0]
    lists_dev = ids_ref.shape[1]
    block_rows = lists_dev * LIST_LEN
    block_groups = lists_dev // GROUP_LISTS
    chunks = block_groups
    block_steps = block_groups // STEP_GROUPS
    width = rows_q // dims
    x, z, s = lax.axis_index('rep'), lax.axis_index('dim'), lax.axis_index('shard')
    twin, across, far = flip(s, 1), flip(s, 2), flip(flip(s, 1), 2)
    other_x = 1 - x

    def at(**place):
        return {'rep': x, 'dim': z, 'shard': s, **place}

    def step_rows(step):
        return pl.ds(pl.multiple_of(step * STEP_ROWS, STEP_ROWS), STEP_ROWS)

    def remote(src, dst, send, recv, device):
        return pltpu.make_async_remote_copy(src_ref=src, dst_ref=dst, send_sem=send, recv_sem=recv,
                                            device_id=device, device_id_type=MESH)

    def await_recv(buffer, semaphore):
        remote(buffer, buffer, send_i, semaphore, at()).wait_recv()

    def await_send(buffer, semaphore):
        remote(buffer, buffer, semaphore, recv_i, at()).wait_send()

    def load_list(block):
        return pltpu.make_async_copy(l_hbm.at[step_rows(block)], raw.at[step_rows(block)], load_l.at[block])

    queries_in = pltpu.make_async_copy(q_hbm, qv, load_q)

    def own_copy(block):
        return remote(vecs.at[step_rows(block)], vecs.at[step_rows(block_steps + block)],
                      send_o, recv_o.at[block], at(shard=twin))

    def piece(group, chunk):
        first = pl.multiple_of(group * GROUP_ROWS + chunk % 2 * PIECE_ROWS, PIECE_ROWS)
        return vecs.at[pl.ds(first, PIECE_ROWS)]

    def slot(chunk, which):
        return piece(2 * block_groups + STEP_GROUPS * (chunk // 2) + which, chunk)

    def y_copy(chunk):
        return remote(piece(chunks // 2 * x + chunk // 2, chunk), slot(chunk, 0), send_y, recv_y.at[chunk % REUSE], at(shard=across))

    def x_copy(chunk):
        return remote(slot(chunk, 0), slot(chunk, 1), send_x, recv_x.at[chunk % REUSE], at(rep=other_x))

    def dy_copy(chunk):
        return remote(slot(chunk, 0), slot(chunk, 2), send_d, recv_d.at[chunk // 2], at(shard=twin))

    def dx_copy(chunk):
        return remote(slot(chunk, 1), slot(chunk, 3), send_d, recv_d.at[chunk // 2], at(shard=twin))

    def id_copy(which, peer):
        return remote(ids_ref, ids_all.at[s], send_i, recv_i, at(shard=peer))

    outer = z % 3 == 0
    mate, far_outer = flip(z, 1), jnp.where(z < 2, dims - 1, 0)
    far_inner = flip(far_outer, 1)

    def part_copy(target, place, half):
        return remote(acc.at[target, half], parts.at[place, half], send_r, recv_r.at[place, half], at(dim=mate))

    def merged_copy(merge, half):
        return remote(parts.at[merge, half], parts.at[3, half], send_r, recv_r.at[3, half],
                      at(dim=(far_outer, far_inner)[merge]))

    def part_wait(place, half):
        await_recv(parts.at[place, half], recv_r.at[place, half])

    def res_copy(target, half):
        return remote(res.at[z, half], res.at[z, half], send_g, recv_g, at(dim=target))

    def target_at(turn):
        first, second, third = (jnp.where(outer, one, two) for one, two in ((far_outer, mate), (far_inner, far_outer), (mate, far_inner)))
        return jnp.where(turn == 0, first, jnp.where(turn == 1, second, jnp.where(turn == 2, third, z)))

    def block_at(turn):
        return (block_steps // 2 * x + turn) % block_steps

    load_list(block_at(0)).start()
    probes_in = pltpu.make_async_copy(probes_hbm, probes_ref, load_p)
    ids_in = pltpu.make_async_copy(ids_hbm, ids_ref, load_i)
    ids_in.start()
    probes_in.start()
    queries_in.start()
    for turn in range(1, block_steps):
        load_list(block_at(turn)).start()

    barrier = pltpu.get_barrier_semaphore()
    peers = [at(shard=twin), at(shard=across), at(shard=far), at(rep=other_x)]
    peers += [at(dim=(z + hop) % dims) for hop in range(1, dims)]
    for peer in peers:
        pl.semaphore_signal(barrier, inc=1, device_id=peer, device_id_type=MESH)

    row = lax.broadcasted_iota(jnp.int32, (STEP_ROWS, STEP_ROWS), 0)
    col = lax.broadcasted_iota(jnp.int32, (STEP_ROWS, STEP_ROWS), 1)
    source = (row // GROUP_ROWS) * GROUP_ROWS + (row % GROUP_LISTS) * LIST_LEN + (row // GROUP_LISTS) % LIST_LEN
    perm[...] = jnp.where(col == source, 1.0, 0.0).astype(jnp.bfloat16)

    def arrange(turn):
        block = block_at(turn)
        moved = jnp.dot(perm[...], raw[step_rows(block), :], preferred_element_type=jnp.float32)
        vecs[step_rows(block), :] = moved.astype(jnp.bfloat16)

    window = 2 * STEP_GROUPS
    load_list(block_at(0)).wait()
    arrange(0)
    pl.semaphore_wait(barrier, len(peers))
    for chunk in range(window):
        y_copy(chunk).start()
    acc[...] = jnp.zeros_like(acc)
    ids_in.wait()
    for which, peer in enumerate((twin, across, far)):
        id_copy(which, peer).start()
    ids_all[s] = ids_ref[...]
    probes_in.wait()
    queries_in.wait()

    def name_candidates(tile, carry):
        cols = pl.ds(pl.multiple_of(z * width + tile * LANES, LANES), LANES)
        probe = probes_ref[:, cols]
        lane, page = probe % LANES, probe // LANES
        pages = lists_dev // LANES
        for member in range(LIST_LEN):
            got = jnp.zeros((probe.shape[0], LANES), jnp.int32)
            for number in range(4 * pages):
                table = ids_all[number // pages, member:member + 1, (number % pages) * LANES:(number % pages + 1) * LANES]
                table = jnp.broadcast_to(table, (probe.shape[0], LANES))
                picked = jnp.take_along_axis(table, lane, axis=1, mode='promise_in_bounds')
                got = jnp.where(page == number, picked, got)
            tiles_half = width // 2 // LANES
            place = pl.ds(pl.multiple_of(tile % tiles_half * LANES, LANES), LANES)
            cand_ids[tile // tiles_half, member, :, place] = got.astype(jnp.float32)
        return carry

    def list_block(step):
        return jnp.where(step < block_steps, block_at(step), step % block_steps)

    def score(step, heads, part):
        lists = vecs[step_rows(jnp.where(step < block_steps, block_at(step), step)), :]
        rows = pl.ds(pl.multiple_of(part * width, width), width)
        scores = lax.dot_general(lists, qv[rows, :], (((1,), (1,)), ((), ())), preferred_element_type=jnp.float32)
        for tile in range(width // LANES):
            probe = probes_ref[:, pl.ds(pl.multiple_of(part * width + tile * LANES, LANES), LANES)]
            low, head = probe % GROUP_LISTS, probe // GROUP_LISTS
            hits = [head == want for want in heads]
            lanes = slice(tile * LANES, (tile + 1) * LANES)
            half, place = divmod(tile * LANES, width // 2)
            kept_lanes = slice(place, place + LANES)
            for member in range(LIST_LEN):
                kept = acc[part, half, member, :, kept_lanes]
                for group, hit in enumerate(hits):
                    first = group * GROUP_ROWS + member * GROUP_LISTS
                    picked = jnp.take_along_axis(scores[first:first + GROUP_LISTS, lanes], low, axis=0, mode='promise_in_bounds')
                    kept = jnp.where(hit, picked, kept)
                acc[part, half, member, :, kept_lanes] = kept

    def heads_at(step):
        local = step < 2 * block_steps
        group = step - 2 * block_steps
        base = block_groups * jnp.where(step < block_steps, s, twin) + STEP_GROUPS * list_block(step)
        heads = []
        for which in range(STEP_GROUPS):
            home = across if which < 2 else far
            side = x if which % 2 == 0 else other_x
            heads.append(jnp.where(local, base + which, block_groups * home + chunks // 2 * side + group))
        return heads

    last = 2 * block_steps + chunks // 2 - 1

    spare_copy = remote(piece(chunks // 2 * other_x + (chunks - 1) // 2, chunks - 1), slot(chunks - 1, 1),
                        send_x, recv_x.at[REUSE], at(shard=across))

    def pass_y(chunk):
        y_copy(chunk).wait_recv()
        if not (isinstance(chunk, int) and chunk == chunks - 1):
            x_copy(chunk).start()
        dy_copy(chunk).start()

        @pl.when(chunk + window < chunks)
        def _():
            y_copy(chunk + window).start()

        @pl.when(chunk + window == chunks)
        def _():
            spare_copy.start()

    def pass_x(chunk):
        if isinstance(chunk, int) and chunk == chunks - 1:
            spare_copy.wait_recv()
        else:
            x_copy(chunk).wait_recv()
        dx_copy(chunk).start()

    def await_step(step):
        await_recv(vecs.at[pl.ds(0, 4 * PIECE_ROWS)], recv_d.at[step - 2 * block_steps])

    def score_all(step):
        heads = heads_at(step)
        for part in range(dims):
            score(step, heads, part)

    def early(step, carry):
        own_copy(block_at(step)).start()

        @pl.when(step >= 1)
        def _():
            pass_y(step - 1)

        @pl.when(step >= 5)
        def _():
            pass_x(step - 5)
        load_list(block_at(step + 1)).wait()
        score_all(step)
        arrange(step + 1)
        return carry

    def middle(step, carry):
        pass_y(step - 1)
        pass_x(step - 5)

        @pl.when(step == block_steps - 1)
        def _():
            own_copy(block_at(step)).start()

        @pl.when((step >= block_steps) & (step < 2 * block_steps))
        def _():
            own_copy(step - block_steps).wait_recv()

        @pl.when(step >= 2 * block_steps)
        def _():
            await_step(step)
        score_all(step)
        return carry

    late_plan = {
        last - 5: 'y25 x21 x22',
        last - 4: 'y26 x23 y27 x24',
        last - 3: 'y28 x25 y29 x26',
        last - 2: 'y30 x27 y31 x28',
        last - 1: 'x31 x29',
    }

    def late(step, carry):
        for when, plan in late_plan.items():
            @pl.when(step == when)
            def _(plan=plan):
                for word in plan.split():
                    (pass_y if word[0] == 'y' else pass_x)(int(word[1:]))

        @pl.when(step == last - 1)
        def _():
            await_recv(ids_all.at[pl.ds(0, 3)], recv_i)
            lax.fori_loop(0, width // LANES, name_candidates, 0)
            pass_x(chunks - 2)
        await_step(step)
        score_all(step)
        return carry

    lax.fori_loop(0, block_steps - 1, early, 0)
    lax.fori_loop(block_steps - 1, last - 5, middle, 0)
    lax.fori_loop(last - 5, last, late, 0)
    await_step(jnp.int32(last))
    last_heads = heads_at(jnp.int32(last))

    def finish(turn, carry):
        @pl.when(outer & (turn == 1))
        def _():
            part_copy(far_outer, 0, 0).start()

        @pl.when(outer & (turn == 2))
        def _():
            part_copy(far_inner, 1, 0).start()
            part_copy(far_outer, 0, 1).start()
            part_copy(far_inner, 1, 1).start()

        @pl.when(jnp.where(outer, turn == 3, turn == 1))
        def _():
            for half in range(2):
                part_copy(mate, 2, half).start()
        score(jnp.int32(last), last_heads, target_at(turn))
        return carry

    lax.fori_loop(0, dims, finish, 0)

    @pl.when(jnp.logical_not(outer))
    def _():
        for half in range(2):
            for merge, target in enumerate((far_outer, far_inner)):
                part_wait(merge, half)
                parts[merge, half] += acc[target, half]
                merged_copy(merge, half).start()

    tiles = width // 2 // LANES
    for half in range(2):
        for place in (2, 3):
            part_wait(place, half)
        scores, names = [], []
        for member in range(LIST_LEN):
            total = acc[z, half, member] + parts[2, half, member] + parts[3, half, member]
            name = cand_ids[half, member]
            real = name >= 0.0
            scores.append(jnp.where(real, total, -jnp.inf))
            names.append(jnp.where(real, name, BIG))
        for place in range(TOP_K):
            best = functools.reduce(jnp.maximum, scores)
            best = jnp.max(best, axis=0, keepdims=True)
            tied = [jnp.where(score_j == best, name_j, BIG) for score_j, name_j in zip(scores, names)]
            first = jnp.min(functools.reduce(jnp.minimum, tied), axis=0, keepdims=True)
            for tile in range(tiles):
                lanes = slice(tile * LANES, (tile + 1) * LANES)
                line = place * tiles + tile
                res[z, half, line:line + 1, :] = best[:, lanes]
                res[z, half, TOP_K * tiles + line:TOP_K * tiles + line + 1, :] = first[:, lanes]
            if place + 1 < TOP_K:
                scores = [jnp.where(name_j == first, -jnp.inf, score_j) for score_j, name_j in zip(scores, names)]
        if half == 0:
            await_send(vecs.at[pl.ds(0, block_rows)], send_o)
            await_send(ids_all.at[pl.ds(0, 3)], send_i)
        else:
            await_send(vecs.at[pl.ds(0, chunks * PIECE_ROWS)], send_y)
            await_send(vecs.at[pl.ds(0, chunks * PIECE_ROWS)], send_x)
            await_send(vecs.at[pl.ds(0, 2 * chunks * PIECE_ROWS)], send_d)
        for which in range(dims - 1):
            res_copy(target_at(which), half).start()

    await_send(parts.at[pl.ds(0, 3)], send_r)
    await_send(res.at[pl.ds(0, dims - 1)], send_g)
    await_recv(res.at[pl.ds(0, dims - 1)], recv_g)


def place_kernel(res, out_s, out_i):
    dims, halves, lines, _ = res.shape
    tiles = lines // (2 * TOP_K)
    for part in range(dims):
        for half in range(halves):
            for tile in range(tiles):
                first = ((part * halves + half) * tiles + tile) * LANES
                out_s[:, first:first + LANES] = res[part, half, pl.ds(tile, TOP_K, stride=tiles), :]
                out_i[:, first:first + LANES] = res[part, half, pl.ds(TOP_K * tiles + tile, TOP_K, stride=tiles), :].astype(jnp.int32)


def solution(mesh):
    dims = mesh.shape['dim']
    row_spec = P(('rep', 'shard'), None)

    def local_search(queries, list_vecs, list_ids, probes):
        rows_q, depth = queries.shape
        lists_dev, list_len, _ = list_vecs.shape
        probe_count = probes.shape[1]
        block_rows = lists_dev * list_len
        block_steps = block_rows // STEP_ROWS
        chunks = lists_dev // GROUP_LISTS
        width = rows_q // dims
        dma = pltpu.SemaphoreType.DMA
        any_spec = pl.BlockSpec(memory_space=pl.ANY)
        vmem_spec = pl.BlockSpec(memory_space=pltpu.VMEM)
        found = pl.pallas_call(
            functools.partial(search_kernel, dims),
            out_shape=pltpu.VMEM((dims, 2, TOP_K * width // LANES, LANES), jnp.float32),
            in_specs=[any_spec] * 4,
            out_specs=vmem_spec,
            scratch_shapes=[
                pltpu.VMEM((block_rows, depth), jnp.bfloat16),
                pltpu.VMEM((rows_q, depth), jnp.bfloat16),
                pltpu.VMEM((4 * block_rows, depth), jnp.bfloat16),
                pltpu.VMEM((STEP_ROWS, STEP_ROWS), jnp.bfloat16),
                pltpu.VMEM((dims, 2, LIST_LEN, probe_count, width // 2), jnp.float32),
                pltpu.VMEM((4, 2, LIST_LEN, probe_count, width // 2), jnp.float32),
                pltpu.VMEM((4, LIST_LEN, lists_dev), jnp.int32),
                pltpu.VMEM((2, LIST_LEN, probe_count, width // 2), jnp.float32),
                pltpu.VMEM((probe_count, rows_q), jnp.int32),
                pltpu.VMEM((LIST_LEN, lists_dev), jnp.int32),
                dma, dma,
                dma((block_steps,)), dma,
                dma, dma((block_steps,)),
                dma, dma((REUSE,)), dma, dma((REUSE + 1,)),
                dma, dma((chunks // 2,)),
                dma, dma, dma, dma((4, 2)), dma, dma,
            ],
            compiler_params=pltpu.CompilerParams(collective_id=0, has_side_effects=True, vmem_limit_bytes=60 * 2**20),
            name='ivf_search',
        )(queries, list_vecs.reshape(block_rows, depth), probes.T, list_ids.T)
        scores, ids = pl.pallas_call(
            place_kernel,
            out_shape=(jax.ShapeDtypeStruct((TOP_K, rows_q), jnp.float32),
                       jax.ShapeDtypeStruct((TOP_K, rows_q), jnp.int32)),
            in_specs=[vmem_spec],
            out_specs=(vmem_spec, vmem_spec),
            compiler_params=pltpu.CompilerParams(vmem_limit_bytes=4 * 2**20),
            name='place',
        )(found)
        return scores.T, ids.T

    return jax.shard_map(local_search, mesh=mesh,
                         in_specs=(P(('rep', 'shard'), 'dim'), P('shard', None, 'dim'), P('shard', None), row_spec),
                         out_specs=(row_spec, row_spec), check_vma=False)
```

```python
import functools

import jax
import jax.numpy as jnp
from jax import lax
from jax.experimental import pallas as pl
from jax.experimental.pallas import tpu as pltpu
from jax.sharding import PartitionSpec as P

TOP_K = 10
LIST_LEN = 8
GROUP_LISTS = 8
GROUP_ROWS = GROUP_LISTS * LIST_LEN
STEP_GROUPS = 4
STEP_ROWS = STEP_GROUPS * GROUP_ROWS
PIECE_ROWS = GROUP_ROWS // 2
LANES = 128
REUSE = 16
MESH = pl.DeviceIdType.MESH
BIG = 1e9


def flip(index, bit):
    return index + bit - 2 * bit * ((index // bit) % 2)


def search_kernel(dims, q_hbm, l_hbm, probes_hbm, ids_hbm, res,
                  raw, qv, vecs, perm, acc, parts, ids_all, cand_ids, probes_ref, ids_ref, load_p, load_i,
                  load_l, load_q, send_o, recv_o, send_y, recv_y, send_x, recv_x,
                  send_d, recv_d, send_i, recv_i, send_r, recv_r, send_g, recv_g):
    rows_q = qv.shape[0]
    lists_dev = ids_ref.shape[1]
    block_rows = lists_dev * LIST_LEN
    block_groups = lists_dev // GROUP_LISTS
    chunks = block_groups
    block_steps = block_groups // STEP_GROUPS
    width = rows_q // dims
    x, z, s = lax.axis_index('rep'), lax.axis_index('dim'), lax.axis_index('shard')
    twin, across, far = flip(s, 1), flip(s, 2), flip(flip(s, 1), 2)
    other_x = 1 - x

    def at(**place):
        return {'rep': x, 'dim': z, 'shard': s, **place}

    def step_rows(step):
        return pl.ds(pl.multiple_of(step * STEP_ROWS, STEP_ROWS), STEP_ROWS)

    def remote(src, dst, send, recv, device):
        return pltpu.make_async_remote_copy(src_ref=src, dst_ref=dst, send_sem=send, recv_sem=recv,
                                            device_id=device, device_id_type=MESH)

    def await_recv(buffer, semaphore):
        remote(buffer, buffer, send_i, semaphore, at()).wait_recv()

    def await_send(buffer, semaphore):
        remote(buffer, buffer, semaphore, recv_i, at()).wait_send()

    def load_list(block):
        return pltpu.make_async_copy(l_hbm.at[step_rows(block)], raw.at[step_rows(block)], load_l.at[block])

    queries_in = pltpu.make_async_copy(q_hbm, qv, load_q)

    def own_copy(block):
        return remote(vecs.at[step_rows(block)], vecs.at[step_rows(block_steps + block)],
                      send_o, recv_o.at[block], at(shard=twin))

    def piece(group, chunk):
        first = pl.multiple_of(group * GROUP_ROWS + chunk % 2 * PIECE_ROWS, PIECE_ROWS)
        return vecs.at[pl.ds(first, PIECE_ROWS)]

    def slot(chunk, which):
        return piece(2 * block_groups + STEP_GROUPS * (chunk // 2) + which, chunk)

    def y_copy(chunk):
        return remote(piece(chunks // 2 * x + chunk // 2, chunk), slot(chunk, 0), send_y, recv_y.at[chunk % REUSE], at(shard=across))

    def x_copy(chunk):
        return remote(slot(chunk, 0), slot(chunk, 1), send_x, recv_x.at[chunk % REUSE], at(rep=other_x))

    def dy_copy(chunk):
        return remote(slot(chunk, 0), slot(chunk, 2), send_d, recv_d.at[chunk // 2], at(shard=twin))

    def dx_copy(chunk):
        return remote(slot(chunk, 1), slot(chunk, 3), send_d, recv_d.at[chunk // 2], at(shard=twin))

    def id_copy(which, peer):
        return remote(ids_ref, ids_all.at[s], send_i, recv_i, at(shard=peer))

    outer = z % 3 == 0
    mate, far_outer = flip(z, 1), jnp.where(z < 2, dims - 1, 0)
    far_inner = flip(far_outer, 1)

    def part_copy(target, place, half):
        return remote(acc.at[target, half], parts.at[place, half], send_r, recv_r.at[place, half], at(dim=mate))

    def merged_copy(merge, half):
        return remote(parts.at[merge, half], parts.at[3, half], send_r, recv_r.at[3, half],
                      at(dim=(far_outer, far_inner)[merge]))

    def part_wait(place, half):
        await_recv(parts.at[place, half], recv_r.at[place, half])

    def res_copy(target, half):
        return remote(res.at[z, half], res.at[z, half], send_g, recv_g, at(dim=target))

    def target_at(turn):
        first, second, third = (jnp.where(outer, one, two) for one, two in ((far_outer, mate), (far_inner, far_outer), (mate, far_inner)))
        return jnp.where(turn == 0, first, jnp.where(turn == 1, second, jnp.where(turn == 2, third, z)))

    def block_at(turn):
        return (block_steps // 2 * x + turn) % block_steps

    barrier = pltpu.get_barrier_semaphore()
    peers = [at(dim=(z + hop) % dims) for hop in (2, 1, 3)]
    peers += [at(shard=twin), at(shard=across), at(shard=far), at(rep=other_x)]

    def greet(some):
        for peer in some:
            pl.semaphore_signal(barrier, inc=1, device_id=peer, device_id_type=MESH)

    load_list(block_at(0)).start()
    greet(peers[:3])
    probes_in = pltpu.make_async_copy(probes_hbm, probes_ref, load_p)
    ids_in = pltpu.make_async_copy(ids_hbm, ids_ref, load_i)
    ids_in.start()
    probes_in.start()
    queries_in.start()
    greet(peers[3:])
    for turn in range(1, block_steps):
        load_list(block_at(turn)).start()

    row = lax.broadcasted_iota(jnp.int32, (STEP_ROWS, STEP_ROWS), 0)
    col = lax.broadcasted_iota(jnp.int32, (STEP_ROWS, STEP_ROWS), 1)
    source = (row // GROUP_ROWS) * GROUP_ROWS + (row % GROUP_LISTS) * LIST_LEN + (row // GROUP_LISTS) % LIST_LEN
    perm[...] = jnp.where(col == source, 1.0, 0.0).astype(jnp.bfloat16)

    def arrange(turn):
        block = block_at(turn)
        moved = jnp.dot(perm[...], raw[step_rows(block), :], preferred_element_type=jnp.float32)
        vecs[step_rows(block), :] = moved.astype(jnp.bfloat16)

    window = 2 * STEP_GROUPS
    load_list(block_at(0)).wait()
    arrange(0)
    pl.semaphore_wait(barrier, len(peers))
    for chunk in range(window):
        y_copy(chunk).start()
    acc[...] = jnp.zeros_like(acc)
    ids_in.wait()
    for which, peer in enumerate((twin, across, far)):
        id_copy(which, peer).start()
    ids_all[s] = ids_ref[...]
    probes_in.wait()
    queries_in.wait()

    def name_candidates(tile, carry):
        cols = pl.ds(pl.multiple_of(z * width + tile * LANES, LANES), LANES)
        probe = probes_ref[:, cols]
        lane, page = probe % LANES, probe // LANES
        pages = lists_dev // LANES
        for member in range(LIST_LEN):
            got = jnp.zeros((probe.shape[0], LANES), jnp.int32)
            for number in range(4 * pages):
                table = ids_all[number // pages, member:member + 1, (number % pages) * LANES:(number % pages + 1) * LANES]
                table = jnp.broadcast_to(table, (probe.shape[0], LANES))
                picked = jnp.take_along_axis(table, lane, axis=1, mode='promise_in_bounds')
                got = jnp.where(page == number, picked, got)
            tiles_half = width // 2 // LANES
            place = pl.ds(pl.multiple_of(tile % tiles_half * LANES, LANES), LANES)
            cand_ids[tile // tiles_half, member, :, place] = got.astype(jnp.float32)
        return carry

    def list_block(step):
        return jnp.where(step < block_steps, block_at(step), step % block_steps)

    def score(step, heads, part):
        lists = vecs[step_rows(jnp.where(step < block_steps, block_at(step), step)), :]
        rows = pl.ds(pl.multiple_of(part * width, width), width)
        scores = lax.dot_general(lists, qv[rows, :], (((1,), (1,)), ((), ())), preferred_element_type=jnp.float32)
        for tile in range(width // LANES):
            probe = probes_ref[:, pl.ds(pl.multiple_of(part * width + tile * LANES, LANES), LANES)]
            low, head = probe % GROUP_LISTS, probe // GROUP_LISTS
            hits = [head == want for want in heads]
            lanes = slice(tile * LANES, (tile + 1) * LANES)
            half, place = divmod(tile * LANES, width // 2)
            kept_lanes = slice(place, place + LANES)
            for member in range(LIST_LEN):
                kept = acc[part, half, member, :, kept_lanes]
                for group, hit in enumerate(hits):
                    first = group * GROUP_ROWS + member * GROUP_LISTS
                    picked = jnp.take_along_axis(scores[first:first + GROUP_LISTS, lanes], low, axis=0, mode='promise_in_bounds')
                    kept = jnp.where(hit, picked, kept)
                acc[part, half, member, :, kept_lanes] = kept

    def heads_at(step):
        local = step < 2 * block_steps
        group = step - 2 * block_steps
        base = block_groups * jnp.where(step < block_steps, s, twin) + STEP_GROUPS * list_block(step)
        heads = []
        for which in range(STEP_GROUPS):
            home = across if which < 2 else far
            side = x if which % 2 == 0 else other_x
            heads.append(jnp.where(local, base + which, block_groups * home + chunks // 2 * side + group))
        return heads

    last = 2 * block_steps + chunks // 2 - 1

    spare_copy = remote(piece(chunks // 2 * other_x + (chunks - 1) // 2, chunks - 1), slot(chunks - 1, 1),
                        send_x, recv_x.at[REUSE], at(shard=across))

    def pass_y(chunk):
        y_copy(chunk).wait_recv()
        if not (isinstance(chunk, int) and chunk == chunks - 1):
            x_copy(chunk).start()
        dy_copy(chunk).start()

        @pl.when(chunk + window < chunks)
        def _():
            y_copy(chunk + window).start()

        @pl.when(chunk + window == chunks)
        def _():
            spare_copy.start()

    def pass_x(chunk):
        if isinstance(chunk, int) and chunk == chunks - 1:
            spare_copy.wait_recv()
        else:
            x_copy(chunk).wait_recv()
        dx_copy(chunk).start()

    def await_step(step):
        await_recv(vecs.at[pl.ds(0, 4 * PIECE_ROWS)], recv_d.at[step - 2 * block_steps])

    def score_all(step):
        heads = heads_at(step)
        for part in range(dims):
            score(step, heads, part)

    def early(step, carry):
        own_copy(block_at(step)).start()

        @pl.when(step >= 1)
        def _():
            pass_y(step - 1)

        @pl.when(step >= 5)
        def _():
            pass_x(step - 5)
        load_list(block_at(step + 1)).wait()
        score_all(step)
        arrange(step + 1)
        return carry

    def middle(step, carry):
        pass_y(step - 1)
        pass_x(step - 5)

        @pl.when(step == block_steps - 1)
        def _():
            own_copy(block_at(step)).start()

        @pl.when((step >= block_steps) & (step < 2 * block_steps))
        def _():
            own_copy(step - block_steps).wait_recv()

        @pl.when(step >= 2 * block_steps)
        def _():
            await_step(step)
        score_all(step)
        return carry

    late_plan = {
        last - 5: 'y25 x21 x22',
        last - 4: 'y26 x23 y27 x24',
        last - 3: 'y28 x25 y29 x26',
        last - 2: 'y30 x27 y31 x28',
        last - 1: 'x31 x29',
    }

    def late(step, carry):
        for when, plan in late_plan.items():
            @pl.when(step == when)
            def _(plan=plan):
                for word in plan.split():
                    (pass_y if word[0] == 'y' else pass_x)(int(word[1:]))

        @pl.when(step == last - 1)
        def _():
            await_recv(ids_all.at[pl.ds(0, 3)], recv_i)
            lax.fori_loop(0, width // LANES, name_candidates, 0)
            pass_x(chunks - 2)
        await_step(step)
        score_all(step)
        return carry

    lax.fori_loop(0, block_steps - 1, early, 0)
    lax.fori_loop(block_steps - 1, last - 5, middle, 0)
    lax.fori_loop(last - 5, last, late, 0)
    await_step(jnp.int32(last))
    last_heads = heads_at(jnp.int32(last))

    leads, follows = outer & (s % 2 == 0), outer & (s % 2 == 1)

    def finish(turn, carry):
        @pl.when(leads & (turn == 1))
        def _():
            part_copy(far_outer, 0, 0).start()

        @pl.when(leads & (turn == 2))
        def _():
            part_copy(far_inner, 1, 0).start()
            part_copy(far_outer, 0, 1).start()
            part_copy(far_inner, 1, 1).start()

        @pl.when((leads & (turn == 3)) | (jnp.logical_not(outer) & (turn == 1)))
        def _():
            for half in range(2):
                part_copy(mate, 2, half).start()
        score(jnp.int32(last), last_heads, target_at(turn))
        return carry

    lax.fori_loop(0, dims, finish, 0)

    @pl.when(follows)
    def _():
        part_wait(2, 0)
        for half in range(2):
            part_copy(far_outer, 0, half).start()
            part_copy(far_inner, 1, half).start()
        for half in range(2):
            part_copy(mate, 2, half).start()

    @pl.when(jnp.logical_not(outer))
    def _():
        for half in range(2):
            for merge, target in enumerate((far_outer, far_inner)):
                part_wait(merge, half)
                parts[merge, half] += acc[target, half]
                merged_copy(merge, half).start()

    tiles = width // 2 // LANES
    for half in range(2):
        if half == 0:
            @pl.when(jnp.logical_not(follows))
            def _():
                part_wait(2, 0)
        else:
            part_wait(2, 1)
        part_wait(3, half)
        scores, names = [], []
        for member in range(LIST_LEN):
            total = acc[z, half, member] + parts[2, half, member] + parts[3, half, member]
            name = cand_ids[half, member]
            real = name >= 0.0
            scores.append(jnp.where(real, total, -jnp.inf))
            names.append(jnp.where(real, name, BIG))
        for place in range(TOP_K):
            best = functools.reduce(jnp.maximum, scores)
            best = jnp.max(best, axis=0, keepdims=True)
            tied = [jnp.where(score_j == best, name_j, BIG) for score_j, name_j in zip(scores, names)]
            first = jnp.min(functools.reduce(jnp.minimum, tied), axis=0, keepdims=True)
            for tile in range(tiles):
                lanes = slice(tile * LANES, (tile + 1) * LANES)
                line = place * tiles + tile
                res[z, half, line:line + 1, :] = best[:, lanes]
                res[z, half, TOP_K * tiles + line:TOP_K * tiles + line + 1, :] = first[:, lanes]
            if place + 1 < TOP_K:
                scores = [jnp.where(name_j == first, -jnp.inf, score_j) for score_j, name_j in zip(scores, names)]
        if half == 0:
            await_send(vecs.at[pl.ds(0, block_rows)], send_o)
            await_send(ids_all.at[pl.ds(0, 3)], send_i)
        else:
            await_send(vecs.at[pl.ds(0, chunks * PIECE_ROWS)], send_y)
            await_send(vecs.at[pl.ds(0, chunks * PIECE_ROWS)], send_x)
            await_send(vecs.at[pl.ds(0, 2 * chunks * PIECE_ROWS)], send_d)
        for which in range(dims - 1):
            res_copy(target_at(which), half).start()

    await_send(parts.at[pl.ds(0, 3)], send_r)
    await_send(res.at[pl.ds(0, dims - 1)], send_g)
    await_recv(res.at[pl.ds(0, dims - 1)], recv_g)


def place_kernel(res, out_s, out_i):
    dims, halves, lines, _ = res.shape
    tiles = lines // (2 * TOP_K)
    for part in range(dims):
        for half in range(halves):
            for tile in range(tiles):
                first = ((part * halves + half) * tiles + tile) * LANES
                out_s[:, first:first + LANES] = res[part, half, pl.ds(tile, TOP_K, stride=tiles), :]
                out_i[:, first:first + LANES] = res[part, half, pl.ds(TOP_K * tiles + tile, TOP_K, stride=tiles), :].astype(jnp.int32)


def solution(mesh):
    dims = mesh.shape['dim']
    row_spec = P(('rep', 'shard'), None)

    def local_search(queries, list_vecs, list_ids, probes):
        rows_q, depth = queries.shape
        lists_dev, list_len, _ = list_vecs.shape
        probe_count = probes.shape[1]
        block_rows = lists_dev * list_len
        block_steps = block_rows // STEP_ROWS
        chunks = lists_dev // GROUP_LISTS
        width = rows_q // dims
        dma = pltpu.SemaphoreType.DMA
        any_spec = pl.BlockSpec(memory_space=pl.ANY)
        vmem_spec = pl.BlockSpec(memory_space=pltpu.VMEM)
        found = pl.pallas_call(
            functools.partial(search_kernel, dims),
            out_shape=pltpu.VMEM((dims, 2, TOP_K * width // LANES, LANES), jnp.float32),
            in_specs=[any_spec] * 4,
            out_specs=vmem_spec,
            scratch_shapes=[
                pltpu.VMEM((block_rows, depth), jnp.bfloat16),
                pltpu.VMEM((rows_q, depth), jnp.bfloat16),
                pltpu.VMEM((4 * block_rows, depth), jnp.bfloat16),
                pltpu.VMEM((STEP_ROWS, STEP_ROWS), jnp.bfloat16),
                pltpu.VMEM((dims, 2, LIST_LEN, probe_count, width // 2), jnp.float32),
                pltpu.VMEM((4, 2, LIST_LEN, probe_count, width // 2), jnp.float32),
                pltpu.VMEM((4, LIST_LEN, lists_dev), jnp.int32),
                pltpu.VMEM((2, LIST_LEN, probe_count, width // 2), jnp.float32),
                pltpu.VMEM((probe_count, rows_q), jnp.int32),
                pltpu.VMEM((LIST_LEN, lists_dev), jnp.int32),
                dma, dma,
                dma((block_steps,)), dma,
                dma, dma((block_steps,)),
                dma, dma((REUSE,)), dma, dma((REUSE + 1,)),
                dma, dma((chunks // 2,)),
                dma, dma, dma, dma((4, 2)), dma, dma,
            ],
            compiler_params=pltpu.CompilerParams(collective_id=0, has_side_effects=True, vmem_limit_bytes=60 * 2**20),
            name='ivf_search',
        )(queries, list_vecs.reshape(block_rows, depth), probes.T, list_ids.T)
        scores, ids = pl.pallas_call(
            place_kernel,
            out_shape=(jax.ShapeDtypeStruct((TOP_K, rows_q), jnp.float32),
                       jax.ShapeDtypeStruct((TOP_K, rows_q), jnp.int32)),
            in_specs=[vmem_spec],
            out_specs=(vmem_spec, vmem_spec),
            compiler_params=pltpu.CompilerParams(vmem_limit_bytes=4 * 2**20),
            name='place',
        )(found)
        return scores.T, ids.T

    return jax.shard_map(local_search, mesh=mesh,
                         in_specs=(P(('rep', 'shard'), 'dim'), P('shard', None, 'dim'), P('shard', None), row_spec),
                         out_specs=(row_spec, row_spec), check_vma=False)
```

```python
import functools

import jax
import jax.numpy as jnp
from jax import lax
from jax.experimental import pallas as pl
from jax.experimental.pallas import tpu as pltpu
from jax.sharding import PartitionSpec as P

TOP_K = 10
LIST_LEN = 8
GROUP_LISTS = 8
GROUP_ROWS = GROUP_LISTS * LIST_LEN
STEP_GROUPS = 4
STEP_ROWS = STEP_GROUPS * GROUP_ROWS
PIECE_ROWS = GROUP_ROWS // 2
LANES = 128
REUSE = 16
MESH = pl.DeviceIdType.MESH
BIG = 1e9


def flip(index, bit):
    return index + bit - 2 * bit * ((index // bit) % 2)


def search_kernel(dims, q_hbm, l_hbm, probes_hbm, ids_hbm, res,
                  raw, qv, vecs, perm, acc, parts, ids_all, cand_ids, probes_ref, ids_ref, load_p, load_i,
                  load_l, load_q, send_o, recv_o, send_y, recv_y, send_x, recv_x,
                  send_d, recv_d, send_i, recv_i, send_r, recv_r, send_g, recv_g):
    rows_q = qv.shape[0]
    lists_dev = ids_ref.shape[1]
    block_rows = lists_dev * LIST_LEN
    block_groups = lists_dev // GROUP_LISTS
    chunks = block_groups
    block_steps = block_groups // STEP_GROUPS
    width = rows_q // dims
    x, z, s = lax.axis_index('rep'), lax.axis_index('dim'), lax.axis_index('shard')
    twin, across, far = flip(s, 1), flip(s, 2), flip(flip(s, 1), 2)
    other_x = 1 - x

    def at(**place):
        return {'rep': x, 'dim': z, 'shard': s, **place}

    def step_rows(step):
        return pl.ds(pl.multiple_of(step * STEP_ROWS, STEP_ROWS), STEP_ROWS)

    def remote(src, dst, send, recv, device):
        return pltpu.make_async_remote_copy(src_ref=src, dst_ref=dst, send_sem=send, recv_sem=recv,
                                            device_id=device, device_id_type=MESH)

    def await_recv(buffer, semaphore):
        remote(buffer, buffer, send_i, semaphore, at()).wait_recv()

    def await_send(buffer, semaphore):
        remote(buffer, buffer, semaphore, recv_i, at()).wait_send()

    def load_list(block):
        return pltpu.make_async_copy(l_hbm.at[step_rows(block)], raw.at[step_rows(block)], load_l.at[block])

    queries_in = pltpu.make_async_copy(q_hbm, qv, load_q)

    def own_copy(block):
        return remote(vecs.at[step_rows(block)], vecs.at[step_rows(block_steps + block)],
                      send_o, recv_o.at[block], at(shard=twin))

    def piece(group, chunk):
        first = pl.multiple_of(group * GROUP_ROWS + chunk % 2 * PIECE_ROWS, PIECE_ROWS)
        return vecs.at[pl.ds(first, PIECE_ROWS)]

    def slot(chunk, which):
        return piece(2 * block_groups + STEP_GROUPS * (chunk // 2) + which, chunk)

    def y_copy(chunk):
        return remote(piece(chunks // 2 * x + chunk // 2, chunk), slot(chunk, 0), send_y, recv_y.at[chunk % REUSE], at(shard=across))

    def x_copy(chunk):
        return remote(slot(chunk, 0), slot(chunk, 1), send_x, recv_x.at[chunk % REUSE], at(rep=other_x))

    def dy_copy(chunk):
        return remote(slot(chunk, 0), slot(chunk, 2), send_d, recv_d.at[chunk // 2], at(shard=twin))

    def dx_copy(chunk):
        return remote(slot(chunk, 1), slot(chunk, 3), send_d, recv_d.at[chunk // 2], at(shard=twin))

    def id_copy(which, peer):
        return remote(ids_ref, ids_all.at[s], send_i, recv_i, at(shard=peer))

    outer = z % 3 == 0
    mate, far_outer = flip(z, 1), jnp.where(z < 2, dims - 1, 0)
    far_inner = flip(far_outer, 1)

    def part_copy(target, place, half):
        return remote(acc.at[target, half], parts.at[place, half], send_r, recv_r.at[place, half], at(dim=mate))

    def merged_copy(merge, half):
        return remote(parts.at[merge, half], parts.at[3, half], send_r, recv_r.at[3, half],
                      at(dim=(far_outer, far_inner)[merge]))

    def part_wait(place, half):
        await_recv(parts.at[place, half], recv_r.at[place, half])

    def res_copy(target, half):
        return remote(res.at[z, half], res.at[z, half], send_g, recv_g, at(dim=target))

    def target_at(turn):
        first, second, third = (jnp.where(outer, one, two) for one, two in ((far_outer, mate), (far_inner, far_outer), (mate, far_inner)))
        return jnp.where(turn == 0, first, jnp.where(turn == 1, second, jnp.where(turn == 2, third, z)))

    def block_at(turn):
        return (block_steps // 2 * x + turn) % block_steps

    barrier = pltpu.get_barrier_semaphore()
    peers = [at(dim=(z + hop) % dims) for hop in (2, 1, 3)]
    peers += [at(shard=twin), at(shard=across), at(shard=far), at(rep=other_x)]

    def greet(some):
        for peer in some:
            pl.semaphore_signal(barrier, inc=1, device_id=peer, device_id_type=MESH)

    load_list(block_at(0)).start()
    greet(peers[:3])
    probes_in = pltpu.make_async_copy(probes_hbm, probes_ref, load_p)
    ids_in = pltpu.make_async_copy(ids_hbm, ids_ref, load_i)
    ids_in.start()
    probes_in.start()
    queries_in.start()
    greet(peers[3:])
    for turn in range(1, block_steps):
        load_list(block_at(turn)).start()

    row = lax.broadcasted_iota(jnp.int32, (STEP_ROWS, STEP_ROWS), 0)
    col = lax.broadcasted_iota(jnp.int32, (STEP_ROWS, STEP_ROWS), 1)
    source = (row // GROUP_ROWS) * GROUP_ROWS + (row % GROUP_LISTS) * LIST_LEN + (row // GROUP_LISTS) % LIST_LEN
    perm[...] = jnp.where(col == source, 1.0, 0.0).astype(jnp.bfloat16)

    def arrange(turn):
        block = block_at(turn)
        moved = jnp.dot(perm[...], raw[step_rows(block), :], preferred_element_type=jnp.float32)
        vecs[step_rows(block), :] = moved.astype(jnp.bfloat16)

    window = 2 * STEP_GROUPS
    load_list(block_at(0)).wait()
    arrange(0)
    pl.semaphore_wait(barrier, len(peers))
    for chunk in range(window):
        y_copy(chunk).start()
    acc[...] = jnp.zeros_like(acc)
    ids_in.wait()
    for which, peer in enumerate((twin, across, far)):
        id_copy(which, peer).start()
    ids_all[s] = ids_ref[...]
    probes_in.wait()
    queries_in.wait()

    def name_candidates(tile, carry):
        cols = pl.ds(pl.multiple_of(z * width + tile * LANES, LANES), LANES)
        probe = probes_ref[:, cols]
        lane, page = probe % LANES, probe // LANES
        pages = lists_dev // LANES
        for member in range(LIST_LEN):
            got = jnp.zeros((probe.shape[0], LANES), jnp.int32)
            for number in range(4 * pages):
                table = ids_all[number // pages, member:member + 1, (number % pages) * LANES:(number % pages + 1) * LANES]
                table = jnp.broadcast_to(table, (probe.shape[0], LANES))
                picked = jnp.take_along_axis(table, lane, axis=1, mode='promise_in_bounds')
                got = jnp.where(page == number, picked, got)
            tiles_half = width // 2 // LANES
            place = pl.ds(pl.multiple_of(tile % tiles_half * LANES, LANES), LANES)
            cand_ids[tile // tiles_half, member, :, place] = got.astype(jnp.float32)
        return carry

    def list_block(step):
        return jnp.where(step < block_steps, block_at(step), step % block_steps)

    def score(step, heads, part):
        lists = vecs[step_rows(jnp.where(step < block_steps, block_at(step), step)), :]
        rows = pl.ds(pl.multiple_of(part * width, width), width)
        scores = lax.dot_general(lists, qv[rows, :], (((1,), (1,)), ((), ())), preferred_element_type=jnp.float32)
        for tile in range(width // LANES):
            probe = probes_ref[:, pl.ds(pl.multiple_of(part * width + tile * LANES, LANES), LANES)]
            low, head = probe % GROUP_LISTS, probe // GROUP_LISTS
            hits = [head == want for want in heads]
            lanes = slice(tile * LANES, (tile + 1) * LANES)
            half, place = divmod(tile * LANES, width // 2)
            kept_lanes = slice(place, place + LANES)
            for member in range(LIST_LEN):
                kept = acc[part, half, member, :, kept_lanes]
                for group, hit in enumerate(hits):
                    first = group * GROUP_ROWS + member * GROUP_LISTS
                    picked = jnp.take_along_axis(scores[first:first + GROUP_LISTS, lanes], low, axis=0, mode='promise_in_bounds')
                    kept = jnp.where(hit, picked, kept)
                acc[part, half, member, :, kept_lanes] = kept

    def heads_at(step):
        local = step < 2 * block_steps
        group = step - 2 * block_steps
        base = block_groups * jnp.where(step < block_steps, s, twin) + STEP_GROUPS * list_block(step)
        heads = []
        for which in range(STEP_GROUPS):
            home = across if which < 2 else far
            side = x if which % 2 == 0 else other_x
            heads.append(jnp.where(local, base + which, block_groups * home + chunks // 2 * side + group))
        return heads

    last = 2 * block_steps + chunks // 2 - 1

    spare_copy = remote(piece(chunks // 2 * other_x + (chunks - 1) // 2, chunks - 1), slot(chunks - 1, 1),
                        send_x, recv_x.at[REUSE], at(shard=across))

    def pass_y(chunk):
        y_copy(chunk).wait_recv()
        if not (isinstance(chunk, int) and chunk == chunks - 1):
            x_copy(chunk).start()
        dy_copy(chunk).start()

        @pl.when(chunk + window < chunks)
        def _():
            y_copy(chunk + window).start()

        @pl.when(chunk + window == chunks)
        def _():
            spare_copy.start()

    def pass_x(chunk):
        if isinstance(chunk, int) and chunk == chunks - 1:
            spare_copy.wait_recv()
        else:
            x_copy(chunk).wait_recv()
        dx_copy(chunk).start()

    def await_step(step):
        await_recv(vecs.at[pl.ds(0, 4 * PIECE_ROWS)], recv_d.at[step - 2 * block_steps])

    def score_all(step):
        heads = heads_at(step)
        for part in range(dims):
            score(step, heads, part)

    def early(step, carry):
        own_copy(block_at(step)).start()

        @pl.when(step >= 1)
        def _():
            pass_y(step - 1)

        @pl.when(step >= 5)
        def _():
            pass_x(step - 5)
        load_list(block_at(step + 1)).wait()
        score_all(step)
        arrange(step + 1)
        return carry

    def middle(step, carry):
        pass_y(step - 1)
        pass_x(step - 5)

        @pl.when(step == block_steps - 1)
        def _():
            own_copy(block_at(step)).start()

        @pl.when((step >= block_steps) & (step < 2 * block_steps))
        def _():
            own_copy(step - block_steps).wait_recv()

        @pl.when(step >= 2 * block_steps)
        def _():
            await_step(step)
        score_all(step)
        return carry

    late_plan = {
        last - 5: 'y25 x21 x22',
        last - 4: 'y26 x23 y27 x24',
        last - 3: 'y28 x25 y29 x26',
        last - 2: 'y30 x27 y31 x28',
        last - 1: 'x31 x29',
    }

    def late(step, carry):
        for when, plan in late_plan.items():
            @pl.when(step == when)
            def _(plan=plan):
                for word in plan.split():
                    (pass_y if word[0] == 'y' else pass_x)(int(word[1:]))

        @pl.when(step == last - 1)
        def _():
            await_recv(ids_all.at[pl.ds(0, 3)], recv_i)
            lax.fori_loop(0, width // LANES, name_candidates, 0)
            pass_x(chunks - 2)
        await_step(step)
        score_all(step)
        return carry

    lax.fori_loop(0, block_steps - 1, early, 0)
    lax.fori_loop(block_steps - 1, last - 5, middle, 0)
    lax.fori_loop(last - 5, last, late, 0)
    await_step(jnp.int32(last))
    last_heads = heads_at(jnp.int32(last))

    leads, follows = outer & (s % 2 == 0), outer & (s % 2 == 1)

    def finish(turn, carry):
        @pl.when(leads & (turn == 1))
        def _():
            part_copy(far_outer, 0, 0).start()

        @pl.when(leads & (turn == 2))
        def _():
            part_copy(far_inner, 1, 0).start()
            part_copy(far_outer, 0, 1).start()
            part_copy(far_inner, 1, 1).start()

        @pl.when((leads & (turn == 3)) | (jnp.logical_not(outer) & (turn == 1)))
        def _():
            for half in range(2):
                part_copy(mate, 2, half).start()
        score(jnp.int32(last), last_heads, target_at(turn))
        return carry

    lax.fori_loop(0, dims, finish, 0)

    @pl.when(follows)
    def _():
        for half in range(2):
            part_copy(far_outer, 0, half).start()
            part_copy(far_inner, 1, half).start()
        for half in range(2):
            part_copy(mate, 2, half).start()

    @pl.when(jnp.logical_not(outer))
    def _():
        for half in range(2):
            for merge, target in enumerate((far_outer, far_inner)):
                part_wait(merge, half)
                parts[merge, half] += acc[target, half]
                merged_copy(merge, half).start()

    tiles = width // 2 // LANES
    for half in range(2):
        part_wait(2, half)
        part_wait(3, half)
        scores, names = [], []
        for member in range(LIST_LEN):
            total = acc[z, half, member] + parts[2, half, member] + parts[3, half, member]
            name = cand_ids[half, member]
            real = name >= 0.0
            scores.append(jnp.where(real, total, -jnp.inf))
            names.append(jnp.where(real, name, BIG))
        for place in range(TOP_K):
            best = functools.reduce(jnp.maximum, scores)
            best = jnp.max(best, axis=0, keepdims=True)
            tied = [jnp.where(score_j == best, name_j, BIG) for score_j, name_j in zip(scores, names)]
            first = jnp.min(functools.reduce(jnp.minimum, tied), axis=0, keepdims=True)
            for tile in range(tiles):
                lanes = slice(tile * LANES, (tile + 1) * LANES)
                line = place * tiles + tile
                res[z, half, line:line + 1, :] = best[:, lanes]
                res[z, half, TOP_K * tiles + line:TOP_K * tiles + line + 1, :] = first[:, lanes]
            if place + 1 < TOP_K:
                scores = [jnp.where(name_j == first, -jnp.inf, score_j) for score_j, name_j in zip(scores, names)]
        if half == 0:
            await_send(vecs.at[pl.ds(0, block_rows)], send_o)
            await_send(ids_all.at[pl.ds(0, 3)], send_i)
        else:
            await_send(vecs.at[pl.ds(0, chunks * PIECE_ROWS)], send_y)
            await_send(vecs.at[pl.ds(0, chunks * PIECE_ROWS)], send_x)
            await_send(vecs.at[pl.ds(0, 2 * chunks * PIECE_ROWS)], send_d)
        for which in range(dims - 1):
            res_copy(target_at(which), half).start()

    await_send(parts.at[pl.ds(0, 3)], send_r)
    await_send(res.at[pl.ds(0, dims - 1)], send_g)
    await_recv(res.at[pl.ds(0, dims - 1)], recv_g)


def place_kernel(res, out_s, out_i):
    dims, halves, lines, _ = res.shape
    tiles = lines // (2 * TOP_K)
    for part in range(dims):
        for half in range(halves):
            for tile in range(tiles):
                first = ((part * halves + half) * tiles + tile) * LANES
                out_s[:, first:first + LANES] = res[part, half, pl.ds(tile, TOP_K, stride=tiles), :]
                out_i[:, first:first + LANES] = res[part, half, pl.ds(TOP_K * tiles + tile, TOP_K, stride=tiles), :].astype(jnp.int32)


def solution(mesh):
    dims = mesh.shape['dim']
    row_spec = P(('rep', 'shard'), None)

    def local_search(queries, list_vecs, list_ids, probes):
        rows_q, depth = queries.shape
        lists_dev, list_len, _ = list_vecs.shape
        probe_count = probes.shape[1]
        block_rows = lists_dev * list_len
        block_steps = block_rows // STEP_ROWS
        chunks = lists_dev // GROUP_LISTS
        width = rows_q // dims
        dma = pltpu.SemaphoreType.DMA
        any_spec = pl.BlockSpec(memory_space=pl.ANY)
        vmem_spec = pl.BlockSpec(memory_space=pltpu.VMEM)
        found = pl.pallas_call(
            functools.partial(search_kernel, dims),
            out_shape=pltpu.VMEM((dims, 2, TOP_K * width // LANES, LANES), jnp.float32),
            in_specs=[any_spec] * 4,
            out_specs=vmem_spec,
            scratch_shapes=[
                pltpu.VMEM((block_rows, depth), jnp.bfloat16),
                pltpu.VMEM((rows_q, depth), jnp.bfloat16),
                pltpu.VMEM((4 * block_rows, depth), jnp.bfloat16),
                pltpu.VMEM((STEP_ROWS, STEP_ROWS), jnp.bfloat16),
                pltpu.VMEM((dims, 2, LIST_LEN, probe_count, width // 2), jnp.float32),
                pltpu.VMEM((4, 2, LIST_LEN, probe_count, width // 2), jnp.float32),
                pltpu.VMEM((4, LIST_LEN, lists_dev), jnp.int32),
                pltpu.VMEM((2, LIST_LEN, probe_count, width // 2), jnp.float32),
                pltpu.VMEM((probe_count, rows_q), jnp.int32),
                pltpu.VMEM((LIST_LEN, lists_dev), jnp.int32),
                dma, dma,
                dma((block_steps,)), dma,
                dma, dma((block_steps,)),
                dma, dma((REUSE,)), dma, dma((REUSE + 1,)),
                dma, dma((chunks // 2,)),
                dma, dma, dma, dma((4, 2)), dma, dma,
            ],
            compiler_params=pltpu.CompilerParams(collective_id=0, has_side_effects=True, vmem_limit_bytes=60 * 2**20),
            name='ivf_search',
        )(queries, list_vecs.reshape(block_rows, depth), probes.T, list_ids.T)
        scores, ids = pl.pallas_call(
            place_kernel,
            out_shape=(jax.ShapeDtypeStruct((TOP_K, rows_q), jnp.float32),
                       jax.ShapeDtypeStruct((TOP_K, rows_q), jnp.int32)),
            in_specs=[vmem_spec],
            out_specs=(vmem_spec, vmem_spec),
            compiler_params=pltpu.CompilerParams(vmem_limit_bytes=4 * 2**20),
            name='place',
        )(found)
        return scores.T, ids.T

    return jax.shard_map(local_search, mesh=mesh,
                         in_specs=(P(('rep', 'shard'), 'dim'), P('shard', None, 'dim'), P('shard', None), row_spec),
                         out_specs=(row_spec, row_spec), check_vma=False)
```

```python
import functools

import jax
import jax.numpy as jnp
from jax import lax
from jax.experimental import pallas as pl
from jax.experimental.pallas import tpu as pltpu
from jax.sharding import PartitionSpec as P

TOP_K = 10
LIST_LEN = 8
GROUP_LISTS = 8
GROUP_ROWS = GROUP_LISTS * LIST_LEN
STEP_GROUPS = 4
STEP_ROWS = STEP_GROUPS * GROUP_ROWS
PIECE_ROWS = GROUP_ROWS // 2
LANES = 128
REUSE_Y, REUSE_X = 8, 12
MESH = pl.DeviceIdType.MESH
BIG = 1e9


def flip(index, bit):
    return index + bit - 2 * bit * ((index // bit) % 2)


def search_kernel(dims, q_hbm, l_hbm, probes_hbm, ids_hbm, res,
                  raw, qv, vecs, perm, acc, parts, ids_all, cand_ids, probes_ref, ids_ref, load_p, load_i,
                  load_l, load_q, send_o, recv_o, send_y, recv_y, send_x, recv_x,
                  send_d, recv_d, send_i, recv_i, send_r, recv_r, send_g, recv_g):
    rows_q = qv.shape[0]
    lists_dev = ids_ref.shape[1]
    block_rows = lists_dev * LIST_LEN
    block_groups = lists_dev // GROUP_LISTS
    chunks = block_groups
    block_steps = block_groups // STEP_GROUPS
    width = rows_q // dims
    x, z, s = lax.axis_index('rep'), lax.axis_index('dim'), lax.axis_index('shard')
    twin, across, far = flip(s, 1), flip(s, 2), flip(flip(s, 1), 2)
    other_x = 1 - x

    def at(**place):
        return {'rep': x, 'dim': z, 'shard': s, **place}

    def step_rows(step):
        return pl.ds(pl.multiple_of(step * STEP_ROWS, STEP_ROWS), STEP_ROWS)

    def remote(src, dst, send, recv, device):
        return pltpu.make_async_remote_copy(src_ref=src, dst_ref=dst, send_sem=send, recv_sem=recv,
                                            device_id=device, device_id_type=MESH)

    def await_recv(buffer, semaphore):
        remote(buffer, buffer, send_i, semaphore, at()).wait_recv()

    def await_send(buffer, semaphore):
        remote(buffer, buffer, semaphore, recv_i, at()).wait_send()

    def load_lists(number):
        half = block_steps // 2
        first, count = ((half * x, 1), (half * x + 1, half - 1), (half * other_x, half))[number]
        rows = pl.ds(pl.multiple_of(first * STEP_ROWS, STEP_ROWS), count * STEP_ROWS)
        return pltpu.make_async_copy(l_hbm.at[rows], raw.at[rows], load_l.at[number])

    queries_in = pltpu.make_async_copy(q_hbm, qv, load_q)

    def own_copy(block):
        return remote(vecs.at[step_rows(block)], vecs.at[step_rows(block_steps + block)],
                      send_o, recv_o.at[(block // (block_steps // 2) + x) % 2], at(shard=twin))

    def piece(group, chunk):
        first = pl.multiple_of(group * GROUP_ROWS + chunk % 2 * PIECE_ROWS, PIECE_ROWS)
        return vecs.at[pl.ds(first, PIECE_ROWS)]

    def slot(chunk, which):
        return piece(2 * block_groups + STEP_GROUPS * (chunk // 2) + which, chunk)

    def y_copy(chunk):
        return remote(piece(chunks // 2 * x + chunk // 2, chunk), slot(chunk, 0), send_y, recv_y.at[chunk % REUSE_Y], at(shard=across))

    def x_copy(chunk):
        return remote(slot(chunk, 0), slot(chunk, 1), send_x, recv_x.at[chunk % REUSE_X], at(rep=other_x))

    def dy_copy(chunk):
        return remote(slot(chunk, 0), slot(chunk, 2), send_d, recv_d.at[chunk // 2], at(shard=twin))

    def dx_copy(chunk):
        return remote(slot(chunk, 1), slot(chunk, 3), send_d, recv_d.at[chunk // 2], at(shard=twin))

    def id_copy(which, peer):
        return remote(ids_ref, ids_all.at[s], send_i, recv_i, at(shard=peer))

    outer = z % 3 == 0
    mate, far_outer = flip(z, 1), jnp.where(z < 2, dims - 1, 0)
    far_inner = flip(far_outer, 1)

    def part_copy(target, place, half):
        return remote(acc.at[target, half], parts.at[place, half], send_r, recv_r.at[place, half], at(dim=mate))

    def merged_copy(merge, half):
        return remote(parts.at[merge, half], parts.at[3, half], send_r, recv_r.at[3, half],
                      at(dim=(far_outer, far_inner)[merge]))

    def part_wait(place, half):
        await_recv(parts.at[place, half], recv_r.at[place, half])

    def res_copy(target, half):
        return remote(res.at[z, half], res.at[z, half], send_g, recv_g, at(dim=target))

    def target_at(turn):
        first, second, third = (jnp.where(outer, one, two) for one, two in ((far_outer, mate), (far_inner, far_outer), (mate, far_inner)))
        return jnp.where(turn == 0, first, jnp.where(turn == 1, second, jnp.where(turn == 2, third, z)))

    def block_at(turn):
        return (block_steps // 2 * x + turn) % block_steps

    barrier = pltpu.get_barrier_semaphore()
    peers = [at(dim=(z + hop) % dims) for hop in (2, 1, 3)]
    peers += [at(shard=twin), at(shard=across), at(shard=far), at(rep=other_x)]

    def greet(some):
        for peer in some:
            pl.semaphore_signal(barrier, inc=1, device_id=peer, device_id_type=MESH)

    load_lists(0).start()
    greet(peers[:3])
    probes_in = pltpu.make_async_copy(probes_hbm, probes_ref, load_p)
    ids_in = pltpu.make_async_copy(ids_hbm, ids_ref, load_i)
    ids_in.start()
    probes_in.start()
    queries_in.start()
    greet(peers[3:])
    load_lists(1).start()
    load_lists(2).start()

    row = lax.broadcasted_iota(jnp.int32, (STEP_ROWS, STEP_ROWS), 0)
    col = lax.broadcasted_iota(jnp.int32, (STEP_ROWS, STEP_ROWS), 1)
    source = (row // GROUP_ROWS) * GROUP_ROWS + (row % GROUP_LISTS) * LIST_LEN + (row // GROUP_LISTS) % LIST_LEN
    perm[...] = jnp.where(col == source, 1.0, 0.0).astype(jnp.bfloat16)

    def arrange(turn):
        block = block_at(turn)
        moved = jnp.dot(perm[...], raw[step_rows(block), :], preferred_element_type=jnp.float32)
        vecs[step_rows(block), :] = moved.astype(jnp.bfloat16)

    window = REUSE_Y // 2
    load_lists(0).wait()
    arrange(0)
    pl.semaphore_wait(barrier, len(peers))
    for chunk in range(window):
        y_copy(chunk).start()
    acc[...] = jnp.zeros_like(acc)
    ids_in.wait()
    for which, peer in enumerate((twin, across, far)):
        id_copy(which, peer).start()
    ids_all[s] = ids_ref[...]
    probes_in.wait()
    queries_in.wait()

    def name_candidates(tile, carry):
        cols = pl.ds(pl.multiple_of(z * width + tile * LANES, LANES), LANES)
        probe = probes_ref[:, cols]
        lane, page = probe % LANES, probe // LANES
        pages = lists_dev // LANES
        for member in range(LIST_LEN):
            got = jnp.zeros((probe.shape[0], LANES), jnp.int32)
            for number in range(4 * pages):
                table = ids_all[number // pages, member:member + 1, (number % pages) * LANES:(number % pages + 1) * LANES]
                table = jnp.broadcast_to(table, (probe.shape[0], LANES))
                picked = jnp.take_along_axis(table, lane, axis=1, mode='promise_in_bounds')
                got = jnp.where(page == number, picked, got)
            tiles_half = width // 2 // LANES
            place = pl.ds(pl.multiple_of(tile % tiles_half * LANES, LANES), LANES)
            cand_ids[tile // tiles_half, member, :, place] = got.astype(jnp.float32)
        return carry

    def list_block(step):
        return block_at(step % block_steps)

    def score(step, heads, part):
        lists = vecs[step_rows(jnp.where(step < 2 * block_steps, step // block_steps * block_steps + list_block(step), step)), :]
        rows = pl.ds(pl.multiple_of(part * width, width), width)
        scores = lax.dot_general(lists, qv[rows, :], (((1,), (1,)), ((), ())), preferred_element_type=jnp.float32)
        for tile in range(width // LANES):
            probe = probes_ref[:, pl.ds(pl.multiple_of(part * width + tile * LANES, LANES), LANES)]
            low, head = probe % GROUP_LISTS, probe // GROUP_LISTS
            hits = [head == want for want in heads]
            lanes = slice(tile * LANES, (tile + 1) * LANES)
            half, place = divmod(tile * LANES, width // 2)
            kept_lanes = slice(place, place + LANES)
            for member in range(LIST_LEN):
                kept = acc[part, half, member, :, kept_lanes]
                for group, hit in enumerate(hits):
                    first = group * GROUP_ROWS + member * GROUP_LISTS
                    picked = jnp.take_along_axis(scores[first:first + GROUP_LISTS, lanes], low, axis=0, mode='promise_in_bounds')
                    kept = jnp.where(hit, picked, kept)
                acc[part, half, member, :, kept_lanes] = kept

    def heads_at(step):
        local = step < 2 * block_steps
        group = step - 2 * block_steps
        base = block_groups * jnp.where(step < block_steps, s, twin) + STEP_GROUPS * list_block(step)
        heads = []
        for which in range(STEP_GROUPS):
            home = across if which < 2 else far
            side = x if which % 2 == 0 else other_x
            heads.append(jnp.where(local, base + which, block_groups * home + chunks // 2 * side + group))
        return heads

    last = 2 * block_steps + chunks // 2 - 1

    spare_copy = remote(piece(chunks // 2 * other_x + (chunks - 1) // 2, chunks - 1), slot(chunks - 1, 1),
                        send_x, recv_x.at[REUSE_X], at(shard=across))

    def pass_y(chunk):
        y_copy(chunk).wait_recv()
        if not (isinstance(chunk, int) and chunk == chunks - 1):
            x_copy(chunk).start()
        dy_copy(chunk).start()

        @pl.when(chunk + window < chunks)
        def _():
            y_copy(chunk + window).start()

        @pl.when(chunk + window == chunks)
        def _():
            spare_copy.start()

    def pass_x(chunk):
        if isinstance(chunk, int) and chunk == chunks - 1:
            spare_copy.wait_recv()
        else:
            x_copy(chunk).wait_recv()
        dx_copy(chunk).start()

    def await_step(step):
        await_recv(vecs.at[pl.ds(0, 4 * PIECE_ROWS)], recv_d.at[step - 2 * block_steps])

    def score_all(step):
        heads = heads_at(step)
        for part in range(dims):
            score(step, heads, part)

    def early(step, carry):
        own_copy(block_at(step)).start()

        @pl.when(step >= 1)
        def _():
            pass_y(step - 1)

        @pl.when(step >= 5)
        def _():
            pass_x(step - 5)

        @pl.when(step == 0)
        def _():
            load_lists(1).wait()

        @pl.when(step == block_steps // 2 - 1)
        def _():
            load_lists(2).wait()
        score_all(step)
        arrange(step + 1)
        return carry

    def middle(step, carry):
        pass_y(step - 1)
        pass_x(step - 5)

        @pl.when(step == block_steps - 1)
        def _():
            own_copy(block_at(step)).start()

        @pl.when((step == block_steps) | (step == block_steps + block_steps // 2))
        def _():
            await_recv(vecs.at[pl.ds(0, block_rows // 2)], recv_o.at[step // (block_steps // 2) - 2])

        @pl.when(step >= 2 * block_steps)
        def _():
            await_step(step)
        score_all(step)
        return carry

    late_plan = {
        last - 5: 'y25 x21 x22',
        last - 4: 'y26 x23 y27 x24',
        last - 3: 'y28 x25 names y29 x26',
        last - 2: 'y30 x27 y31 x28 x29',
        last - 1: 'x31 x30',
    }

    def late(step, carry):
        for when, plan in late_plan.items():
            @pl.when(step == when)
            def _(plan=plan):
                for word in plan.split():
                    if word == 'names':
                        await_recv(ids_all.at[pl.ds(0, 3)], recv_i)
                        lax.fori_loop(0, width // LANES, name_candidates, 0)
                    else:
                        (pass_y if word[0] == 'y' else pass_x)(int(word[1:]))

        await_step(step)
        score_all(step)
        return carry

    lax.fori_loop(0, block_steps - 1, early, 0)
    lax.fori_loop(block_steps - 1, last - 5, middle, 0)
    lax.fori_loop(last - 5, last, late, 0)
    await_step(jnp.int32(last))
    last_heads = heads_at(jnp.int32(last))

    leads, follows = outer & (s % 2 == 0), outer & (s % 2 == 1)

    def finish(turn, carry):
        @pl.when(leads & (turn == 1))
        def _():
            part_copy(far_outer, 0, 0).start()

        @pl.when(leads & (turn == 2))
        def _():
            part_copy(far_inner, 1, 0).start()
            part_copy(far_outer, 0, 1).start()
            part_copy(far_inner, 1, 1).start()

        @pl.when((leads & (turn == 3)) | (jnp.logical_not(outer) & (turn == 1)))
        def _():
            for half in range(2):
                part_copy(mate, 2, half).start()
        score(jnp.int32(last), last_heads, target_at(turn))
        return carry

    lax.fori_loop(0, dims, finish, 0)

    @pl.when(follows)
    def _():
        for half in range(2):
            part_copy(far_outer, 0, half).start()
            part_copy(far_inner, 1, half).start()
        for half in range(2):
            part_copy(mate, 2, half).start()

    @pl.when(jnp.logical_not(outer))
    def _():
        for half in range(2):
            for merge, target in enumerate((far_outer, far_inner)):
                part_wait(merge, half)
                parts[merge, half] += acc[target, half]
                merged_copy(merge, half).start()

    tiles = width // 2 // LANES
    for half in range(2):
        part_wait(2, half)
        part_wait(3, half)
        scores, names = [], []
        for member in range(LIST_LEN):
            total = acc[z, half, member] + parts[2, half, member] + parts[3, half, member]
            name = cand_ids[half, member]
            real = name >= 0.0
            scores.append(jnp.where(real, total, -jnp.inf))
            names.append(jnp.where(real, name, BIG))
        for place in range(TOP_K):
            best = functools.reduce(jnp.maximum, scores)
            best = jnp.max(best, axis=0, keepdims=True)
            tied = [jnp.where(score_j == best, name_j, BIG) for score_j, name_j in zip(scores, names)]
            first = jnp.min(functools.reduce(jnp.minimum, tied), axis=0, keepdims=True)
            for tile in range(tiles):
                lanes = slice(tile * LANES, (tile + 1) * LANES)
                line = place * tiles + tile
                res[z, half, line:line + 1, :] = best[:, lanes]
                res[z, half, TOP_K * tiles + line:TOP_K * tiles + line + 1, :] = first[:, lanes]
            if place + 1 < TOP_K:
                scores = [jnp.where(name_j == first, -jnp.inf, score_j) for score_j, name_j in zip(scores, names)]
        if half == 0:
            await_send(vecs.at[pl.ds(0, block_rows)], send_o)
            await_send(ids_all.at[pl.ds(0, 3)], send_i)
        else:
            await_send(vecs.at[pl.ds(0, chunks * PIECE_ROWS)], send_y)
            await_send(vecs.at[pl.ds(0, chunks * PIECE_ROWS)], send_x)
            await_send(vecs.at[pl.ds(0, 2 * chunks * PIECE_ROWS)], send_d)
        for which in range(dims - 1):
            res_copy(target_at(which), half).start()

    await_send(parts.at[pl.ds(0, 3)], send_r)
    await_send(res.at[pl.ds(0, dims - 1)], send_g)
    await_recv(res.at[pl.ds(0, dims - 1)], recv_g)


def place_kernel(res, out_s, out_i):
    dims, halves, lines, _ = res.shape
    tiles = lines // (2 * TOP_K)
    for part in range(dims):
        for half in range(halves):
            for tile in range(tiles):
                first = ((part * halves + half) * tiles + tile) * LANES
                out_s[:, first:first + LANES] = res[part, half, pl.ds(tile, TOP_K, stride=tiles), :]
                out_i[:, first:first + LANES] = res[part, half, pl.ds(TOP_K * tiles + tile, TOP_K, stride=tiles), :].astype(jnp.int32)


def solution(mesh):
    dims = mesh.shape['dim']
    row_spec = P(('rep', 'shard'), None)

    def local_search(queries, list_vecs, list_ids, probes):
        rows_q, depth = queries.shape
        lists_dev, list_len, _ = list_vecs.shape
        probe_count = probes.shape[1]
        block_rows = lists_dev * list_len
        block_steps = block_rows // STEP_ROWS
        chunks = lists_dev // GROUP_LISTS
        width = rows_q // dims
        dma = pltpu.SemaphoreType.DMA
        any_spec = pl.BlockSpec(memory_space=pl.ANY)
        vmem_spec = pl.BlockSpec(memory_space=pltpu.VMEM)
        found = pl.pallas_call(
            functools.partial(search_kernel, dims),
            out_shape=pltpu.VMEM((dims, 2, TOP_K * width // LANES, LANES), jnp.float32),
            in_specs=[any_spec] * 4,
            out_specs=vmem_spec,
            scratch_shapes=[
                pltpu.VMEM((block_rows, depth), jnp.bfloat16),
                pltpu.VMEM((rows_q, depth), jnp.bfloat16),
                pltpu.VMEM((4 * block_rows, depth), jnp.bfloat16),
                pltpu.VMEM((STEP_ROWS, STEP_ROWS), jnp.bfloat16),
                pltpu.VMEM((dims, 2, LIST_LEN, probe_count, width // 2), jnp.float32),
                pltpu.VMEM((4, 2, LIST_LEN, probe_count, width // 2), jnp.float32),
                pltpu.VMEM((4, LIST_LEN, lists_dev), jnp.int32),
                pltpu.VMEM((2, LIST_LEN, probe_count, width // 2), jnp.float32),
                pltpu.VMEM((probe_count, rows_q), jnp.int32),
                pltpu.VMEM((LIST_LEN, lists_dev), jnp.int32),
                dma, dma,
                dma((3,)), dma,
                dma, dma((2,)),
                dma, dma((REUSE_Y,)), dma, dma((REUSE_X + 1,)),
                dma, dma((chunks // 2,)),
                dma, dma, dma, dma((4, 2)), dma, dma,
            ],
            compiler_params=pltpu.CompilerParams(collective_id=0, has_side_effects=True, vmem_limit_bytes=60 * 2**20),
            name='ivf_search',
        )(queries, list_vecs.reshape(block_rows, depth), probes.T, list_ids.T)
        scores, ids = pl.pallas_call(
            place_kernel,
            out_shape=(jax.ShapeDtypeStruct((TOP_K, rows_q), jnp.float32),
                       jax.ShapeDtypeStruct((TOP_K, rows_q), jnp.int32)),
            in_specs=[vmem_spec],
            out_specs=(vmem_spec, vmem_spec),
            compiler_params=pltpu.CompilerParams(vmem_limit_bytes=4 * 2**20),
            name='place',
        )(found)
        return scores.T, ids.T

    return jax.shard_map(local_search, mesh=mesh,
                         in_specs=(P(('rep', 'shard'), 'dim'), P('shard', None, 'dim'), P('shard', None), row_spec),
                         out_specs=(row_spec, row_spec), check_vma=False)
```

```python
import functools

import jax
import jax.numpy as jnp
from jax import lax
from jax.experimental import pallas as pl
from jax.experimental.pallas import tpu as pltpu
from jax.sharding import PartitionSpec as P

TOP_K = 10
LIST_LEN = 8
GROUP_LISTS = 8
GROUP_ROWS = GROUP_LISTS * LIST_LEN
STEP_GROUPS = 4
STEP_ROWS = STEP_GROUPS * GROUP_ROWS
PIECE_ROWS = GROUP_ROWS // 2
LANES = 128
REUSE_Y, REUSE_X = 8, 12
MESH = pl.DeviceIdType.MESH
BIG = 1e9


def flip(index, bit):
    return index + bit - 2 * bit * ((index // bit) % 2)


def search_kernel(dims, q_hbm, l_hbm, probes_hbm, ids_hbm, res,
                  raw, qv, vecs, perm, acc, parts, ids_all, cand_ids, probes_ref, ids_ref, load_p, load_i,
                  load_l, load_q, send_o, recv_o, send_y, recv_y, send_x, recv_x,
                  send_d, recv_d, send_i, recv_i, send_r, recv_r, send_g, recv_g, met):
    rows_q = qv.shape[0]
    lists_dev = ids_ref.shape[1]
    block_rows = lists_dev * LIST_LEN
    block_groups = lists_dev // GROUP_LISTS
    chunks = block_groups
    block_steps = block_groups // STEP_GROUPS
    width = rows_q // dims
    x, z, s = lax.axis_index('rep'), lax.axis_index('dim'), lax.axis_index('shard')
    twin, across, far = flip(s, 1), flip(s, 2), flip(flip(s, 1), 2)
    other_x = 1 - x

    def at(**place):
        return {'rep': x, 'dim': z, 'shard': s, **place}

    def step_rows(step):
        return pl.ds(pl.multiple_of(step * STEP_ROWS, STEP_ROWS), STEP_ROWS)

    def remote(src, dst, send, recv, device):
        return pltpu.make_async_remote_copy(src_ref=src, dst_ref=dst, send_sem=send, recv_sem=recv,
                                            device_id=device, device_id_type=MESH)

    def await_recv(buffer, semaphore):
        remote(buffer, buffer, send_i, semaphore, at()).wait_recv()

    def await_send(buffer, semaphore):
        remote(buffer, buffer, semaphore, recv_i, at()).wait_send()

    def load_lists(number):
        half = block_steps // 2
        first, count = ((half * x, 1), (half * x + 1, half - 1), (half * other_x, half))[number]
        rows = pl.ds(pl.multiple_of(first * STEP_ROWS, STEP_ROWS), count * STEP_ROWS)
        return pltpu.make_async_copy(l_hbm.at[rows], raw.at[rows], load_l.at[number])

    queries_in = pltpu.make_async_copy(q_hbm, qv, load_q)

    def own_copy(block):
        return remote(vecs.at[step_rows(block)], vecs.at[step_rows(block_steps + block)],
                      send_o, recv_o.at[(block // (block_steps // 2) + x) % 2], at(shard=twin))

    def piece(group, chunk):
        first = pl.multiple_of(group * GROUP_ROWS + chunk % 2 * PIECE_ROWS, PIECE_ROWS)
        return vecs.at[pl.ds(first, PIECE_ROWS)]

    def slot(chunk, which):
        return piece(2 * block_groups + STEP_GROUPS * (chunk // 2) + which, chunk)

    def y_copy(chunk):
        return remote(piece(chunks // 2 * x + chunk // 2, chunk), slot(chunk, 0), send_y, recv_y.at[chunk % REUSE_Y], at(shard=across))

    def x_copy(chunk):
        return remote(slot(chunk, 0), slot(chunk, 1), send_x, recv_x.at[chunk % REUSE_X], at(rep=other_x))

    def dy_copy(chunk):
        return remote(slot(chunk, 0), slot(chunk, 2), send_d, recv_d.at[chunk // 2], at(shard=twin))

    def dx_copy(chunk):
        return remote(slot(chunk, 1), slot(chunk, 3), send_d, recv_d.at[chunk // 2], at(shard=twin))

    def id_copy(which, peer):
        return remote(ids_ref, ids_all.at[s], send_i, recv_i, at(shard=peer))

    outer = z % 3 == 0
    mate, far_outer = flip(z, 1), jnp.where(z < 2, dims - 1, 0)
    far_inner = flip(far_outer, 1)

    def part_copy(target, place, half):
        return remote(acc.at[target, half], parts.at[place, half], send_r, recv_r.at[place, half], at(dim=mate))

    def merged_copy(merge, half):
        return remote(parts.at[merge, half], parts.at[3, half], send_r, recv_r.at[3, half],
                      at(dim=(far_outer, far_inner)[merge]))

    def part_wait(place, half):
        await_recv(parts.at[place, half], recv_r.at[place, half])

    def res_copy(target, half):
        return remote(res.at[z, half], res.at[z, half], send_g, recv_g, at(dim=target))

    def target_at(turn):
        first, second, third = (jnp.where(outer, one, two) for one, two in ((far_outer, mate), (far_inner, far_outer), (mate, far_inner)))
        return jnp.where(turn == 0, first, jnp.where(turn == 1, second, jnp.where(turn == 2, third, z)))

    def block_at(turn):
        return (block_steps // 2 * x + turn) % block_steps

    barrier = pltpu.get_barrier_semaphore()
    peers = [at(shard=twin), at(shard=across), at(shard=far), at(rep=other_x)]
    beside = jnp.where(outer, 1, 2)

    def tell_line(semaphore):
        @pl.when(z < dims - 1)
        def _():
            pl.semaphore_signal(semaphore, inc=1, device_id=at(dim=(z + 1) % dims), device_id_type=MESH)

        @pl.when(z > 0)
        def _():
            pl.semaphore_signal(semaphore, inc=1, device_id=at(dim=(z + dims - 1) % dims), device_id_type=MESH)

    load_lists(0).start()
    tell_line(barrier)
    probes_in = pltpu.make_async_copy(probes_hbm, probes_ref, load_p)
    ids_in = pltpu.make_async_copy(ids_hbm, ids_ref, load_i)
    ids_in.start()
    probes_in.start()
    queries_in.start()
    for peer in peers:
        pl.semaphore_signal(barrier, inc=1, device_id=peer, device_id_type=MESH)
    load_lists(1).start()
    load_lists(2).start()

    row = lax.broadcasted_iota(jnp.int32, (STEP_ROWS, STEP_ROWS), 0)
    col = lax.broadcasted_iota(jnp.int32, (STEP_ROWS, STEP_ROWS), 1)
    source = (row // GROUP_ROWS) * GROUP_ROWS + (row % GROUP_LISTS) * LIST_LEN + (row // GROUP_LISTS) % LIST_LEN
    perm[...] = jnp.where(col == source, 1.0, 0.0).astype(jnp.bfloat16)

    def arrange(turn):
        block = block_at(turn)
        moved = jnp.dot(perm[...], raw[step_rows(block), :], preferred_element_type=jnp.float32)
        vecs[step_rows(block), :] = moved.astype(jnp.bfloat16)

    window = REUSE_Y // 2
    load_lists(0).wait()
    arrange(0)
    pl.semaphore_wait(barrier, len(peers) + beside)
    for chunk in range(window):
        y_copy(chunk).start()
    tell_line(met.at[0])
    acc[...] = jnp.zeros_like(acc)
    ids_in.wait()
    for which, peer in enumerate((twin, across, far)):
        id_copy(which, peer).start()
    ids_all[s] = ids_ref[...]
    probes_in.wait()
    queries_in.wait()

    def name_candidates(tile, carry):
        cols = pl.ds(pl.multiple_of(z * width + tile * LANES, LANES), LANES)
        probe = probes_ref[:, cols]
        lane, page = probe % LANES, probe // LANES
        pages = lists_dev // LANES
        for member in range(LIST_LEN):
            got = jnp.zeros((probe.shape[0], LANES), jnp.int32)
            for number in range(4 * pages):
                table = ids_all[number // pages, member:member + 1, (number % pages) * LANES:(number % pages + 1) * LANES]
                table = jnp.broadcast_to(table, (probe.shape[0], LANES))
                picked = jnp.take_along_axis(table, lane, axis=1, mode='promise_in_bounds')
                got = jnp.where(page == number, picked, got)
            tiles_half = width // 2 // LANES
            place = pl.ds(pl.multiple_of(tile % tiles_half * LANES, LANES), LANES)
            cand_ids[tile // tiles_half, member, :, place] = got.astype(jnp.float32)
        return carry

    def list_block(step):
        return block_at(step % block_steps)

    def score(step, heads, part):
        lists = vecs[step_rows(jnp.where(step < 2 * block_steps, step // block_steps * block_steps + list_block(step), step)), :]
        rows = pl.ds(pl.multiple_of(part * width, width), width)
        scores = lax.dot_general(lists, qv[rows, :], (((1,), (1,)), ((), ())), preferred_element_type=jnp.float32)
        for tile in range(width // LANES):
            probe = probes_ref[:, pl.ds(pl.multiple_of(part * width + tile * LANES, LANES), LANES)]
            low, head = probe % GROUP_LISTS, probe // GROUP_LISTS
            hits = [head == want for want in heads]
            lanes = slice(tile * LANES, (tile + 1) * LANES)
            half, place = divmod(tile * LANES, width // 2)
            kept_lanes = slice(place, place + LANES)
            for member in range(LIST_LEN):
                kept = acc[part, half, member, :, kept_lanes]
                for group, hit in enumerate(hits):
                    first = group * GROUP_ROWS + member * GROUP_LISTS
                    picked = jnp.take_along_axis(scores[first:first + GROUP_LISTS, lanes], low, axis=0, mode='promise_in_bounds')
                    kept = jnp.where(hit, picked, kept)
                acc[part, half, member, :, kept_lanes] = kept

    def heads_at(step):
        local = step < 2 * block_steps
        group = step - 2 * block_steps
        base = block_groups * jnp.where(step < block_steps, s, twin) + STEP_GROUPS * list_block(step)
        heads = []
        for which in range(STEP_GROUPS):
            home = across if which < 2 else far
            side = x if which % 2 == 0 else other_x
            heads.append(jnp.where(local, base + which, block_groups * home + chunks // 2 * side + group))
        return heads

    last = 2 * block_steps + chunks // 2 - 1

    spare_copy = remote(piece(chunks // 2 * other_x + (chunks - 1) // 2, chunks - 1), slot(chunks - 1, 1),
                        send_x, recv_x.at[REUSE_X], at(shard=across))

    def pass_y(chunk):
        y_copy(chunk).wait_recv()
        if not (isinstance(chunk, int) and chunk == chunks - 1):
            x_copy(chunk).start()
        dy_copy(chunk).start()

        @pl.when(chunk + window < chunks)
        def _():
            y_copy(chunk + window).start()

        @pl.when(chunk + window == chunks)
        def _():
            spare_copy.start()

    def pass_x(chunk):
        if isinstance(chunk, int) and chunk == chunks - 1:
            spare_copy.wait_recv()
        else:
            x_copy(chunk).wait_recv()
        dx_copy(chunk).start()

    def await_step(step):
        await_recv(vecs.at[pl.ds(0, 4 * PIECE_ROWS)], recv_d.at[step - 2 * block_steps])

    def score_all(step):
        heads = heads_at(step)
        for part in range(dims):
            score(step, heads, part)

    def early(step, carry):
        own_copy(block_at(step)).start()

        @pl.when(step >= 1)
        def _():
            pass_y(step - 1)

        @pl.when(step >= 5)
        def _():
            pass_x(step - 5)

        @pl.when(step == 0)
        def _():
            load_lists(1).wait()

        @pl.when(step == block_steps // 2 - 1)
        def _():
            load_lists(2).wait()
        score_all(step)
        arrange(step + 1)
        return carry

    def middle(step, carry):
        pass_y(step - 1)
        pass_x(step - 5)

        @pl.when(step == block_steps - 1)
        def _():
            own_copy(block_at(step)).start()

        @pl.when((step == block_steps) | (step == block_steps + block_steps // 2))
        def _():
            await_recv(vecs.at[pl.ds(0, block_rows // 2)], recv_o.at[step // (block_steps // 2) - 2])

        @pl.when(step >= 2 * block_steps)
        def _():
            await_step(step)
        score_all(step)
        return carry

    late_plan = {
        last - 5: 'y25 x21 x22',
        last - 4: 'y26 x23 y27 x24',
        last - 3: 'y28 x25 names y29 x26',
        last - 2: 'y30 x27 y31 x28 x29',
        last - 1: 'x31 x30',
    }

    def late(step, carry):
        for when, plan in late_plan.items():
            @pl.when(step == when)
            def _(plan=plan):
                for word in plan.split():
                    if word == 'names':
                        await_recv(ids_all.at[pl.ds(0, 3)], recv_i)
                        lax.fori_loop(0, width // LANES, name_candidates, 0)
                    else:
                        (pass_y if word[0] == 'y' else pass_x)(int(word[1:]))

        await_step(step)
        score_all(step)
        return carry

    lax.fori_loop(0, block_steps - 1, early, 0)
    lax.fori_loop(block_steps - 1, last - 5, middle, 0)
    pl.semaphore_wait(met.at[0], beside)
    tell_line(met.at[1])
    lax.fori_loop(last - 5, last, late, 0)
    pl.semaphore_wait(met.at[1], beside)
    await_step(jnp.int32(last))
    last_heads = heads_at(jnp.int32(last))

    leads, follows = outer & (s % 2 == 0), outer & (s % 2 == 1)

    def finish(turn, carry):
        @pl.when(leads & (turn == 1))
        def _():
            part_copy(far_outer, 0, 0).start()

        @pl.when(leads & (turn == 2))
        def _():
            part_copy(far_inner, 1, 0).start()
            part_copy(far_outer, 0, 1).start()
            part_copy(far_inner, 1, 1).start()

        @pl.when((leads & (turn == 3)) | (jnp.logical_not(outer) & (turn == 1)))
        def _():
            for half in range(2):
                part_copy(mate, 2, half).start()
        score(jnp.int32(last), last_heads, target_at(turn))
        return carry

    lax.fori_loop(0, dims, finish, 0)

    @pl.when(follows)
    def _():
        for half in range(2):
            part_copy(far_outer, 0, half).start()
            part_copy(far_inner, 1, half).start()
        for half in range(2):
            part_copy(mate, 2, half).start()

    @pl.when(jnp.logical_not(outer))
    def _():
        for half in range(2):
            for merge, target in enumerate((far_outer, far_inner)):
                part_wait(merge, half)
                parts[merge, half] += acc[target, half]
                merged_copy(merge, half).start()

    tiles = width // 2 // LANES
    for half in range(2):
        part_wait(2, half)
        part_wait(3, half)
        scores, names = [], []
        for member in range(LIST_LEN):
            total = acc[z, half, member] + parts[2, half, member] + parts[3, half, member]
            name = cand_ids[half, member]
            real = name >= 0.0
            scores.append(jnp.where(real, total, -jnp.inf))
            names.append(jnp.where(real, name, BIG))
        for place in range(TOP_K):
            best = functools.reduce(jnp.maximum, scores)
            best = jnp.max(best, axis=0, keepdims=True)
            tied = [jnp.where(score_j == best, name_j, BIG) for score_j, name_j in zip(scores, names)]
            first = jnp.min(functools.reduce(jnp.minimum, tied), axis=0, keepdims=True)
            for tile in range(tiles):
                lanes = slice(tile * LANES, (tile + 1) * LANES)
                line = place * tiles + tile
                res[z, half, line:line + 1, :] = best[:, lanes]
                res[z, half, TOP_K * tiles + line:TOP_K * tiles + line + 1, :] = first[:, lanes]
            if place + 1 < TOP_K:
                scores = [jnp.where(name_j == first, -jnp.inf, score_j) for score_j, name_j in zip(scores, names)]
        if half == 0:
            await_send(vecs.at[pl.ds(0, block_rows)], send_o)
            await_send(ids_all.at[pl.ds(0, 3)], send_i)
        else:
            await_send(vecs.at[pl.ds(0, chunks * PIECE_ROWS)], send_y)
            await_send(vecs.at[pl.ds(0, chunks * PIECE_ROWS)], send_x)
            await_send(vecs.at[pl.ds(0, 2 * chunks * PIECE_ROWS)], send_d)
        for which in range(dims - 1):
            res_copy(target_at(which), half).start()

    await_send(parts.at[pl.ds(0, 3)], send_r)
    await_send(res.at[pl.ds(0, dims - 1)], send_g)
    await_recv(res.at[pl.ds(0, dims - 1)], recv_g)


def place_kernel(res, out_s, out_i):
    dims, halves, lines, _ = res.shape
    tiles = lines // (2 * TOP_K)
    for part in range(dims):
        for half in range(halves):
            for tile in range(tiles):
                first = ((part * halves + half) * tiles + tile) * LANES
                out_s[:, first:first + LANES] = res[part, half, pl.ds(tile, TOP_K, stride=tiles), :]
                out_i[:, first:first + LANES] = res[part, half, pl.ds(TOP_K * tiles + tile, TOP_K, stride=tiles), :].astype(jnp.int32)


def solution(mesh):
    dims = mesh.shape['dim']
    row_spec = P(('rep', 'shard'), None)

    def local_search(queries, list_vecs, list_ids, probes):
        rows_q, depth = queries.shape
        lists_dev, list_len, _ = list_vecs.shape
        probe_count = probes.shape[1]
        block_rows = lists_dev * list_len
        block_steps = block_rows // STEP_ROWS
        chunks = lists_dev // GROUP_LISTS
        width = rows_q // dims
        dma = pltpu.SemaphoreType.DMA
        any_spec = pl.BlockSpec(memory_space=pl.ANY)
        vmem_spec = pl.BlockSpec(memory_space=pltpu.VMEM)
        found = pl.pallas_call(
            functools.partial(search_kernel, dims),
            out_shape=pltpu.VMEM((dims, 2, TOP_K * width // LANES, LANES), jnp.float32),
            in_specs=[any_spec] * 4,
            out_specs=vmem_spec,
            scratch_shapes=[
                pltpu.VMEM((block_rows, depth), jnp.bfloat16),
                pltpu.VMEM((rows_q, depth), jnp.bfloat16),
                pltpu.VMEM((4 * block_rows, depth), jnp.bfloat16),
                pltpu.VMEM((STEP_ROWS, STEP_ROWS), jnp.bfloat16),
                pltpu.VMEM((dims, 2, LIST_LEN, probe_count, width // 2), jnp.float32),
                pltpu.VMEM((4, 2, LIST_LEN, probe_count, width // 2), jnp.float32),
                pltpu.VMEM((4, LIST_LEN, lists_dev), jnp.int32),
                pltpu.VMEM((2, LIST_LEN, probe_count, width // 2), jnp.float32),
                pltpu.VMEM((probe_count, rows_q), jnp.int32),
                pltpu.VMEM((LIST_LEN, lists_dev), jnp.int32),
                dma, dma,
                dma((3,)), dma,
                dma, dma((2,)),
                dma, dma((REUSE_Y,)), dma, dma((REUSE_X + 1,)),
                dma, dma((chunks // 2,)),
                dma, dma, dma, dma((4, 2)), dma, dma,
                pltpu.SemaphoreType.REGULAR((2,)),
            ],
            compiler_params=pltpu.CompilerParams(collective_id=0, has_side_effects=True, vmem_limit_bytes=60 * 2**20),
            name='ivf_search',
        )(queries, list_vecs.reshape(block_rows, depth), probes.T, list_ids.T)
        scores, ids = pl.pallas_call(
            place_kernel,
            out_shape=(jax.ShapeDtypeStruct((TOP_K, rows_q), jnp.float32),
                       jax.ShapeDtypeStruct((TOP_K, rows_q), jnp.int32)),
            in_specs=[vmem_spec],
            out_specs=(vmem_spec, vmem_spec),
            compiler_params=pltpu.CompilerParams(vmem_limit_bytes=4 * 2**20),
            name='place',
        )(found)
        return scores.T, ids.T

    return jax.shard_map(local_search, mesh=mesh,
                         in_specs=(P(('rep', 'shard'), 'dim'), P('shard', None, 'dim'), P('shard', None), row_spec),
                         out_specs=(row_spec, row_spec), check_vma=False)
```

```python
import functools

import jax
import jax.numpy as jnp
from jax import lax
from jax.experimental import pallas as pl
from jax.experimental.pallas import tpu as pltpu
from jax.sharding import PartitionSpec as P

TOP_K = 10
LIST_LEN = 8
GROUP_LISTS = 8
GROUP_ROWS = GROUP_LISTS * LIST_LEN
STEP_GROUPS = 4
STEP_ROWS = STEP_GROUPS * GROUP_ROWS
PIECE_ROWS = GROUP_ROWS // 2
LANES = 128
REUSE_Y, REUSE_X = 8, 12
MESH = pl.DeviceIdType.MESH
BIG = 1e9


def flip(index, bit):
    return index + bit - 2 * bit * ((index // bit) % 2)


def search_kernel(dims, q_hbm, l_hbm, probes_hbm, ids_hbm, res,
                  raw, qv, vecs, perm, acc, parts, ids_all, cand_ids, probes_ref, ids_ref, load_p, load_i,
                  load_l, load_q, send_o, recv_o, send_y, recv_y, send_x, recv_x,
                  send_d, recv_d, send_i, recv_i, send_r, recv_r, send_g, recv_g, met):
    rows_q = qv.shape[0]
    lists_dev = ids_ref.shape[1]
    block_rows = lists_dev * LIST_LEN
    block_groups = lists_dev // GROUP_LISTS
    chunks = block_groups
    block_steps = block_groups // STEP_GROUPS
    width = rows_q // dims
    x, z, s = lax.axis_index('rep'), lax.axis_index('dim'), lax.axis_index('shard')
    twin, across, far = flip(s, 1), flip(s, 2), flip(flip(s, 1), 2)
    other_x = 1 - x

    def at(**place):
        return {'rep': x, 'dim': z, 'shard': s, **place}

    def step_rows(step):
        return pl.ds(pl.multiple_of(step * STEP_ROWS, STEP_ROWS), STEP_ROWS)

    def remote(src, dst, send, recv, device):
        return pltpu.make_async_remote_copy(src_ref=src, dst_ref=dst, send_sem=send, recv_sem=recv,
                                            device_id=device, device_id_type=MESH)

    def await_recv(buffer, semaphore):
        remote(buffer, buffer, send_i, semaphore, at()).wait_recv()

    def await_send(buffer, semaphore):
        remote(buffer, buffer, semaphore, recv_i, at()).wait_send()

    def load_lists(number):
        half = block_steps // 2
        first, count = ((half * x, 1), (half * x + 1, half - 1), (half * other_x, half))[number]
        rows = pl.ds(pl.multiple_of(first * STEP_ROWS, STEP_ROWS), count * STEP_ROWS)
        return pltpu.make_async_copy(l_hbm.at[rows], raw.at[rows], load_l.at[number])

    queries_in = pltpu.make_async_copy(q_hbm, qv, load_q)

    def own_copy(block):
        return remote(vecs.at[step_rows(block)], vecs.at[step_rows(block_steps + block)],
                      send_o, recv_o.at[(block // (block_steps // 2) + x) % 2], at(shard=twin))

    def piece(group, chunk):
        first = pl.multiple_of(group * GROUP_ROWS + chunk % 2 * PIECE_ROWS, PIECE_ROWS)
        return vecs.at[pl.ds(first, PIECE_ROWS)]

    def slot(chunk, which):
        return piece(2 * block_groups + STEP_GROUPS * (chunk // 2) + which, chunk)

    def y_copy(chunk):
        return remote(piece(chunks // 2 * x + chunk // 2, chunk), slot(chunk, 0), send_y, recv_y.at[chunk % REUSE_Y], at(shard=across))

    def x_copy(chunk):
        return remote(slot(chunk, 0), slot(chunk, 1), send_x, recv_x.at[chunk % REUSE_X], at(rep=other_x))

    def dy_copy(chunk):
        return remote(slot(chunk, 0), slot(chunk, 2), send_d, recv_d.at[chunk // 2], at(shard=twin))

    def dx_copy(chunk):
        return remote(slot(chunk, 1), slot(chunk, 3), send_d, recv_d.at[chunk // 2], at(shard=twin))

    def id_copy(which, peer):
        return remote(ids_ref, ids_all.at[s], send_i, recv_i, at(shard=peer))

    outer = z % 3 == 0
    mate, far_outer = flip(z, 1), jnp.where(z < 2, dims - 1, 0)
    far_inner = flip(far_outer, 1)

    def part_copy(target, place, half):
        return remote(acc.at[target, half], parts.at[place, half], send_r, recv_r.at[place, half], at(dim=mate))

    def merged_copy(merge, half):
        return remote(parts.at[merge, half], parts.at[3, half], send_r, recv_r.at[3, half],
                      at(dim=(far_outer, far_inner)[merge]))

    def part_wait(place, half):
        await_recv(parts.at[place, half], recv_r.at[place, half])

    def res_copy(target, half):
        return remote(res.at[z, half], res.at[z, half], send_g, recv_g, at(dim=target))

    def target_at(turn):
        first, second, third = (jnp.where(outer, one, two) for one, two in ((far_outer, mate), (far_inner, far_outer), (mate, far_inner)))
        return jnp.where(turn == 0, first, jnp.where(turn == 1, second, jnp.where(turn == 2, third, z)))

    def block_at(turn):
        return (block_steps // 2 * x + turn) % block_steps

    barrier = pltpu.get_barrier_semaphore()
    peers = [at(shard=twin), at(shard=across), at(shard=far), at(rep=other_x)]
    beside = jnp.where(outer, 1, 2)

    def tell_line(semaphore):
        @pl.when(z < dims - 1)
        def _():
            pl.semaphore_signal(semaphore, inc=1, device_id=at(dim=(z + 1) % dims), device_id_type=MESH)

        @pl.when(z > 0)
        def _():
            pl.semaphore_signal(semaphore, inc=1, device_id=at(dim=(z + dims - 1) % dims), device_id_type=MESH)

    load_lists(0).start()
    tell_line(barrier)
    probes_in = pltpu.make_async_copy(probes_hbm, probes_ref, load_p)
    ids_in = pltpu.make_async_copy(ids_hbm, ids_ref, load_i)
    ids_in.start()
    probes_in.start()
    queries_in.start()
    for peer in peers:
        pl.semaphore_signal(barrier, inc=1, device_id=peer, device_id_type=MESH)
    load_lists(1).start()
    load_lists(2).start()

    row = lax.broadcasted_iota(jnp.int32, (STEP_ROWS, STEP_ROWS), 0)
    col = lax.broadcasted_iota(jnp.int32, (STEP_ROWS, STEP_ROWS), 1)
    source = (row // GROUP_ROWS) * GROUP_ROWS + (row % GROUP_LISTS) * LIST_LEN + (row // GROUP_LISTS) % LIST_LEN
    perm[...] = jnp.where(col == source, 1.0, 0.0).astype(jnp.bfloat16)

    def arrange(turn):
        block = block_at(turn)
        moved = jnp.dot(perm[...], raw[step_rows(block), :], preferred_element_type=jnp.float32)
        vecs[step_rows(block), :] = moved.astype(jnp.bfloat16)

    window = REUSE_Y // 2
    load_lists(0).wait()
    arrange(0)
    pl.semaphore_wait(barrier, len(peers) + beside)
    for chunk in range(window):
        y_copy(chunk).start()
    tell_line(met.at[0])
    acc[...] = jnp.zeros_like(acc)
    ids_in.wait()
    for which, peer in enumerate((twin, across, far)):
        id_copy(which, peer).start()
    ids_all[s] = ids_ref[...]
    probes_in.wait()
    queries_in.wait()

    def name_candidates(tile, carry):
        cols = pl.ds(pl.multiple_of(z * width + tile * LANES, LANES), LANES)
        probe = probes_ref[:, cols]
        lane, page = probe % LANES, probe // LANES
        pages = lists_dev // LANES
        for member in range(LIST_LEN):
            got = jnp.zeros((probe.shape[0], LANES), jnp.int32)
            for number in range(4 * pages):
                table = ids_all[number // pages, member:member + 1, (number % pages) * LANES:(number % pages + 1) * LANES]
                table = jnp.broadcast_to(table, (probe.shape[0], LANES))
                picked = jnp.take_along_axis(table, lane, axis=1, mode='promise_in_bounds')
                got = jnp.where(page == number, picked, got)
            tiles_half = width // 2 // LANES
            place = pl.ds(pl.multiple_of(tile % tiles_half * LANES, LANES), LANES)
            cand_ids[tile // tiles_half, member, :, place] = got.astype(jnp.float32)
        return carry

    def list_block(step):
        return block_at(step % block_steps)

    def score(step, heads, part):
        lists = vecs[step_rows(jnp.where(step < 2 * block_steps, step // block_steps * block_steps + list_block(step), step)), :]
        rows = pl.ds(pl.multiple_of(part * width, width), width)
        scores = lax.dot_general(lists, qv[rows, :], (((1,), (1,)), ((), ())), preferred_element_type=jnp.float32)
        for tile in range(width // LANES):
            probe = probes_ref[:, pl.ds(pl.multiple_of(part * width + tile * LANES, LANES), LANES)]
            low, head = probe % GROUP_LISTS, probe // GROUP_LISTS
            hits = [head == want for want in heads]
            lanes = slice(tile * LANES, (tile + 1) * LANES)
            half, place = divmod(tile * LANES, width // 2)
            kept_lanes = slice(place, place + LANES)
            for member in range(LIST_LEN):
                kept = acc[part, half, member, :, kept_lanes]
                for group, hit in enumerate(hits):
                    first = group * GROUP_ROWS + member * GROUP_LISTS
                    picked = jnp.take_along_axis(scores[first:first + GROUP_LISTS, lanes], low, axis=0, mode='promise_in_bounds')
                    kept = jnp.where(hit, picked, kept)
                acc[part, half, member, :, kept_lanes] = kept

    def heads_at(step):
        local = step < 2 * block_steps
        group = step - 2 * block_steps
        base = block_groups * jnp.where(step < block_steps, s, twin) + STEP_GROUPS * list_block(step)
        heads = []
        for which in range(STEP_GROUPS):
            home = across if which < 2 else far
            side = x if which % 2 == 0 else other_x
            heads.append(jnp.where(local, base + which, block_groups * home + chunks // 2 * side + group))
        return heads

    last = 2 * block_steps + chunks // 2 - 1

    spare_copy = remote(piece(chunks // 2 * other_x + (chunks - 1) // 2, chunks - 1), slot(chunks - 1, 1),
                        send_x, recv_x.at[REUSE_X], at(shard=across))

    def pass_y(chunk):
        y_copy(chunk).wait_recv()
        if not (isinstance(chunk, int) and chunk == chunks - 1):
            x_copy(chunk).start()
        dy_copy(chunk).start()

        @pl.when(chunk + window < chunks)
        def _():
            y_copy(chunk + window).start()

        @pl.when(chunk + window == chunks)
        def _():
            spare_copy.start()

    def pass_x(chunk):
        if isinstance(chunk, int) and chunk == chunks - 1:
            spare_copy.wait_recv()
        else:
            x_copy(chunk).wait_recv()
        dx_copy(chunk).start()

    def await_step(step):
        await_recv(vecs.at[pl.ds(0, 4 * PIECE_ROWS)], recv_d.at[step - 2 * block_steps])

    def score_all(step):
        heads = heads_at(step)
        for part in range(dims):
            score(step, heads, part)

    def early(step, carry):
        own_copy(block_at(step)).start()

        @pl.when(step >= 1)
        def _():
            pass_y(step - 1)

        @pl.when(step >= 5)
        def _():
            pass_x(step - 5)

        @pl.when(step == 0)
        def _():
            load_lists(1).wait()

        @pl.when(step == block_steps // 2 - 1)
        def _():
            load_lists(2).wait()
        score_all(step)
        arrange(step + 1)
        return carry

    def middle(step, carry):
        pass_y(step - 1)
        pass_x(step - 5)

        @pl.when(step == block_steps - 1)
        def _():
            own_copy(block_at(step)).start()

        @pl.when((step == block_steps) | (step == block_steps + block_steps // 2))
        def _():
            await_recv(vecs.at[pl.ds(0, block_rows // 2)], recv_o.at[step // (block_steps // 2) - 2])

        @pl.when(step >= 2 * block_steps)
        def _():
            await_step(step)
        score_all(step)
        return carry

    late_plan = {
        last - 5: ('y25', 'x21', 'x22'),
        last - 4: ('y26', 'x23', 'y27', 'x24'),
        last - 3: ('y28', 'x25', 'names', 'y29', 'x26'),
        last - 2: ('y30', 'x27', 'y31', 'x28', 'x29'),
        last - 1: ('x31', 'x30'),
    }

    def late(step, carry):
        for when, plan in late_plan.items():
            @pl.when(step == when)
            def _(plan=plan):
                for word in plan:
                    if word == 'names':
                        await_recv(ids_all.at[pl.ds(0, 3)], recv_i)
                        lax.fori_loop(0, width // LANES, name_candidates, 0)
                    else:
                        (pass_y if word[0] == 'y' else pass_x)(int(word[1:]))

        await_step(step)
        score_all(step)
        return carry

    lax.fori_loop(0, block_steps - 1, early, 0)
    lax.fori_loop(block_steps - 1, last - 5, middle, 0)
    pl.semaphore_wait(met.at[0], beside)
    tell_line(met.at[1])
    lax.fori_loop(last - 5, last, late, 0)
    pl.semaphore_wait(met.at[1], beside)
    await_step(jnp.int32(last))
    last_heads = heads_at(jnp.int32(last))

    leads, follows = outer & (s % 2 == 0), outer & (s % 2 == 1)

    def finish(turn, carry):
        @pl.when(leads & (turn == 1))
        def _():
            part_copy(far_outer, 0, 0).start()

        @pl.when(leads & (turn == 2))
        def _():
            part_copy(far_inner, 1, 0).start()
            part_copy(far_outer, 0, 1).start()
            part_copy(far_inner, 1, 1).start()

        @pl.when((leads & (turn == 3)) | (jnp.logical_not(outer) & (turn == 1)))
        def _():
            for half in range(2):
                part_copy(mate, 2, half).start()
        score(jnp.int32(last), last_heads, target_at(turn))
        return carry

    lax.fori_loop(0, dims, finish, 0)

    @pl.when(follows)
    def _():
        for half in range(2):
            part_copy(far_outer, 0, half).start()
            part_copy(far_inner, 1, half).start()
        for half in range(2):
            part_copy(mate, 2, half).start()

    @pl.when(jnp.logical_not(outer))
    def _():
        for half in range(2):
            for merge, target in enumerate((far_outer, far_inner)):
                part_wait(merge, half)
                parts[merge, half] += acc[target, half]
                merged_copy(merge, half).start()

    tiles = width // 2 // LANES
    for half in range(2):
        part_wait(2, half)
        part_wait(3, half)
        scores, names = [], []
        for member in range(LIST_LEN):
            total = acc[z, half, member] + parts[2, half, member] + parts[3, half, member]
            name = cand_ids[half, member]
            real = name >= 0.0
            scores.append(jnp.where(real, total, -jnp.inf))
            names.append(jnp.where(real, name, BIG))
        for place in range(TOP_K):
            best = functools.reduce(jnp.maximum, scores)
            best = jnp.max(best, axis=0, keepdims=True)
            tied = [jnp.where(score_j == best, name_j, BIG) for score_j, name_j in zip(scores, names)]
            first = jnp.min(functools.reduce(jnp.minimum, tied), axis=0, keepdims=True)
            for tile in range(tiles):
                lanes = slice(tile * LANES, (tile + 1) * LANES)
                line = place * tiles + tile
                res[z, half, line:line + 1, :] = best[:, lanes]
                res[z, half, TOP_K * tiles + line:TOP_K * tiles + line + 1, :] = first[:, lanes]
            if place + 1 < TOP_K:
                scores = [jnp.where(name_j == first, -jnp.inf, score_j) for score_j, name_j in zip(scores, names)]
        if half == 0:
            await_send(vecs.at[pl.ds(0, block_rows)], send_o)
            await_send(ids_all.at[pl.ds(0, 3)], send_i)
        else:
            await_send(vecs.at[pl.ds(0, chunks * PIECE_ROWS)], send_y)
            await_send(vecs.at[pl.ds(0, chunks * PIECE_ROWS)], send_x)
            await_send(vecs.at[pl.ds(0, 2 * chunks * PIECE_ROWS)], send_d)
        for which in range(dims - 1):
            res_copy(target_at(which), half).start()

    await_send(parts.at[pl.ds(0, 3)], send_r)
    await_send(res.at[pl.ds(0, dims - 1)], send_g)
    await_recv(res.at[pl.ds(0, dims - 1)], recv_g)


def place_kernel(res, out_s, out_i):
    dims, halves, lines, _ = res.shape
    tiles = lines // (2 * TOP_K)
    for part in range(dims):
        for half in range(halves):
            for tile in range(tiles):
                first = ((part * halves + half) * tiles + tile) * LANES
                out_s[:, first:first + LANES] = res[part, half, pl.ds(tile, TOP_K, stride=tiles), :]
                out_i[:, first:first + LANES] = res[part, half, pl.ds(TOP_K * tiles + tile, TOP_K, stride=tiles), :].astype(jnp.int32)


def solution(mesh):
    dims = mesh.shape['dim']
    row_spec = P(('rep', 'shard'), None)

    def local_search(queries, list_vecs, list_ids, probes):
        rows_q, depth = queries.shape
        lists_dev, list_len, _ = list_vecs.shape
        probe_count = probes.shape[1]
        block_rows = lists_dev * list_len
        block_steps = block_rows // STEP_ROWS
        chunks = lists_dev // GROUP_LISTS
        width = rows_q // dims
        dma = pltpu.SemaphoreType.DMA
        any_spec = pl.BlockSpec(memory_space=pl.ANY)
        vmem_spec = pl.BlockSpec(memory_space=pltpu.VMEM)
        found = pl.pallas_call(
            functools.partial(search_kernel, dims),
            out_shape=pltpu.VMEM((dims, 2, TOP_K * width // LANES, LANES), jnp.float32),
            in_specs=[any_spec] * 4,
            out_specs=vmem_spec,
            scratch_shapes=[
                pltpu.VMEM((block_rows, depth), jnp.bfloat16),
                pltpu.VMEM((rows_q, depth), jnp.bfloat16),
                pltpu.VMEM((4 * block_rows, depth), jnp.bfloat16),
                pltpu.VMEM((STEP_ROWS, STEP_ROWS), jnp.bfloat16),
                pltpu.VMEM((dims, 2, LIST_LEN, probe_count, width // 2), jnp.float32),
                pltpu.VMEM((4, 2, LIST_LEN, probe_count, width // 2), jnp.float32),
                pltpu.VMEM((4, LIST_LEN, lists_dev), jnp.int32),
                pltpu.VMEM((2, LIST_LEN, probe_count, width // 2), jnp.float32),
                pltpu.VMEM((probe_count, rows_q), jnp.int32),
                pltpu.VMEM((LIST_LEN, lists_dev), jnp.int32),
                dma, dma,
                dma((3,)), dma,
                dma, dma((2,)),
                dma, dma((REUSE_Y,)), dma, dma((REUSE_X + 1,)),
                dma, dma((chunks // 2,)),
                dma, dma, dma, dma((4, 2)), dma, dma,
                pltpu.SemaphoreType.REGULAR((2,)),
            ],
            compiler_params=pltpu.CompilerParams(collective_id=0, has_side_effects=True, vmem_limit_bytes=60 * 2**20),
            name='ivf_search',
        )(queries, list_vecs.reshape(block_rows, depth), probes.T, list_ids.T)
        scores, ids = pl.pallas_call(
            place_kernel,
            out_shape=(jax.ShapeDtypeStruct((TOP_K, rows_q), jnp.float32),
                       jax.ShapeDtypeStruct((TOP_K, rows_q), jnp.int32)),
            in_specs=[vmem_spec],
            out_specs=(vmem_spec, vmem_spec),
            compiler_params=pltpu.CompilerParams(vmem_limit_bytes=4 * 2**20),
            name='place',
        )(found)
        return scores.T, ids.T

    return jax.shard_map(local_search, mesh=mesh,
                         in_specs=(P(('rep', 'shard'), 'dim'), P('shard', None, 'dim'), P('shard', None), row_spec),
                         out_specs=(row_spec, row_spec), check_vma=False)
```

```python
import functools

import jax
import jax.numpy as jnp
from jax import lax
from jax.experimental import pallas as pl
from jax.experimental.pallas import tpu as pltpu
from jax.sharding import PartitionSpec as P

TOP_K = 10
LIST_LEN = 8
GROUP_LISTS = 8
GROUP_ROWS = GROUP_LISTS * LIST_LEN
STEP_GROUPS = 4
STEP_ROWS = STEP_GROUPS * GROUP_ROWS
PIECE_ROWS = GROUP_ROWS // 2
LANES = 128
REUSE_Y, REUSE_X = 8, 12
MESH = pl.DeviceIdType.MESH
BIG = 1e9


def flip(index, bit):
    return index + bit - 2 * bit * ((index // bit) % 2)


def search_kernel(dims, q_hbm, l_hbm, probes_hbm, ids_hbm, res,
                  raw, qv, vecs, perm, acc, parts, ids_all, cand_ids, probes_ref, ids_ref, load_p, load_i,
                  load_l, load_q, send_o, recv_o, send_y, recv_y, send_x, recv_x,
                  send_d, recv_d, send_i, recv_i, send_r, recv_r, send_g, recv_g, met):
    rows_q = qv.shape[0]
    lists_dev = ids_ref.shape[1]
    block_rows = lists_dev * LIST_LEN
    block_groups = lists_dev // GROUP_LISTS
    chunks = block_groups
    block_steps = block_groups // STEP_GROUPS
    width = rows_q // dims
    row_blocks = 2 * dims
    block_width = rows_q // row_blocks
    x, z, s = lax.axis_index('rep'), lax.axis_index('dim'), lax.axis_index('shard')
    twin, across, far = flip(s, 1), flip(s, 2), flip(flip(s, 1), 2)
    other_x = 1 - x

    def at(**place):
        return {'rep': x, 'dim': z, 'shard': s, **place}

    def step_rows(step):
        return pl.ds(pl.multiple_of(step * STEP_ROWS, STEP_ROWS), STEP_ROWS)

    def remote(src, dst, send, recv, device):
        return pltpu.make_async_remote_copy(src_ref=src, dst_ref=dst, send_sem=send, recv_sem=recv,
                                            device_id=device, device_id_type=MESH)

    def await_recv(buffer, semaphore):
        remote(buffer, buffer, send_i, semaphore, at()).wait_recv()

    def await_send(buffer, semaphore):
        remote(buffer, buffer, semaphore, recv_i, at()).wait_send()

    def load_lists(number):
        half = block_steps // 2
        first, count = ((half * x, 1), (half * x + 1, half - 1), (half * other_x, half))[number]
        rows = pl.ds(pl.multiple_of(first * STEP_ROWS, STEP_ROWS), count * STEP_ROWS)
        return pltpu.make_async_copy(l_hbm.at[rows], raw.at[rows], load_l.at[number])

    queries_in = pltpu.make_async_copy(q_hbm, qv, load_q)

    def own_copy(block):
        return remote(vecs.at[step_rows(block)], vecs.at[step_rows(block_steps + block)],
                      send_o, recv_o.at[(block // (block_steps // 2) + x) % 2], at(shard=twin))

    def piece(group, chunk):
        first = pl.multiple_of(group * GROUP_ROWS + chunk % 2 * PIECE_ROWS, PIECE_ROWS)
        return vecs.at[pl.ds(first, PIECE_ROWS)]

    def slot(chunk, which):
        return piece(2 * block_groups + STEP_GROUPS * (chunk // 2) + which, chunk)

    def y_copy(chunk):
        return remote(piece(chunks // 2 * x + chunk // 2, chunk), slot(chunk, 0), send_y, recv_y.at[chunk % REUSE_Y], at(shard=across))

    def x_copy(chunk):
        return remote(slot(chunk, 0), slot(chunk, 1), send_x, recv_x.at[chunk % REUSE_X], at(rep=other_x))

    def dy_copy(chunk):
        return remote(slot(chunk, 0), slot(chunk, 2), send_d, recv_d.at[chunk // 2], at(shard=twin))

    def dx_copy(chunk):
        return remote(slot(chunk, 1), slot(chunk, 3), send_d, recv_d.at[chunk // 2], at(shard=twin))

    def id_copy(which, peer):
        return remote(ids_ref, ids_all.at[s], send_i, recv_i, at(shard=peer))

    outer, low = z % 3 == 0, z < 2
    mate, far_outer = flip(z, 1), jnp.where(low, dims - 1, 0)
    far_inner = flip(far_outer, 1)
    owned = jnp.where(outer, 3, 1)

    def mirrored(block):
        return jnp.where(low, block, row_blocks - 1 - block)

    def owned_block(turn):
        return mirrored(jnp.where(outer, (turn + 2) % 3, 3))

    def part_copy(block, place):
        return remote(acc.at[block], parts.at[place], send_r, recv_r.at[place], at(dim=mate))

    def merged_copy(merge):
        target, place = (far_inner, 5) if merge == 0 else (far_outer, 2 + merge)
        return remote(parts.at[merge], parts.at[place], send_r, recv_r.at[place], at(dim=target))

    def part_wait(place):
        await_recv(parts.at[place], recv_r.at[place])

    def res_copy(block, turn, hop):
        return remote(res.at[block], res.at[block], send_g.at[turn], recv_g, at(dim=(z + hop) % dims))

    def target_at(turn):
        return jnp.where(low, quarter_order(turn), dims - 1 - quarter_order(turn))

    def quarter_order(turn):
        first, second, third, fourth = (jnp.where(outer, one, two) for one, two in ((2, 1), (1, 0), (3, 2), (0, 3)))
        return jnp.where(turn == 0, first, jnp.where(turn == 1, second, jnp.where(turn == 2, third, fourth)))

    def block_at(turn):
        return (block_steps // 2 * x + turn) % block_steps

    barrier = pltpu.get_barrier_semaphore()
    peers = [at(shard=twin), at(shard=across), at(shard=far), at(rep=other_x)]
    beside = jnp.where(outer, 1, 2)

    def tell_line(semaphore):
        @pl.when(z < dims - 1)
        def _():
            pl.semaphore_signal(semaphore, inc=1, device_id=at(dim=(z + 1) % dims), device_id_type=MESH)

        @pl.when(z > 0)
        def _():
            pl.semaphore_signal(semaphore, inc=1, device_id=at(dim=(z + dims - 1) % dims), device_id_type=MESH)

    load_lists(0).start()
    tell_line(barrier)
    probes_in = pltpu.make_async_copy(probes_hbm, probes_ref, load_p)
    ids_in = pltpu.make_async_copy(ids_hbm, ids_ref, load_i)
    ids_in.start()
    probes_in.start()
    queries_in.start()
    for peer in peers:
        pl.semaphore_signal(barrier, inc=1, device_id=peer, device_id_type=MESH)
    load_lists(1).start()
    load_lists(2).start()

    row = lax.broadcasted_iota(jnp.int32, (STEP_ROWS, STEP_ROWS), 0)
    col = lax.broadcasted_iota(jnp.int32, (STEP_ROWS, STEP_ROWS), 1)
    source = (row // GROUP_ROWS) * GROUP_ROWS + (row % GROUP_LISTS) * LIST_LEN + (row // GROUP_LISTS) % LIST_LEN
    perm[...] = jnp.where(col == source, 1.0, 0.0).astype(jnp.bfloat16)

    def arrange(turn):
        block = block_at(turn)
        moved = jnp.dot(perm[...], raw[step_rows(block), :], preferred_element_type=jnp.float32)
        vecs[step_rows(block), :] = moved.astype(jnp.bfloat16)

    window = REUSE_Y // 2
    load_lists(0).wait()
    arrange(0)
    pl.semaphore_wait(barrier, len(peers) + beside)
    for chunk in range(window):
        y_copy(chunk).start()
    tell_line(met.at[0])
    acc[...] = jnp.zeros_like(acc)
    ids_in.wait()
    for which, peer in enumerate((twin, across, far)):
        id_copy(which, peer).start()
    ids_all[s] = ids_ref[...]
    probes_in.wait()
    queries_in.wait()

    tiles = block_width // LANES

    def name_candidates(number, carry):
        turn, tile = number // tiles, number % tiles
        cols = pl.ds(pl.multiple_of(owned_block(turn) * block_width + tile * LANES, LANES), LANES)
        probe = probes_ref[:, cols]
        lane, page = probe % LANES, probe // LANES
        pages = lists_dev // LANES
        for member in range(LIST_LEN):
            got = jnp.zeros((probe.shape[0], LANES), jnp.int32)
            for number in range(4 * pages):
                table = ids_all[number // pages, member:member + 1, (number % pages) * LANES:(number % pages + 1) * LANES]
                table = jnp.broadcast_to(table, (probe.shape[0], LANES))
                picked = jnp.take_along_axis(table, lane, axis=1, mode='promise_in_bounds')
                got = jnp.where(page == number, picked, got)
            cand_ids[turn, member, :, pl.ds(pl.multiple_of(tile * LANES, LANES), LANES)] = got.astype(jnp.float32)
        return carry

    def list_block(step):
        return block_at(step % block_steps)

    def score(step, heads, part):
        lists = vecs[step_rows(jnp.where(step < 2 * block_steps, step // block_steps * block_steps + list_block(step), step)), :]
        rows = pl.ds(pl.multiple_of(part * width, width), width)
        scores = lax.dot_general(lists, qv[rows, :], (((1,), (1,)), ((), ())), preferred_element_type=jnp.float32)
        for tile in range(width // LANES):
            probe = probes_ref[:, pl.ds(pl.multiple_of(part * width + tile * LANES, LANES), LANES)]
            low, head = probe % GROUP_LISTS, probe // GROUP_LISTS
            hits = [head == want for want in heads]
            lanes = slice(tile * LANES, (tile + 1) * LANES)
            half, place = divmod(tile * LANES, block_width)
            kept_lanes = slice(place, place + LANES)
            for member in range(LIST_LEN):
                kept = acc[2 * part + half, member, :, kept_lanes]
                for group, hit in enumerate(hits):
                    first = group * GROUP_ROWS + member * GROUP_LISTS
                    picked = jnp.take_along_axis(scores[first:first + GROUP_LISTS, lanes], low, axis=0, mode='promise_in_bounds')
                    kept = jnp.where(hit, picked, kept)
                acc[2 * part + half, member, :, kept_lanes] = kept

    def heads_at(step):
        local = step < 2 * block_steps
        group = step - 2 * block_steps
        base = block_groups * jnp.where(step < block_steps, s, twin) + STEP_GROUPS * list_block(step)
        heads = []
        for which in range(STEP_GROUPS):
            home = across if which < 2 else far
            side = x if which % 2 == 0 else other_x
            heads.append(jnp.where(local, base + which, block_groups * home + chunks // 2 * side + group))
        return heads

    last = 2 * block_steps + chunks // 2 - 1

    spare_copy = remote(piece(chunks // 2 * other_x + (chunks - 1) // 2, chunks - 1), slot(chunks - 1, 1),
                        send_x, recv_x.at[REUSE_X], at(shard=across))

    def pass_y(chunk):
        y_copy(chunk).wait_recv()
        if not (isinstance(chunk, int) and chunk == chunks - 1):
            x_copy(chunk).start()
        dy_copy(chunk).start()

        @pl.when(chunk + window < chunks)
        def _():
            y_copy(chunk + window).start()

        @pl.when(chunk + window == chunks)
        def _():
            spare_copy.start()

    def pass_x(chunk):
        if isinstance(chunk, int) and chunk == chunks - 1:
            spare_copy.wait_recv()
        else:
            x_copy(chunk).wait_recv()
        dx_copy(chunk).start()

    def await_step(step):
        await_recv(vecs.at[pl.ds(0, 4 * PIECE_ROWS)], recv_d.at[step - 2 * block_steps])

    def score_all(step):
        heads = heads_at(step)
        for part in range(dims):
            score(step, heads, part)

    def early(step, carry):
        own_copy(block_at(step)).start()

        @pl.when(step >= 1)
        def _():
            pass_y(step - 1)

        @pl.when(step >= 5)
        def _():
            pass_x(step - 5)

        @pl.when(step == 0)
        def _():
            load_lists(1).wait()

        @pl.when(step == block_steps // 2 - 1)
        def _():
            load_lists(2).wait()
        score_all(step)
        arrange(step + 1)
        return carry

    def middle(step, carry):
        pass_y(step - 1)
        pass_x(step - 5)

        @pl.when(step == block_steps - 1)
        def _():
            own_copy(block_at(step)).start()

        @pl.when((step == block_steps) | (step == block_steps + block_steps // 2))
        def _():
            await_recv(vecs.at[pl.ds(0, block_rows // 2)], recv_o.at[step // (block_steps // 2) - 2])

        @pl.when(step >= 2 * block_steps)
        def _():
            await_step(step)
        score_all(step)
        return carry

    late_plan = {
        last - 5: ('y25', 'x21', 'x22'),
        last - 4: ('y26', 'x23', 'y27', 'x24'),
        last - 3: ('y28', 'x25', 'names', 'y29', 'x26'),
        last - 2: ('y30', 'x27', 'y31', 'x28', 'x29'),
        last - 1: ('x31', 'x30'),
    }

    def late(step, carry):
        for when, plan in late_plan.items():
            @pl.when(step == when)
            def _(plan=plan):
                for word in plan:
                    if word == 'names':
                        await_recv(ids_all.at[pl.ds(0, 3)], recv_i)
                        lax.fori_loop(0, owned * tiles, name_candidates, 0)
                    else:
                        (pass_y if word[0] == 'y' else pass_x)(int(word[1:]))

        await_step(step)
        score_all(step)
        return carry

    lax.fori_loop(0, block_steps - 1, early, 0)
    lax.fori_loop(block_steps - 1, last - 5, middle, 0)
    pl.semaphore_wait(met.at[0], beside)
    tell_line(met.at[1])
    lax.fori_loop(last - 5, last, late, 0)
    pl.semaphore_wait(met.at[1], beside)
    await_step(jnp.int32(last))
    last_heads = heads_at(jnp.int32(last))

    leads, follows = outer & (s % 2 == 0), outer & (s % 2 == 1)
    outer_sends = ((4, 0), (5, 1), (3, 4), (7, 2), (6, 3))
    inner_sends = ((2, 0), (0, 1), (1, 2))

    def send_parts(plan):
        for block, place in plan:
            part_copy(mirrored(block), place).start()

    def finish(turn, carry):
        for when, some in ((1, outer_sends[:2]), (2, outer_sends[2:3]), (3, outer_sends[3:])):
            @pl.when(leads & (turn == when))
            def _(some=some):
                send_parts(some)
        for when, some in ((1, inner_sends[:1]), (2, inner_sends[1:])):
            @pl.when(jnp.logical_not(outer) & (turn == when))
            def _(some=some):
                send_parts(some)
        score(jnp.int32(last), last_heads, target_at(turn))
        return carry

    lax.fori_loop(0, dims, finish, 0)

    @pl.when(follows)
    def _():
        send_parts(outer_sends)

    @pl.when(jnp.logical_not(outer))
    def _():
        for merge, block in enumerate((4, 5, 7, 6)):
            part_wait(merge)
            parts[merge] += acc[mirrored(block)]
            merged_copy(merge).start()

    await_send(vecs.at[pl.ds(0, block_rows)], send_o)
    await_send(ids_all.at[pl.ds(0, 3)], send_i)
    await_send(vecs.at[pl.ds(0, chunks * PIECE_ROWS)], send_y)
    await_send(vecs.at[pl.ds(0, chunks * PIECE_ROWS)], send_x)
    await_send(vecs.at[pl.ds(0, 2 * chunks * PIECE_ROWS)], send_d)

    def choose(turn, carry):
        near, cross = jnp.where(outer, turn, 4), jnp.where(outer, 3 + turn, 5)
        part_wait(near)
        part_wait(cross)
        block = owned_block(turn)
        scores, names = [], []
        for member in range(LIST_LEN):
            total = acc[block, member] + parts[near, member] + parts[cross, member]
            name = cand_ids[turn, member]
            real = name >= 0.0
            scores.append(jnp.where(real, total, -jnp.inf))
            names.append(jnp.where(real, name, BIG))
        for place in range(TOP_K):
            best = functools.reduce(jnp.maximum, scores)
            best = jnp.max(best, axis=0, keepdims=True)
            tied = [jnp.where(score_j == best, name_j, BIG) for score_j, name_j in zip(scores, names)]
            first = jnp.min(functools.reduce(jnp.minimum, tied), axis=0, keepdims=True)
            for tile in range(tiles):
                lanes = slice(tile * LANES, (tile + 1) * LANES)
                line = place * tiles + tile
                res[block, line:line + 1, :] = best[:, lanes]
                res[block, TOP_K * tiles + line:TOP_K * tiles + line + 1, :] = first[:, lanes]
            if place + 1 < TOP_K:
                scores = [jnp.where(name_j == first, -jnp.inf, score_j) for score_j, name_j in zip(scores, names)]
        for hop in (2, 1, 3):
            res_copy(block, turn, hop).start()
        return carry

    lax.fori_loop(0, owned, choose, 0)

    def drain(turn, carry):
        await_send(res.at[pl.ds(0, dims - 1)], send_g.at[turn])
        return carry

    lax.fori_loop(0, owned, drain, 0)

    @pl.when(outer)
    def _():
        await_send(acc.at[pl.ds(0, 5)], send_r)
        await_recv(res.at[pl.ds(0, 5)], recv_g)

    @pl.when(jnp.logical_not(outer))
    def _():
        await_send(acc.at[pl.ds(0, 7)], send_r)
        await_recv(res.at[pl.ds(0, 7)], recv_g)


def place_kernel(res, out_s, out_i):
    blocks, lines, _ = res.shape
    tiles = lines // (2 * TOP_K)
    for block in range(blocks):
        for tile in range(tiles):
            first = (block * tiles + tile) * LANES
            out_s[:, first:first + LANES] = res[block, pl.ds(tile, TOP_K, stride=tiles), :]
            out_i[:, first:first + LANES] = res[block, pl.ds(TOP_K * tiles + tile, TOP_K, stride=tiles), :].astype(jnp.int32)


def solution(mesh):
    dims = mesh.shape['dim']
    row_spec = P(('rep', 'shard'), None)

    def local_search(queries, list_vecs, list_ids, probes):
        rows_q, depth = queries.shape
        lists_dev, list_len, _ = list_vecs.shape
        probe_count = probes.shape[1]
        block_rows = lists_dev * list_len
        block_steps = block_rows // STEP_ROWS
        chunks = lists_dev // GROUP_LISTS
        width = rows_q // dims
        dma = pltpu.SemaphoreType.DMA
        any_spec = pl.BlockSpec(memory_space=pl.ANY)
        vmem_spec = pl.BlockSpec(memory_space=pltpu.VMEM)
        found = pl.pallas_call(
            functools.partial(search_kernel, dims),
            out_shape=pltpu.VMEM((2 * dims, TOP_K * width // LANES, LANES), jnp.float32),
            in_specs=[any_spec] * 4,
            out_specs=vmem_spec,
            scratch_shapes=[
                pltpu.VMEM((block_rows, depth), jnp.bfloat16),
                pltpu.VMEM((rows_q, depth), jnp.bfloat16),
                pltpu.VMEM((4 * block_rows, depth), jnp.bfloat16),
                pltpu.VMEM((STEP_ROWS, STEP_ROWS), jnp.bfloat16),
                pltpu.VMEM((2 * dims, LIST_LEN, probe_count, width // 2), jnp.float32),
                pltpu.VMEM((6, LIST_LEN, probe_count, width // 2), jnp.float32),
                pltpu.VMEM((4, LIST_LEN, lists_dev), jnp.int32),
                pltpu.VMEM((3, LIST_LEN, probe_count, width // 2), jnp.float32),
                pltpu.VMEM((probe_count, rows_q), jnp.int32),
                pltpu.VMEM((LIST_LEN, lists_dev), jnp.int32),
                dma, dma,
                dma((3,)), dma,
                dma, dma((2,)),
                dma, dma((REUSE_Y,)), dma, dma((REUSE_X + 1,)),
                dma, dma((chunks // 2,)),
                dma, dma, dma, dma((6,)), dma((3,)), dma,
                pltpu.SemaphoreType.REGULAR((2,)),
            ],
            compiler_params=pltpu.CompilerParams(collective_id=0, has_side_effects=True, vmem_limit_bytes=60 * 2**20),
            name='ivf_search',
        )(queries, list_vecs.reshape(block_rows, depth), probes.T, list_ids.T)
        scores, ids = pl.pallas_call(
            place_kernel,
            out_shape=(jax.ShapeDtypeStruct((TOP_K, rows_q), jnp.float32),
                       jax.ShapeDtypeStruct((TOP_K, rows_q), jnp.int32)),
            in_specs=[vmem_spec],
            out_specs=(vmem_spec, vmem_spec),
            compiler_params=pltpu.CompilerParams(vmem_limit_bytes=4 * 2**20),
            name='place',
        )(found)
        return scores.T, ids.T

    return jax.shard_map(local_search, mesh=mesh,
                         in_specs=(P(('rep', 'shard'), 'dim'), P('shard', None, 'dim'), P('shard', None), row_spec),
                         out_specs=(row_spec, row_spec), check_vma=False)
```

```python
import functools

import jax
import jax.numpy as jnp
from jax import lax
from jax.experimental import pallas as pl
from jax.experimental.pallas import tpu as pltpu
from jax.sharding import PartitionSpec as P

TOP_K = 10
LIST_LEN = 8
GROUP_LISTS = 8
GROUP_ROWS = GROUP_LISTS * LIST_LEN
STEP_GROUPS = 4
STEP_ROWS = STEP_GROUPS * GROUP_ROWS
PIECE_ROWS = GROUP_ROWS // 2
LANES = 128
REUSE_Y, REUSE_X = 8, 12
MESH = pl.DeviceIdType.MESH
BIG = 1e9


def flip(index, bit):
    return index + bit - 2 * bit * ((index // bit) % 2)


def search_kernel(dims, q_hbm, l_hbm, probes_hbm, ids_hbm, res, kept_hbm,
                  raw, qv, vecs, perm, acc, parts, ids_all, cand_ids, probes_ref, ids_ref, load_p, load_i, keep_sem,
                  load_l, load_q, send_o, recv_o, send_y, recv_y, send_x, recv_x,
                  send_d, recv_d, send_i, recv_i, send_r, recv_r, send_g, recv_g, met):
    rows_q = qv.shape[0]
    lists_dev = ids_ref.shape[1]
    block_rows = lists_dev * LIST_LEN
    block_groups = lists_dev // GROUP_LISTS
    chunks = block_groups
    block_steps = block_groups // STEP_GROUPS
    width = rows_q // dims
    x, z, s = lax.axis_index('rep'), lax.axis_index('dim'), lax.axis_index('shard')
    twin, across, far = flip(s, 1), flip(s, 2), flip(flip(s, 1), 2)
    other_x = 1 - x

    def at(**place):
        return {'rep': x, 'dim': z, 'shard': s, **place}

    def step_rows(step):
        return pl.ds(pl.multiple_of(step * STEP_ROWS, STEP_ROWS), STEP_ROWS)

    def remote(src, dst, send, recv, device):
        return pltpu.make_async_remote_copy(src_ref=src, dst_ref=dst, send_sem=send, recv_sem=recv,
                                            device_id=device, device_id_type=MESH)

    def await_recv(buffer, semaphore):
        remote(buffer, buffer, send_i, semaphore, at()).wait_recv()

    def await_send(buffer, semaphore):
        remote(buffer, buffer, semaphore, recv_i, at()).wait_send()

    def load_lists(number):
        half = block_steps // 2
        first, count = ((half * x, 1), (half * x + 1, half - 1), (half * other_x, half))[number]
        rows = pl.ds(pl.multiple_of(first * STEP_ROWS, STEP_ROWS), count * STEP_ROWS)
        return pltpu.make_async_copy(l_hbm.at[rows], raw.at[rows], load_l.at[number])

    queries_in = pltpu.make_async_copy(q_hbm, qv, load_q)

    def own_copy(block):
        return remote(vecs.at[step_rows(block)], vecs.at[step_rows(block_steps + block)],
                      send_o, recv_o.at[(block // (block_steps // 2) + x) % 2], at(shard=twin))

    def piece(group, chunk):
        first = pl.multiple_of(group * GROUP_ROWS + chunk % 2 * PIECE_ROWS, PIECE_ROWS)
        return vecs.at[pl.ds(first, PIECE_ROWS)]

    def slot(chunk, which):
        return piece(2 * block_groups + STEP_GROUPS * (chunk // 2) + which, chunk)

    early_chunks = STEP_ROWS // PIECE_ROWS

    def y_copy(chunk, source=None):
        source = piece(chunks // 2 * x + chunk // 2, chunk) if source is None else source
        return remote(source, slot(chunk, 0), send_y, recv_y.at[chunk % REUSE_Y], at(shard=across))

    def y_send(chunk):
        @pl.when(chunk < early_chunks)
        def _():
            y_copy(chunk).start()

        @pl.when((chunk >= early_chunks) & (chunk < chunks))
        def _():
            y_copy(chunk, kept_hbm.at[pl.ds(pl.multiple_of(chunk * PIECE_ROWS, PIECE_ROWS), PIECE_ROWS)]).start()

    def keep(turn):
        rows = pl.ds(pl.multiple_of(turn * STEP_ROWS, STEP_ROWS), STEP_ROWS)
        return pltpu.make_async_copy(vecs.at[step_rows(block_at(turn))], kept_hbm.at[rows], keep_sem)

    def x_copy(chunk):
        return remote(slot(chunk, 0), slot(chunk, 1), send_x, recv_x.at[chunk % REUSE_X], at(rep=other_x))

    def whole(group, which):
        return vecs.at[pl.ds(pl.multiple_of((2 * block_groups + STEP_GROUPS * group + which) * GROUP_ROWS, GROUP_ROWS), GROUP_ROWS)]

    def twin_copy(group, which):
        return remote(whole(group, which), whole(group, which + 2), send_d, recv_d.at[group], at(shard=twin))

    def twin_piece(chunk, which):
        return remote(slot(chunk, which), slot(chunk, which + 2), send_d, recv_d.at[chunk // 2], at(shard=twin))

    def pair_up(chunk, which):
        if isinstance(chunk, int):
            if which == 1 and chunk // 2 == chunks // 2 - 1:
                twin_piece(chunk, which).start()
            elif chunk % 2 == 1:
                twin_copy(chunk // 2, which).start()
        else:
            @pl.when(chunk % 2 == 1)
            def _():
                twin_copy(chunk // 2, which).start()

    def id_copy(which, peer):
        return remote(ids_ref, ids_all.at[s], send_i, recv_i, at(shard=peer))

    outer = z % 3 == 0
    mate, far_outer = flip(z, 1), jnp.where(z < 2, dims - 1, 0)
    far_inner = flip(far_outer, 1)

    def part_copy(target, place, half):
        return remote(acc.at[target, half], parts.at[place, half], send_r, recv_r.at[place, half], at(dim=mate))

    def merged_copy(merge, half):
        return remote(parts.at[merge, half], parts.at[3, half], send_r, recv_r.at[3, half],
                      at(dim=(far_outer, far_inner)[merge]))

    def part_wait(place, half):
        await_recv(parts.at[place, half], recv_r.at[place, half])

    def res_copy(target, half):
        return remote(res.at[z, half], res.at[z, half], send_g, recv_g, at(dim=target))

    def target_at(turn):
        first, second, third = (jnp.where(outer, one, two) for one, two in ((far_outer, mate), (far_inner, far_outer), (mate, far_inner)))
        return jnp.where(turn == 0, first, jnp.where(turn == 1, second, jnp.where(turn == 2, third, z)))

    def block_at(turn):
        return (block_steps // 2 * x + turn) % block_steps

    barrier = pltpu.get_barrier_semaphore()
    peers = [at(shard=twin), at(shard=across), at(shard=far), at(rep=other_x)]
    beside = jnp.where(outer, 1, 2)

    def tell_line(semaphore):
        @pl.when(z < dims - 1)
        def _():
            pl.semaphore_signal(semaphore, inc=1, device_id=at(dim=(z + 1) % dims), device_id_type=MESH)

        @pl.when(z > 0)
        def _():
            pl.semaphore_signal(semaphore, inc=1, device_id=at(dim=(z + dims - 1) % dims), device_id_type=MESH)

    load_lists(0).start()
    tell_line(barrier)
    probes_in = pltpu.make_async_copy(probes_hbm, probes_ref, load_p)
    ids_in = pltpu.make_async_copy(ids_hbm, ids_ref, load_i)
    ids_in.start()
    probes_in.start()
    queries_in.start()
    for peer in peers:
        pl.semaphore_signal(barrier, inc=1, device_id=peer, device_id_type=MESH)
    load_lists(1).start()
    load_lists(2).start()

    row = lax.broadcasted_iota(jnp.int32, (STEP_ROWS, STEP_ROWS), 0)
    col = lax.broadcasted_iota(jnp.int32, (STEP_ROWS, STEP_ROWS), 1)
    source = (row // GROUP_ROWS) * GROUP_ROWS + (row % GROUP_LISTS) * LIST_LEN + (row // GROUP_LISTS) % LIST_LEN
    perm[...] = jnp.where(col == source, 1.0, 0.0).astype(jnp.bfloat16)

    def arrange(turn):
        block = block_at(turn)
        moved = jnp.dot(perm[...], raw[step_rows(block), :], preferred_element_type=jnp.float32)
        vecs[step_rows(block), :] = moved.astype(jnp.bfloat16)

    window = REUSE_Y // 2
    load_lists(0).wait()
    arrange(0)
    pl.semaphore_wait(barrier, len(peers) + beside)
    for chunk in range(window):
        y_copy(chunk).start()
    tell_line(met.at[0])
    acc[...] = jnp.zeros_like(acc)
    ids_in.wait()
    for which, peer in enumerate((twin, across, far)):
        id_copy(which, peer).start()
    ids_all[s] = ids_ref[...]
    probes_in.wait()
    queries_in.wait()

    def name_candidates(tile, carry):
        cols = pl.ds(pl.multiple_of(z * width + tile * LANES, LANES), LANES)
        probe = probes_ref[:, cols]
        lane, page = probe % LANES, probe // LANES
        pages = lists_dev // LANES
        for member in range(LIST_LEN):
            got = jnp.zeros((probe.shape[0], LANES), jnp.int32)
            for number in range(4 * pages):
                table = ids_all[number // pages, member:member + 1, (number % pages) * LANES:(number % pages + 1) * LANES]
                table = jnp.broadcast_to(table, (probe.shape[0], LANES))
                picked = jnp.take_along_axis(table, lane, axis=1, mode='promise_in_bounds')
                got = jnp.where(page == number, picked, got)
            tiles_half = width // 2 // LANES
            place = pl.ds(pl.multiple_of(tile % tiles_half * LANES, LANES), LANES)
            cand_ids[tile // tiles_half, member, :, place] = got.astype(jnp.float32)
        return carry

    def list_block(step):
        return block_at(step % block_steps)

    def score(step, heads, part):
        lists = vecs[step_rows(jnp.where(step < 2 * block_steps, step // block_steps * block_steps + list_block(step), step)), :]
        rows = pl.ds(pl.multiple_of(part * width, width), width)
        scores = lax.dot_general(lists, qv[rows, :], (((1,), (1,)), ((), ())), preferred_element_type=jnp.float32)
        for tile in range(width // LANES):
            probe = probes_ref[:, pl.ds(pl.multiple_of(part * width + tile * LANES, LANES), LANES)]
            low, head = probe % GROUP_LISTS, probe // GROUP_LISTS
            hits = [head == want for want in heads]
            lanes = slice(tile * LANES, (tile + 1) * LANES)
            half, place = divmod(tile * LANES, width // 2)
            kept_lanes = slice(place, place + LANES)
            for member in range(LIST_LEN):
                kept = acc[part, half, member, :, kept_lanes]
                for group, hit in enumerate(hits):
                    first = group * GROUP_ROWS + member * GROUP_LISTS
                    picked = jnp.take_along_axis(scores[first:first + GROUP_LISTS, lanes], low, axis=0, mode='promise_in_bounds')
                    kept = jnp.where(hit, picked, kept)
                acc[part, half, member, :, kept_lanes] = kept

    def heads_at(step):
        local = step < 2 * block_steps
        group = step - 2 * block_steps
        base = block_groups * jnp.where(step < block_steps, s, twin) + STEP_GROUPS * list_block(step)
        heads = []
        for which in range(STEP_GROUPS):
            home = across if which < 2 else far
            side = x if which % 2 == 0 else other_x
            heads.append(jnp.where(local, base + which, block_groups * home + chunks // 2 * side + group))
        return heads

    last = 2 * block_steps + chunks // 2 - 1

    spare_copy = remote(piece(chunks // 2 * other_x + (chunks - 1) // 2, chunks - 1), slot(chunks - 1, 1),
                        send_x, recv_x.at[REUSE_X], at(shard=across))

    def pass_y(chunk):
        y_copy(chunk).wait_recv()
        if not (isinstance(chunk, int) and chunk == chunks - 1):
            x_copy(chunk).start()
        pair_up(chunk, 0)
        y_send(chunk + window)

        @pl.when(chunk + window == chunks)
        def _():
            spare_copy.start()

    def pass_x(chunk):
        if isinstance(chunk, int) and chunk == chunks - 1:
            spare_copy.wait_recv()
        else:
            x_copy(chunk).wait_recv()
        pair_up(chunk, 1)

    def await_step(step):
        await_recv(vecs.at[pl.ds(0, 4 * PIECE_ROWS)], recv_d.at[step - 2 * block_steps])

    def score_all(step):
        heads = heads_at(step)
        for part in range(dims):
            score(step, heads, part)

    def early(step, carry):
        own_copy(block_at(step)).start()
        half = block_steps // 2

        @pl.when((step >= 2) & (step <= half))
        def _():
            keep(step - 1).wait()

        @pl.when((step >= 1) & (step < half))
        def _():
            keep(step).start()

        @pl.when(step >= 1)
        def _():
            pass_y(step - 1)

        @pl.when(step >= 5)
        def _():
            pass_x(step - 5)

        @pl.when(step == 0)
        def _():
            load_lists(1).wait()

        @pl.when(step == block_steps // 2 - 1)
        def _():
            load_lists(2).wait()
        score_all(step)
        arrange(step + 1)
        return carry

    def middle(step, carry):
        pass_y(step - 1)
        pass_x(step - 5)

        @pl.when(step == block_steps - 1)
        def _():
            own_copy(block_at(step)).start()

        @pl.when((step == block_steps) | (step == block_steps + block_steps // 2))
        def _():
            await_recv(vecs.at[pl.ds(0, block_rows // 2)], recv_o.at[step // (block_steps // 2) - 2])

        @pl.when(step >= 2 * block_steps)
        def _():
            await_step(step)
        score_all(step)
        return carry

    late_plan = {
        last - 5: ('y25', 'x21', 'x22'),
        last - 4: ('y26', 'x23', 'y27', 'x24'),
        last - 3: ('y28', 'x25', 'names', 'y29', 'x26'),
        last - 2: ('y30', 'x27', 'y31', 'x28', 'x29'),
        last - 1: ('x31', 'x30'),
    }

    def late(step, carry):
        for when, plan in late_plan.items():
            @pl.when(step == when)
            def _(plan=plan):
                for word in plan:
                    if word == 'names':
                        await_recv(ids_all.at[pl.ds(0, 3)], recv_i)
                        lax.fori_loop(0, width // LANES, name_candidates, 0)
                    else:
                        (pass_y if word[0] == 'y' else pass_x)(int(word[1:]))

        await_step(step)
        score_all(step)
        return carry

    lax.fori_loop(0, block_steps - 1, early, 0)
    lax.fori_loop(block_steps - 1, last - 5, middle, 0)
    pl.semaphore_wait(met.at[0], beside)
    tell_line(met.at[1])
    lax.fori_loop(last - 5, last, late, 0)
    pl.semaphore_wait(met.at[1], beside)
    await_step(jnp.int32(last))
    last_heads = heads_at(jnp.int32(last))

    leads, follows = outer & (s % 2 == 0), outer & (s % 2 == 1)

    def finish(turn, carry):
        @pl.when(leads & (turn == 1))
        def _():
            part_copy(far_outer, 0, 0).start()

        @pl.when(leads & (turn == 2))
        def _():
            part_copy(far_inner, 1, 0).start()
            part_copy(far_outer, 0, 1).start()
            part_copy(far_inner, 1, 1).start()

        @pl.when((leads & (turn == 3)) | (jnp.logical_not(outer) & (turn == 1)))
        def _():
            for half in range(2):
                part_copy(mate, 2, half).start()
        score(jnp.int32(last), last_heads, target_at(turn))
        return carry

    lax.fori_loop(0, dims, finish, 0)

    @pl.when(follows)
    def _():
        for half in range(2):
            part_copy(far_outer, 0, half).start()
            part_copy(far_inner, 1, half).start()
        for half in range(2):
            part_copy(mate, 2, half).start()

    @pl.when(jnp.logical_not(outer))
    def _():
        for half in range(2):
            for merge, target in enumerate((far_outer, far_inner)):
                part_wait(merge, half)
                parts[merge, half] += acc[target, half]
                merged_copy(merge, half).start()

    tiles = width // 2 // LANES
    for half in range(2):
        part_wait(2, half)
        part_wait(3, half)
        scores, names = [], []
        for member in range(LIST_LEN):
            total = acc[z, half, member] + parts[2, half, member] + parts[3, half, member]
            name = cand_ids[half, member]
            real = name >= 0.0
            scores.append(jnp.where(real, total, -jnp.inf))
            names.append(jnp.where(real, name, BIG))
        for place in range(TOP_K):
            best = functools.reduce(jnp.maximum, scores)
            best = jnp.max(best, axis=0, keepdims=True)
            tied = [jnp.where(score_j == best, name_j, BIG) for score_j, name_j in zip(scores, names)]
            first = jnp.min(functools.reduce(jnp.minimum, tied), axis=0, keepdims=True)
            for tile in range(tiles):
                lanes = slice(tile * LANES, (tile + 1) * LANES)
                line = place * tiles + tile
                res[z, half, line:line + 1, :] = best[:, lanes]
                res[z, half, TOP_K * tiles + line:TOP_K * tiles + line + 1, :] = first[:, lanes]
            if place + 1 < TOP_K:
                scores = [jnp.where(name_j == first, -jnp.inf, score_j) for score_j, name_j in zip(scores, names)]
        if half == 0:
            await_send(vecs.at[pl.ds(0, block_rows)], send_o)
            await_send(ids_all.at[pl.ds(0, 3)], send_i)
        else:
            await_send(vecs.at[pl.ds(0, chunks * PIECE_ROWS)], send_y)
            await_send(vecs.at[pl.ds(0, chunks * PIECE_ROWS)], send_x)
            await_send(vecs.at[pl.ds(0, 2 * chunks * PIECE_ROWS)], send_d)
        for which in range(dims - 1):
            res_copy(target_at(which), half).start()

    await_send(parts.at[pl.ds(0, 3)], send_r)
    await_send(res.at[pl.ds(0, dims - 1)], send_g)
    await_recv(res.at[pl.ds(0, dims - 1)], recv_g)


def place_kernel(res, out_s, out_i):
    dims, halves, lines, _ = res.shape
    tiles = lines // (2 * TOP_K)
    for part in range(dims):
        for half in range(halves):
            for tile in range(tiles):
                first = ((part * halves + half) * tiles + tile) * LANES
                out_s[:, first:first + LANES] = res[part, half, pl.ds(tile, TOP_K, stride=tiles), :]
                out_i[:, first:first + LANES] = res[part, half, pl.ds(TOP_K * tiles + tile, TOP_K, stride=tiles), :].astype(jnp.int32)


def solution(mesh):
    dims = mesh.shape['dim']
    row_spec = P(('rep', 'shard'), None)

    def local_search(queries, list_vecs, list_ids, probes):
        rows_q, depth = queries.shape
        lists_dev, list_len, _ = list_vecs.shape
        probe_count = probes.shape[1]
        block_rows = lists_dev * list_len
        block_steps = block_rows // STEP_ROWS
        chunks = lists_dev // GROUP_LISTS
        width = rows_q // dims
        dma = pltpu.SemaphoreType.DMA
        any_spec = pl.BlockSpec(memory_space=pl.ANY)
        vmem_spec = pl.BlockSpec(memory_space=pltpu.VMEM)
        found, _ = pl.pallas_call(
            functools.partial(search_kernel, dims),
            out_shape=(pltpu.VMEM((dims, 2, TOP_K * width // LANES, LANES), jnp.float32),
                       jax.ShapeDtypeStruct((block_rows // 2, depth), jnp.bfloat16)),
            in_specs=[any_spec] * 4,
            out_specs=(vmem_spec, any_spec),
            scratch_shapes=[
                pltpu.VMEM((block_rows, depth), jnp.bfloat16),
                pltpu.VMEM((rows_q, depth), jnp.bfloat16),
                pltpu.VMEM((4 * block_rows, depth), jnp.bfloat16),
                pltpu.VMEM((STEP_ROWS, STEP_ROWS), jnp.bfloat16),
                pltpu.VMEM((dims, 2, LIST_LEN, probe_count, width // 2), jnp.float32),
                pltpu.VMEM((4, 2, LIST_LEN, probe_count, width // 2), jnp.float32),
                pltpu.VMEM((4, LIST_LEN, lists_dev), jnp.int32),
                pltpu.VMEM((2, LIST_LEN, probe_count, width // 2), jnp.float32),
                pltpu.VMEM((probe_count, rows_q), jnp.int32),
                pltpu.VMEM((LIST_LEN, lists_dev), jnp.int32),
                dma, dma, dma,
                dma((3,)), dma,
                dma, dma((2,)),
                dma, dma((REUSE_Y,)), dma, dma((REUSE_X + 1,)),
                dma, dma((chunks // 2,)),
                dma, dma, dma, dma((4, 2)), dma, dma,
                pltpu.SemaphoreType.REGULAR((2,)),
            ],
            compiler_params=pltpu.CompilerParams(collective_id=0, has_side_effects=True, vmem_limit_bytes=60 * 2**20),
            name='ivf_search',
        )(queries, list_vecs.reshape(block_rows, depth), probes.T, list_ids.T)
        scores, ids = pl.pallas_call(
            place_kernel,
            out_shape=(jax.ShapeDtypeStruct((TOP_K, rows_q), jnp.float32),
                       jax.ShapeDtypeStruct((TOP_K, rows_q), jnp.int32)),
            in_specs=[vmem_spec],
            out_specs=(vmem_spec, vmem_spec),
            compiler_params=pltpu.CompilerParams(vmem_limit_bytes=4 * 2**20),
            name='place',
        )(found)
        return scores.T, ids.T

    return jax.shard_map(local_search, mesh=mesh,
                         in_specs=(P(('rep', 'shard'), 'dim'), P('shard', None, 'dim'), P('shard', None), row_spec),
                         out_specs=(row_spec, row_spec), check_vma=False)
```

```python
import functools

import jax
import jax.numpy as jnp
from jax import lax
from jax.experimental import pallas as pl
from jax.experimental.pallas import tpu as pltpu
from jax.sharding import PartitionSpec as P

TOP_K = 10
LIST_LEN = 8
GROUP_LISTS = 8
GROUP_ROWS = GROUP_LISTS * LIST_LEN
STEP_GROUPS = 4
STEP_ROWS = STEP_GROUPS * GROUP_ROWS
PIECE_ROWS = GROUP_ROWS // 2
LANES = 128
REUSE_Y, REUSE_X = 8, 12
MESH = pl.DeviceIdType.MESH
BIG = 1e9


def flip(index, bit):
    return index + bit - 2 * bit * ((index // bit) % 2)


def search_kernel(dims, q_hbm, l_hbm, probes_hbm, ids_hbm, res,
                  raw, qv, vecs, perm, acc, parts, ids_all, cand_ids, probes_ref, ids_ref, load_p, load_i,
                  load_l, load_q, send_o, recv_o, send_y, recv_y, send_x, recv_x,
                  send_d, recv_d, send_i, recv_i, send_r, recv_r, send_g, recv_g, met):
    rows_q = qv.shape[0]
    lists_dev = ids_ref.shape[1]
    block_rows = lists_dev * LIST_LEN
    block_groups = lists_dev // GROUP_LISTS
    chunks = block_groups
    block_steps = block_groups // STEP_GROUPS
    width = rows_q // dims
    x, z, s = lax.axis_index('rep'), lax.axis_index('dim'), lax.axis_index('shard')
    twin, across, far = flip(s, 1), flip(s, 2), flip(flip(s, 1), 2)
    other_x = 1 - x

    def at(**place):
        return {'rep': x, 'dim': z, 'shard': s, **place}

    def step_rows(step):
        return pl.ds(pl.multiple_of(step * STEP_ROWS, STEP_ROWS), STEP_ROWS)

    def remote(src, dst, send, recv, device):
        return pltpu.make_async_remote_copy(src_ref=src, dst_ref=dst, send_sem=send, recv_sem=recv,
                                            device_id=device, device_id_type=MESH)

    def await_recv(buffer, semaphore):
        remote(buffer, buffer, send_i, semaphore, at()).wait_recv()

    def await_send(buffer, semaphore):
        remote(buffer, buffer, semaphore, recv_i, at()).wait_send()

    def load_lists(number):
        half = block_steps // 2
        first, count = ((half * x, 1), (half * x + 1, half - 1), (half * other_x, half))[number]
        rows = pl.ds(pl.multiple_of(first * STEP_ROWS, STEP_ROWS), count * STEP_ROWS)
        return pltpu.make_async_copy(l_hbm.at[rows], raw.at[rows], load_l.at[number])

    queries_in = pltpu.make_async_copy(q_hbm, qv, load_q)

    def own_copy(block):
        return remote(vecs.at[step_rows(block)], vecs.at[step_rows(block_steps + block)],
                      send_o, recv_o.at[(block // (block_steps // 2) + x) % 2], at(shard=twin))

    def piece(group, chunk):
        first = pl.multiple_of(group * GROUP_ROWS + chunk % 2 * PIECE_ROWS, PIECE_ROWS)
        return vecs.at[pl.ds(first, PIECE_ROWS)]

    def slot(chunk, which):
        return piece(2 * block_groups + STEP_GROUPS * (chunk // 2) + which, chunk)

    def y_copy(chunk):
        return remote(piece(chunks // 2 * x + chunk // 2, chunk), slot(chunk, 0), send_y, recv_y.at[chunk % REUSE_Y], at(shard=across))

    def x_copy(chunk):
        return remote(slot(chunk, 0), slot(chunk, 1), send_x, recv_x.at[chunk % REUSE_X], at(rep=other_x))

    def whole(group, which):
        return vecs.at[pl.ds(pl.multiple_of((2 * block_groups + STEP_GROUPS * group + which) * GROUP_ROWS, GROUP_ROWS), GROUP_ROWS)]

    def twin_copy(group, which):
        return remote(whole(group, which), whole(group, which + 2), send_d, recv_d.at[group], at(shard=twin))

    def twin_piece(chunk, which):
        return remote(slot(chunk, which), slot(chunk, which + 2), send_d, recv_d.at[chunk // 2], at(shard=twin))

    def pair_up(chunk, which):
        if isinstance(chunk, int):
            if which == 1 and chunk // 2 == chunks // 2 - 1:
                twin_piece(chunk, which).start()
            elif chunk % 2 == 1:
                twin_copy(chunk // 2, which).start()
        else:
            @pl.when(chunk % 2 == 1)
            def _():
                twin_copy(chunk // 2, which).start()

    def id_copy(which, peer):
        return remote(ids_ref, ids_all.at[s], send_i, recv_i, at(shard=peer))

    outer = z % 3 == 0
    mate, far_outer = flip(z, 1), jnp.where(z < 2, dims - 1, 0)
    far_inner = flip(far_outer, 1)

    def part_copy(target, place, half):
        return remote(acc.at[target, half], parts.at[place, half], send_r, recv_r.at[place, half], at(dim=mate))

    def merged_copy(merge, half):
        return remote(parts.at[merge, half], parts.at[3, half], send_r, recv_r.at[3, half],
                      at(dim=(far_outer, far_inner)[merge]))

    def part_wait(place, half):
        await_recv(parts.at[place, half], recv_r.at[place, half])

    def res_copy(target, half):
        return remote(res.at[z, half], res.at[z, half], send_g, recv_g, at(dim=target))

    def target_at(turn):
        first, second, third = (jnp.where(outer, one, two) for one, two in ((far_outer, mate), (far_inner, far_outer), (mate, far_inner)))
        return jnp.where(turn == 0, first, jnp.where(turn == 1, second, jnp.where(turn == 2, third, z)))

    def block_at(turn):
        return (block_steps // 2 * x + turn) % block_steps

    barrier = pltpu.get_barrier_semaphore()
    peers = [at(shard=twin), at(shard=across), at(shard=far), at(rep=other_x)]
    beside = jnp.where(outer, 1, 2)

    def tell_line(semaphore):
        @pl.when(z < dims - 1)
        def _():
            pl.semaphore_signal(semaphore, inc=1, device_id=at(dim=(z + 1) % dims), device_id_type=MESH)

        @pl.when(z > 0)
        def _():
            pl.semaphore_signal(semaphore, inc=1, device_id=at(dim=(z + dims - 1) % dims), device_id_type=MESH)

    load_lists(0).start()
    tell_line(barrier)
    probes_in = pltpu.make_async_copy(probes_hbm, probes_ref, load_p)
    ids_in = pltpu.make_async_copy(ids_hbm, ids_ref, load_i)
    ids_in.start()
    probes_in.start()
    queries_in.start()
    for peer in peers:
        pl.semaphore_signal(barrier, inc=1, device_id=peer, device_id_type=MESH)
    load_lists(1).start()
    load_lists(2).start()

    row = lax.broadcasted_iota(jnp.int32, (STEP_ROWS, STEP_ROWS), 0)
    col = lax.broadcasted_iota(jnp.int32, (STEP_ROWS, STEP_ROWS), 1)
    source = (row // GROUP_ROWS) * GROUP_ROWS + (row % GROUP_LISTS) * LIST_LEN + (row // GROUP_LISTS) % LIST_LEN
    perm[...] = jnp.where(col == source, 1.0, 0.0).astype(jnp.bfloat16)

    def arrange(turn):
        block = block_at(turn)
        moved = jnp.dot(perm[...], raw[step_rows(block), :], preferred_element_type=jnp.float32)
        vecs[step_rows(block), :] = moved.astype(jnp.bfloat16)

    window = REUSE_Y // 2
    load_lists(0).wait()
    arrange(0)
    pl.semaphore_wait(barrier, len(peers) + beside)
    for chunk in range(window):
        y_copy(chunk).start()
    tell_line(met.at[0])
    acc[...] = jnp.zeros_like(acc)
    ids_in.wait()
    for which, peer in enumerate((twin, across, far)):
        id_copy(which, peer).start()
    ids_all[s] = ids_ref[...]
    probes_in.wait()
    queries_in.wait()

    def name_candidates(tile, carry):
        cols = pl.ds(pl.multiple_of(z * width + tile * LANES, LANES), LANES)
        probe = probes_ref[:, cols]
        lane, page = probe % LANES, probe // LANES
        pages = lists_dev // LANES
        for member in range(LIST_LEN):
            got = jnp.zeros((probe.shape[0], LANES), jnp.int32)
            for number in range(4 * pages):
                table = ids_all[number // pages, member:member + 1, (number % pages) * LANES:(number % pages + 1) * LANES]
                table = jnp.broadcast_to(table, (probe.shape[0], LANES))
                picked = jnp.take_along_axis(table, lane, axis=1, mode='promise_in_bounds')
                got = jnp.where(page == number, picked, got)
            tiles_half = width // 2 // LANES
            place = pl.ds(pl.multiple_of(tile % tiles_half * LANES, LANES), LANES)
            cand_ids[tile // tiles_half, member, :, place] = got.astype(jnp.float32)
        return carry

    def list_block(step):
        return block_at(step % block_steps)

    def score(step, heads, part):
        lists = vecs[step_rows(jnp.where(step < 2 * block_steps, step // block_steps * block_steps + list_block(step), step)), :]
        rows = pl.ds(pl.multiple_of(part * width, width), width)
        scores = lax.dot_general(lists, qv[rows, :], (((1,), (1,)), ((), ())), preferred_element_type=jnp.float32)
        for tile in range(width // LANES):
            probe = probes_ref[:, pl.ds(pl.multiple_of(part * width + tile * LANES, LANES), LANES)]
            low, head = probe % GROUP_LISTS, probe // GROUP_LISTS
            hits = [head == want for want in heads]
            lanes = slice(tile * LANES, (tile + 1) * LANES)
            half, place = divmod(tile * LANES, width // 2)
            kept_lanes = slice(place, place + LANES)
            for member in range(LIST_LEN):
                kept = acc[part, half, member, :, kept_lanes]
                for group, hit in enumerate(hits):
                    first = group * GROUP_ROWS + member * GROUP_LISTS
                    picked = jnp.take_along_axis(scores[first:first + GROUP_LISTS, lanes], low, axis=0, mode='promise_in_bounds')
                    kept = jnp.where(hit, picked, kept)
                acc[part, half, member, :, kept_lanes] = kept

    def heads_at(step):
        local = step < 2 * block_steps
        group = step - 2 * block_steps
        base = block_groups * jnp.where(step < block_steps, s, twin) + STEP_GROUPS * list_block(step)
        heads = []
        for which in range(STEP_GROUPS):
            home = across if which < 2 else far
            side = x if which % 2 == 0 else other_x
            heads.append(jnp.where(local, base + which, block_groups * home + chunks // 2 * side + group))
        return heads

    last = 2 * block_steps + chunks // 2 - 1

    spare_copy = remote(piece(chunks // 2 * other_x + (chunks - 1) // 2, chunks - 1), slot(chunks - 1, 1),
                        send_x, recv_x.at[REUSE_X], at(shard=across))

    def pass_y(chunk):
        y_copy(chunk).wait_recv()
        if not (isinstance(chunk, int) and chunk == chunks - 1):
            x_copy(chunk).start()
        pair_up(chunk, 0)

        @pl.when(chunk + window < chunks)
        def _():
            y_copy(chunk + window).start()

        @pl.when(chunk + window == chunks)
        def _():
            spare_copy.start()

    def pass_x(chunk):
        if isinstance(chunk, int) and chunk == chunks - 1:
            spare_copy.wait_recv()
        else:
            x_copy(chunk).wait_recv()
        pair_up(chunk, 1)

    def await_step(step):
        await_recv(vecs.at[pl.ds(0, 4 * PIECE_ROWS)], recv_d.at[step - 2 * block_steps])

    def score_all(step):
        heads = heads_at(step)
        for part in range(dims):
            score(step, heads, part)

    def early(step, carry):
        own_copy(block_at(step)).start()

        @pl.when(step >= 1)
        def _():
            pass_y(step - 1)

        @pl.when(step >= 5)
        def _():
            pass_x(step - 5)

        @pl.when(step == 0)
        def _():
            load_lists(1).wait()

        @pl.when(step == block_steps // 2 - 1)
        def _():
            load_lists(2).wait()
        score_all(step)
        arrange(step + 1)
        return carry

    def middle(step, carry):
        pass_y(step - 1)
        pass_x(step - 5)

        @pl.when(step == block_steps - 1)
        def _():
            own_copy(block_at(step)).start()

        @pl.when((step == block_steps) | (step == block_steps + block_steps // 2))
        def _():
            await_recv(vecs.at[pl.ds(0, block_rows // 2)], recv_o.at[step // (block_steps // 2) - 2])

        @pl.when(step >= 2 * block_steps)
        def _():
            await_step(step)
        score_all(step)
        return carry

    late_plan = {
        last - 5: ('y25', 'x21', 'x22'),
        last - 4: ('y26', 'x23', 'y27', 'x24'),
        last - 3: ('y28', 'x25', 'names', 'y29', 'x26'),
        last - 2: ('y30', 'x27', 'y31', 'x28', 'x29'),
        last - 1: ('x31', 'x30'),
    }

    def late(step, carry):
        for when, plan in late_plan.items():
            @pl.when(step == when)
            def _(plan=plan):
                for word in plan:
                    if word == 'names':
                        await_recv(ids_all.at[pl.ds(0, 3)], recv_i)
                        lax.fori_loop(0, width // LANES, name_candidates, 0)
                    else:
                        (pass_y if word[0] == 'y' else pass_x)(int(word[1:]))

        await_step(step)
        score_all(step)
        return carry

    lax.fori_loop(0, block_steps - 1, early, 0)
    lax.fori_loop(block_steps - 1, last - 5, middle, 0)
    pl.semaphore_wait(met.at[0], beside)
    tell_line(met.at[1])
    lax.fori_loop(last - 5, last, late, 0)
    pl.semaphore_wait(met.at[1], beside)
    await_step(jnp.int32(last))
    last_heads = heads_at(jnp.int32(last))

    leads, follows = outer & (s % 2 == 0), outer & (s % 2 == 1)

    def finish(turn, carry):
        @pl.when(leads & (turn == 1))
        def _():
            part_copy(far_outer, 0, 0).start()

        @pl.when(leads & (turn == 2))
        def _():
            part_copy(far_inner, 1, 0).start()
            part_copy(far_outer, 0, 1).start()
            part_copy(far_inner, 1, 1).start()

        @pl.when((leads & (turn == 3)) | (jnp.logical_not(outer) & (turn == 1)))
        def _():
            for half in range(2):
                part_copy(mate, 2, half).start()
        score(jnp.int32(last), last_heads, target_at(turn))
        return carry

    lax.fori_loop(0, dims, finish, 0)

    @pl.when(follows)
    def _():
        for half in range(2):
            part_copy(far_outer, 0, half).start()
            part_copy(far_inner, 1, half).start()
        for half in range(2):
            part_copy(mate, 2, half).start()

    @pl.when(jnp.logical_not(outer))
    def _():
        for half in range(2):
            for merge, target in enumerate((far_outer, far_inner)):
                part_wait(merge, half)
                parts[merge, half] += acc[target, half]
                merged_copy(merge, half).start()

    tiles = width // 2 // LANES
    for half in range(2):
        part_wait(2, half)
        part_wait(3, half)
        scores, names = [], []
        for member in range(LIST_LEN):
            total = acc[z, half, member] + parts[2, half, member] + parts[3, half, member]
            name = cand_ids[half, member]
            real = name >= 0.0
            scores.append(jnp.where(real, total, -jnp.inf))
            names.append(jnp.where(real, name, BIG))
        for place in range(TOP_K):
            best = functools.reduce(jnp.maximum, scores)
            best = jnp.max(best, axis=0, keepdims=True)
            tied = [jnp.where(score_j == best, name_j, BIG) for score_j, name_j in zip(scores, names)]
            first = jnp.min(functools.reduce(jnp.minimum, tied), axis=0, keepdims=True)
            for tile in range(tiles):
                lanes = slice(tile * LANES, (tile + 1) * LANES)
                line = place * tiles + tile
                res[z, half, line:line + 1, :] = best[:, lanes]
                res[z, half, TOP_K * tiles + line:TOP_K * tiles + line + 1, :] = first[:, lanes]
            if place + 1 < TOP_K:
                scores = [jnp.where(name_j == first, -jnp.inf, score_j) for score_j, name_j in zip(scores, names)]
        if half == 0:
            await_send(vecs.at[pl.ds(0, block_rows)], send_o)
            await_send(ids_all.at[pl.ds(0, 3)], send_i)
        else:
            await_send(vecs.at[pl.ds(0, chunks * PIECE_ROWS)], send_y)
            await_send(vecs.at[pl.ds(0, chunks * PIECE_ROWS)], send_x)
            await_send(vecs.at[pl.ds(0, 2 * chunks * PIECE_ROWS)], send_d)
        for which in range(dims - 1):
            res_copy(target_at(which), half).start()

    await_send(parts.at[pl.ds(0, 3)], send_r)
    await_send(res.at[pl.ds(0, dims - 1)], send_g)
    await_recv(res.at[pl.ds(0, dims - 1)], recv_g)


def place_kernel(res, out_s, out_i):
    dims, halves, lines, _ = res.shape
    tiles = lines // (2 * TOP_K)
    for part in range(dims):
        for half in range(halves):
            for tile in range(tiles):
                first = ((part * halves + half) * tiles + tile) * LANES
                out_s[:, first:first + LANES] = res[part, half, pl.ds(tile, TOP_K, stride=tiles), :]
                out_i[:, first:first + LANES] = res[part, half, pl.ds(TOP_K * tiles + tile, TOP_K, stride=tiles), :].astype(jnp.int32)


def solution(mesh):
    dims = mesh.shape['dim']
    row_spec = P(('rep', 'shard'), None)

    def local_search(queries, list_vecs, list_ids, probes):
        rows_q, depth = queries.shape
        lists_dev, list_len, _ = list_vecs.shape
        probe_count = probes.shape[1]
        block_rows = lists_dev * list_len
        block_steps = block_rows // STEP_ROWS
        chunks = lists_dev // GROUP_LISTS
        width = rows_q // dims
        dma = pltpu.SemaphoreType.DMA
        any_spec = pl.BlockSpec(memory_space=pl.ANY)
        vmem_spec = pl.BlockSpec(memory_space=pltpu.VMEM)
        found = pl.pallas_call(
            functools.partial(search_kernel, dims),
            out_shape=pltpu.VMEM((dims, 2, TOP_K * width // LANES, LANES), jnp.float32),
            in_specs=[any_spec] * 4,
            out_specs=vmem_spec,
            scratch_shapes=[
                pltpu.VMEM((block_rows, depth), jnp.bfloat16),
                pltpu.VMEM((rows_q, depth), jnp.bfloat16),
                pltpu.VMEM((4 * block_rows, depth), jnp.bfloat16),
                pltpu.VMEM((STEP_ROWS, STEP_ROWS), jnp.bfloat16),
                pltpu.VMEM((dims, 2, LIST_LEN, probe_count, width // 2), jnp.float32),
                pltpu.VMEM((4, 2, LIST_LEN, probe_count, width // 2), jnp.float32),
                pltpu.VMEM((4, LIST_LEN, lists_dev), jnp.int32),
                pltpu.VMEM((2, LIST_LEN, probe_count, width // 2), jnp.float32),
                pltpu.VMEM((probe_count, rows_q), jnp.int32),
                pltpu.VMEM((LIST_LEN, lists_dev), jnp.int32),
                dma, dma,
                dma((3,)), dma,
                dma, dma((2,)),
                dma, dma((REUSE_Y,)), dma, dma((REUSE_X + 1,)),
                dma, dma((chunks // 2,)),
                dma, dma, dma, dma((4, 2)), dma, dma,
                pltpu.SemaphoreType.REGULAR((2,)),
            ],
            compiler_params=pltpu.CompilerParams(collective_id=0, has_side_effects=True, vmem_limit_bytes=60 * 2**20),
            name='ivf_search',
        )(queries, list_vecs.reshape(block_rows, depth), probes.T, list_ids.T)
        scores, ids = pl.pallas_call(
            place_kernel,
            out_shape=(jax.ShapeDtypeStruct((TOP_K, rows_q), jnp.float32),
                       jax.ShapeDtypeStruct((TOP_K, rows_q), jnp.int32)),
            in_specs=[vmem_spec],
            out_specs=(vmem_spec, vmem_spec),
            compiler_params=pltpu.CompilerParams(vmem_limit_bytes=4 * 2**20),
            name='place',
        )(found)
        return scores.T, ids.T

    return jax.shard_map(local_search, mesh=mesh,
                         in_specs=(P(('rep', 'shard'), 'dim'), P('shard', None, 'dim'), P('shard', None), row_spec),
                         out_specs=(row_spec, row_spec), check_vma=False)
```

```python
import functools

import jax
import jax.numpy as jnp
from jax import lax
from jax.experimental import pallas as pl
from jax.experimental.pallas import tpu as pltpu
from jax.sharding import PartitionSpec as P

TOP_K = 10
LIST_LEN = 8
GROUP_LISTS = 8
GROUP_ROWS = GROUP_LISTS * LIST_LEN
STEP_GROUPS = 4
STEP_ROWS = STEP_GROUPS * GROUP_ROWS
PIECE_ROWS = GROUP_ROWS // 2
LANES = 128
REUSE_Y, REUSE_X = 8, 12
MESH = pl.DeviceIdType.MESH
BIG = 1e9


def flip(index, bit):
    return index + bit - 2 * bit * ((index // bit) % 2)


def search_kernel(dims, q_hbm, l_hbm, probes_hbm, ids_hbm, res,
                  raw, qv, vecs, perm, acc, parts, ids_all, cand_ids, probes_ref, ids_ref, load_p, load_i,
                  load_l, load_q, send_o, recv_o, send_y, recv_y, send_x, recv_x,
                  send_d, recv_d, send_i, recv_i, send_r, recv_r, send_g, recv_g, met):
    rows_q = qv.shape[0]
    lists_dev = ids_ref.shape[1]
    block_rows = lists_dev * LIST_LEN
    block_groups = lists_dev // GROUP_LISTS
    chunks = block_groups
    block_steps = block_groups // STEP_GROUPS
    width = rows_q // dims
    x, z, s = lax.axis_index('rep'), lax.axis_index('dim'), lax.axis_index('shard')
    twin, across, far = flip(s, 1), flip(s, 2), flip(flip(s, 1), 2)
    other_x = 1 - x

    def at(**place):
        return {'rep': x, 'dim': z, 'shard': s, **place}

    def step_rows(step):
        return pl.ds(pl.multiple_of(step * STEP_ROWS, STEP_ROWS), STEP_ROWS)

    def remote(src, dst, send, recv, device):
        return pltpu.make_async_remote_copy(src_ref=src, dst_ref=dst, send_sem=send, recv_sem=recv,
                                            device_id=device, device_id_type=MESH)

    def await_recv(buffer, semaphore):
        remote(buffer, buffer, send_i, semaphore, at()).wait_recv()

    def await_send(buffer, semaphore):
        remote(buffer, buffer, semaphore, recv_i, at()).wait_send()

    def load_lists(number):
        half = block_steps // 2
        first, count = ((half * x, 1), (half * x + 1, half - 1), (half * other_x, half))[number]
        rows = pl.ds(pl.multiple_of(first * STEP_ROWS, STEP_ROWS), count * STEP_ROWS)
        return pltpu.make_async_copy(l_hbm.at[rows], raw.at[rows], load_l.at[number])

    queries_in = pltpu.make_async_copy(q_hbm, qv, load_q)

    def own_copy(block):
        return remote(vecs.at[step_rows(block)], vecs.at[step_rows(block_steps + block)],
                      send_o, recv_o.at[(block // (block_steps // 2) + x) % 2], at(shard=twin))

    def piece(group, chunk):
        first = pl.multiple_of(group * GROUP_ROWS + chunk % 2 * PIECE_ROWS, PIECE_ROWS)
        return vecs.at[pl.ds(first, PIECE_ROWS)]

    def slot(chunk, which):
        return piece(2 * block_groups + STEP_GROUPS * (chunk // 2) + which, chunk)

    def y_copy(chunk):
        return remote(piece(chunks // 2 * x + chunk // 2, chunk), slot(chunk, 0), send_y, recv_y.at[chunk % REUSE_Y], at(shard=across))

    def x_copy(chunk):
        return remote(slot(chunk, 0), slot(chunk, 1), send_x, recv_x.at[chunk % REUSE_X], at(rep=other_x))

    def dy_copy(chunk):
        return remote(slot(chunk, 0), slot(chunk, 2), send_d, recv_d.at[chunk // 2], at(shard=twin))

    def dx_copy(chunk):
        return remote(slot(chunk, 1), slot(chunk, 3), send_d, recv_d.at[chunk // 2], at(shard=twin))

    def id_copy(which, peer):
        return remote(ids_ref, ids_all.at[s], send_i, recv_i, at(shard=peer))

    outer = z % 3 == 0
    mate, far_outer = flip(z, 1), jnp.where(z < 2, dims - 1, 0)
    far_inner = flip(far_outer, 1)

    def landed(place, half, sub=0):
        return recv_r.at[12 + half if place == 2 else 4 * min(place, 2) + 2 * half + sub]

    def some_members(sub):
        return pl.ds(sub * (LIST_LEN // 2), LIST_LEN // 2)

    def near_copy(half):
        return remote(acc.at[mate, half], parts.at[2, half], send_r, landed(2, half), at(dim=mate))

    def cross_copy(target, place, half, sub):
        return remote(acc.at[target, half, some_members(sub)], parts.at[place, half, some_members(sub)], send_r,
                      landed(place, half, sub), at(dim=mate))

    def merged_copy(merge, half, sub):
        return remote(parts.at[merge, half, some_members(sub)], parts.at[3, half, some_members(sub)], send_r,
                      landed(3, half, sub), at(dim=(far_outer, far_inner)[merge]))

    def part_wait(place, half, sub):
        await_recv(parts.at[place, half, some_members(sub)], landed(place, half, sub))

    def res_copy(target, half):
        return remote(res.at[z, half], res.at[z, half], send_g, recv_g, at(dim=target))

    def target_at(turn):
        first, second, third = (jnp.where(outer, one, two) for one, two in ((far_outer, mate), (far_inner, far_outer), (mate, far_inner)))
        return jnp.where(turn == 0, first, jnp.where(turn == 1, second, jnp.where(turn == 2, third, z)))

    def block_at(turn):
        return (block_steps // 2 * x + turn) % block_steps

    barrier = pltpu.get_barrier_semaphore()
    peers = [at(shard=twin), at(shard=across), at(shard=far), at(rep=other_x)]
    beside = jnp.where(outer, 1, 2)

    def tell_line(semaphore):
        @pl.when(z < dims - 1)
        def _():
            pl.semaphore_signal(semaphore, inc=1, device_id=at(dim=(z + 1) % dims), device_id_type=MESH)

        @pl.when(z > 0)
        def _():
            pl.semaphore_signal(semaphore, inc=1, device_id=at(dim=(z + dims - 1) % dims), device_id_type=MESH)

    load_lists(0).start()
    tell_line(barrier)
    probes_in = pltpu.make_async_copy(probes_hbm, probes_ref, load_p)
    ids_in = pltpu.make_async_copy(ids_hbm, ids_ref, load_i)
    ids_in.start()
    probes_in.start()
    queries_in.start()
    for peer in peers:
        pl.semaphore_signal(barrier, inc=1, device_id=peer, device_id_type=MESH)
    load_lists(1).start()
    load_lists(2).start()

    row = lax.broadcasted_iota(jnp.int32, (STEP_ROWS, STEP_ROWS), 0)
    col = lax.broadcasted_iota(jnp.int32, (STEP_ROWS, STEP_ROWS), 1)
    source = (row // GROUP_ROWS) * GROUP_ROWS + (row % GROUP_LISTS) * LIST_LEN + (row // GROUP_LISTS) % LIST_LEN
    perm[...] = jnp.where(col == source, 1.0, 0.0).astype(jnp.bfloat16)

    def arrange(turn):
        block = block_at(turn)
        moved = jnp.dot(perm[...], raw[step_rows(block), :], preferred_element_type=jnp.float32)
        vecs[step_rows(block), :] = moved.astype(jnp.bfloat16)

    window = REUSE_Y // 2
    load_lists(0).wait()
    arrange(0)
    pl.semaphore_wait(barrier, len(peers) + beside)
    for chunk in range(window):
        y_copy(chunk).start()
    tell_line(met.at[0])
    acc[...] = jnp.zeros_like(acc)
    ids_in.wait()
    for which, peer in enumerate((twin, across, far)):
        id_copy(which, peer).start()
    ids_all[s] = ids_ref[...]
    probes_in.wait()
    queries_in.wait()

    def name_candidates(tile, carry):
        cols = pl.ds(pl.multiple_of(z * width + tile * LANES, LANES), LANES)
        probe = probes_ref[:, cols]
        lane, page = probe % LANES, probe // LANES
        pages = lists_dev // LANES
        for member in range(LIST_LEN):
            got = jnp.zeros((probe.shape[0], LANES), jnp.int32)
            for number in range(4 * pages):
                table = ids_all[number // pages, member:member + 1, (number % pages) * LANES:(number % pages + 1) * LANES]
                table = jnp.broadcast_to(table, (probe.shape[0], LANES))
                picked = jnp.take_along_axis(table, lane, axis=1, mode='promise_in_bounds')
                got = jnp.where(page == number, picked, got)
            tiles_half = width // 2 // LANES
            place = pl.ds(pl.multiple_of(tile % tiles_half * LANES, LANES), LANES)
            cand_ids[tile // tiles_half, member, :, place] = got.astype(jnp.float32)
        return carry

    def list_block(step):
        return block_at(step % block_steps)

    def score(step, heads, part):
        lists = vecs[step_rows(jnp.where(step < 2 * block_steps, step // block_steps * block_steps + list_block(step), step)), :]
        rows = pl.ds(pl.multiple_of(part * width, width), width)
        scores = lax.dot_general(lists, qv[rows, :], (((1,), (1,)), ((), ())), preferred_element_type=jnp.float32)
        for tile in range(width // LANES):
            probe = probes_ref[:, pl.ds(pl.multiple_of(part * width + tile * LANES, LANES), LANES)]
            low, head = probe % GROUP_LISTS, probe // GROUP_LISTS
            hits = [head == want for want in heads]
            lanes = slice(tile * LANES, (tile + 1) * LANES)
            half, place = divmod(tile * LANES, width // 2)
            kept_lanes = slice(place, place + LANES)
            for member in range(LIST_LEN):
                kept = acc[part, half, member, :, kept_lanes]
                for group, hit in enumerate(hits):
                    first = group * GROUP_ROWS + member * GROUP_LISTS
                    picked = jnp.take_along_axis(scores[first:first + GROUP_LISTS, lanes], low, axis=0, mode='promise_in_bounds')
                    kept = jnp.where(hit, picked, kept)
                acc[part, half, member, :, kept_lanes] = kept

    def heads_at(step):
        local = step < 2 * block_steps
        group = step - 2 * block_steps
        base = block_groups * jnp.where(step < block_steps, s, twin) + STEP_GROUPS * list_block(step)
        heads = []
        for which in range(STEP_GROUPS):
            home = across if which < 2 else far
            side = x if which % 2 == 0 else other_x
            heads.append(jnp.where(local, base + which, block_groups * home + chunks // 2 * side + group))
        return heads

    last = 2 * block_steps + chunks // 2 - 1

    spare_copy = remote(piece(chunks // 2 * other_x + (chunks - 1) // 2, chunks - 1), slot(chunks - 1, 1),
                        send_x, recv_x.at[REUSE_X], at(shard=across))

    def pass_y(chunk):
        y_copy(chunk).wait_recv()
        if not (isinstance(chunk, int) and chunk == chunks - 1):
            x_copy(chunk).start()
        dy_copy(chunk).start()

        @pl.when(chunk + window < chunks)
        def _():
            y_copy(chunk + window).start()

        @pl.when(chunk + window == chunks)
        def _():
            spare_copy.start()

    def pass_x(chunk):
        if isinstance(chunk, int) and chunk == chunks - 1:
            spare_copy.wait_recv()
        else:
            x_copy(chunk).wait_recv()
        dx_copy(chunk).start()

    def await_step(step):
        await_recv(vecs.at[pl.ds(0, 4 * PIECE_ROWS)], recv_d.at[step - 2 * block_steps])

    def score_all(step):
        heads = heads_at(step)
        for part in range(dims):
            score(step, heads, part)

    def early(step, carry):
        own_copy(block_at(step)).start()

        @pl.when(step >= 1)
        def _():
            pass_y(step - 1)

        @pl.when(step >= 5)
        def _():
            pass_x(step - 5)

        @pl.when(step == 0)
        def _():
            load_lists(1).wait()

        @pl.when(step == block_steps // 2 - 1)
        def _():
            load_lists(2).wait()
        score_all(step)
        arrange(step + 1)
        return carry

    def middle(step, carry):
        pass_y(step - 1)
        pass_x(step - 5)

        @pl.when(step == block_steps - 1)
        def _():
            own_copy(block_at(step)).start()

        @pl.when((step == block_steps) | (step == block_steps + block_steps // 2))
        def _():
            await_recv(vecs.at[pl.ds(0, block_rows // 2)], recv_o.at[step // (block_steps // 2) - 2])

        @pl.when(step >= 2 * block_steps)
        def _():
            await_step(step)
        score_all(step)
        return carry

    late_plan = {
        last - 5: ('y25', 'x21', 'x22'),
        last - 4: ('y26', 'x23', 'y27', 'x24'),
        last - 3: ('y28', 'x25', 'names', 'y29', 'x26'),
        last - 2: ('y30', 'x27', 'y31', 'x28', 'x29'),
        last - 1: ('x31', 'x30'),
    }

    def late(step, carry):
        for when, plan in late_plan.items():
            @pl.when(step == when)
            def _(plan=plan):
                for word in plan:
                    if word == 'names':
                        await_recv(ids_all.at[pl.ds(0, 3)], recv_i)
                        lax.fori_loop(0, width // LANES, name_candidates, 0)
                    else:
                        (pass_y if word[0] == 'y' else pass_x)(int(word[1:]))

        await_step(step)
        score_all(step)
        return carry

    lax.fori_loop(0, block_steps - 1, early, 0)
    lax.fori_loop(block_steps - 1, last - 5, middle, 0)
    pl.semaphore_wait(met.at[0], beside)
    tell_line(met.at[1])
    lax.fori_loop(last - 5, last, late, 0)
    pl.semaphore_wait(met.at[1], beside)
    await_step(jnp.int32(last))
    last_heads = heads_at(jnp.int32(last))

    leads, follows = outer & (s % 2 == 0), outer & (s % 2 == 1)

    def send_cross(*plan):
        for far_place, half in plan:
            for sub in range(2):
                cross_copy((far_outer, far_inner)[far_place], far_place, half, sub).start()

    def send_near():
        for half in range(2):
            near_copy(half).start()

    def finish(turn, carry):
        @pl.when(leads & (turn == 1))
        def _():
            send_cross((0, 0))

        @pl.when(leads & (turn == 2))
        def _():
            send_cross((1, 0), (0, 1), (1, 1))

        @pl.when(follows & (turn == 3))
        def _():
            send_cross((0, 0), (1, 0))

        @pl.when((leads & (turn == 3)) | (jnp.logical_not(outer) & (turn == 1)))
        def _():
            send_near()
        score(jnp.int32(last), last_heads, target_at(turn))
        return carry

    lax.fori_loop(0, dims, finish, 0)

    @pl.when(follows)
    def _():
        send_cross((0, 1), (1, 1))
        send_near()

    @pl.when(jnp.logical_not(outer))
    def _():
        for half in range(2):
            for merge, target in enumerate((far_outer, far_inner)):
                for sub in range(2):
                    part_wait(merge, half, sub)
                    parts[merge, half, some_members(sub)] += acc[target, half, some_members(sub)]
                    merged_copy(merge, half, sub).start()

    tiles = width // 2 // LANES
    for half in range(2):
        await_recv(parts.at[2, half], landed(2, half))
        for sub in range(2):
            part_wait(3, half, sub)
        scores, names = [], []
        for member in range(LIST_LEN):
            total = acc[z, half, member] + parts[2, half, member] + parts[3, half, member]
            name = cand_ids[half, member]
            real = name >= 0.0
            scores.append(jnp.where(real, total, -jnp.inf))
            names.append(jnp.where(real, name, BIG))
        for place in range(TOP_K):
            best = functools.reduce(jnp.maximum, scores)
            best = jnp.max(best, axis=0, keepdims=True)
            tied = [jnp.where(score_j == best, name_j, BIG) for score_j, name_j in zip(scores, names)]
            first = jnp.min(functools.reduce(jnp.minimum, tied), axis=0, keepdims=True)
            for tile in range(tiles):
                lanes = slice(tile * LANES, (tile + 1) * LANES)
                line = place * tiles + tile
                res[z, half, line:line + 1, :] = best[:, lanes]
                res[z, half, TOP_K * tiles + line:TOP_K * tiles + line + 1, :] = first[:, lanes]
            if place + 1 < TOP_K:
                scores = [jnp.where(name_j == first, -jnp.inf, score_j) for score_j, name_j in zip(scores, names)]
        if half == 0:
            await_send(vecs.at[pl.ds(0, block_rows)], send_o)
            await_send(ids_all.at[pl.ds(0, 3)], send_i)
        else:
            await_send(vecs.at[pl.ds(0, chunks * PIECE_ROWS)], send_y)
            await_send(vecs.at[pl.ds(0, chunks * PIECE_ROWS)], send_x)
            await_send(vecs.at[pl.ds(0, 2 * chunks * PIECE_ROWS)], send_d)
        for which in range(dims - 1):
            res_copy(target_at(which), half).start()

    await_send(parts.at[pl.ds(0, 3)], send_r)
    await_send(res.at[pl.ds(0, dims - 1)], send_g)
    await_recv(res.at[pl.ds(0, dims - 1)], recv_g)


def place_kernel(res, out_s, out_i):
    dims, halves, lines, _ = res.shape
    tiles = lines // (2 * TOP_K)
    for part in range(dims):
        for half in range(halves):
            for tile in range(tiles):
                first = ((part * halves + half) * tiles + tile) * LANES
                out_s[:, first:first + LANES] = res[part, half, pl.ds(tile, TOP_K, stride=tiles), :]
                out_i[:, first:first + LANES] = res[part, half, pl.ds(TOP_K * tiles + tile, TOP_K, stride=tiles), :].astype(jnp.int32)


def solution(mesh):
    dims = mesh.shape['dim']
    row_spec = P(('rep', 'shard'), None)

    def local_search(queries, list_vecs, list_ids, probes):
        rows_q, depth = queries.shape
        lists_dev, list_len, _ = list_vecs.shape
        probe_count = probes.shape[1]
        block_rows = lists_dev * list_len
        block_steps = block_rows // STEP_ROWS
        chunks = lists_dev // GROUP_LISTS
        width = rows_q // dims
        dma = pltpu.SemaphoreType.DMA
        any_spec = pl.BlockSpec(memory_space=pl.ANY)
        vmem_spec = pl.BlockSpec(memory_space=pltpu.VMEM)
        found = pl.pallas_call(
            functools.partial(search_kernel, dims),
            out_shape=pltpu.VMEM((dims, 2, TOP_K * width // LANES, LANES), jnp.float32),
            in_specs=[any_spec] * 4,
            out_specs=vmem_spec,
            scratch_shapes=[
                pltpu.VMEM((block_rows, depth), jnp.bfloat16),
                pltpu.VMEM((rows_q, depth), jnp.bfloat16),
                pltpu.VMEM((4 * block_rows, depth), jnp.bfloat16),
                pltpu.VMEM((STEP_ROWS, STEP_ROWS), jnp.bfloat16),
                pltpu.VMEM((dims, 2, LIST_LEN, probe_count, width // 2), jnp.float32),
                pltpu.VMEM((4, 2, LIST_LEN, probe_count, width // 2), jnp.float32),
                pltpu.VMEM((4, LIST_LEN, lists_dev), jnp.int32),
                pltpu.VMEM((2, LIST_LEN, probe_count, width // 2), jnp.float32),
                pltpu.VMEM((probe_count, rows_q), jnp.int32),
                pltpu.VMEM((LIST_LEN, lists_dev), jnp.int32),
                dma, dma,
                dma((3,)), dma,
                dma, dma((2,)),
                dma, dma((REUSE_Y,)), dma, dma((REUSE_X + 1,)),
                dma, dma((chunks // 2,)),
                dma, dma, dma, dma((14,)), dma, dma,
                pltpu.SemaphoreType.REGULAR((2,)),
            ],
            compiler_params=pltpu.CompilerParams(collective_id=0, has_side_effects=True, vmem_limit_bytes=60 * 2**20),
            name='ivf_search',
        )(queries, list_vecs.reshape(block_rows, depth), probes.T, list_ids.T)
        scores, ids = pl.pallas_call(
            place_kernel,
            out_shape=(jax.ShapeDtypeStruct((TOP_K, rows_q), jnp.float32),
                       jax.ShapeDtypeStruct((TOP_K, rows_q), jnp.int32)),
            in_specs=[vmem_spec],
            out_specs=(vmem_spec, vmem_spec),
            compiler_params=pltpu.CompilerParams(vmem_limit_bytes=4 * 2**20),
            name='place',
        )(found)
        return scores.T, ids.T

    return jax.shard_map(local_search, mesh=mesh,
                         in_specs=(P(('rep', 'shard'), 'dim'), P('shard', None, 'dim'), P('shard', None), row_spec),
                         out_specs=(row_spec, row_spec), check_vma=False)
```

```python
import functools

import jax
import jax.numpy as jnp
from jax import lax
from jax.experimental import pallas as pl
from jax.experimental.pallas import tpu as pltpu
from jax.sharding import PartitionSpec as P

TOP_K = 10
LIST_LEN = 8
GROUP_LISTS = 8
GROUP_ROWS = GROUP_LISTS * LIST_LEN
STEP_GROUPS = 4
STEP_ROWS = STEP_GROUPS * GROUP_ROWS
PIECE_ROWS = GROUP_ROWS // 2
LANES = 128
REUSE_Y, REUSE_X = 8, 12
MESH = pl.DeviceIdType.MESH
BIG = 1e9


def flip(index, bit):
    return index + bit - 2 * bit * ((index // bit) % 2)


def search_kernel(dims, q_hbm, l_hbm, probes_hbm, ids_hbm, res,
                  raw, qv, vecs, perm, acc, parts, ids_all, cand_ids, probes_ref, ids_ref, load_p, load_i,
                  load_l, load_q, send_o, recv_o, send_y, recv_y, send_x, recv_x,
                  send_d, recv_d, send_i, recv_i, send_r, recv_r, send_g, recv_g, met):
    rows_q = qv.shape[0]
    lists_dev = ids_ref.shape[1]
    block_rows = lists_dev * LIST_LEN
    block_groups = lists_dev // GROUP_LISTS
    chunks = block_groups
    block_steps = block_groups // STEP_GROUPS
    width = rows_q // dims
    x, z, s = lax.axis_index('rep'), lax.axis_index('dim'), lax.axis_index('shard')
    twin, across, far = flip(s, 1), flip(s, 2), flip(flip(s, 1), 2)
    other_x = 1 - x

    def at(**place):
        return {'rep': x, 'dim': z, 'shard': s, **place}

    def step_rows(step):
        return pl.ds(pl.multiple_of(step * STEP_ROWS, STEP_ROWS), STEP_ROWS)

    def remote(src, dst, send, recv, device):
        return pltpu.make_async_remote_copy(src_ref=src, dst_ref=dst, send_sem=send, recv_sem=recv,
                                            device_id=device, device_id_type=MESH)

    def await_recv(buffer, semaphore):
        remote(buffer, buffer, send_i, semaphore, at()).wait_recv()

    def await_send(buffer, semaphore):
        remote(buffer, buffer, semaphore, recv_i, at()).wait_send()

    def load_lists(number):
        half = block_steps // 2
        first, count = ((half * x, 1), (half * x + 1, half - 1), (half * other_x, half))[number]
        rows = pl.ds(pl.multiple_of(first * STEP_ROWS, STEP_ROWS), count * STEP_ROWS)
        return pltpu.make_async_copy(l_hbm.at[rows], raw.at[rows], load_l.at[number])

    queries_in = pltpu.make_async_copy(q_hbm, qv, load_q)

    def send_own(block):
        for part in range(STEP_ROWS // PIECE_ROWS):
            first = pl.multiple_of(block * STEP_ROWS + part * PIECE_ROWS, PIECE_ROWS)
            remote(vecs.at[pl.ds(first, PIECE_ROWS)], vecs.at[pl.ds(block_rows + first, PIECE_ROWS)],
                   send_o, recv_o.at[(block // (block_steps // 2) + x) % 2], at(shard=twin)).start()

    def piece(group, chunk):
        first = pl.multiple_of(group * GROUP_ROWS + chunk % 2 * PIECE_ROWS, PIECE_ROWS)
        return vecs.at[pl.ds(first, PIECE_ROWS)]

    def slot(chunk, which):
        return piece(2 * block_groups + STEP_GROUPS * (chunk // 2) + which, chunk)

    def y_copy(chunk):
        return remote(piece(chunks // 2 * x + chunk // 2, chunk), slot(chunk, 0), send_y, recv_y.at[chunk % REUSE_Y], at(shard=across))

    def x_copy(chunk):
        return remote(slot(chunk, 0), slot(chunk, 1), send_x, recv_x.at[chunk % REUSE_X], at(rep=other_x))

    def dy_copy(chunk):
        return remote(slot(chunk, 0), slot(chunk, 2), send_d, recv_d.at[chunk // 2], at(shard=twin))

    def dx_copy(chunk):
        return remote(slot(chunk, 1), slot(chunk, 3), send_d, recv_d.at[chunk // 2], at(shard=twin))

    def id_copy(which, peer):
        return remote(ids_ref, ids_all.at[s], send_i, recv_i, at(shard=peer))

    outer = z % 3 == 0
    mate, far_outer = flip(z, 1), jnp.where(z < 2, dims - 1, 0)
    far_inner = flip(far_outer, 1)

    def landed(place, half, sub=0):
        return recv_r.at[12 + half if place == 2 else 4 * min(place, 2) + 2 * half + sub]

    def some_members(sub):
        return pl.ds(sub * (LIST_LEN // 2), LIST_LEN // 2)

    def near_copy(half):
        return remote(acc.at[mate, half], parts.at[2, half], send_r, landed(2, half), at(dim=mate))

    def cross_copy(target, place, half, sub):
        return remote(acc.at[target, half, some_members(sub)], parts.at[place, half, some_members(sub)], send_r,
                      landed(place, half, sub), at(dim=mate))

    def merged_copy(merge, half, sub):
        return remote(parts.at[merge, half, some_members(sub)], parts.at[3, half, some_members(sub)], send_r,
                      landed(3, half, sub), at(dim=(far_outer, far_inner)[merge]))

    def part_wait(place, half, sub):
        await_recv(parts.at[place, half, some_members(sub)], landed(place, half, sub))

    def res_copy(target, half):
        return remote(res.at[z, half], res.at[z, half], send_g, recv_g, at(dim=target))

    def target_at(turn):
        first, second, third = (jnp.where(outer, one, two) for one, two in ((far_outer, mate), (far_inner, far_outer), (mate, far_inner)))
        return jnp.where(turn == 0, first, jnp.where(turn == 1, second, jnp.where(turn == 2, third, z)))

    def block_at(turn):
        return (block_steps // 2 * x + turn) % block_steps

    barrier = pltpu.get_barrier_semaphore()
    peers = [at(shard=twin), at(shard=across), at(shard=far), at(rep=other_x)]
    beside = jnp.where(outer, 1, 2)

    def tell_line(semaphore):
        @pl.when(z < dims - 1)
        def _():
            pl.semaphore_signal(semaphore, inc=1, device_id=at(dim=(z + 1) % dims), device_id_type=MESH)

        @pl.when(z > 0)
        def _():
            pl.semaphore_signal(semaphore, inc=1, device_id=at(dim=(z + dims - 1) % dims), device_id_type=MESH)

    load_lists(0).start()
    tell_line(barrier)
    probes_in = pltpu.make_async_copy(probes_hbm, probes_ref, load_p)
    ids_in = pltpu.make_async_copy(ids_hbm, ids_ref, load_i)
    ids_in.start()
    probes_in.start()
    queries_in.start()
    for peer in peers:
        pl.semaphore_signal(barrier, inc=1, device_id=peer, device_id_type=MESH)
    load_lists(1).start()
    load_lists(2).start()

    row = lax.broadcasted_iota(jnp.int32, (STEP_ROWS, STEP_ROWS), 0)
    col = lax.broadcasted_iota(jnp.int32, (STEP_ROWS, STEP_ROWS), 1)
    source = (row // GROUP_ROWS) * GROUP_ROWS + (row % GROUP_LISTS) * LIST_LEN + (row // GROUP_LISTS) % LIST_LEN
    perm[...] = jnp.where(col == source, 1.0, 0.0).astype(jnp.bfloat16)

    def arrange(turn):
        block = block_at(turn)
        moved = jnp.dot(perm[...], raw[step_rows(block), :], preferred_element_type=jnp.float32)
        vecs[step_rows(block), :] = moved.astype(jnp.bfloat16)

    window = REUSE_Y // 2
    load_lists(0).wait()
    arrange(0)
    pl.semaphore_wait(barrier, len(peers) + beside)
    for chunk in range(window):
        y_copy(chunk).start()
    tell_line(met.at[0])
    acc[...] = jnp.zeros_like(acc)
    ids_in.wait()
    for which, peer in enumerate((twin, across, far)):
        id_copy(which, peer).start()
    ids_all[s] = ids_ref[...]
    probes_in.wait()
    queries_in.wait()

    def name_candidates(tile, carry):
        cols = pl.ds(pl.multiple_of(z * width + tile * LANES, LANES), LANES)
        probe = probes_ref[:, cols]
        lane, page = probe % LANES, probe // LANES
        pages = lists_dev // LANES
        for member in range(LIST_LEN):
            got = jnp.zeros((probe.shape[0], LANES), jnp.int32)
            for number in range(4 * pages):
                table = ids_all[number // pages, member:member + 1, (number % pages) * LANES:(number % pages + 1) * LANES]
                table = jnp.broadcast_to(table, (probe.shape[0], LANES))
                picked = jnp.take_along_axis(table, lane, axis=1, mode='promise_in_bounds')
                got = jnp.where(page == number, picked, got)
            tiles_half = width // 2 // LANES
            place = pl.ds(pl.multiple_of(tile % tiles_half * LANES, LANES), LANES)
            cand_ids[tile // tiles_half, member, :, place] = got.astype(jnp.float32)
        return carry

    def list_block(step):
        return block_at(step % block_steps)

    def score(step, heads, part):
        lists = vecs[step_rows(jnp.where(step < 2 * block_steps, step // block_steps * block_steps + list_block(step), step)), :]
        rows = pl.ds(pl.multiple_of(part * width, width), width)
        scores = lax.dot_general(lists, qv[rows, :], (((1,), (1,)), ((), ())), preferred_element_type=jnp.float32)
        for tile in range(width // LANES):
            probe = probes_ref[:, pl.ds(pl.multiple_of(part * width + tile * LANES, LANES), LANES)]
            low, head = probe % GROUP_LISTS, probe // GROUP_LISTS
            hits = [head == want for want in heads]
            lanes = slice(tile * LANES, (tile + 1) * LANES)
            half, place = divmod(tile * LANES, width // 2)
            kept_lanes = slice(place, place + LANES)
            for member in range(LIST_LEN):
                kept = acc[part, half, member, :, kept_lanes]
                for group, hit in enumerate(hits):
                    first = group * GROUP_ROWS + member * GROUP_LISTS
                    picked = jnp.take_along_axis(scores[first:first + GROUP_LISTS, lanes], low, axis=0, mode='promise_in_bounds')
                    kept = jnp.where(hit, picked, kept)
                acc[part, half, member, :, kept_lanes] = kept

    def heads_at(step):
        local = step < 2 * block_steps
        group = step - 2 * block_steps
        base = block_groups * jnp.where(step < block_steps, s, twin) + STEP_GROUPS * list_block(step)
        heads = []
        for which in range(STEP_GROUPS):
            home = across if which < 2 else far
            side = x if which % 2 == 0 else other_x
            heads.append(jnp.where(local, base + which, block_groups * home + chunks // 2 * side + group))
        return heads

    last = 2 * block_steps + chunks // 2 - 1

    spare_copy = remote(piece(chunks // 2 * other_x + (chunks - 1) // 2, chunks - 1), slot(chunks - 1, 1),
                        send_x, recv_x.at[REUSE_X], at(shard=across))

    def pass_y(chunk):
        y_copy(chunk).wait_recv()
        if not (isinstance(chunk, int) and chunk == chunks - 1):
            x_copy(chunk).start()
        dy_copy(chunk).start()

        @pl.when(chunk + window < chunks)
        def _():
            y_copy(chunk + window).start()

        @pl.when(chunk + window == chunks)
        def _():
            spare_copy.start()

    def pass_x(chunk):
        if isinstance(chunk, int) and chunk == chunks - 1:
            spare_copy.wait_recv()
        else:
            x_copy(chunk).wait_recv()
        dx_copy(chunk).start()

    def await_step(step):
        await_recv(vecs.at[pl.ds(0, 4 * PIECE_ROWS)], recv_d.at[step - 2 * block_steps])

    def score_all(step):
        heads = heads_at(step)
        for part in range(dims):
            score(step, heads, part)

    def early(step, carry):
        send_own(block_at(step))

        @pl.when(step >= 1)
        def _():
            pass_y(step - 1)

        @pl.when(step >= 5)
        def _():
            pass_x(step - 5)

        @pl.when(step == 0)
        def _():
            load_lists(1).wait()

        @pl.when(step == block_steps // 2 - 1)
        def _():
            load_lists(2).wait()
        score_all(step)
        arrange(step + 1)
        return carry

    def middle(step, carry):
        pass_y(step - 1)
        pass_x(step - 5)

        @pl.when(step == block_steps - 1)
        def _():
            send_own(block_at(step))

        @pl.when((step == block_steps) | (step == block_steps + block_steps // 2))
        def _():
            await_recv(vecs.at[pl.ds(0, block_rows // 2)], recv_o.at[step // (block_steps // 2) - 2])

        @pl.when(step >= 2 * block_steps)
        def _():
            await_step(step)
        score_all(step)
        return carry

    late_plan = {
        last - 5: ('y25', 'x21', 'x22'),
        last - 4: ('y26', 'x23', 'y27', 'x24'),
        last - 3: ('y28', 'x25', 'names', 'y29', 'x26'),
        last - 2: ('y30', 'x27', 'y31', 'x28', 'x29'),
        last - 1: ('x31', 'x30'),
    }

    def late(step, carry):
        for when, plan in late_plan.items():
            @pl.when(step == when)
            def _(plan=plan):
                for word in plan:
                    if word == 'names':
                        await_recv(ids_all.at[pl.ds(0, 3)], recv_i)
                        lax.fori_loop(0, width // LANES, name_candidates, 0)
                    else:
                        (pass_y if word[0] == 'y' else pass_x)(int(word[1:]))

        await_step(step)
        score_all(step)
        return carry

    lax.fori_loop(0, block_steps - 1, early, 0)
    lax.fori_loop(block_steps - 1, last - 5, middle, 0)
    pl.semaphore_wait(met.at[0], beside)
    tell_line(met.at[1])
    lax.fori_loop(last - 5, last, late, 0)
    pl.semaphore_wait(met.at[1], beside)
    await_step(jnp.int32(last))
    last_heads = heads_at(jnp.int32(last))

    leads, follows = outer & (s % 2 == 0), outer & (s % 2 == 1)

    def send_cross(*plan):
        for far_place, half in plan:
            for sub in range(2):
                cross_copy((far_outer, far_inner)[far_place], far_place, half, sub).start()

    def send_near():
        for half in range(2):
            near_copy(half).start()

    def finish(turn, carry):
        @pl.when(leads & (turn == 1))
        def _():
            send_cross((0, 0))

        @pl.when(leads & (turn == 2))
        def _():
            send_cross((1, 0), (0, 1), (1, 1))

        @pl.when(follows & (turn == 3))
        def _():
            send_cross((0, 0), (1, 0))

        @pl.when((leads & (turn == 3)) | (jnp.logical_not(outer) & (turn == 1)))
        def _():
            send_near()
        score(jnp.int32(last), last_heads, target_at(turn))
        return carry

    lax.fori_loop(0, dims, finish, 0)

    @pl.when(follows)
    def _():
        send_cross((0, 1), (1, 1))
        send_near()

    @pl.when(jnp.logical_not(outer))
    def _():
        for half in range(2):
            for merge, target in enumerate((far_outer, far_inner)):
                for sub in range(2):
                    part_wait(merge, half, sub)
                    parts[merge, half, some_members(sub)] += acc[target, half, some_members(sub)]
                    merged_copy(merge, half, sub).start()

    tiles = width // 2 // LANES
    for half in range(2):
        await_recv(parts.at[2, half], landed(2, half))
        for sub in range(2):
            part_wait(3, half, sub)
        scores, names = [], []
        for member in range(LIST_LEN):
            total = acc[z, half, member] + parts[2, half, member] + parts[3, half, member]
            name = cand_ids[half, member]
            real = name >= 0.0
            scores.append(jnp.where(real, total, -jnp.inf))
            names.append(jnp.where(real, name, BIG))
        for place in range(TOP_K):
            best = functools.reduce(jnp.maximum, scores)
            best = jnp.max(best, axis=0, keepdims=True)
            tied = [jnp.where(score_j == best, name_j, BIG) for score_j, name_j in zip(scores, names)]
            first = jnp.min(functools.reduce(jnp.minimum, tied), axis=0, keepdims=True)
            for tile in range(tiles):
                lanes = slice(tile * LANES, (tile + 1) * LANES)
                line = place * tiles + tile
                res[z, half, line:line + 1, :] = best[:, lanes]
                res[z, half, TOP_K * tiles + line:TOP_K * tiles + line + 1, :] = first[:, lanes]
            if place + 1 < TOP_K:
                scores = [jnp.where(name_j == first, -jnp.inf, score_j) for score_j, name_j in zip(scores, names)]
        if half == 0:
            await_send(vecs.at[pl.ds(0, block_rows)], send_o)
            await_send(ids_all.at[pl.ds(0, 3)], send_i)
        else:
            await_send(vecs.at[pl.ds(0, chunks * PIECE_ROWS)], send_y)
            await_send(vecs.at[pl.ds(0, chunks * PIECE_ROWS)], send_x)
            await_send(vecs.at[pl.ds(0, 2 * chunks * PIECE_ROWS)], send_d)
        for which in range(dims - 1):
            res_copy(target_at(which), half).start()

    await_send(parts.at[pl.ds(0, 3)], send_r)
    await_send(res.at[pl.ds(0, dims - 1)], send_g)
    await_recv(res.at[pl.ds(0, dims - 1)], recv_g)


def place_kernel(res, out_s, out_i):
    dims, halves, lines, _ = res.shape
    tiles = lines // (2 * TOP_K)
    for part in range(dims):
        for half in range(halves):
            for tile in range(tiles):
                first = ((part * halves + half) * tiles + tile) * LANES
                out_s[:, first:first + LANES] = res[part, half, pl.ds(tile, TOP_K, stride=tiles), :]
                out_i[:, first:first + LANES] = res[part, half, pl.ds(TOP_K * tiles + tile, TOP_K, stride=tiles), :].astype(jnp.int32)


def solution(mesh):
    dims = mesh.shape['dim']
    row_spec = P(('rep', 'shard'), None)

    def local_search(queries, list_vecs, list_ids, probes):
        rows_q, depth = queries.shape
        lists_dev, list_len, _ = list_vecs.shape
        probe_count = probes.shape[1]
        block_rows = lists_dev * list_len
        block_steps = block_rows // STEP_ROWS
        chunks = lists_dev // GROUP_LISTS
        width = rows_q // dims
        dma = pltpu.SemaphoreType.DMA
        any_spec = pl.BlockSpec(memory_space=pl.ANY)
        vmem_spec = pl.BlockSpec(memory_space=pltpu.VMEM)
        found = pl.pallas_call(
            functools.partial(search_kernel, dims),
            out_shape=pltpu.VMEM((dims, 2, TOP_K * width // LANES, LANES), jnp.float32),
            in_specs=[any_spec] * 4,
            out_specs=vmem_spec,
            scratch_shapes=[
                pltpu.VMEM((block_rows, depth), jnp.bfloat16),
                pltpu.VMEM((rows_q, depth), jnp.bfloat16),
                pltpu.VMEM((4 * block_rows, depth), jnp.bfloat16),
                pltpu.VMEM((STEP_ROWS, STEP_ROWS), jnp.bfloat16),
                pltpu.VMEM((dims, 2, LIST_LEN, probe_count, width // 2), jnp.float32),
                pltpu.VMEM((4, 2, LIST_LEN, probe_count, width // 2), jnp.float32),
                pltpu.VMEM((4, LIST_LEN, lists_dev), jnp.int32),
                pltpu.VMEM((2, LIST_LEN, probe_count, width // 2), jnp.float32),
                pltpu.VMEM((probe_count, rows_q), jnp.int32),
                pltpu.VMEM((LIST_LEN, lists_dev), jnp.int32),
                dma, dma,
                dma((3,)), dma,
                dma, dma((2,)),
                dma, dma((REUSE_Y,)), dma, dma((REUSE_X + 1,)),
                dma, dma((chunks // 2,)),
                dma, dma, dma, dma((14,)), dma, dma,
                pltpu.SemaphoreType.REGULAR((2,)),
            ],
            compiler_params=pltpu.CompilerParams(collective_id=0, has_side_effects=True, vmem_limit_bytes=60 * 2**20),
            name='ivf_search',
        )(queries, list_vecs.reshape(block_rows, depth), probes.T, list_ids.T)
        scores, ids = pl.pallas_call(
            place_kernel,
            out_shape=(jax.ShapeDtypeStruct((TOP_K, rows_q), jnp.float32),
                       jax.ShapeDtypeStruct((TOP_K, rows_q), jnp.int32)),
            in_specs=[vmem_spec],
            out_specs=(vmem_spec, vmem_spec),
            compiler_params=pltpu.CompilerParams(vmem_limit_bytes=4 * 2**20),
            name='place',
        )(found)
        return scores.T, ids.T

    return jax.shard_map(local_search, mesh=mesh,
                         in_specs=(P(('rep', 'shard'), 'dim'), P('shard', None, 'dim'), P('shard', None), row_spec),
                         out_specs=(row_spec, row_spec), check_vma=False)
```

```python
import functools

import jax
import jax.numpy as jnp
from jax import lax
from jax.experimental import pallas as pl
from jax.experimental.pallas import tpu as pltpu
from jax.sharding import PartitionSpec as P

TOP_K = 10
LIST_LEN = 8
GROUP_LISTS = 8
GROUP_ROWS = GROUP_LISTS * LIST_LEN
STEP_GROUPS = 4
STEP_ROWS = STEP_GROUPS * GROUP_ROWS
PIECE_ROWS = GROUP_ROWS // 2
LANES = 128
REUSE_Y, REUSE_X = 8, 12
MESH = pl.DeviceIdType.MESH
BIG = 1e9


def flip(index, bit):
    return index + bit - 2 * bit * ((index // bit) % 2)


def search_kernel(dims, q_hbm, l_hbm, probes_hbm, ids_hbm, res,
                  raw, qv, vecs, perm, acc, parts, ids_all, cand_ids, probes_ref, ids_ref, load_p, load_i,
                  load_l, load_q, send_o, recv_o, send_y, recv_y, send_x, recv_x,
                  send_d, recv_d, send_i, recv_i, send_r, recv_r, send_g, recv_g, met):
    rows_q = qv.shape[0]
    lists_dev = ids_ref.shape[1]
    block_rows = lists_dev * LIST_LEN
    block_groups = lists_dev // GROUP_LISTS
    chunks = block_groups
    block_steps = block_groups // STEP_GROUPS
    width = rows_q // dims
    x, z, s = lax.axis_index('rep'), lax.axis_index('dim'), lax.axis_index('shard')
    twin, across, far = flip(s, 1), flip(s, 2), flip(flip(s, 1), 2)
    other_x = 1 - x

    def at(**place):
        return {'rep': x, 'dim': z, 'shard': s, **place}

    def step_rows(step):
        return pl.ds(pl.multiple_of(step * STEP_ROWS, STEP_ROWS), STEP_ROWS)

    def remote(src, dst, send, recv, device):
        return pltpu.make_async_remote_copy(src_ref=src, dst_ref=dst, send_sem=send, recv_sem=recv,
                                            device_id=device, device_id_type=MESH)

    def await_recv(buffer, semaphore):
        remote(buffer, buffer, send_i, semaphore, at()).wait_recv()

    def await_send(buffer, semaphore):
        remote(buffer, buffer, semaphore, recv_i, at()).wait_send()

    def load_lists(number):
        half = block_steps // 2
        first, count = ((half * x, 1), (half * x + 1, half - 1), (half * other_x, half))[number]
        rows = pl.ds(pl.multiple_of(first * STEP_ROWS, STEP_ROWS), count * STEP_ROWS)
        return pltpu.make_async_copy(l_hbm.at[rows], raw.at[rows], load_l.at[number])

    queries_in = pltpu.make_async_copy(q_hbm, qv, load_q)

    def own_copy(block):
        return remote(vecs.at[step_rows(block)], vecs.at[step_rows(block_steps + block)],
                      send_o, recv_o.at[(block // (block_steps // 2) + x) % 2], at(shard=twin))

    def piece(group, chunk):
        first = pl.multiple_of(group * GROUP_ROWS + chunk % 2 * PIECE_ROWS, PIECE_ROWS)
        return vecs.at[pl.ds(first, PIECE_ROWS)]

    def slot(chunk, which):
        return piece(2 * block_groups + STEP_GROUPS * (chunk // 2) + which, chunk)

    def y_copy(chunk):
        return remote(piece(chunks // 2 * x + chunk // 2, chunk), slot(chunk, 0), send_y, recv_y.at[chunk % REUSE_Y], at(shard=across))

    def x_copy(chunk):
        return remote(slot(chunk, 0), slot(chunk, 1), send_x, recv_x.at[chunk % REUSE_X], at(rep=other_x))

    def dy_copy(chunk):
        return remote(slot(chunk, 0), slot(chunk, 2), send_d, recv_d.at[chunk // 2], at(shard=twin))

    def dx_copy(chunk):
        return remote(slot(chunk, 1), slot(chunk, 3), send_d, recv_d.at[chunk // 2], at(shard=twin))

    def id_copy(which, peer):
        return remote(ids_ref, ids_all.at[s], send_i, recv_i, at(shard=peer))

    outer = z % 3 == 0
    mate, far_outer = flip(z, 1), jnp.where(z < 2, dims - 1, 0)
    far_inner = flip(far_outer, 1)

    def landed(place, half, sub=0):
        return recv_r.at[12 + half if place == 2 else 4 * min(place, 2) + 2 * half + sub]

    def some_members(sub):
        return pl.ds(sub * (LIST_LEN // 2), LIST_LEN // 2)

    def near_copy(half):
        return remote(acc.at[mate, half], parts.at[2, half], send_r, landed(2, half), at(dim=mate))

    def cross_copy(target, place, half, sub):
        return remote(acc.at[target, half, some_members(sub)], parts.at[place, half, some_members(sub)], send_r,
                      landed(place, half, sub), at(dim=mate))

    def merged_copy(merge, half, sub):
        return remote(parts.at[merge, half, some_members(sub)], parts.at[3, half, some_members(sub)], send_r,
                      landed(3, half, sub), at(dim=(far_outer, far_inner)[merge]))

    def part_wait(place, half, sub):
        await_recv(parts.at[place, half, some_members(sub)], landed(place, half, sub))

    def res_copy(target, half):
        return remote(res.at[z, half], res.at[z, half], send_g, recv_g, at(dim=target))

    def target_at(turn):
        first, second, third = (jnp.where(outer, one, two) for one, two in ((far_outer, mate), (far_inner, far_outer), (mate, far_inner)))
        return jnp.where(turn == 0, first, jnp.where(turn == 1, second, jnp.where(turn == 2, third, z)))

    def block_at(turn):
        return (block_steps // 2 * x + turn) % block_steps

    barrier = pltpu.get_barrier_semaphore()
    peers = [at(shard=twin), at(shard=across), at(shard=far), at(rep=other_x)]
    beside = jnp.where(outer, 1, 2)

    def tell_line(semaphore):
        @pl.when(z < dims - 1)
        def _():
            pl.semaphore_signal(semaphore, inc=1, device_id=at(dim=(z + 1) % dims), device_id_type=MESH)

        @pl.when(z > 0)
        def _():
            pl.semaphore_signal(semaphore, inc=1, device_id=at(dim=(z + dims - 1) % dims), device_id_type=MESH)

    load_lists(0).start()
    tell_line(barrier)
    probes_in = pltpu.make_async_copy(probes_hbm, probes_ref, load_p)
    ids_in = pltpu.make_async_copy(ids_hbm, ids_ref, load_i)
    ids_in.start()
    probes_in.start()
    queries_in.start()
    for peer in peers:
        pl.semaphore_signal(barrier, inc=1, device_id=peer, device_id_type=MESH)
    load_lists(1).start()
    load_lists(2).start()

    row = lax.broadcasted_iota(jnp.int32, (STEP_ROWS, STEP_ROWS), 0)
    col = lax.broadcasted_iota(jnp.int32, (STEP_ROWS, STEP_ROWS), 1)
    source = (row // GROUP_ROWS) * GROUP_ROWS + (row % GROUP_LISTS) * LIST_LEN + (row // GROUP_LISTS) % LIST_LEN
    perm[...] = jnp.where(col == source, 1.0, 0.0).astype(jnp.bfloat16)

    def arrange(turn):
        block = block_at(turn)
        moved = jnp.dot(perm[...], raw[step_rows(block), :], preferred_element_type=jnp.float32)
        vecs[step_rows(block), :] = moved.astype(jnp.bfloat16)

    window = REUSE_Y // 2
    load_lists(0).wait()
    arrange(0)
    pl.semaphore_wait(barrier, len(peers) + beside)
    for chunk in range(window):
        y_copy(chunk).start()
    tell_line(met.at[0])
    acc[...] = jnp.zeros_like(acc)
    ids_in.wait()
    for which, peer in enumerate((twin, across, far)):
        id_copy(which, peer).start()
    ids_all[s] = ids_ref[...]
    probes_in.wait()
    queries_in.wait()

    def name_candidates(tile, carry):
        cols = pl.ds(pl.multiple_of(z * width + tile * LANES, LANES), LANES)
        probe = probes_ref[:, cols]
        lane, page = probe % LANES, probe // LANES
        pages = lists_dev // LANES
        for member in range(LIST_LEN):
            got = jnp.zeros((probe.shape[0], LANES), jnp.int32)
            for number in range(4 * pages):
                table = ids_all[number // pages, member:member + 1, (number % pages) * LANES:(number % pages + 1) * LANES]
                table = jnp.broadcast_to(table, (probe.shape[0], LANES))
                picked = jnp.take_along_axis(table, lane, axis=1, mode='promise_in_bounds')
                got = jnp.where(page == number, picked, got)
            tiles_half = width // 2 // LANES
            place = pl.ds(pl.multiple_of(tile % tiles_half * LANES, LANES), LANES)
            cand_ids[tile // tiles_half, member, :, place] = got.astype(jnp.float32)
        return carry

    def list_block(step):
        return block_at(step % block_steps)

    def score(step, heads, part):
        lists = vecs[step_rows(jnp.where(step < 2 * block_steps, step // block_steps * block_steps + list_block(step), step)), :]
        rows = pl.ds(pl.multiple_of(part * width, width), width)
        scores = lax.dot_general(lists, qv[rows, :], (((1,), (1,)), ((), ())), preferred_element_type=jnp.float32)
        for tile in range(width // LANES):
            probe = probes_ref[:, pl.ds(pl.multiple_of(part * width + tile * LANES, LANES), LANES)]
            low, head = probe % GROUP_LISTS, probe // GROUP_LISTS
            hits = [head == want for want in heads]
            lanes = slice(tile * LANES, (tile + 1) * LANES)
            half, place = divmod(tile * LANES, width // 2)
            kept_lanes = slice(place, place + LANES)
            for member in range(LIST_LEN):
                kept = acc[part, half, member, :, kept_lanes]
                for group, hit in enumerate(hits):
                    first = group * GROUP_ROWS + member * GROUP_LISTS
                    picked = jnp.take_along_axis(scores[first:first + GROUP_LISTS, lanes], low, axis=0, mode='promise_in_bounds')
                    kept = jnp.where(hit, picked, kept)
                acc[part, half, member, :, kept_lanes] = kept

    def heads_at(step):
        local = step < 2 * block_steps
        group = step - 2 * block_steps
        base = block_groups * jnp.where(step < block_steps, s, twin) + STEP_GROUPS * list_block(step)
        heads = []
        for which in range(STEP_GROUPS):
            home = across if which < 2 else far
            side = x if which % 2 == 0 else other_x
            heads.append(jnp.where(local, base + which, block_groups * home + chunks // 2 * side + group))
        return heads

    last = 2 * block_steps + chunks // 2 - 1

    spare_copy = remote(piece(chunks // 2 * other_x + (chunks - 1) // 2, chunks - 1), slot(chunks - 1, 1),
                        send_x, recv_x.at[REUSE_X], at(shard=across))

    split = chunks - 2

    def split_half(buffer, half):
        return buffer.at[pl.ds(half * (PIECE_ROWS // 2), PIECE_ROWS // 2)]

    def y_half(half):
        return remote(split_half(piece(chunks // 2 * x + split // 2, split), half), split_half(slot(split, 0), half),
                      send_y, recv_y.at[REUSE_Y + half], at(shard=across))

    def x_half(half):
        return remote(split_half(slot(split, 0), half), split_half(slot(split, 1), half),
                      send_x, recv_x.at[REUSE_X + 1 + half], at(rep=other_x))

    def d_half(which, half):
        return remote(split_half(slot(split, which), half), split_half(slot(split, which + 2), half),
                      send_d, recv_d.at[split // 2], at(shard=twin))

    def pass_split(which):
        for half in range(2):
            if which == 0:
                y_half(half).wait_recv()
                x_half(half).start()
            else:
                x_half(half).wait_recv()
            d_half(which, half).start()

    def pass_y(chunk):
        y_copy(chunk).wait_recv()
        if not (isinstance(chunk, int) and chunk == chunks - 1):
            x_copy(chunk).start()
        dy_copy(chunk).start()

        if isinstance(chunk, int) and chunk + window == split:
            for half in range(2):
                y_half(half).start()
        else:
            @pl.when(chunk + window < chunks)
            def _():
                y_copy(chunk + window).start()

        @pl.when(chunk + window == chunks)
        def _():
            spare_copy.start()

    def pass_x(chunk):
        if isinstance(chunk, int) and chunk == chunks - 1:
            spare_copy.wait_recv()
        else:
            x_copy(chunk).wait_recv()
        dx_copy(chunk).start()

    def await_step(step):
        await_recv(vecs.at[pl.ds(0, 4 * PIECE_ROWS)], recv_d.at[step - 2 * block_steps])

    def score_all(step):
        heads = heads_at(step)
        for part in range(dims):
            score(step, heads, part)

    def early(step, carry):
        own_copy(block_at(step)).start()

        @pl.when(step >= 1)
        def _():
            pass_y(step - 1)

        @pl.when(step >= 5)
        def _():
            pass_x(step - 5)

        @pl.when(step == 0)
        def _():
            load_lists(1).wait()

        @pl.when(step == block_steps // 2 - 1)
        def _():
            load_lists(2).wait()
        score_all(step)
        arrange(step + 1)
        return carry

    def middle(step, carry):
        pass_y(step - 1)
        pass_x(step - 5)

        @pl.when(step == block_steps - 1)
        def _():
            own_copy(block_at(step)).start()

        @pl.when((step == block_steps) | (step == block_steps + block_steps // 2))
        def _():
            await_recv(vecs.at[pl.ds(0, block_rows // 2)], recv_o.at[step // (block_steps // 2) - 2])

        @pl.when(step >= 2 * block_steps)
        def _():
            await_step(step)
        score_all(step)
        return carry

    late_plan = {
        last - 5: ('y25', 'x21', 'x22'),
        last - 4: ('y26', 'x23', 'y27', 'x24'),
        last - 3: ('y28', 'x25', 'names', 'y29', 'x26'),
        last - 2: ('y30', 'x27', 'y31', 'x28', 'x29'),
        last - 1: ('x31', 'x30'),
    }

    def late(step, carry):
        for when, plan in late_plan.items():
            @pl.when(step == when)
            def _(plan=plan):
                for word in plan:
                    if word == 'names':
                        await_recv(ids_all.at[pl.ds(0, 3)], recv_i)
                        lax.fori_loop(0, width // LANES, name_candidates, 0)
                    else:
                        which, number = 'yx'.index(word[0]), int(word[1:])
                        if number == split:
                            pass_split(which)
                        else:
                            (pass_y, pass_x)[which](number)

        await_step(step)
        score_all(step)
        return carry

    lax.fori_loop(0, block_steps - 1, early, 0)
    lax.fori_loop(block_steps - 1, last - 5, middle, 0)
    pl.semaphore_wait(met.at[0], beside)
    tell_line(met.at[1])
    lax.fori_loop(last - 5, last, late, 0)
    pl.semaphore_wait(met.at[1], beside)
    await_step(jnp.int32(last))
    last_heads = heads_at(jnp.int32(last))

    leads, follows = outer & (s % 2 == 0), outer & (s % 2 == 1)

    def send_cross(*plan):
        for far_place, half in plan:
            for sub in range(2):
                cross_copy((far_outer, far_inner)[far_place], far_place, half, sub).start()

    def send_near():
        for half in range(2):
            near_copy(half).start()

    def finish(turn, carry):
        @pl.when(leads & (turn == 1))
        def _():
            send_cross((0, 0))

        @pl.when(leads & (turn == 2))
        def _():
            send_cross((1, 0), (0, 1), (1, 1))

        @pl.when(follows & (turn == 3))
        def _():
            send_cross((0, 0), (1, 0))

        @pl.when((leads & (turn == 3)) | (jnp.logical_not(outer) & (turn == 1)))
        def _():
            send_near()
        score(jnp.int32(last), last_heads, target_at(turn))
        return carry

    lax.fori_loop(0, dims, finish, 0)

    @pl.when(follows)
    def _():
        send_cross((0, 1), (1, 1))
        send_near()

    @pl.when(jnp.logical_not(outer))
    def _():
        for half in range(2):
            for merge, target in enumerate((far_outer, far_inner)):
                for sub in range(2):
                    part_wait(merge, half, sub)
                    parts[merge, half, some_members(sub)] += acc[target, half, some_members(sub)]
                    merged_copy(merge, half, sub).start()

    tiles = width // 2 // LANES
    for half in range(2):
        await_recv(parts.at[2, half], landed(2, half))
        for sub in range(2):
            part_wait(3, half, sub)
        scores, names = [], []
        for member in range(LIST_LEN):
            total = acc[z, half, member] + parts[2, half, member] + parts[3, half, member]
            name = cand_ids[half, member]
            real = name >= 0.0
            scores.append(jnp.where(real, total, -jnp.inf))
            names.append(jnp.where(real, name, BIG))
        for place in range(TOP_K):
            best = functools.reduce(jnp.maximum, scores)
            best = jnp.max(best, axis=0, keepdims=True)
            tied = [jnp.where(score_j == best, name_j, BIG) for score_j, name_j in zip(scores, names)]
            first = jnp.min(functools.reduce(jnp.minimum, tied), axis=0, keepdims=True)
            for tile in range(tiles):
                lanes = slice(tile * LANES, (tile + 1) * LANES)
                line = place * tiles + tile
                res[z, half, line:line + 1, :] = best[:, lanes]
                res[z, half, TOP_K * tiles + line:TOP_K * tiles + line + 1, :] = first[:, lanes]
            if place + 1 < TOP_K:
                scores = [jnp.where(name_j == first, -jnp.inf, score_j) for score_j, name_j in zip(scores, names)]
        if half == 0:
            await_send(vecs.at[pl.ds(0, block_rows)], send_o)
            await_send(ids_all.at[pl.ds(0, 3)], send_i)
        else:
            await_send(vecs.at[pl.ds(0, chunks * PIECE_ROWS)], send_y)
            await_send(vecs.at[pl.ds(0, chunks * PIECE_ROWS)], send_x)
            await_send(vecs.at[pl.ds(0, 2 * chunks * PIECE_ROWS)], send_d)
        for which in range(dims - 1):
            res_copy(target_at(which), half).start()

    await_send(parts.at[pl.ds(0, 3)], send_r)
    await_send(res.at[pl.ds(0, dims - 1)], send_g)
    await_recv(res.at[pl.ds(0, dims - 1)], recv_g)


def place_kernel(res, out_s, out_i):
    dims, halves, lines, _ = res.shape
    tiles = lines // (2 * TOP_K)
    for part in range(dims):
        for half in range(halves):
            for tile in range(tiles):
                first = ((part * halves + half) * tiles + tile) * LANES
                out_s[:, first:first + LANES] = res[part, half, pl.ds(tile, TOP_K, stride=tiles), :]
                out_i[:, first:first + LANES] = res[part, half, pl.ds(TOP_K * tiles + tile, TOP_K, stride=tiles), :].astype(jnp.int32)


def solution(mesh):
    dims = mesh.shape['dim']
    row_spec = P(('rep', 'shard'), None)

    def local_search(queries, list_vecs, list_ids, probes):
        rows_q, depth = queries.shape
        lists_dev, list_len, _ = list_vecs.shape
        probe_count = probes.shape[1]
        block_rows = lists_dev * list_len
        block_steps = block_rows // STEP_ROWS
        chunks = lists_dev // GROUP_LISTS
        width = rows_q // dims
        dma = pltpu.SemaphoreType.DMA
        any_spec = pl.BlockSpec(memory_space=pl.ANY)
        vmem_spec = pl.BlockSpec(memory_space=pltpu.VMEM)
        found = pl.pallas_call(
            functools.partial(search_kernel, dims),
            out_shape=pltpu.VMEM((dims, 2, TOP_K * width // LANES, LANES), jnp.float32),
            in_specs=[any_spec] * 4,
            out_specs=vmem_spec,
            scratch_shapes=[
                pltpu.VMEM((block_rows, depth), jnp.bfloat16),
                pltpu.VMEM((rows_q, depth), jnp.bfloat16),
                pltpu.VMEM((4 * block_rows, depth), jnp.bfloat16),
                pltpu.VMEM((STEP_ROWS, STEP_ROWS), jnp.bfloat16),
                pltpu.VMEM((dims, 2, LIST_LEN, probe_count, width // 2), jnp.float32),
                pltpu.VMEM((4, 2, LIST_LEN, probe_count, width // 2), jnp.float32),
                pltpu.VMEM((4, LIST_LEN, lists_dev), jnp.int32),
                pltpu.VMEM((2, LIST_LEN, probe_count, width // 2), jnp.float32),
                pltpu.VMEM((probe_count, rows_q), jnp.int32),
                pltpu.VMEM((LIST_LEN, lists_dev), jnp.int32),
                dma, dma,
                dma((3,)), dma,
                dma, dma((2,)),
                dma, dma((REUSE_Y + 2,)), dma, dma((REUSE_X + 3,)),
                dma, dma((chunks // 2,)),
                dma, dma, dma, dma((14,)), dma, dma,
                pltpu.SemaphoreType.REGULAR((2,)),
            ],
            compiler_params=pltpu.CompilerParams(collective_id=0, has_side_effects=True, vmem_limit_bytes=60 * 2**20),
            name='ivf_search',
        )(queries, list_vecs.reshape(block_rows, depth), probes.T, list_ids.T)
        scores, ids = pl.pallas_call(
            place_kernel,
            out_shape=(jax.ShapeDtypeStruct((TOP_K, rows_q), jnp.float32),
                       jax.ShapeDtypeStruct((TOP_K, rows_q), jnp.int32)),
            in_specs=[vmem_spec],
            out_specs=(vmem_spec, vmem_spec),
            compiler_params=pltpu.CompilerParams(vmem_limit_bytes=4 * 2**20),
            name='place',
        )(found)
        return scores.T, ids.T

    return jax.shard_map(local_search, mesh=mesh,
                         in_specs=(P(('rep', 'shard'), 'dim'), P('shard', None, 'dim'), P('shard', None), row_spec),
                         out_specs=(row_spec, row_spec), check_vma=False)
```

```python
import functools

import jax
import jax.numpy as jnp
from jax import lax
from jax.experimental import pallas as pl
from jax.experimental.pallas import tpu as pltpu
from jax.sharding import PartitionSpec as P

TOP_K = 10
LIST_LEN = 8
GROUP_LISTS = 8
GROUP_ROWS = GROUP_LISTS * LIST_LEN
STEP_GROUPS = 4
STEP_ROWS = STEP_GROUPS * GROUP_ROWS
PIECE_ROWS = GROUP_ROWS // 2
LANES = 128
REUSE_Y, REUSE_X = 8, 12
MESH = pl.DeviceIdType.MESH
BIG = 1e9


def flip(index, bit):
    return index + bit - 2 * bit * ((index // bit) % 2)


def search_kernel(dims, q_hbm, l_hbm, probes_hbm, ids_hbm, res,
                  raw, qv, vecs, perm, acc, parts, ids_all, cand_ids, probes_ref, ids_ref, load_p, load_i,
                  load_l, load_q, send_o, recv_o, send_y, recv_y, send_x, recv_x,
                  send_d, recv_d, send_i, recv_i, send_r, recv_r, send_g, recv_g, met):
    rows_q = qv.shape[0]
    lists_dev = ids_ref.shape[1]
    block_rows = lists_dev * LIST_LEN
    block_groups = lists_dev // GROUP_LISTS
    chunks = block_groups
    block_steps = block_groups // STEP_GROUPS
    width = rows_q // dims
    x, z, s = lax.axis_index('rep'), lax.axis_index('dim'), lax.axis_index('shard')
    twin, across, far = flip(s, 1), flip(s, 2), flip(flip(s, 1), 2)
    other_x = 1 - x

    def at(**place):
        return {'rep': x, 'dim': z, 'shard': s, **place}

    def step_rows(step):
        return pl.ds(pl.multiple_of(step * STEP_ROWS, STEP_ROWS), STEP_ROWS)

    def remote(src, dst, send, recv, device):
        return pltpu.make_async_remote_copy(src_ref=src, dst_ref=dst, send_sem=send, recv_sem=recv,
                                            device_id=device, device_id_type=MESH)

    def await_recv(buffer, semaphore):
        remote(buffer, buffer, send_i, semaphore, at()).wait_recv()

    def await_send(buffer, semaphore):
        remote(buffer, buffer, semaphore, recv_i, at()).wait_send()

    def load_lists(number):
        half = block_steps // 2
        first, count = ((half * x, 1), (half * x + 1, half - 1), (half * other_x, half))[number]
        rows = pl.ds(pl.multiple_of(first * STEP_ROWS, STEP_ROWS), count * STEP_ROWS)
        return pltpu.make_async_copy(l_hbm.at[rows], raw.at[rows], load_l.at[number])

    queries_in = pltpu.make_async_copy(q_hbm, qv, load_q)

    def own_copy(block):
        return remote(vecs.at[step_rows(block)], vecs.at[step_rows(block_steps + block)],
                      send_o, recv_o.at[(block // (block_steps // 2) + x) % 2], at(shard=twin))

    def piece(group, chunk):
        first = pl.multiple_of(group * GROUP_ROWS + chunk % 2 * PIECE_ROWS, PIECE_ROWS)
        return vecs.at[pl.ds(first, PIECE_ROWS)]

    def slot(chunk, which):
        return piece(2 * block_groups + STEP_GROUPS * (chunk // 2) + which, chunk)

    def y_copy(chunk):
        return remote(piece(chunks // 2 * x + chunk // 2, chunk), slot(chunk, 0), send_y, recv_y.at[chunk % REUSE_Y], at(shard=across))

    def x_copy(chunk):
        return remote(slot(chunk, 0), slot(chunk, 1), send_x, recv_x.at[chunk % REUSE_X], at(rep=other_x))

    def dy_copy(chunk):
        return remote(slot(chunk, 0), slot(chunk, 2), send_d, recv_d.at[chunk // 2], at(shard=twin))

    def dx_copy(chunk):
        return remote(slot(chunk, 1), slot(chunk, 3), send_d, recv_d.at[chunk // 2], at(shard=twin))

    def id_copy(which, peer):
        return remote(ids_ref, ids_all.at[s], send_i, recv_i, at(shard=peer))

    outer = z % 3 == 0
    mate, far_outer = flip(z, 1), jnp.where(z < 2, dims - 1, 0)
    far_inner = flip(far_outer, 1)

    def landed(place, half, sub=0):
        return recv_r.at[12 + half if place == 2 else 4 * min(place, 2) + 2 * half + sub]

    def some_members(sub):
        return pl.ds(sub * (LIST_LEN // 2), LIST_LEN // 2)

    def near_copy(half):
        return remote(acc.at[mate, half], parts.at[2, half], send_r, landed(2, half), at(dim=mate))

    def cross_copy(target, place, half, sub):
        return remote(acc.at[target, half, some_members(sub)], parts.at[place, half, some_members(sub)], send_r,
                      landed(place, half, sub), at(dim=mate))

    def merged_copy(merge, half, sub):
        return remote(parts.at[merge, half, some_members(sub)], parts.at[3, half, some_members(sub)], send_r,
                      landed(3, half, sub), at(dim=(far_outer, far_inner)[merge]))

    def part_wait(place, half, sub):
        await_recv(parts.at[place, half, some_members(sub)], landed(place, half, sub))

    def res_copy(target, half):
        return remote(res.at[z, half], res.at[z, half], send_g, recv_g, at(dim=target))

    def target_at(turn):
        first, second, third = (jnp.where(outer, one, two) for one, two in ((far_outer, mate), (far_inner, far_outer), (mate, far_inner)))
        return jnp.where(turn == 0, first, jnp.where(turn == 1, second, jnp.where(turn == 2, third, z)))

    def block_at(turn):
        return (block_steps // 2 * x + turn) % block_steps

    barrier = pltpu.get_barrier_semaphore()
    peers = [at(shard=twin), at(shard=across), at(shard=far), at(rep=other_x)]
    beside = jnp.where(outer, 1, 2)

    def tell_line(semaphore):
        @pl.when(z < dims - 1)
        def _():
            pl.semaphore_signal(semaphore, inc=1, device_id=at(dim=(z + 1) % dims), device_id_type=MESH)

        @pl.when(z > 0)
        def _():
            pl.semaphore_signal(semaphore, inc=1, device_id=at(dim=(z + dims - 1) % dims), device_id_type=MESH)

    load_lists(0).start()
    tell_line(barrier)
    probes_in = pltpu.make_async_copy(probes_hbm, probes_ref, load_p)
    ids_in = pltpu.make_async_copy(ids_hbm, ids_ref, load_i)
    ids_in.start()
    probes_in.start()
    queries_in.start()
    for peer in peers:
        pl.semaphore_signal(barrier, inc=1, device_id=peer, device_id_type=MESH)
    load_lists(1).start()
    load_lists(2).start()

    row = lax.broadcasted_iota(jnp.int32, (STEP_ROWS, STEP_ROWS), 0)
    col = lax.broadcasted_iota(jnp.int32, (STEP_ROWS, STEP_ROWS), 1)
    source = (row // GROUP_ROWS) * GROUP_ROWS + (row % GROUP_LISTS) * LIST_LEN + (row // GROUP_LISTS) % LIST_LEN
    perm[...] = jnp.where(col == source, 1.0, 0.0).astype(jnp.bfloat16)

    def arrange(turn):
        block = block_at(turn)
        moved = jnp.dot(perm[...], raw[step_rows(block), :], preferred_element_type=jnp.float32)
        vecs[step_rows(block), :] = moved.astype(jnp.bfloat16)

    window = REUSE_Y // 2
    load_lists(0).wait()
    arrange(0)
    pl.semaphore_wait(barrier, len(peers) + beside)
    for chunk in range(window):
        y_copy(chunk).start()
    tell_line(met.at[0])
    acc[...] = jnp.zeros_like(acc)
    ids_in.wait()
    for which, peer in enumerate((twin, across, far)):
        id_copy(which, peer).start()
    ids_all[s] = ids_ref[...]
    probes_in.wait()
    queries_in.wait()

    def name_candidates(tile, carry):
        cols = pl.ds(pl.multiple_of(z * width + tile * LANES, LANES), LANES)
        probe = probes_ref[:, cols]
        lane, page = probe % LANES, probe // LANES
        pages = lists_dev // LANES
        for member in range(LIST_LEN):
            got = jnp.zeros((probe.shape[0], LANES), jnp.int32)
            for number in range(4 * pages):
                table = ids_all[number // pages, member:member + 1, (number % pages) * LANES:(number % pages + 1) * LANES]
                table = jnp.broadcast_to(table, (probe.shape[0], LANES))
                picked = jnp.take_along_axis(table, lane, axis=1, mode='promise_in_bounds')
                got = jnp.where(page == number, picked, got)
            tiles_half = width // 2 // LANES
            place = pl.ds(pl.multiple_of(tile % tiles_half * LANES, LANES), LANES)
            cand_ids[tile // tiles_half, member, :, place] = got.astype(jnp.float32)
        return carry

    def list_block(step):
        return block_at(step % block_steps)

    def score(step, heads, part):
        lists = vecs[step_rows(jnp.where(step < 2 * block_steps, step // block_steps * block_steps + list_block(step), step)), :]
        rows = pl.ds(pl.multiple_of(part * width, width), width)
        scores = lax.dot_general(lists, qv[rows, :], (((1,), (1,)), ((), ())), preferred_element_type=jnp.float32)
        for tile in range(width // LANES):
            probe = probes_ref[:, pl.ds(pl.multiple_of(part * width + tile * LANES, LANES), LANES)]
            low, head = probe % GROUP_LISTS, probe // GROUP_LISTS
            hits = [head == want for want in heads]
            lanes = slice(tile * LANES, (tile + 1) * LANES)
            half, place = divmod(tile * LANES, width // 2)
            kept_lanes = slice(place, place + LANES)
            for member in range(LIST_LEN):
                kept = acc[part, half, member, :, kept_lanes]
                for group, hit in enumerate(hits):
                    first = group * GROUP_ROWS + member * GROUP_LISTS
                    picked = jnp.take_along_axis(scores[first:first + GROUP_LISTS, lanes], low, axis=0, mode='promise_in_bounds')
                    kept = jnp.where(hit, picked, kept)
                acc[part, half, member, :, kept_lanes] = kept

    def heads_at(step):
        local = step < 2 * block_steps
        group = step - 2 * block_steps
        base = block_groups * jnp.where(step < block_steps, s, twin) + STEP_GROUPS * list_block(step)
        heads = []
        for which in range(STEP_GROUPS):
            home = across if which < 2 else far
            side = x if which % 2 == 0 else other_x
            heads.append(jnp.where(local, base + which, block_groups * home + chunks // 2 * side + group))
        return heads

    last = 2 * block_steps + chunks // 2 - 1

    spare_copy = remote(piece(chunks // 2 * other_x + (chunks - 1) // 2, chunks - 1), slot(chunks - 1, 1),
                        send_x, recv_x.at[REUSE_X], at(shard=across))

    split = chunks - 2

    def split_half(buffer, half):
        return buffer.at[pl.ds(half * (PIECE_ROWS // 2), PIECE_ROWS // 2)]

    def y_half(half):
        return remote(split_half(piece(chunks // 2 * x + split // 2, split), half), split_half(slot(split, 0), half),
                      send_y, recv_y.at[REUSE_Y + half], at(shard=across))

    def x_half(half):
        return remote(split_half(slot(split, 0), half), split_half(slot(split, 1), half),
                      send_x, recv_x.at[REUSE_X + 1 + half], at(rep=other_x))

    def d_half(which, half):
        return remote(split_half(slot(split, which), half), split_half(slot(split, which + 2), half),
                      send_d, recv_d.at[split // 2], at(shard=twin))

    def pass_split(which):
        for half in range(2):
            if which == 0:
                y_half(half).wait_recv()
                x_half(half).start()
            else:
                x_half(half).wait_recv()
            d_half(which, half).start()

    def pass_y(chunk):
        y_copy(chunk).wait_recv()
        if not (isinstance(chunk, int) and chunk == chunks - 1):
            x_copy(chunk).start()
        dy_copy(chunk).start()

        if isinstance(chunk, int) and chunk + window == split:
            for half in range(2):
                y_half(half).start()
        else:
            @pl.when(chunk + window < chunks)
            def _():
                y_copy(chunk + window).start()

        @pl.when(chunk + window == chunks)
        def _():
            spare_copy.start()

    def pass_x(chunk):
        if isinstance(chunk, int) and chunk == chunks - 1:
            spare_copy.wait_recv()
        else:
            x_copy(chunk).wait_recv()
        dx_copy(chunk).start()

    def await_step(step):
        await_recv(vecs.at[pl.ds(0, 4 * PIECE_ROWS)], recv_d.at[step - 2 * block_steps])

    def score_all(step):
        heads = heads_at(step)
        for part in range(dims):
            score(step, heads, part)

    def early(step, carry):
        own_copy(block_at(step)).start()

        @pl.when(step >= 1)
        def _():
            pass_y(step - 1)

        @pl.when(step >= 5)
        def _():
            pass_x(step - 5)

        @pl.when(step == 0)
        def _():
            load_lists(1).wait()

        @pl.when(step == block_steps // 2 - 1)
        def _():
            load_lists(2).wait()
        score_all(step)
        arrange(step + 1)
        return carry

    def middle(step, carry):
        pass_y(step - 1)
        pass_x(step - 5)

        @pl.when(step == block_steps - 1)
        def _():
            own_copy(block_at(step)).start()

        @pl.when((step == block_steps) | (step == block_steps + block_steps // 2))
        def _():
            await_recv(vecs.at[pl.ds(0, block_rows // 2)], recv_o.at[step // (block_steps // 2) - 2])

        @pl.when(step >= 2 * block_steps)
        def _():
            await_step(step)
        score_all(step)
        return carry

    late_plan = {
        last - 5: ('y25', 'x21', 'x22'),
        last - 4: ('y26', 'x23', 'y27', 'x24'),
        last - 3: ('y28', 'x25', 'names', 'y29', 'x26'),
        last - 2: ('y30', 'x27', 'y31', 'x28', 'x29'),
        last - 1: ('x31', 'x30'),
    }

    def late(step, carry):
        for when, plan in late_plan.items():
            @pl.when(step == when)
            def _(plan=plan):
                for word in plan:
                    if word == 'names':
                        await_recv(ids_all.at[pl.ds(0, 3)], recv_i)
                        lax.fori_loop(0, width // LANES, name_candidates, 0)
                    else:
                        which, number = 'yx'.index(word[0]), int(word[1:])
                        if number == split:
                            pass_split(which)
                        else:
                            (pass_y, pass_x)[which](number)

        await_step(step)
        score_all(step)
        return carry

    lax.fori_loop(0, block_steps - 1, early, 0)
    lax.fori_loop(block_steps - 1, last - 5, middle, 0)
    pl.semaphore_wait(met.at[0], beside)
    tell_line(met.at[1])
    lax.fori_loop(last - 5, last, late, 0)
    pl.semaphore_wait(met.at[1], beside)
    await_step(jnp.int32(last))
    last_heads = heads_at(jnp.int32(last))

    leads, follows = outer & (s % 2 == 0), outer & (s % 2 == 1)

    def send_cross(*plan):
        for far_place, half in plan:
            for sub in range(2):
                cross_copy((far_outer, far_inner)[far_place], far_place, half, sub).start()

    def send_near():
        for half in range(2):
            near_copy(half).start()

    def finish(turn, carry):
        @pl.when(leads & (turn == 1))
        def _():
            send_cross((0, 0))

        @pl.when(leads & (turn == 2))
        def _():
            send_cross((1, 0), (0, 1), (1, 1))

        @pl.when(follows & (turn == 3))
        def _():
            send_cross((0, 0), (1, 0))

        @pl.when((leads & (turn == 3)) | (jnp.logical_not(outer) & (turn == 1)))
        def _():
            send_near()
        score(jnp.int32(last), last_heads, target_at(turn))
        return carry

    lax.fori_loop(0, dims, finish, 0)

    @pl.when(follows)
    def _():
        send_cross((0, 1), (1, 1))
        send_near()

    @pl.when(jnp.logical_not(outer))
    def _():
        for half in range(2):
            for merge, target in enumerate((far_outer, far_inner)):
                for sub in range(2):
                    part_wait(merge, half, sub)
                    parts[merge, half, some_members(sub)] += acc[target, half, some_members(sub)]
                    merged_copy(merge, half, sub).start()

    tiles = width // 2 // LANES
    for half in range(2):
        await_recv(parts.at[2, half], landed(2, half))
        for sub in range(2):
            part_wait(3, half, sub)
        scores, names = [], []
        for member in range(LIST_LEN):
            total = acc[z, half, member] + parts[2, half, member] + parts[3, half, member]
            name = cand_ids[half, member]
            real = name >= 0.0
            scores.append(jnp.where(real, total, -jnp.inf))
            names.append(jnp.where(real, name, BIG))
        for place in range(TOP_K):
            best = functools.reduce(jnp.maximum, scores)
            best = jnp.max(best, axis=0, keepdims=True)
            tied = [jnp.where(score_j == best, name_j, BIG) for score_j, name_j in zip(scores, names)]
            first = jnp.min(functools.reduce(jnp.minimum, tied), axis=0, keepdims=True)
            for tile in range(tiles):
                lanes = slice(tile * LANES, (tile + 1) * LANES)
                line = place * tiles + tile
                res[z, half, line:line + 1, :] = best[:, lanes]
                res[z, half, TOP_K * tiles + line:TOP_K * tiles + line + 1, :] = first[:, lanes]
            if place + 1 < TOP_K:
                scores = [jnp.where(name_j == first, -jnp.inf, score_j) for score_j, name_j in zip(scores, names)]
        if half == 0:
            await_send(vecs.at[pl.ds(0, block_rows)], send_o)
            await_send(ids_all.at[pl.ds(0, 3)], send_i)
        else:
            await_send(vecs.at[pl.ds(0, chunks * PIECE_ROWS)], send_y)
            await_send(vecs.at[pl.ds(0, chunks * PIECE_ROWS)], send_x)
            await_send(vecs.at[pl.ds(0, 2 * chunks * PIECE_ROWS)], send_d)
        for which in range(dims - 1):
            res_copy(jnp.where(which < z, which, which + 1), half).start()

    await_send(parts.at[pl.ds(0, 3)], send_r)
    await_send(res.at[pl.ds(0, dims - 1)], send_g)
    await_recv(res.at[pl.ds(0, dims - 1)], recv_g)


def place_kernel(res, out_s, out_i):
    dims, halves, lines, _ = res.shape
    tiles = lines // (2 * TOP_K)
    for part in range(dims):
        for half in range(halves):
            for tile in range(tiles):
                first = ((part * halves + half) * tiles + tile) * LANES
                out_s[:, first:first + LANES] = res[part, half, pl.ds(tile, TOP_K, stride=tiles), :]
                out_i[:, first:first + LANES] = res[part, half, pl.ds(TOP_K * tiles + tile, TOP_K, stride=tiles), :].astype(jnp.int32)


def solution(mesh):
    dims = mesh.shape['dim']
    row_spec = P(('rep', 'shard'), None)

    def local_search(queries, list_vecs, list_ids, probes):
        rows_q, depth = queries.shape
        lists_dev, list_len, _ = list_vecs.shape
        probe_count = probes.shape[1]
        block_rows = lists_dev * list_len
        block_steps = block_rows // STEP_ROWS
        chunks = lists_dev // GROUP_LISTS
        width = rows_q // dims
        dma = pltpu.SemaphoreType.DMA
        any_spec = pl.BlockSpec(memory_space=pl.ANY)
        vmem_spec = pl.BlockSpec(memory_space=pltpu.VMEM)
        found = pl.pallas_call(
            functools.partial(search_kernel, dims),
            out_shape=pltpu.VMEM((dims, 2, TOP_K * width // LANES, LANES), jnp.float32),
            in_specs=[any_spec] * 4,
            out_specs=vmem_spec,
            scratch_shapes=[
                pltpu.VMEM((block_rows, depth), jnp.bfloat16),
                pltpu.VMEM((rows_q, depth), jnp.bfloat16),
                pltpu.VMEM((4 * block_rows, depth), jnp.bfloat16),
                pltpu.VMEM((STEP_ROWS, STEP_ROWS), jnp.bfloat16),
                pltpu.VMEM((dims, 2, LIST_LEN, probe_count, width // 2), jnp.float32),
                pltpu.VMEM((4, 2, LIST_LEN, probe_count, width // 2), jnp.float32),
                pltpu.VMEM((4, LIST_LEN, lists_dev), jnp.int32),
                pltpu.VMEM((2, LIST_LEN, probe_count, width // 2), jnp.float32),
                pltpu.VMEM((probe_count, rows_q), jnp.int32),
                pltpu.VMEM((LIST_LEN, lists_dev), jnp.int32),
                dma, dma,
                dma((3,)), dma,
                dma, dma((2,)),
                dma, dma((REUSE_Y + 2,)), dma, dma((REUSE_X + 3,)),
                dma, dma((chunks // 2,)),
                dma, dma, dma, dma((14,)), dma, dma,
                pltpu.SemaphoreType.REGULAR((2,)),
            ],
            compiler_params=pltpu.CompilerParams(collective_id=0, has_side_effects=True, vmem_limit_bytes=60 * 2**20),
            name='ivf_search',
        )(queries, list_vecs.reshape(block_rows, depth), probes.T, list_ids.T)
        scores, ids = pl.pallas_call(
            place_kernel,
            out_shape=(jax.ShapeDtypeStruct((TOP_K, rows_q), jnp.float32),
                       jax.ShapeDtypeStruct((TOP_K, rows_q), jnp.int32)),
            in_specs=[vmem_spec],
            out_specs=(vmem_spec, vmem_spec),
            compiler_params=pltpu.CompilerParams(vmem_limit_bytes=4 * 2**20),
            name='place',
        )(found)
        return scores.T, ids.T

    return jax.shard_map(local_search, mesh=mesh,
                         in_specs=(P(('rep', 'shard'), 'dim'), P('shard', None, 'dim'), P('shard', None), row_spec),
                         out_specs=(row_spec, row_spec), check_vma=False)
```

```python
import functools

import jax
import jax.numpy as jnp
from jax import lax
from jax.experimental import pallas as pl
from jax.experimental.pallas import tpu as pltpu
from jax.sharding import PartitionSpec as P

TOP_K = 10
LIST_LEN = 8
GROUP_LISTS = 8
GROUP_ROWS = GROUP_LISTS * LIST_LEN
STEP_GROUPS = 4
STEP_ROWS = STEP_GROUPS * GROUP_ROWS
PIECE_ROWS = GROUP_ROWS // 2
LANES = 128
REUSE_Y, REUSE_X = 8, 12
MESH = pl.DeviceIdType.MESH
BIG = 1e9


def flip(index, bit):
    return index + bit - 2 * bit * ((index // bit) % 2)


def search_kernel(dims, q_hbm, l_hbm, probes_hbm, ids_hbm, res,
                  raw, qv, vecs, perm, acc, parts, ids_all, cand_ids, probes_ref, ids_ref, load_p, load_i,
                  load_l, load_q, send_o, recv_o, send_y, recv_y, send_x, recv_x,
                  send_d, recv_d, send_i, recv_i, send_r, recv_r, send_g, recv_g, met):
    rows_q = qv.shape[0]
    lists_dev = ids_ref.shape[1]
    block_rows = lists_dev * LIST_LEN
    block_groups = lists_dev // GROUP_LISTS
    chunks = block_groups
    block_steps = block_groups // STEP_GROUPS
    width = rows_q // dims
    x, z, s = lax.axis_index('rep'), lax.axis_index('dim'), lax.axis_index('shard')
    twin, across, far = flip(s, 1), flip(s, 2), flip(flip(s, 1), 2)
    other_x = 1 - x

    def at(**place):
        return {'rep': x, 'dim': z, 'shard': s, **place}

    def step_rows(step):
        return pl.ds(pl.multiple_of(step * STEP_ROWS, STEP_ROWS), STEP_ROWS)

    def remote(src, dst, send, recv, device):
        return pltpu.make_async_remote_copy(src_ref=src, dst_ref=dst, send_sem=send, recv_sem=recv,
                                            device_id=device, device_id_type=MESH)

    def await_recv(buffer, semaphore):
        remote(buffer, buffer, send_i, semaphore, at()).wait_recv()

    def await_send(buffer, semaphore):
        remote(buffer, buffer, semaphore, recv_i, at()).wait_send()

    def load_lists(number):
        half = block_steps // 2
        first, count = ((half * x, 1), (half * x + 1, half - 1), (half * other_x, half))[number]
        rows = pl.ds(pl.multiple_of(first * STEP_ROWS, STEP_ROWS), count * STEP_ROWS)
        return pltpu.make_async_copy(l_hbm.at[rows], raw.at[rows], load_l.at[number])

    queries_in = pltpu.make_async_copy(q_hbm, qv, load_q)

    def own_copy(block):
        return remote(vecs.at[step_rows(block)], vecs.at[step_rows(block_steps + block)],
                      send_o, recv_o.at[(block // (block_steps // 2) + x) % 2], at(shard=twin))

    def piece(group, chunk):
        first = pl.multiple_of(group * GROUP_ROWS + chunk % 2 * PIECE_ROWS, PIECE_ROWS)
        return vecs.at[pl.ds(first, PIECE_ROWS)]

    def slot(chunk, which):
        return piece(2 * block_groups + STEP_GROUPS * (chunk // 2) + which, chunk)

    def y_copy(chunk):
        return remote(piece(chunks // 2 * x + chunk // 2, chunk), slot(chunk, 0), send_y, recv_y.at[chunk % REUSE_Y], at(shard=across))

    def x_copy(chunk):
        return remote(slot(chunk, 0), slot(chunk, 1), send_x, recv_x.at[chunk % REUSE_X], at(rep=other_x))

    def dy_copy(chunk):
        return remote(slot(chunk, 0), slot(chunk, 2), send_d, recv_d.at[chunk // 2], at(shard=twin))

    def dx_copy(chunk):
        return remote(slot(chunk, 1), slot(chunk, 3), send_d, recv_d.at[chunk // 2], at(shard=twin))

    def id_copy(which, peer):
        return remote(ids_ref, ids_all.at[s], send_i, recv_i, at(shard=peer))

    outer = z % 3 == 0
    mate, far_outer = flip(z, 1), jnp.where(z < 2, dims - 1, 0)
    far_inner = flip(far_outer, 1)

    def landed(place, half, sub=0):
        return recv_r.at[12 + half if place == 2 else 4 * min(place, 2) + 2 * half + sub]

    def some_members(sub):
        return pl.ds(sub * (LIST_LEN // 2), LIST_LEN // 2)

    def near_copy(half):
        return remote(acc.at[mate, half], parts.at[2, half], send_r, landed(2, half), at(dim=mate))

    def cross_copy(target, place, half, sub):
        return remote(acc.at[target, half, some_members(sub)], parts.at[place, half, some_members(sub)], send_r,
                      landed(place, half, sub), at(dim=mate))

    def merged_copy(merge, half, sub):
        return remote(parts.at[merge, half, some_members(sub)], parts.at[3, half, some_members(sub)], send_r,
                      landed(3, half, sub), at(dim=(far_outer, far_inner)[merge]))

    def part_wait(place, half, sub):
        await_recv(parts.at[place, half, some_members(sub)], landed(place, half, sub))

    def res_copy(target, half):
        return remote(res.at[z, half], res.at[z, half], send_g, recv_g, at(dim=target))

    def target_at(turn):
        first, second, third = (jnp.where(outer, one, two) for one, two in ((far_inner, mate), (far_outer, far_inner), (mate, far_outer)))
        return jnp.where(turn == 0, first, jnp.where(turn == 1, second, jnp.where(turn == 2, third, z)))

    def block_at(turn):
        return (block_steps // 2 * x + turn) % block_steps

    barrier = pltpu.get_barrier_semaphore()
    peers = [at(shard=twin), at(shard=across), at(shard=far), at(rep=other_x)]
    beside = jnp.where(outer, 1, 2)

    def tell_line(semaphore):
        @pl.when(z < dims - 1)
        def _():
            pl.semaphore_signal(semaphore, inc=1, device_id=at(dim=(z + 1) % dims), device_id_type=MESH)

        @pl.when(z > 0)
        def _():
            pl.semaphore_signal(semaphore, inc=1, device_id=at(dim=(z + dims - 1) % dims), device_id_type=MESH)

    load_lists(0).start()
    tell_line(barrier)
    probes_in = pltpu.make_async_copy(probes_hbm, probes_ref, load_p)
    ids_in = pltpu.make_async_copy(ids_hbm, ids_ref, load_i)
    ids_in.start()
    probes_in.start()
    queries_in.start()
    for peer in peers:
        pl.semaphore_signal(barrier, inc=1, device_id=peer, device_id_type=MESH)
    load_lists(1).start()
    load_lists(2).start()

    row = lax.broadcasted_iota(jnp.int32, (STEP_ROWS, STEP_ROWS), 0)
    col = lax.broadcasted_iota(jnp.int32, (STEP_ROWS, STEP_ROWS), 1)
    source = (row // GROUP_ROWS) * GROUP_ROWS + (row % GROUP_LISTS) * LIST_LEN + (row // GROUP_LISTS) % LIST_LEN
    perm[...] = jnp.where(col == source, 1.0, 0.0).astype(jnp.bfloat16)

    def arrange(turn):
        block = block_at(turn)
        moved = jnp.dot(perm[...], raw[step_rows(block), :], preferred_element_type=jnp.float32)
        vecs[step_rows(block), :] = moved.astype(jnp.bfloat16)

    window = REUSE_Y // 2
    load_lists(0).wait()
    arrange(0)
    pl.semaphore_wait(barrier, len(peers) + beside)
    for chunk in range(window):
        y_copy(chunk).start()
    tell_line(met.at[0])
    acc[...] = jnp.zeros_like(acc)
    ids_in.wait()
    for which, peer in enumerate((twin, across, far)):
        id_copy(which, peer).start()
    ids_all[s] = ids_ref[...]
    probes_in.wait()
    queries_in.wait()

    def name_candidates(tile, carry):
        cols = pl.ds(pl.multiple_of(z * width + tile * LANES, LANES), LANES)
        probe = probes_ref[:, cols]
        lane, page = probe % LANES, probe // LANES
        pages = lists_dev // LANES
        for member in range(LIST_LEN):
            got = jnp.zeros((probe.shape[0], LANES), jnp.int32)
            for number in range(4 * pages):
                table = ids_all[number // pages, member:member + 1, (number % pages) * LANES:(number % pages + 1) * LANES]
                table = jnp.broadcast_to(table, (probe.shape[0], LANES))
                picked = jnp.take_along_axis(table, lane, axis=1, mode='promise_in_bounds')
                got = jnp.where(page == number, picked, got)
            tiles_half = width // 2 // LANES
            place = pl.ds(pl.multiple_of(tile % tiles_half * LANES, LANES), LANES)
            cand_ids[tile // tiles_half, member, :, place] = got.astype(jnp.float32)
        return carry

    def list_block(step):
        return block_at(step % block_steps)

    def score(step, heads, part):
        lists = vecs[step_rows(jnp.where(step < 2 * block_steps, step // block_steps * block_steps + list_block(step), step)), :]
        rows = pl.ds(pl.multiple_of(part * width, width), width)
        scores = lax.dot_general(lists, qv[rows, :], (((1,), (1,)), ((), ())), preferred_element_type=jnp.float32)
        for tile in range(width // LANES):
            probe = probes_ref[:, pl.ds(pl.multiple_of(part * width + tile * LANES, LANES), LANES)]
            low, head = probe % GROUP_LISTS, probe // GROUP_LISTS
            hits = [head == want for want in heads]
            lanes = slice(tile * LANES, (tile + 1) * LANES)
            half, place = divmod(tile * LANES, width // 2)
            kept_lanes = slice(place, place + LANES)
            for member in range(LIST_LEN):
                kept = acc[part, half, member, :, kept_lanes]
                for group, hit in enumerate(hits):
                    first = group * GROUP_ROWS + member * GROUP_LISTS
                    picked = jnp.take_along_axis(scores[first:first + GROUP_LISTS, lanes], low, axis=0, mode='promise_in_bounds')
                    kept = jnp.where(hit, picked, kept)
                acc[part, half, member, :, kept_lanes] = kept

    def heads_at(step):
        local = step < 2 * block_steps
        group = step - 2 * block_steps
        base = block_groups * jnp.where(step < block_steps, s, twin) + STEP_GROUPS * list_block(step)
        heads = []
        for which in range(STEP_GROUPS):
            home = across if which < 2 else far
            side = x if which % 2 == 0 else other_x
            heads.append(jnp.where(local, base + which, block_groups * home + chunks // 2 * side + group))
        return heads

    last = 2 * block_steps + chunks // 2 - 1

    spare_copy = remote(piece(chunks // 2 * other_x + (chunks - 1) // 2, chunks - 1), slot(chunks - 1, 1),
                        send_x, recv_x.at[REUSE_X], at(shard=across))

    split = chunks - 2

    def split_half(buffer, half):
        return buffer.at[pl.ds(half * (PIECE_ROWS // 2), PIECE_ROWS // 2)]

    def y_half(half):
        return remote(split_half(piece(chunks // 2 * x + split // 2, split), half), split_half(slot(split, 0), half),
                      send_y, recv_y.at[REUSE_Y + half], at(shard=across))

    def x_half(half):
        return remote(split_half(slot(split, 0), half), split_half(slot(split, 1), half),
                      send_x, recv_x.at[REUSE_X + 1 + half], at(rep=other_x))

    def d_half(which, half):
        return remote(split_half(slot(split, which), half), split_half(slot(split, which + 2), half),
                      send_d, recv_d.at[split // 2], at(shard=twin))

    def pass_split(which):
        for half in range(2):
            if which == 0:
                y_half(half).wait_recv()
                x_half(half).start()
            else:
                x_half(half).wait_recv()
            d_half(which, half).start()

    def pass_y(chunk):
        y_copy(chunk).wait_recv()
        if not (isinstance(chunk, int) and chunk == chunks - 1):
            x_copy(chunk).start()
        dy_copy(chunk).start()

        if isinstance(chunk, int) and chunk + window == split:
            for half in range(2):
                y_half(half).start()
        else:
            @pl.when(chunk + window < chunks)
            def _():
                y_copy(chunk + window).start()

        @pl.when(chunk + window == chunks)
        def _():
            spare_copy.start()

    def pass_x(chunk):
        if isinstance(chunk, int) and chunk == chunks - 1:
            spare_copy.wait_recv()
        else:
            x_copy(chunk).wait_recv()
        dx_copy(chunk).start()

    def await_step(step):
        await_recv(vecs.at[pl.ds(0, 4 * PIECE_ROWS)], recv_d.at[step - 2 * block_steps])

    def score_all(step):
        heads = heads_at(step)
        for part in range(dims):
            score(step, heads, part)

    def early(step, carry):
        own_copy(block_at(step)).start()

        @pl.when(step >= 1)
        def _():
            pass_y(step - 1)

        @pl.when(step >= 5)
        def _():
            pass_x(step - 5)

        @pl.when(step == 0)
        def _():
            load_lists(1).wait()

        @pl.when(step == block_steps // 2 - 1)
        def _():
            load_lists(2).wait()
        score_all(step)
        arrange(step + 1)
        return carry

    def middle(step, carry):
        pass_y(step - 1)
        pass_x(step - 5)

        @pl.when(step == block_steps - 1)
        def _():
            own_copy(block_at(step)).start()

        @pl.when((step == block_steps) | (step == block_steps + block_steps // 2))
        def _():
            await_recv(vecs.at[pl.ds(0, block_rows // 2)], recv_o.at[step // (block_steps // 2) - 2])

        @pl.when(step >= 2 * block_steps)
        def _():
            await_step(step)
        score_all(step)
        return carry

    late_plan = {
        last - 5: ('y25', 'x21', 'x22'),
        last - 4: ('y26', 'x23', 'y27', 'x24'),
        last - 3: ('y28', 'x25', 'names', 'y29', 'x26'),
        last - 2: ('y30', 'x27', 'y31', 'x28', 'x29'),
        last - 1: ('x31', 'x30'),
    }

    def late(step, carry):
        for when, plan in late_plan.items():
            @pl.when(step == when)
            def _(plan=plan):
                for word in plan:
                    if word == 'names':
                        await_recv(ids_all.at[pl.ds(0, 3)], recv_i)
                        lax.fori_loop(0, width // LANES, name_candidates, 0)
                    else:
                        which, number = 'yx'.index(word[0]), int(word[1:])
                        if number == split:
                            pass_split(which)
                        else:
                            (pass_y, pass_x)[which](number)

        await_step(step)
        score_all(step)
        return carry

    lax.fori_loop(0, block_steps - 1, early, 0)
    lax.fori_loop(block_steps - 1, last - 5, middle, 0)
    pl.semaphore_wait(met.at[0], beside)
    tell_line(met.at[1])
    lax.fori_loop(last - 5, last, late, 0)
    pl.semaphore_wait(met.at[1], beside)
    await_step(jnp.int32(last))
    last_heads = heads_at(jnp.int32(last))

    leads, follows = outer & (s % 2 == 0), outer & (s % 2 == 1)

    def send_cross(*plan):
        for far_place, half in plan:
            for sub in range(2):
                cross_copy((far_outer, far_inner)[far_place], far_place, half, sub).start()

    def send_near():
        for half in range(2):
            near_copy(half).start()

    def finish(turn, carry):
        @pl.when(leads & (turn == 1))
        def _():
            send_cross((1, 0))

        @pl.when(leads & (turn == 2))
        def _():
            send_cross((0, 0), (1, 1), (0, 1))

        @pl.when(follows & (turn == 3))
        def _():
            send_cross((1, 0), (0, 0))

        @pl.when((leads & (turn == 3)) | (jnp.logical_not(outer) & (turn == 1)))
        def _():
            send_near()
        score(jnp.int32(last), last_heads, target_at(turn))
        return carry

    lax.fori_loop(0, dims, finish, 0)

    @pl.when(follows)
    def _():
        send_cross((1, 1), (0, 1))
        send_near()

    @pl.when(jnp.logical_not(outer))
    def _():
        for half in range(2):
            for merge, target in ((1, far_inner), (0, far_outer)):
                for sub in range(2):
                    part_wait(merge, half, sub)
                    parts[merge, half, some_members(sub)] += acc[target, half, some_members(sub)]
                    merged_copy(merge, half, sub).start()

    tiles = width // 2 // LANES
    for half in range(2):
        await_recv(parts.at[2, half], landed(2, half))
        for sub in range(2):
            part_wait(3, half, sub)
        scores, names = [], []
        for member in range(LIST_LEN):
            total = acc[z, half, member] + parts[2, half, member] + parts[3, half, member]
            name = cand_ids[half, member]
            real = name >= 0.0
            scores.append(jnp.where(real, total, -jnp.inf))
            names.append(jnp.where(real, name, BIG))
        for place in range(TOP_K):
            best = functools.reduce(jnp.maximum, scores)
            best = jnp.max(best, axis=0, keepdims=True)
            tied = [jnp.where(score_j == best, name_j, BIG) for score_j, name_j in zip(scores, names)]
            first = jnp.min(functools.reduce(jnp.minimum, tied), axis=0, keepdims=True)
            for tile in range(tiles):
                lanes = slice(tile * LANES, (tile + 1) * LANES)
                line = place * tiles + tile
                res[z, half, line:line + 1, :] = best[:, lanes]
                res[z, half, TOP_K * tiles + line:TOP_K * tiles + line + 1, :] = first[:, lanes]
            if place + 1 < TOP_K:
                scores = [jnp.where(name_j == first, -jnp.inf, score_j) for score_j, name_j in zip(scores, names)]
        if half == 0:
            await_send(vecs.at[pl.ds(0, block_rows)], send_o)
            await_send(ids_all.at[pl.ds(0, 3)], send_i)
        else:
            await_send(vecs.at[pl.ds(0, chunks * PIECE_ROWS)], send_y)
            await_send(vecs.at[pl.ds(0, chunks * PIECE_ROWS)], send_x)
            await_send(vecs.at[pl.ds(0, 2 * chunks * PIECE_ROWS)], send_d)
        for which in range(dims - 1):
            res_copy(jnp.where(which < z, which, which + 1), half).start()

    await_send(parts.at[pl.ds(0, 3)], send_r)
    await_send(res.at[pl.ds(0, dims - 1)], send_g)
    await_recv(res.at[pl.ds(0, dims - 1)], recv_g)


def place_kernel(res, out_s, out_i):
    dims, halves, lines, _ = res.shape
    tiles = lines // (2 * TOP_K)
    for part in range(dims):
        for half in range(halves):
            for tile in range(tiles):
                first = ((part * halves + half) * tiles + tile) * LANES
                out_s[:, first:first + LANES] = res[part, half, pl.ds(tile, TOP_K, stride=tiles), :]
                out_i[:, first:first + LANES] = res[part, half, pl.ds(TOP_K * tiles + tile, TOP_K, stride=tiles), :].astype(jnp.int32)


def solution(mesh):
    dims = mesh.shape['dim']
    row_spec = P(('rep', 'shard'), None)

    def local_search(queries, list_vecs, list_ids, probes):
        rows_q, depth = queries.shape
        lists_dev, list_len, _ = list_vecs.shape
        probe_count = probes.shape[1]
        block_rows = lists_dev * list_len
        block_steps = block_rows // STEP_ROWS
        chunks = lists_dev // GROUP_LISTS
        width = rows_q // dims
        dma = pltpu.SemaphoreType.DMA
        any_spec = pl.BlockSpec(memory_space=pl.ANY)
        vmem_spec = pl.BlockSpec(memory_space=pltpu.VMEM)
        found = pl.pallas_call(
            functools.partial(search_kernel, dims),
            out_shape=pltpu.VMEM((dims, 2, TOP_K * width // LANES, LANES), jnp.float32),
            in_specs=[any_spec] * 4,
            out_specs=vmem_spec,
            scratch_shapes=[
                pltpu.VMEM((block_rows, depth), jnp.bfloat16),
                pltpu.VMEM((rows_q, depth), jnp.bfloat16),
                pltpu.VMEM((4 * block_rows, depth), jnp.bfloat16),
                pltpu.VMEM((STEP_ROWS, STEP_ROWS), jnp.bfloat16),
                pltpu.VMEM((dims, 2, LIST_LEN, probe_count, width // 2), jnp.float32),
                pltpu.VMEM((4, 2, LIST_LEN, probe_count, width // 2), jnp.float32),
                pltpu.VMEM((4, LIST_LEN, lists_dev), jnp.int32),
                pltpu.VMEM((2, LIST_LEN, probe_count, width // 2), jnp.float32),
                pltpu.VMEM((probe_count, rows_q), jnp.int32),
                pltpu.VMEM((LIST_LEN, lists_dev), jnp.int32),
                dma, dma,
                dma((3,)), dma,
                dma, dma((2,)),
                dma, dma((REUSE_Y + 2,)), dma, dma((REUSE_X + 3,)),
                dma, dma((chunks // 2,)),
                dma, dma, dma, dma((14,)), dma, dma,
                pltpu.SemaphoreType.REGULAR((2,)),
            ],
            compiler_params=pltpu.CompilerParams(collective_id=0, has_side_effects=True, vmem_limit_bytes=60 * 2**20),
            name='ivf_search',
        )(queries, list_vecs.reshape(block_rows, depth), probes.T, list_ids.T)
        scores, ids = pl.pallas_call(
            place_kernel,
            out_shape=(jax.ShapeDtypeStruct((TOP_K, rows_q), jnp.float32),
                       jax.ShapeDtypeStruct((TOP_K, rows_q), jnp.int32)),
            in_specs=[vmem_spec],
            out_specs=(vmem_spec, vmem_spec),
            compiler_params=pltpu.CompilerParams(vmem_limit_bytes=4 * 2**20),
            name='place',
        )(found)
        return scores.T, ids.T

    return jax.shard_map(local_search, mesh=mesh,
                         in_specs=(P(('rep', 'shard'), 'dim'), P('shard', None, 'dim'), P('shard', None), row_spec),
                         out_specs=(row_spec, row_spec), check_vma=False)
```

```python
import functools

import jax
import jax.numpy as jnp
from jax import lax
from jax.experimental import pallas as pl
from jax.experimental.pallas import tpu as pltpu
from jax.sharding import PartitionSpec as P

TOP_K = 10
LIST_LEN = 8
GROUP_LISTS = 8
GROUP_ROWS = GROUP_LISTS * LIST_LEN
STEP_GROUPS = 4
STEP_ROWS = STEP_GROUPS * GROUP_ROWS
PIECE_ROWS = GROUP_ROWS // 2
LANES = 128
REUSE_Y, REUSE_X = 8, 12
MESH = pl.DeviceIdType.MESH
BIG = 1e9


def flip(index, bit):
    return index + bit - 2 * bit * ((index // bit) % 2)


def search_kernel(dims, q_hbm, l_hbm, probes_hbm, ids_hbm, res,
                  raw, qv, vecs, perm, acc, parts, ids_all, cand_ids, probes_ref, ids_ref, load_p, load_i,
                  load_l, load_q, send_o, recv_o, send_y, recv_y, send_x, recv_x,
                  send_d, recv_d, send_i, recv_i, send_r, recv_r, send_g, recv_g, met):
    rows_q = qv.shape[0]
    lists_dev = ids_ref.shape[1]
    block_rows = lists_dev * LIST_LEN
    block_groups = lists_dev // GROUP_LISTS
    chunks = block_groups
    block_steps = block_groups // STEP_GROUPS
    width = rows_q // dims
    x, z, s = lax.axis_index('rep'), lax.axis_index('dim'), lax.axis_index('shard')
    twin, across, far = flip(s, 1), flip(s, 2), flip(flip(s, 1), 2)
    other_x = 1 - x

    def at(**place):
        return {'rep': x, 'dim': z, 'shard': s, **place}

    def step_rows(step):
        return pl.ds(pl.multiple_of(step * STEP_ROWS, STEP_ROWS), STEP_ROWS)

    def remote(src, dst, send, recv, device):
        return pltpu.make_async_remote_copy(src_ref=src, dst_ref=dst, send_sem=send, recv_sem=recv,
                                            device_id=device, device_id_type=MESH)

    def await_recv(buffer, semaphore):
        remote(buffer, buffer, send_i, semaphore, at()).wait_recv()

    def await_send(buffer, semaphore):
        remote(buffer, buffer, semaphore, recv_i, at()).wait_send()

    def load_lists(number):
        half = block_steps // 2
        first, count = ((half * x, 1), (half * x + 1, half - 1), (half * other_x, half))[number]
        rows = pl.ds(pl.multiple_of(first * STEP_ROWS, STEP_ROWS), count * STEP_ROWS)
        return pltpu.make_async_copy(l_hbm.at[rows], raw.at[rows], load_l.at[number])

    queries_in = pltpu.make_async_copy(q_hbm, qv, load_q)

    def own_copy(block):
        return remote(vecs.at[step_rows(block)], vecs.at[step_rows(block_steps + block)],
                      send_o, recv_o.at[(block // (block_steps // 2) + x) % 2], at(shard=twin))

    def piece(group, chunk):
        first = pl.multiple_of(group * GROUP_ROWS + chunk % 2 * PIECE_ROWS, PIECE_ROWS)
        return vecs.at[pl.ds(first, PIECE_ROWS)]

    def slot(chunk, which):
        return piece(2 * block_groups + STEP_GROUPS * (chunk // 2) + which, chunk)

    def y_copy(chunk):
        return remote(piece(chunks // 2 * x + chunk // 2, chunk), slot(chunk, 0), send_y, recv_y.at[chunk % REUSE_Y], at(shard=across))

    def x_copy(chunk):
        return remote(slot(chunk, 0), slot(chunk, 1), send_x, recv_x.at[chunk % REUSE_X], at(rep=other_x))

    def dy_copy(chunk):
        return remote(slot(chunk, 0), slot(chunk, 2), send_d, recv_d.at[chunk // 2], at(shard=twin))

    def dx_copy(chunk):
        return remote(slot(chunk, 1), slot(chunk, 3), send_d, recv_d.at[chunk // 2], at(shard=twin))

    def id_copy(which, peer):
        return remote(ids_ref, ids_all.at[s], send_i, recv_i, at(shard=peer))

    outer = z % 3 == 0
    mate, far_outer = flip(z, 1), jnp.where(z < 2, dims - 1, 0)
    far_inner = flip(far_outer, 1)

    def landed(place, half, sub=0):
        return recv_r.at[12 + half if place == 2 else 4 * min(place, 2) + 2 * half + sub]

    def some_members(sub):
        return pl.ds(sub * (LIST_LEN // 2), LIST_LEN // 2)

    def near_copy(half):
        return remote(acc.at[mate, half], parts.at[2, half], send_r, landed(2, half), at(dim=mate))

    def cross_copy(target, place, half, sub):
        return remote(acc.at[target, half, some_members(sub)], parts.at[place, half, some_members(sub)], send_r,
                      landed(place, half, sub), at(dim=mate))

    def merged_copy(merge, half, sub):
        return remote(parts.at[merge, half, some_members(sub)], parts.at[3, half, some_members(sub)], send_r,
                      landed(3, half, sub), at(dim=(far_outer, far_inner)[merge]))

    def part_wait(place, half, sub):
        await_recv(parts.at[place, half, some_members(sub)], landed(place, half, sub))

    def res_copy(target, half):
        return remote(res.at[z, half], res.at[z, half], send_g, recv_g, at(dim=target))

    def target_at(turn):
        first, second, third = (jnp.where(outer, one, two) for one, two in ((far_inner, mate), (far_outer, far_inner), (mate, far_outer)))
        return jnp.where(turn == 0, first, jnp.where(turn == 1, second, jnp.where(turn == 2, third, z)))

    def block_at(turn):
        return (block_steps // 2 * x + turn) % block_steps

    barrier = pltpu.get_barrier_semaphore()
    peers = [at(shard=twin), at(shard=across), at(shard=far), at(rep=other_x)]
    beside = jnp.where(outer, 1, 2)

    def tell_line(semaphore):
        @pl.when(z < dims - 1)
        def _():
            pl.semaphore_signal(semaphore, inc=1, device_id=at(dim=(z + 1) % dims), device_id_type=MESH)

        @pl.when(z > 0)
        def _():
            pl.semaphore_signal(semaphore, inc=1, device_id=at(dim=(z + dims - 1) % dims), device_id_type=MESH)

    load_lists(0).start()
    tell_line(barrier)
    probes_in = pltpu.make_async_copy(probes_hbm, probes_ref, load_p)
    ids_in = pltpu.make_async_copy(ids_hbm, ids_ref, load_i)
    ids_in.start()
    probes_in.start()
    queries_in.start()
    for peer in peers:
        pl.semaphore_signal(barrier, inc=1, device_id=peer, device_id_type=MESH)
    load_lists(1).start()
    load_lists(2).start()

    row = lax.broadcasted_iota(jnp.int32, (STEP_ROWS, STEP_ROWS), 0)
    col = lax.broadcasted_iota(jnp.int32, (STEP_ROWS, STEP_ROWS), 1)
    source = (row // GROUP_ROWS) * GROUP_ROWS + (row % GROUP_LISTS) * LIST_LEN + (row // GROUP_LISTS) % LIST_LEN
    perm[...] = jnp.where(col == source, 1.0, 0.0).astype(jnp.bfloat16)

    def arrange(turn):
        block = block_at(turn)
        moved = jnp.dot(perm[...], raw[step_rows(block), :], preferred_element_type=jnp.float32)
        vecs[step_rows(block), :] = moved.astype(jnp.bfloat16)

    window = REUSE_Y // 2
    load_lists(0).wait()
    arrange(0)
    pl.semaphore_wait(barrier, len(peers) + beside)
    for chunk in range(window):
        y_copy(chunk).start()
    tell_line(met.at[0])
    acc[...] = jnp.zeros_like(acc)
    ids_in.wait()
    for which, peer in enumerate((twin, across, far)):
        id_copy(which, peer).start()
    ids_all[s] = ids_ref[...]
    probes_in.wait()
    queries_in.wait()

    def name_candidates(tile, carry):
        cols = pl.ds(pl.multiple_of(z * width + tile * LANES, LANES), LANES)
        probe = probes_ref[:, cols]
        lane, page = probe % LANES, probe // LANES
        pages = lists_dev // LANES
        for member in range(LIST_LEN):
            got = jnp.zeros((probe.shape[0], LANES), jnp.int32)
            for number in range(4 * pages):
                table = ids_all[number // pages, member:member + 1, (number % pages) * LANES:(number % pages + 1) * LANES]
                table = jnp.broadcast_to(table, (probe.shape[0], LANES))
                picked = jnp.take_along_axis(table, lane, axis=1, mode='promise_in_bounds')
                got = jnp.where(page == number, picked, got)
            tiles_half = width // 2 // LANES
            place = pl.ds(pl.multiple_of(tile % tiles_half * LANES, LANES), LANES)
            cand_ids[tile // tiles_half, member, :, place] = got.astype(jnp.float32)
        return carry

    def list_block(step):
        return block_at(step % block_steps)

    def score(step, heads, part):
        lists = vecs[step_rows(jnp.where(step < 2 * block_steps, step // block_steps * block_steps + list_block(step), step)), :]
        rows = pl.ds(pl.multiple_of(part * width, width), width)
        scores = lax.dot_general(lists, qv[rows, :], (((1,), (1,)), ((), ())), preferred_element_type=jnp.float32)
        for tile in range(width // LANES):
            probe = probes_ref[:, pl.ds(pl.multiple_of(part * width + tile * LANES, LANES), LANES)]
            low, head = probe % GROUP_LISTS, probe // GROUP_LISTS
            hits = [head == want for want in heads]
            lanes = slice(tile * LANES, (tile + 1) * LANES)
            half, place = divmod(tile * LANES, width // 2)
            kept_lanes = slice(place, place + LANES)
            for member in range(LIST_LEN):
                kept = acc[part, half, member, :, kept_lanes]
                for group, hit in enumerate(hits):
                    first = group * GROUP_ROWS + member * GROUP_LISTS
                    picked = jnp.take_along_axis(scores[first:first + GROUP_LISTS, lanes], low, axis=0, mode='promise_in_bounds')
                    kept = jnp.where(hit, picked, kept)
                acc[part, half, member, :, kept_lanes] = kept

    def heads_at(step):
        local = step < 2 * block_steps
        group = step - 2 * block_steps
        base = block_groups * jnp.where(step < block_steps, s, twin) + STEP_GROUPS * list_block(step)
        heads = []
        for which in range(STEP_GROUPS):
            home = across if which < 2 else far
            side = x if which % 2 == 0 else other_x
            heads.append(jnp.where(local, base + which, block_groups * home + chunks // 2 * side + group))
        return heads

    last = 2 * block_steps + chunks // 2 - 1

    spare_copy = remote(piece(chunks // 2 * other_x + (chunks - 1) // 2, chunks - 1), slot(chunks - 1, 1),
                        send_x, recv_x.at[REUSE_X], at(shard=across))

    split = chunks - 2

    def split_half(buffer, half):
        return buffer.at[pl.ds(half * (PIECE_ROWS // 2), PIECE_ROWS // 2)]

    def y_half(half):
        return remote(split_half(piece(chunks // 2 * x + split // 2, split), half), split_half(slot(split, 0), half),
                      send_y, recv_y.at[REUSE_Y + half], at(shard=across))

    def x_half(half):
        return remote(split_half(slot(split, 0), half), split_half(slot(split, 1), half),
                      send_x, recv_x.at[REUSE_X + 1 + half], at(rep=other_x))

    def d_half(which, half):
        return remote(split_half(slot(split, which), half), split_half(slot(split, which + 2), half),
                      send_d, recv_d.at[split // 2], at(shard=twin))

    def pass_split(which):
        for half in range(2):
            if which == 0:
                y_half(half).wait_recv()
                x_half(half).start()
            else:
                x_half(half).wait_recv()
            d_half(which, half).start()

    def pass_y(chunk):
        y_copy(chunk).wait_recv()
        if not (isinstance(chunk, int) and chunk == chunks - 1):
            x_copy(chunk).start()
        dy_copy(chunk).start()

        if isinstance(chunk, int) and chunk + window == split:
            for half in range(2):
                y_half(half).start()
        else:
            @pl.when(chunk + window < chunks)
            def _():
                y_copy(chunk + window).start()

        @pl.when(chunk + window == chunks)
        def _():
            spare_copy.start()

    def pass_x(chunk):
        if isinstance(chunk, int) and chunk == chunks - 1:
            spare_copy.wait_recv()
        else:
            x_copy(chunk).wait_recv()
        dx_copy(chunk).start()

    def await_step(step):
        await_recv(vecs.at[pl.ds(0, 4 * PIECE_ROWS)], recv_d.at[step - 2 * block_steps])

    def score_all(step):
        heads = heads_at(step)
        for part in range(dims):
            score(step, heads, part)

    def early(step, carry):
        own_copy(block_at(step)).start()

        @pl.when(step >= 1)
        def _():
            pass_y(step - 1)

        @pl.when(step >= 5)
        def _():
            pass_x(step - 5)

        @pl.when(step == 0)
        def _():
            load_lists(1).wait()

        @pl.when(step == block_steps // 2 - 1)
        def _():
            load_lists(2).wait()
        score_all(step)
        arrange(step + 1)
        return carry

    def middle(step, carry):
        pass_y(step - 1)
        pass_x(step - 5)

        @pl.when(step == block_steps - 1)
        def _():
            own_copy(block_at(step)).start()

        @pl.when((step == block_steps) | (step == block_steps + block_steps // 2))
        def _():
            await_recv(vecs.at[pl.ds(0, block_rows // 2)], recv_o.at[step // (block_steps // 2) - 2])

        @pl.when(step >= 2 * block_steps)
        def _():
            await_step(step)
        score_all(step)
        return carry

    late_plan = {
        last - 5: ('y25', 'x21', 'x22'),
        last - 4: ('y26', 'x23', 'y27', 'x24'),
        last - 3: ('y28', 'x25', 'names', 'y29', 'x26'),
        last - 2: ('y30', 'x27', 'y31', 'x28', 'x29'),
        last - 1: ('x31', 'x30'),
    }

    def late(step, carry):
        for when, plan in late_plan.items():
            @pl.when(step == when)
            def _(plan=plan):
                for word in plan:
                    if word == 'names':
                        await_recv(ids_all.at[pl.ds(0, 3)], recv_i)
                        lax.fori_loop(0, width // LANES, name_candidates, 0)
                    else:
                        which, number = 'yx'.index(word[0]), int(word[1:])
                        if number == split:
                            pass_split(which)
                        else:
                            (pass_y, pass_x)[which](number)

        await_step(step)
        score_all(step)
        return carry

    lax.fori_loop(0, block_steps - 1, early, 0)
    lax.fori_loop(block_steps - 1, last - 5, middle, 0)
    pl.semaphore_wait(met.at[0], beside)
    tell_line(met.at[1])
    lax.fori_loop(last - 5, last, late, 0)
    pl.semaphore_wait(met.at[1], beside)
    await_step(jnp.int32(last))
    last_heads = heads_at(jnp.int32(last))

    leads, follows = outer & (s % 2 == 0), outer & (s % 2 == 1)

    def send_cross(*plan):
        for far_place, half in plan:
            for sub in range(2):
                cross_copy((far_outer, far_inner)[far_place], far_place, half, sub).start()

    def send_near():
        for half in range(2):
            near_copy(half).start()

    def finish(turn, carry):
        @pl.when(leads & (turn == 1))
        def _():
            send_cross((1, 0))

        @pl.when(leads & (turn == 2))
        def _():
            send_cross((0, 0))

        @pl.when(follows & (turn == 3))
        def _():
            send_cross((1, 0), (0, 0))

        @pl.when((leads & (turn == 3)) | (jnp.logical_not(outer) & (turn == 1)))
        def _():
            send_near()

        @pl.when(leads & (turn == 3))
        def _():
            send_cross((1, 1), (0, 1))
        score(jnp.int32(last), last_heads, target_at(turn))
        return carry

    lax.fori_loop(0, dims, finish, 0)

    @pl.when(follows)
    def _():
        send_near()
        send_cross((1, 1), (0, 1))

    @pl.when(jnp.logical_not(outer))
    def _():
        for half in range(2):
            for merge, target in ((1, far_inner), (0, far_outer)):
                for sub in range(2):
                    part_wait(merge, half, sub)
                    parts[merge, half, some_members(sub)] += acc[target, half, some_members(sub)]
                    merged_copy(merge, half, sub).start()

    tiles = width // 2 // LANES
    for half in range(2):
        await_recv(parts.at[2, half], landed(2, half))
        for sub in range(2):
            part_wait(3, half, sub)
        scores, names = [], []
        for member in range(LIST_LEN):
            total = acc[z, half, member] + parts[2, half, member] + parts[3, half, member]
            name = cand_ids[half, member]
            real = name >= 0.0
            scores.append(jnp.where(real, total, -jnp.inf))
            names.append(jnp.where(real, name, BIG))
        for place in range(TOP_K):
            best = functools.reduce(jnp.maximum, scores)
            best = jnp.max(best, axis=0, keepdims=True)
            tied = [jnp.where(score_j == best, name_j, BIG) for score_j, name_j in zip(scores, names)]
            first = jnp.min(functools.reduce(jnp.minimum, tied), axis=0, keepdims=True)
            for tile in range(tiles):
                lanes = slice(tile * LANES, (tile + 1) * LANES)
                line = place * tiles + tile
                res[z, half, line:line + 1, :] = best[:, lanes]
                res[z, half, TOP_K * tiles + line:TOP_K * tiles + line + 1, :] = first[:, lanes]
            if place + 1 < TOP_K:
                scores = [jnp.where(name_j == first, -jnp.inf, score_j) for score_j, name_j in zip(scores, names)]
        if half == 0:
            await_send(vecs.at[pl.ds(0, block_rows)], send_o)
            await_send(ids_all.at[pl.ds(0, 3)], send_i)
        else:
            await_send(vecs.at[pl.ds(0, chunks * PIECE_ROWS)], send_y)
            await_send(vecs.at[pl.ds(0, chunks * PIECE_ROWS)], send_x)
            await_send(vecs.at[pl.ds(0, 2 * chunks * PIECE_ROWS)], send_d)
        for which in range(dims - 1):
            res_copy(jnp.where(which < z, which, which + 1), half).start()

    await_send(parts.at[pl.ds(0, 3)], send_r)
    await_send(res.at[pl.ds(0, dims - 1)], send_g)
    await_recv(res.at[pl.ds(0, dims - 1)], recv_g)


def place_kernel(res, out_s, out_i):
    dims, halves, lines, _ = res.shape
    tiles = lines // (2 * TOP_K)
    for part in range(dims):
        for half in range(halves):
            for tile in range(tiles):
                first = ((part * halves + half) * tiles + tile) * LANES
                out_s[:, first:first + LANES] = res[part, half, pl.ds(tile, TOP_K, stride=tiles), :]
                out_i[:, first:first + LANES] = res[part, half, pl.ds(TOP_K * tiles + tile, TOP_K, stride=tiles), :].astype(jnp.int32)


def solution(mesh):
    dims = mesh.shape['dim']
    row_spec = P(('rep', 'shard'), None)

    def local_search(queries, list_vecs, list_ids, probes):
        rows_q, depth = queries.shape
        lists_dev, list_len, _ = list_vecs.shape
        probe_count = probes.shape[1]
        block_rows = lists_dev * list_len
        block_steps = block_rows // STEP_ROWS
        chunks = lists_dev // GROUP_LISTS
        width = rows_q // dims
        dma = pltpu.SemaphoreType.DMA
        any_spec = pl.BlockSpec(memory_space=pl.ANY)
        vmem_spec = pl.BlockSpec(memory_space=pltpu.VMEM)
        found = pl.pallas_call(
            functools.partial(search_kernel, dims),
            out_shape=pltpu.VMEM((dims, 2, TOP_K * width // LANES, LANES), jnp.float32),
            in_specs=[any_spec] * 4,
            out_specs=vmem_spec,
            scratch_shapes=[
                pltpu.VMEM((block_rows, depth), jnp.bfloat16),
                pltpu.VMEM((rows_q, depth), jnp.bfloat16),
                pltpu.VMEM((4 * block_rows, depth), jnp.bfloat16),
                pltpu.VMEM((STEP_ROWS, STEP_ROWS), jnp.bfloat16),
                pltpu.VMEM((dims, 2, LIST_LEN, probe_count, width // 2), jnp.float32),
                pltpu.VMEM((4, 2, LIST_LEN, probe_count, width // 2), jnp.float32),
                pltpu.VMEM((4, LIST_LEN, lists_dev), jnp.int32),
                pltpu.VMEM((2, LIST_LEN, probe_count, width // 2), jnp.float32),
                pltpu.VMEM((probe_count, rows_q), jnp.int32),
                pltpu.VMEM((LIST_LEN, lists_dev), jnp.int32),
                dma, dma,
                dma((3,)), dma,
                dma, dma((2,)),
                dma, dma((REUSE_Y + 2,)), dma, dma((REUSE_X + 3,)),
                dma, dma((chunks // 2,)),
                dma, dma, dma, dma((14,)), dma, dma,
                pltpu.SemaphoreType.REGULAR((2,)),
            ],
            compiler_params=pltpu.CompilerParams(collective_id=0, has_side_effects=True, vmem_limit_bytes=60 * 2**20),
            name='ivf_search',
        )(queries, list_vecs.reshape(block_rows, depth), probes.T, list_ids.T)
        scores, ids = pl.pallas_call(
            place_kernel,
            out_shape=(jax.ShapeDtypeStruct((TOP_K, rows_q), jnp.float32),
                       jax.ShapeDtypeStruct((TOP_K, rows_q), jnp.int32)),
            in_specs=[vmem_spec],
            out_specs=(vmem_spec, vmem_spec),
            compiler_params=pltpu.CompilerParams(vmem_limit_bytes=4 * 2**20),
            name='place',
        )(found)
        return scores.T, ids.T

    return jax.shard_map(local_search, mesh=mesh,
                         in_specs=(P(('rep', 'shard'), 'dim'), P('shard', None, 'dim'), P('shard', None), row_spec),
                         out_specs=(row_spec, row_spec), check_vma=False)
```

```python
import functools

import jax
import jax.numpy as jnp
from jax import lax
from jax.experimental import pallas as pl
from jax.experimental.pallas import tpu as pltpu
from jax.sharding import PartitionSpec as P

TOP_K = 10
LIST_LEN = 8
GROUP_LISTS = 8
GROUP_ROWS = GROUP_LISTS * LIST_LEN
STEP_GROUPS = 4
STEP_ROWS = STEP_GROUPS * GROUP_ROWS
PIECE_ROWS = GROUP_ROWS // 2
LANES = 128
REUSE_Y, REUSE_X = 8, 12
SUBS = 4
MESH = pl.DeviceIdType.MESH
BIG = 1e9


def flip(index, bit):
    return index + bit - 2 * bit * ((index // bit) % 2)


def search_kernel(dims, q_hbm, l_hbm, probes_hbm, ids_hbm, res,
                  raw, qv, vecs, perm, acc, parts, ids_all, cand_ids, probes_ref, ids_ref, load_p, load_i,
                  load_l, load_q, send_o, recv_o, send_y, recv_y, send_x, recv_x,
                  send_d, recv_d, send_i, recv_i, send_r, recv_r, send_g, recv_g, met):
    rows_q = qv.shape[0]
    lists_dev = ids_ref.shape[1]
    block_rows = lists_dev * LIST_LEN
    block_groups = lists_dev // GROUP_LISTS
    chunks = block_groups
    block_steps = block_groups // STEP_GROUPS
    width = rows_q // dims
    x, z, s = lax.axis_index('rep'), lax.axis_index('dim'), lax.axis_index('shard')
    twin, across, far = flip(s, 1), flip(s, 2), flip(flip(s, 1), 2)
    other_x = 1 - x

    def at(**place):
        return {'rep': x, 'dim': z, 'shard': s, **place}

    def step_rows(step):
        return pl.ds(pl.multiple_of(step * STEP_ROWS, STEP_ROWS), STEP_ROWS)

    def remote(src, dst, send, recv, device):
        return pltpu.make_async_remote_copy(src_ref=src, dst_ref=dst, send_sem=send, recv_sem=recv,
                                            device_id=device, device_id_type=MESH)

    def await_recv(buffer, semaphore):
        remote(buffer, buffer, send_i, semaphore, at()).wait_recv()

    def await_send(buffer, semaphore):
        remote(buffer, buffer, semaphore, recv_i, at()).wait_send()

    def load_lists(number):
        half = block_steps // 2
        first, count = ((half * x, 1), (half * x + 1, half - 1), (half * other_x, half))[number]
        rows = pl.ds(pl.multiple_of(first * STEP_ROWS, STEP_ROWS), count * STEP_ROWS)
        return pltpu.make_async_copy(l_hbm.at[rows], raw.at[rows], load_l.at[number])

    queries_in = pltpu.make_async_copy(q_hbm, qv, load_q)

    def own_copy(block):
        return remote(vecs.at[step_rows(block)], vecs.at[step_rows(block_steps + block)],
                      send_o, recv_o.at[(block // (block_steps // 2) + x) % 2], at(shard=twin))

    def piece(group, chunk):
        first = pl.multiple_of(group * GROUP_ROWS + chunk % 2 * PIECE_ROWS, PIECE_ROWS)
        return vecs.at[pl.ds(first, PIECE_ROWS)]

    def slot(chunk, which):
        return piece(2 * block_groups + STEP_GROUPS * (chunk // 2) + which, chunk)

    def y_copy(chunk):
        return remote(piece(chunks // 2 * x + chunk // 2, chunk), slot(chunk, 0), send_y, recv_y.at[chunk % REUSE_Y], at(shard=across))

    def x_copy(chunk):
        return remote(slot(chunk, 0), slot(chunk, 1), send_x, recv_x.at[chunk % REUSE_X], at(rep=other_x))

    def dy_copy(chunk):
        return remote(slot(chunk, 0), slot(chunk, 2), send_d, recv_d.at[chunk // 2], at(shard=twin))

    def dx_copy(chunk):
        return remote(slot(chunk, 1), slot(chunk, 3), send_d, recv_d.at[chunk // 2], at(shard=twin))

    def id_copy(which, peer):
        return remote(ids_ref, ids_all.at[s], send_i, recv_i, at(shard=peer))

    outer = z % 3 == 0
    mate, far_outer = flip(z, 1), jnp.where(z < 2, dims - 1, 0)
    far_inner = flip(far_outer, 1)

    def landed(place, half, sub=0):
        return recv_r.at[6 * SUBS + half if place == 2 else (2 * min(place, 2) + half) * SUBS + sub]

    def some_members(sub):
        return pl.ds(sub * (LIST_LEN // SUBS), LIST_LEN // SUBS)

    def near_copy(half):
        return remote(acc.at[mate, half], parts.at[2, half], send_r, landed(2, half), at(dim=mate))

    def cross_copy(target, place, half, sub):
        return remote(acc.at[target, half, some_members(sub)], parts.at[place, half, some_members(sub)], send_r,
                      landed(place, half, sub), at(dim=mate))

    def merged_copy(merge, half, sub):
        return remote(parts.at[merge, half, some_members(sub)], parts.at[3, half, some_members(sub)], send_r,
                      landed(3, half, sub), at(dim=(far_outer, far_inner)[merge]))

    def part_wait(place, half, sub):
        await_recv(parts.at[place, half, some_members(sub)], landed(place, half, sub))

    def res_copy(target, half):
        return remote(res.at[z, half], res.at[z, half], send_g, recv_g, at(dim=target))

    def target_at(turn):
        first, second, third = (jnp.where(outer, one, two) for one, two in ((far_inner, mate), (far_outer, far_inner), (mate, far_outer)))
        return jnp.where(turn == 0, first, jnp.where(turn == 1, second, jnp.where(turn == 2, third, z)))

    def block_at(turn):
        return (block_steps // 2 * x + turn) % block_steps

    barrier = pltpu.get_barrier_semaphore()
    peers = [at(shard=twin), at(shard=across), at(shard=far), at(rep=other_x)]
    beside = jnp.where(outer, 1, 2)

    def tell_line(semaphore):
        @pl.when(z < dims - 1)
        def _():
            pl.semaphore_signal(semaphore, inc=1, device_id=at(dim=(z + 1) % dims), device_id_type=MESH)

        @pl.when(z > 0)
        def _():
            pl.semaphore_signal(semaphore, inc=1, device_id=at(dim=(z + dims - 1) % dims), device_id_type=MESH)

    load_lists(0).start()
    tell_line(barrier)
    probes_in = pltpu.make_async_copy(probes_hbm, probes_ref, load_p)
    ids_in = pltpu.make_async_copy(ids_hbm, ids_ref, load_i)
    ids_in.start()
    probes_in.start()
    queries_in.start()
    for peer in peers:
        pl.semaphore_signal(barrier, inc=1, device_id=peer, device_id_type=MESH)
    load_lists(1).start()
    load_lists(2).start()

    row = lax.broadcasted_iota(jnp.int32, (STEP_ROWS, STEP_ROWS), 0)
    col = lax.broadcasted_iota(jnp.int32, (STEP_ROWS, STEP_ROWS), 1)
    source = (row // GROUP_ROWS) * GROUP_ROWS + (row % GROUP_LISTS) * LIST_LEN + (row // GROUP_LISTS) % LIST_LEN
    perm[...] = jnp.where(col == source, 1.0, 0.0).astype(jnp.bfloat16)

    def arrange(turn):
        block = block_at(turn)
        moved = jnp.dot(perm[...], raw[step_rows(block), :], preferred_element_type=jnp.float32)
        vecs[step_rows(block), :] = moved.astype(jnp.bfloat16)

    window = REUSE_Y // 2
    load_lists(0).wait()
    arrange(0)
    pl.semaphore_wait(barrier, len(peers) + beside)
    for chunk in range(window):
        y_copy(chunk).start()
    tell_line(met.at[0])
    acc[...] = jnp.zeros_like(acc)
    ids_in.wait()
    for which, peer in enumerate((twin, across, far)):
        id_copy(which, peer).start()
    ids_all[s] = ids_ref[...]
    probes_in.wait()
    queries_in.wait()

    def name_candidates(tile, carry):
        cols = pl.ds(pl.multiple_of(z * width + tile * LANES, LANES), LANES)
        probe = probes_ref[:, cols]
        lane, page = probe % LANES, probe // LANES
        pages = lists_dev // LANES
        for member in range(LIST_LEN):
            got = jnp.zeros((probe.shape[0], LANES), jnp.int32)
            for number in range(4 * pages):
                table = ids_all[number // pages, member:member + 1, (number % pages) * LANES:(number % pages + 1) * LANES]
                table = jnp.broadcast_to(table, (probe.shape[0], LANES))
                picked = jnp.take_along_axis(table, lane, axis=1, mode='promise_in_bounds')
                got = jnp.where(page == number, picked, got)
            tiles_half = width // 2 // LANES
            place = pl.ds(pl.multiple_of(tile % tiles_half * LANES, LANES), LANES)
            cand_ids[tile // tiles_half, member, :, place] = got.astype(jnp.float32)
        return carry

    def list_block(step):
        return block_at(step % block_steps)

    def score(step, heads, part):
        lists = vecs[step_rows(jnp.where(step < 2 * block_steps, step // block_steps * block_steps + list_block(step), step)), :]
        rows = pl.ds(pl.multiple_of(part * width, width), width)
        scores = lax.dot_general(lists, qv[rows, :], (((1,), (1,)), ((), ())), preferred_element_type=jnp.float32)
        for tile in range(width // LANES):
            probe = probes_ref[:, pl.ds(pl.multiple_of(part * width + tile * LANES, LANES), LANES)]
            low, head = probe % GROUP_LISTS, probe // GROUP_LISTS
            hits = [head == want for want in heads]
            lanes = slice(tile * LANES, (tile + 1) * LANES)
            half, place = divmod(tile * LANES, width // 2)
            kept_lanes = slice(place, place + LANES)
            for member in range(LIST_LEN):
                kept = acc[part, half, member, :, kept_lanes]
                for group, hit in enumerate(hits):
                    first = group * GROUP_ROWS + member * GROUP_LISTS
                    picked = jnp.take_along_axis(scores[first:first + GROUP_LISTS, lanes], low, axis=0, mode='promise_in_bounds')
                    kept = jnp.where(hit, picked, kept)
                acc[part, half, member, :, kept_lanes] = kept

    def heads_at(step):
        local = step < 2 * block_steps
        group = step - 2 * block_steps
        base = block_groups * jnp.where(step < block_steps, s, twin) + STEP_GROUPS * list_block(step)
        heads = []
        for which in range(STEP_GROUPS):
            home = across if which < 2 else far
            side = x if which % 2 == 0 else other_x
            heads.append(jnp.where(local, base + which, block_groups * home + chunks // 2 * side + group))
        return heads

    last = 2 * block_steps + chunks // 2 - 1

    spare_copy = remote(piece(chunks // 2 * other_x + (chunks - 1) // 2, chunks - 1), slot(chunks - 1, 1),
                        send_x, recv_x.at[REUSE_X], at(shard=across))

    split = chunks - 2

    def split_half(buffer, half):
        return buffer.at[pl.ds(half * (PIECE_ROWS // 2), PIECE_ROWS // 2)]

    def y_half(half):
        return remote(split_half(piece(chunks // 2 * x + split // 2, split), half), split_half(slot(split, 0), half),
                      send_y, recv_y.at[REUSE_Y + half], at(shard=across))

    def x_half(half):
        return remote(split_half(slot(split, 0), half), split_half(slot(split, 1), half),
                      send_x, recv_x.at[REUSE_X + 1 + half], at(rep=other_x))

    def d_half(which, half):
        return remote(split_half(slot(split, which), half), split_half(slot(split, which + 2), half),
                      send_d, recv_d.at[split // 2], at(shard=twin))

    def pass_split(which):
        for half in range(2):
            if which == 0:
                y_half(half).wait_recv()
                x_half(half).start()
            else:
                x_half(half).wait_recv()
            d_half(which, half).start()

    def pass_y(chunk):
        y_copy(chunk).wait_recv()
        if not (isinstance(chunk, int) and chunk == chunks - 1):
            x_copy(chunk).start()
        dy_copy(chunk).start()

        if isinstance(chunk, int) and chunk + window == split:
            for half in range(2):
                y_half(half).start()
        else:
            @pl.when(chunk + window < chunks)
            def _():
                y_copy(chunk + window).start()

        @pl.when(chunk + window == chunks)
        def _():
            spare_copy.start()

    def pass_x(chunk):
        if isinstance(chunk, int) and chunk == chunks - 1:
            spare_copy.wait_recv()
        else:
            x_copy(chunk).wait_recv()
        dx_copy(chunk).start()

    def await_step(step):
        await_recv(vecs.at[pl.ds(0, 4 * PIECE_ROWS)], recv_d.at[step - 2 * block_steps])

    def score_all(step):
        heads = heads_at(step)
        for part in range(dims):
            score(step, heads, part)

    def early(step, carry):
        own_copy(block_at(step)).start()

        @pl.when(step >= 1)
        def _():
            pass_y(step - 1)

        @pl.when(step >= 5)
        def _():
            pass_x(step - 5)

        @pl.when(step == 0)
        def _():
            load_lists(1).wait()

        @pl.when(step == block_steps // 2 - 1)
        def _():
            load_lists(2).wait()
        score_all(step)
        arrange(step + 1)
        return carry

    def middle(step, carry):
        pass_y(step - 1)
        pass_x(step - 5)

        @pl.when(step == block_steps - 1)
        def _():
            own_copy(block_at(step)).start()

        @pl.when((step == block_steps) | (step == block_steps + block_steps // 2))
        def _():
            await_recv(vecs.at[pl.ds(0, block_rows // 2)], recv_o.at[step // (block_steps // 2) - 2])

        @pl.when(step >= 2 * block_steps)
        def _():
            await_step(step)
        score_all(step)
        return carry

    late_plan = {
        last - 5: ('y25', 'x21', 'x22'),
        last - 4: ('y26', 'x23', 'y27', 'x24'),
        last - 3: ('y28', 'x25', 'names', 'y29', 'x26'),
        last - 2: ('y30', 'x27', 'y31', 'x28', 'x29'),
        last - 1: ('x31', 'x30'),
    }

    def late(step, carry):
        for when, plan in late_plan.items():
            @pl.when(step == when)
            def _(plan=plan):
                for word in plan:
                    if word == 'names':
                        await_recv(ids_all.at[pl.ds(0, 3)], recv_i)
                        lax.fori_loop(0, width // LANES, name_candidates, 0)
                    else:
                        which, number = 'yx'.index(word[0]), int(word[1:])
                        if number == split:
                            pass_split(which)
                        else:
                            (pass_y, pass_x)[which](number)

        await_step(step)
        score_all(step)
        return carry

    lax.fori_loop(0, block_steps - 1, early, 0)
    lax.fori_loop(block_steps - 1, last - 5, middle, 0)
    pl.semaphore_wait(met.at[0], beside)
    tell_line(met.at[1])
    lax.fori_loop(last - 5, last, late, 0)
    pl.semaphore_wait(met.at[1], beside)
    await_step(jnp.int32(last))
    last_heads = heads_at(jnp.int32(last))

    leads, follows = outer & (s % 2 == 0), outer & (s % 2 == 1)

    def send_cross(*plan):
        for far_place, half in plan:
            for sub in range(SUBS):
                cross_copy((far_outer, far_inner)[far_place], far_place, half, sub).start()

    def send_near():
        for half in range(2):
            near_copy(half).start()

    def finish(turn, carry):
        @pl.when(leads & (turn == 1))
        def _():
            send_cross((1, 0))

        @pl.when(leads & (turn == 2))
        def _():
            send_cross((0, 0), (1, 1), (0, 1))

        @pl.when(follows & (turn == 3))
        def _():
            send_cross((1, 0), (0, 0))

        @pl.when((leads & (turn == 3)) | (jnp.logical_not(outer) & (turn == 1)))
        def _():
            send_near()
        score(jnp.int32(last), last_heads, target_at(turn))
        return carry

    lax.fori_loop(0, dims, finish, 0)

    @pl.when(follows)
    def _():
        send_cross((1, 1), (0, 1))
        send_near()

    @pl.when(jnp.logical_not(outer))
    def _():
        for half in range(2):
            for merge, target in ((1, far_inner), (0, far_outer)):
                for sub in range(SUBS):
                    part_wait(merge, half, sub)
                    parts[merge, half, some_members(sub)] += acc[target, half, some_members(sub)]
                    merged_copy(merge, half, sub).start()

    tiles = width // 2 // LANES
    for half in range(2):
        await_recv(parts.at[2, half], landed(2, half))
        for sub in range(SUBS):
            part_wait(3, half, sub)
        scores, names = [], []
        for member in range(LIST_LEN):
            total = acc[z, half, member] + parts[2, half, member] + parts[3, half, member]
            name = cand_ids[half, member]
            real = name >= 0.0
            scores.append(jnp.where(real, total, -jnp.inf))
            names.append(jnp.where(real, name, BIG))
        for place in range(TOP_K):
            best = functools.reduce(jnp.maximum, scores)
            best = jnp.max(best, axis=0, keepdims=True)
            tied = [jnp.where(score_j == best, name_j, BIG) for score_j, name_j in zip(scores, names)]
            first = jnp.min(functools.reduce(jnp.minimum, tied), axis=0, keepdims=True)
            for tile in range(tiles):
                lanes = slice(tile * LANES, (tile + 1) * LANES)
                line = place * tiles + tile
                res[z, half, line:line + 1, :] = best[:, lanes]
                res[z, half, TOP_K * tiles + line:TOP_K * tiles + line + 1, :] = first[:, lanes]
            if place + 1 < TOP_K:
                scores = [jnp.where(name_j == first, -jnp.inf, score_j) for score_j, name_j in zip(scores, names)]
        if half == 0:
            await_send(vecs.at[pl.ds(0, block_rows)], send_o)
            await_send(ids_all.at[pl.ds(0, 3)], send_i)
        else:
            await_send(vecs.at[pl.ds(0, chunks * PIECE_ROWS)], send_y)
            await_send(vecs.at[pl.ds(0, chunks * PIECE_ROWS)], send_x)
            await_send(vecs.at[pl.ds(0, 2 * chunks * PIECE_ROWS)], send_d)
        for which in range(dims - 1):
            res_copy(jnp.where(which < z, which, which + 1), half).start()

    await_send(parts.at[pl.ds(0, 3)], send_r)
    await_send(res.at[pl.ds(0, dims - 1)], send_g)
    await_recv(res.at[pl.ds(0, dims - 1)], recv_g)


def place_kernel(res, out_s, out_i):
    dims, halves, lines, _ = res.shape
    tiles = lines // (2 * TOP_K)
    for part in range(dims):
        for half in range(halves):
            for tile in range(tiles):
                first = ((part * halves + half) * tiles + tile) * LANES
                out_s[:, first:first + LANES] = res[part, half, pl.ds(tile, TOP_K, stride=tiles), :]
                out_i[:, first:first + LANES] = res[part, half, pl.ds(TOP_K * tiles + tile, TOP_K, stride=tiles), :].astype(jnp.int32)


def solution(mesh):
    dims = mesh.shape['dim']
    row_spec = P(('rep', 'shard'), None)

    def local_search(queries, list_vecs, list_ids, probes):
        rows_q, depth = queries.shape
        lists_dev, list_len, _ = list_vecs.shape
        probe_count = probes.shape[1]
        block_rows = lists_dev * list_len
        block_steps = block_rows // STEP_ROWS
        chunks = lists_dev // GROUP_LISTS
        width = rows_q // dims
        dma = pltpu.SemaphoreType.DMA
        any_spec = pl.BlockSpec(memory_space=pl.ANY)
        vmem_spec = pl.BlockSpec(memory_space=pltpu.VMEM)
        found = pl.pallas_call(
            functools.partial(search_kernel, dims),
            out_shape=pltpu.VMEM((dims, 2, TOP_K * width // LANES, LANES), jnp.float32),
            in_specs=[any_spec] * 4,
            out_specs=vmem_spec,
            scratch_shapes=[
                pltpu.VMEM((block_rows, depth), jnp.bfloat16),
                pltpu.VMEM((rows_q, depth), jnp.bfloat16),
                pltpu.VMEM((4 * block_rows, depth), jnp.bfloat16),
                pltpu.VMEM((STEP_ROWS, STEP_ROWS), jnp.bfloat16),
                pltpu.VMEM((dims, 2, LIST_LEN, probe_count, width // 2), jnp.float32),
                pltpu.VMEM((4, 2, LIST_LEN, probe_count, width // 2), jnp.float32),
                pltpu.VMEM((4, LIST_LEN, lists_dev), jnp.int32),
                pltpu.VMEM((2, LIST_LEN, probe_count, width // 2), jnp.float32),
                pltpu.VMEM((probe_count, rows_q), jnp.int32),
                pltpu.VMEM((LIST_LEN, lists_dev), jnp.int32),
                dma, dma,
                dma((3,)), dma,
                dma, dma((2,)),
                dma, dma((REUSE_Y + 2,)), dma, dma((REUSE_X + 3,)),
                dma, dma((chunks // 2,)),
                dma, dma, dma, dma((6 * SUBS + 2,)), dma, dma,
                pltpu.SemaphoreType.REGULAR((2,)),
            ],
            compiler_params=pltpu.CompilerParams(collective_id=0, has_side_effects=True, vmem_limit_bytes=60 * 2**20),
            name='ivf_search',
        )(queries, list_vecs.reshape(block_rows, depth), probes.T, list_ids.T)
        scores, ids = pl.pallas_call(
            place_kernel,
            out_shape=(jax.ShapeDtypeStruct((TOP_K, rows_q), jnp.float32),
                       jax.ShapeDtypeStruct((TOP_K, rows_q), jnp.int32)),
            in_specs=[vmem_spec],
            out_specs=(vmem_spec, vmem_spec),
            compiler_params=pltpu.CompilerParams(vmem_limit_bytes=4 * 2**20),
            name='place',
        )(found)
        return scores.T, ids.T

    return jax.shard_map(local_search, mesh=mesh,
                         in_specs=(P(('rep', 'shard'), 'dim'), P('shard', None, 'dim'), P('shard', None), row_spec),
                         out_specs=(row_spec, row_spec), check_vma=False)
```

```python
import functools

import jax
import jax.numpy as jnp
from jax import lax
from jax.experimental import pallas as pl
from jax.experimental.pallas import tpu as pltpu
from jax.sharding import PartitionSpec as P

TOP_K = 10
LIST_LEN = 8
GROUP_LISTS = 8
GROUP_ROWS = GROUP_LISTS * LIST_LEN
STEP_GROUPS = 4
STEP_ROWS = STEP_GROUPS * GROUP_ROWS
PIECE_ROWS = GROUP_ROWS // 2
LANES = 128
REUSE_Y, REUSE_X = 8, 12
MESH = pl.DeviceIdType.MESH
BIG = 1e9


def flip(index, bit):
    return index + bit - 2 * bit * ((index // bit) % 2)


def search_kernel(dims, q_hbm, l_hbm, probes_hbm, ids_hbm, res,
                  raw, qv, vecs, perm, acc, parts, ids_all, cand_ids, probes_ref, ids_ref, load_p, load_i,
                  load_l, load_q, send_o, recv_o, send_y, recv_y, send_x, recv_x,
                  send_d, recv_d, send_i, recv_i, send_r, recv_r, send_g, recv_g, met):
    rows_q = qv.shape[0]
    lists_dev = ids_ref.shape[1]
    block_rows = lists_dev * LIST_LEN
    block_groups = lists_dev // GROUP_LISTS
    chunks = block_groups
    block_steps = block_groups // STEP_GROUPS
    width = rows_q // dims
    x, z, s = lax.axis_index('rep'), lax.axis_index('dim'), lax.axis_index('shard')
    twin, across, far = flip(s, 1), flip(s, 2), flip(flip(s, 1), 2)
    other_x = 1 - x

    def at(**place):
        return {'rep': x, 'dim': z, 'shard': s, **place}

    def step_rows(step):
        return pl.ds(pl.multiple_of(step * STEP_ROWS, STEP_ROWS), STEP_ROWS)

    def remote(src, dst, send, recv, device):
        return pltpu.make_async_remote_copy(src_ref=src, dst_ref=dst, send_sem=send, recv_sem=recv,
                                            device_id=device, device_id_type=MESH)

    def await_recv(buffer, semaphore):
        remote(buffer, buffer, send_i, semaphore, at()).wait_recv()

    def await_send(buffer, semaphore):
        remote(buffer, buffer, semaphore, recv_i, at()).wait_send()

    def load_lists(number):
        half = block_steps // 2
        first, count = ((half * x, 1), (half * x + 1, half - 1), (half * other_x, half))[number]
        rows = pl.ds(pl.multiple_of(first * STEP_ROWS, STEP_ROWS), count * STEP_ROWS)
        return pltpu.make_async_copy(l_hbm.at[rows], raw.at[rows], load_l.at[number])

    queries_in = pltpu.make_async_copy(q_hbm, qv, load_q)

    def own_copy(block):
        return remote(vecs.at[step_rows(block)], vecs.at[step_rows(block_steps + block)],
                      send_o, recv_o.at[(block // (block_steps // 2) + x) % 2], at(shard=twin))

    def piece(group, chunk):
        first = pl.multiple_of(group * GROUP_ROWS + chunk % 2 * PIECE_ROWS, PIECE_ROWS)
        return vecs.at[pl.ds(first, PIECE_ROWS)]

    def slot(chunk, which):
        return piece(2 * block_groups + STEP_GROUPS * (chunk // 2) + which, chunk)

    def y_copy(chunk):
        return remote(piece(chunks // 2 * x + chunk // 2, chunk), slot(chunk, 0), send_y, recv_y.at[chunk % REUSE_Y], at(shard=across))

    def x_copy(chunk):
        return remote(slot(chunk, 0), slot(chunk, 1), send_x, recv_x.at[chunk % REUSE_X], at(rep=other_x))

    def dy_copy(chunk):
        return remote(slot(chunk, 0), slot(chunk, 2), send_d, recv_d.at[chunk // 2], at(shard=twin))

    def dx_copy(chunk):
        return remote(slot(chunk, 1), slot(chunk, 3), send_d, recv_d.at[chunk // 2], at(shard=twin))

    def id_copy(which, peer):
        return remote(ids_ref, ids_all.at[s], send_i, recv_i, at(shard=peer))

    outer = z % 3 == 0
    mate, far_outer = flip(z, 1), jnp.where(z < 2, dims - 1, 0)
    far_inner = flip(far_outer, 1)

    def landed(place, half, sub=0):
        return recv_r.at[12 + half if place == 2 else 4 * min(place, 2) + 2 * half + sub]

    def some_members(sub):
        return pl.ds(sub * (LIST_LEN // 2), LIST_LEN // 2)

    def near_copy(half):
        return remote(acc.at[mate, half], parts.at[2, half], send_r, landed(2, half), at(dim=mate))

    def cross_copy(target, place, half, sub):
        return remote(acc.at[target, half, some_members(sub)], parts.at[place, half, some_members(sub)], send_r,
                      landed(place, half, sub), at(dim=mate))

    def merged_copy(merge, half, sub):
        return remote(parts.at[merge, half, some_members(sub)], parts.at[3, half, some_members(sub)], send_r,
                      landed(3, half, sub), at(dim=(far_outer, far_inner)[merge]))

    def part_wait(place, half, sub):
        await_recv(parts.at[place, half, some_members(sub)], landed(place, half, sub))

    def res_copy(target, half):
        return remote(res.at[z, half], res.at[z, half], send_g, recv_g, at(dim=target))

    def target_at(turn):
        first, second, third = (jnp.where(outer, one, two) for one, two in ((far_inner, mate), (far_outer, far_inner), (mate, far_outer)))
        return jnp.where(turn == 0, first, jnp.where(turn == 1, second, jnp.where(turn == 2, third, z)))

    def block_at(turn):
        return (block_steps // 2 * x + turn) % block_steps

    barrier = pltpu.get_barrier_semaphore()
    peers = [at(shard=twin), at(shard=across), at(shard=far), at(rep=other_x)]
    beside = jnp.where(outer, 1, 2)

    def tell_line(semaphore):
        @pl.when(z < dims - 1)
        def _():
            pl.semaphore_signal(semaphore, inc=1, device_id=at(dim=(z + 1) % dims), device_id_type=MESH)

        @pl.when(z > 0)
        def _():
            pl.semaphore_signal(semaphore, inc=1, device_id=at(dim=(z + dims - 1) % dims), device_id_type=MESH)

    load_lists(0).start()
    tell_line(barrier)
    probes_in = pltpu.make_async_copy(probes_hbm, probes_ref, load_p)
    ids_in = pltpu.make_async_copy(ids_hbm, ids_ref, load_i)
    ids_in.start()
    probes_in.start()
    queries_in.start()
    for peer in peers:
        pl.semaphore_signal(barrier, inc=1, device_id=peer, device_id_type=MESH)
    load_lists(1).start()
    load_lists(2).start()

    row = lax.broadcasted_iota(jnp.int32, (STEP_ROWS, STEP_ROWS), 0)
    col = lax.broadcasted_iota(jnp.int32, (STEP_ROWS, STEP_ROWS), 1)
    source = (row // GROUP_ROWS) * GROUP_ROWS + (row % GROUP_LISTS) * LIST_LEN + (row // GROUP_LISTS) % LIST_LEN
    perm[...] = jnp.where(col == source, 1.0, 0.0).astype(jnp.bfloat16)

    def arrange(turn):
        block = block_at(turn)
        moved = jnp.dot(perm[...], raw[step_rows(block), :], preferred_element_type=jnp.float32)
        vecs[step_rows(block), :] = moved.astype(jnp.bfloat16)

    window = REUSE_Y // 2
    load_lists(0).wait()
    arrange(0)
    pl.semaphore_wait(barrier, len(peers) + beside)
    for chunk in range(window):
        y_copy(chunk).start()
    tell_line(met.at[0])
    acc[...] = jnp.zeros_like(acc)
    ids_in.wait()
    for which, peer in enumerate((twin, across, far)):
        id_copy(which, peer).start()
    ids_all[s] = ids_ref[...]
    probes_in.wait()
    queries_in.wait()

    def name_candidates(tile, carry):
        cols = pl.ds(pl.multiple_of(z * width + tile * LANES, LANES), LANES)
        probe = probes_ref[:, cols]
        lane, page = probe % LANES, probe // LANES
        pages = lists_dev // LANES
        for member in range(LIST_LEN):
            got = jnp.zeros((probe.shape[0], LANES), jnp.int32)
            for number in range(4 * pages):
                table = ids_all[number // pages, member:member + 1, (number % pages) * LANES:(number % pages + 1) * LANES]
                table = jnp.broadcast_to(table, (probe.shape[0], LANES))
                picked = jnp.take_along_axis(table, lane, axis=1, mode='promise_in_bounds')
                got = jnp.where(page == number, picked, got)
            tiles_half = width // 2 // LANES
            place = pl.ds(pl.multiple_of(tile % tiles_half * LANES, LANES), LANES)
            cand_ids[tile // tiles_half, member, :, place] = got.astype(jnp.float32)
        return carry

    def list_block(step):
        return block_at(step % block_steps)

    def score(step, heads, part):
        lists = vecs[step_rows(jnp.where(step < 2 * block_steps, step // block_steps * block_steps + list_block(step), step)), :]
        rows = pl.ds(pl.multiple_of(part * width, width), width)
        scores = lax.dot_general(lists, qv[rows, :], (((1,), (1,)), ((), ())), preferred_element_type=jnp.float32)
        for tile in range(width // LANES):
            probe = probes_ref[:, pl.ds(pl.multiple_of(part * width + tile * LANES, LANES), LANES)]
            low, head = probe % GROUP_LISTS, probe // GROUP_LISTS
            hits = [head == want for want in heads]
            lanes = slice(tile * LANES, (tile + 1) * LANES)
            half, place = divmod(tile * LANES, width // 2)
            kept_lanes = slice(place, place + LANES)
            for member in range(LIST_LEN):
                kept = acc[part, half, member, :, kept_lanes]
                for group, hit in enumerate(hits):
                    first = group * GROUP_ROWS + member * GROUP_LISTS
                    picked = jnp.take_along_axis(scores[first:first + GROUP_LISTS, lanes], low, axis=0, mode='promise_in_bounds')
                    kept = jnp.where(hit, picked, kept)
                acc[part, half, member, :, kept_lanes] = kept

    def heads_at(step):
        local = step < 2 * block_steps
        group = step - 2 * block_steps
        base = block_groups * jnp.where(step < block_steps, s, twin) + STEP_GROUPS * list_block(step)
        heads = []
        for which in range(STEP_GROUPS):
            home = across if which < 2 else far
            side = x if which % 2 == 0 else other_x
            heads.append(jnp.where(local, base + which, block_groups * home + chunks // 2 * side + group))
        return heads

    last = 2 * block_steps + chunks // 2 - 1

    spare_copy = remote(piece(chunks // 2 * other_x + (chunks - 1) // 2, chunks - 1), slot(chunks - 1, 1),
                        send_x, recv_x.at[REUSE_X], at(shard=across))

    split = chunks - 2

    def split_half(buffer, half):
        return buffer.at[pl.ds(half * (PIECE_ROWS // 2), PIECE_ROWS // 2)]

    def y_half(half):
        return remote(split_half(piece(chunks // 2 * x + split // 2, split), half), split_half(slot(split, 0), half),
                      send_y, recv_y.at[REUSE_Y + half], at(shard=across))

    def x_half(half):
        return remote(split_half(slot(split, 0), half), split_half(slot(split, 1), half),
                      send_x, recv_x.at[REUSE_X + 1 + half], at(rep=other_x))

    def d_half(which, half):
        return remote(split_half(slot(split, which), half), split_half(slot(split, which + 2), half),
                      send_d, recv_d.at[split // 2], at(shard=twin))

    def pass_split(which):
        for half in range(2):
            if which == 0:
                y_half(half).wait_recv()
                x_half(half).start()
            else:
                x_half(half).wait_recv()
            d_half(which, half).start()

    def pass_y(chunk):
        y_copy(chunk).wait_recv()
        if not (isinstance(chunk, int) and chunk == chunks - 1):
            x_copy(chunk).start()
        dy_copy(chunk).start()

        if isinstance(chunk, int) and chunk + window == split:
            for half in range(2):
                y_half(half).start()
        else:
            @pl.when(chunk + window < chunks)
            def _():
                y_copy(chunk + window).start()

        @pl.when(chunk + window == chunks)
        def _():
            spare_copy.start()

    def pass_x(chunk):
        if isinstance(chunk, int) and chunk == chunks - 1:
            spare_copy.wait_recv()
        else:
            x_copy(chunk).wait_recv()
        dx_copy(chunk).start()

    def await_step(step):
        await_recv(vecs.at[pl.ds(0, 4 * PIECE_ROWS)], recv_d.at[step - 2 * block_steps])

    def score_all(step):
        heads = heads_at(step)
        for part in range(dims):
            score(step, heads, part)

    def early(step, carry):
        own_copy(block_at(step)).start()

        @pl.when(step >= 1)
        def _():
            pass_y(step - 1)

        @pl.when(step >= 5)
        def _():
            pass_x(step - 5)

        @pl.when(step == 0)
        def _():
            load_lists(1).wait()

        @pl.when(step == block_steps // 2 - 1)
        def _():
            load_lists(2).wait()
        score_all(step)
        arrange(step + 1)
        return carry

    def middle(step, carry):
        pass_y(step - 1)
        pass_x(step - 5)

        @pl.when(step == block_steps - 1)
        def _():
            own_copy(block_at(step)).start()

        @pl.when((step == block_steps) | (step == block_steps + block_steps // 2))
        def _():
            await_recv(vecs.at[pl.ds(0, block_rows // 2)], recv_o.at[step // (block_steps // 2) - 2])

        @pl.when(step >= 2 * block_steps)
        def _():
            await_step(step)
        score_all(step)
        return carry

    late_plan = {
        last - 5: ('y25', 'x21', 'x22'),
        last - 4: ('y26', 'x23', 'y27', 'x24'),
        last - 3: ('y28', 'x25', 'names', 'y29', 'x26'),
        last - 2: ('y30', 'x27', 'y31', 'x28', 'x29'),
        last - 1: ('x31', 'x30'),
    }

    def late(step, carry):
        for when, plan in late_plan.items():
            @pl.when(step == when)
            def _(plan=plan):
                for word in plan:
                    if word == 'names':
                        await_recv(ids_all.at[pl.ds(0, 3)], recv_i)
                        lax.fori_loop(0, width // LANES, name_candidates, 0)
                    else:
                        which, number = 'yx'.index(word[0]), int(word[1:])
                        if number == split:
                            pass_split(which)
                        else:
                            (pass_y, pass_x)[which](number)

        await_step(step)
        score_all(step)
        return carry

    lax.fori_loop(0, block_steps - 1, early, 0)
    lax.fori_loop(block_steps - 1, last - 5, middle, 0)
    pl.semaphore_wait(met.at[0], beside)
    tell_line(met.at[1])
    lax.fori_loop(last - 5, last, late, 0)
    pl.semaphore_wait(met.at[1], beside)
    await_step(jnp.int32(last))
    last_heads = heads_at(jnp.int32(last))

    leads, follows = outer & (s % 2 == 0), outer & (s % 2 == 1)

    def send_cross(*plan):
        for far_place, half in plan:
            for sub in range(2):
                cross_copy((far_outer, far_inner)[far_place], far_place, half, sub).start()

    def send_near():
        for half in range(2):
            near_copy(half).start()

    def finish(turn, carry):
        @pl.when(leads & (turn == 1))
        def _():
            send_cross((1, 0))

        @pl.when(leads & (turn == 2))
        def _():
            send_cross((0, 0), (1, 1), (0, 1))

        @pl.when(follows & (turn == 2))
        def _():
            send_cross((1, 0))

        @pl.when(follows & (turn == 3))
        def _():
            send_cross((0, 0))

        @pl.when((leads & (turn == 3)) | (jnp.logical_not(outer) & (turn == 1)))
        def _():
            send_near()
        score(jnp.int32(last), last_heads, target_at(turn))
        return carry

    lax.fori_loop(0, dims, finish, 0)

    @pl.when(follows)
    def _():
        send_cross((1, 1), (0, 1))
        send_near()

    @pl.when(jnp.logical_not(outer))
    def _():
        for half in range(2):
            for merge, target in ((1, far_inner), (0, far_outer)):
                for sub in range(2):
                    part_wait(merge, half, sub)
                    parts[merge, half, some_members(sub)] += acc[target, half, some_members(sub)]
                    merged_copy(merge, half, sub).start()

    tiles = width // 2 // LANES
    for half in range(2):
        await_recv(parts.at[2, half], landed(2, half))
        for sub in range(2):
            part_wait(3, half, sub)
        scores, names = [], []
        for member in range(LIST_LEN):
            total = acc[z, half, member] + parts[2, half, member] + parts[3, half, member]
            name = cand_ids[half, member]
            real = name >= 0.0
            scores.append(jnp.where(real, total, -jnp.inf))
            names.append(jnp.where(real, name, BIG))
        for place in range(TOP_K):
            best = functools.reduce(jnp.maximum, scores)
            best = jnp.max(best, axis=0, keepdims=True)
            tied = [jnp.where(score_j == best, name_j, BIG) for score_j, name_j in zip(scores, names)]
            first = jnp.min(functools.reduce(jnp.minimum, tied), axis=0, keepdims=True)
            for tile in range(tiles):
                lanes = slice(tile * LANES, (tile + 1) * LANES)
                line = place * tiles + tile
                res[z, half, line:line + 1, :] = best[:, lanes]
                res[z, half, TOP_K * tiles + line:TOP_K * tiles + line + 1, :] = first[:, lanes]
            if place + 1 < TOP_K:
                scores = [jnp.where(name_j == first, -jnp.inf, score_j) for score_j, name_j in zip(scores, names)]
        if half == 0:
            await_send(vecs.at[pl.ds(0, block_rows)], send_o)
            await_send(ids_all.at[pl.ds(0, 3)], send_i)
        else:
            await_send(vecs.at[pl.ds(0, chunks * PIECE_ROWS)], send_y)
            await_send(vecs.at[pl.ds(0, chunks * PIECE_ROWS)], send_x)
            await_send(vecs.at[pl.ds(0, 2 * chunks * PIECE_ROWS)], send_d)
        for which in range(dims - 1):
            res_copy(jnp.where(which < z, which, which + 1), half).start()

    await_send(parts.at[pl.ds(0, 3)], send_r)
    await_send(res.at[pl.ds(0, dims - 1)], send_g)
    await_recv(res.at[pl.ds(0, dims - 1)], recv_g)


def place_kernel(res, out_s, out_i):
    dims, halves, lines, _ = res.shape
    tiles = lines // (2 * TOP_K)
    for part in range(dims):
        for half in range(halves):
            for tile in range(tiles):
                first = ((part * halves + half) * tiles + tile) * LANES
                out_s[:, first:first + LANES] = res[part, half, pl.ds(tile, TOP_K, stride=tiles), :]
                out_i[:, first:first + LANES] = res[part, half, pl.ds(TOP_K * tiles + tile, TOP_K, stride=tiles), :].astype(jnp.int32)


def solution(mesh):
    dims = mesh.shape['dim']
    row_spec = P(('rep', 'shard'), None)

    def local_search(queries, list_vecs, list_ids, probes):
        rows_q, depth = queries.shape
        lists_dev, list_len, _ = list_vecs.shape
        probe_count = probes.shape[1]
        block_rows = lists_dev * list_len
        block_steps = block_rows // STEP_ROWS
        chunks = lists_dev // GROUP_LISTS
        width = rows_q // dims
        dma = pltpu.SemaphoreType.DMA
        any_spec = pl.BlockSpec(memory_space=pl.ANY)
        vmem_spec = pl.BlockSpec(memory_space=pltpu.VMEM)
        found = pl.pallas_call(
            functools.partial(search_kernel, dims),
            out_shape=pltpu.VMEM((dims, 2, TOP_K * width // LANES, LANES), jnp.float32),
            in_specs=[any_spec] * 4,
            out_specs=vmem_spec,
            scratch_shapes=[
                pltpu.VMEM((block_rows, depth), jnp.bfloat16),
                pltpu.VMEM((rows_q, depth), jnp.bfloat16),
                pltpu.VMEM((4 * block_rows, depth), jnp.bfloat16),
                pltpu.VMEM((STEP_ROWS, STEP_ROWS), jnp.bfloat16),
                pltpu.VMEM((dims, 2, LIST_LEN, probe_count, width // 2), jnp.float32),
                pltpu.VMEM((4, 2, LIST_LEN, probe_count, width // 2), jnp.float32),
                pltpu.VMEM((4, LIST_LEN, lists_dev), jnp.int32),
                pltpu.VMEM((2, LIST_LEN, probe_count, width // 2), jnp.float32),
                pltpu.VMEM((probe_count, rows_q), jnp.int32),
                pltpu.VMEM((LIST_LEN, lists_dev), jnp.int32),
                dma, dma,
                dma((3,)), dma,
                dma, dma((2,)),
                dma, dma((REUSE_Y + 2,)), dma, dma((REUSE_X + 3,)),
                dma, dma((chunks // 2,)),
                dma, dma, dma, dma((14,)), dma, dma,
                pltpu.SemaphoreType.REGULAR((2,)),
            ],
            compiler_params=pltpu.CompilerParams(collective_id=0, has_side_effects=True, vmem_limit_bytes=60 * 2**20),
            name='ivf_search',
        )(queries, list_vecs.reshape(block_rows, depth), probes.T, list_ids.T)
        scores, ids = pl.pallas_call(
            place_kernel,
            out_shape=(jax.ShapeDtypeStruct((TOP_K, rows_q), jnp.float32),
                       jax.ShapeDtypeStruct((TOP_K, rows_q), jnp.int32)),
            in_specs=[vmem_spec],
            out_specs=(vmem_spec, vmem_spec),
            compiler_params=pltpu.CompilerParams(vmem_limit_bytes=4 * 2**20),
            name='place',
        )(found)
        return scores.T, ids.T

    return jax.shard_map(local_search, mesh=mesh,
                         in_specs=(P(('rep', 'shard'), 'dim'), P('shard', None, 'dim'), P('shard', None), row_spec),
                         out_specs=(row_spec, row_spec), check_vma=False)
```
